32 devices in a mesh: fsdp: 8 (over z, y), tp: 4 (over x, core).
Axes of the slice: x: 2, y: 2, z: 4, core: 2. Of those that a mesh axis runs over, the one named last changes fastest.
Arguments:
- tokens: bfloat16 [16, 1024, 768], P('fsdp', 'tp'), may hold values from -12 to 12
- segment_ids: int32 [16, 1024], P('fsdp'), may hold values from 0 to 5, never falling along the last dimension, each value on 1 to 800 neighbouring positions
- query_key_value_weight: bfloat16 [3, 768, 768], P(None, 'fsdp', 'tp'), may hold values from -0.21875 to 0.21875
- w_out: bfloat16 [768, 768], P('tp', 'fsdp'), may hold values from -0.875 to 0.875
- input_weight: bfloat16 [768, 2, 3072], P('fsdp', None, 'tp'), may hold values from -0.21875 to 0.21875
- w_down: bfloat16 [3072, 768], P('tp', 'fsdp'), may hold values from -0.109375 to 0.109375
- norm_gains: bfloat16 [2, 768], P(None, 'fsdp'), may hold values from 0.25 to 1.75
- norm_biases: bfloat16 [2, 768], P(None, 'fsdp'), may hold values from -3 to 3
- cotangent: bfloat16 [16, 1024, 768], P('fsdp', 'tp'), may hold values from -6 to 6
Outputs:
- layer_out: bfloat16 [16, 1024, 768], P('fsdp', 'tp')
- grad_tokens: bfloat16 [16, 1024, 768], P('fsdp', 'tp')
- grad_qkv: float32 [3, 768, 768], P(None, 'fsdp', 'tp')
- output_weight_gradient: float32 [768, 768], P('tp', 'fsdp')
- input_weight_gradient: float32 [768, 2, 3072], P('fsdp', None, 'tp')
- down_weight_gradient: float32 [3072, 768], P('tp', 'fsdp')
- grad_gains: float32 [2, 768], P(None, 'fsdp')
- grad_biases: float32 [2, 768], P(None, 'fsdp')
- stream_rms: float32 [4], replicated
The draws below stay inside these ranges and needn't reach their ends.
All inputs are finite; a program needn't handle non-finite values.
Results may differ from the reference program's by a relative error of at most 0.023.
Values may be sent and summed in bfloat16 or wider, within the bound.
A program may use at most 128 MiB of HBM per device.

```python
import math
import jax
import jax.numpy as jnp
import numpy as np
from jax import lax

D = 768
HEADS = 12
HEAD_DIM = 64
FF = 3072
L = 1024
SEQ_DEV = 2
DOCS = 6
DOC_MOST = 800
SEQUENCES = 16
N_FSDP = 8
N_TP = 4


def draw_tokens(key, part):
    noise_key, factor_key = jax.random.split(key)
    base = jnp.clip(jax.random.normal(noise_key, (SEQUENCES, L, D), jnp.float32), -6.0, 6.0)
    rough = jax.random.uniform(factor_key, (SEQUENCES, L, 1), jnp.float32, 0.7, 1.3)
    ramp = 0.5 + jnp.arange(SEQUENCES).astype(jnp.float32)[:, None, None] / max(SEQUENCES - 1, 1)
    return (base * rough * ramp).astype(jnp.bfloat16)


def level_of(stream_key, shape, cuts, least, largest):
    gain = 1.0
    for position, parts in cuts:
        draws = jax.random.uniform(jax.random.fold_in(jax.random.fold_in(stream_key, 6), position), (parts,), jnp.float32, least / len(cuts), largest / len(cuts))
        gain = gain * jnp.repeat(jnp.exp(draws), shape[position] // parts).reshape((-1,) + (1,) * (len(shape) - 1 - position))
    return gain


def split_up(amount, total, reach, slope):
    weights = [(1 << 20) // math.isqrt(grade ** slope) + 1 for grade in range(2, amount + 1)]
    spare, counts = total - reach - (amount - 1), [1] * (amount - 1)
    while spare > 0:
        movable = [i for i in range(amount - 1) if counts[i] < reach]
        pool, budget = sum([weights[i] for i in movable]), spare
        for i in movable:
            addition = min(reach - counts[i], max(1, budget * weights[i] // pool), spare)
            counts[i] = counts[i] + addition
            spare = spare - addition
    return np.array([reach] + counts)


def uneven_parts(rng, amount, total, bound, slope):
    if amount == 2:
        one = jax.random.randint(rng, (), max(1, total - bound), min(bound, total - 1) + 1)
        return jnp.stack([one, total - one])
    tallies = jnp.asarray(split_up(amount, total, bound, slope), jnp.int32)
    couples = (amount - 1) // 2
    giver, taker = tallies[1:1 + 2 * couples:2], tallies[2:2 + 2 * couples:2]
    margin = jnp.minimum(giver - 1, bound - taker)
    passed = jax.random.randint(jax.random.fold_in(rng, 1), (couples,), 0, 1 << 20) % (margin + 1)
    tallies = tallies.at[1:1 + 2 * couples:2].set(giver - passed).at[2:2 + 2 * couples:2].set(taker + passed)
    return tallies[jax.random.permutation(jax.random.fold_in(rng, 2), amount)]


def gaussian(stream_key, dims, width, reach, cuts=(), held_as=jnp.bfloat16):
    array = width * jax.random.normal(stream_key, dims, jnp.float32)
    if cuts:
        array = array * level_of(stream_key, dims, cuts, -0.22, 0.18)
    return jnp.clip(array, -reach, reach).astype(held_as)


def setup_inputs(seed: int = 0) -> dict:
    seeds = jax.random.split(jax.random.key(seed), 10)
    return {
        "tokens": draw_tokens(jax.random.fold_in(seeds[9], 71), 0),
        "segment_ids": jax.vmap(lambda own: jnp.searchsorted(jnp.cumsum(uneven_parts(own, DOCS, L, DOC_MOST, 1)), jnp.arange(L), side="right"))(jax.random.split(seeds[1], SEQUENCES)).reshape((SEQUENCES, L)).astype(jnp.int32),
        "query_key_value_weight": gaussian(seeds[2], (3, D, D), D ** -0.5, 0.21875, ((1, 8), (2, 4))),
        "w_out": gaussian(seeds[3], (D, D), (D // 16) ** -0.5, 0.875, ((0, 4), (1, 8))),
        "input_weight": gaussian(seeds[4], (D, 2, FF), D ** -0.5, 0.21875, ((0, 8), (2, 4))),
        "w_down": gaussian(seeds[5], (FF, D), FF ** -0.5, 0.109375, ((0, 4), (1, 8))),
        "norm_gains": jnp.clip(1.0 + 0.15 * jax.random.normal(seeds[6], (2, D), jnp.float32), 0.25, 1.75).astype(jnp.bfloat16),
        "norm_biases": gaussian(seeds[7], (2, D), 0.3, 3.0, ((1, 8),)),
        "cotangent": gaussian(seeds[8], (SEQUENCES, L, D), 1.0, 6.0, ((0, 8), (1, 4))),
    }


norm_eps = 1e-05
precision_highest = lax.Precision.HIGHEST

@jax.custom_vjp
def reduced_precision(v):
    return lax.optimization_barrier(v.astype(jnp.bfloat16)).astype(jnp.float32)

@jax.custom_vjp
def reduced_precision_reverse(v):
    return v

def low_keep(v):
    return (reduced_precision(v), None)

def low_pass(kept, grad):
    return (grad,)

def back_keep(v):
    return (v, None)

def back_low(kept, grad):
    return (reduced_precision(grad),)
reduced_precision.defvjp(low_keep, low_pass)
reduced_precision_reverse.defvjp(back_keep, back_low)

def both_round(value):
    return reduced_precision_reverse(reduced_precision(value))

def layer_norm(value, gain_row, bias_row):
    average = lax.optimization_barrier(jnp.mean(value, axis=-1, keepdims=True))
    centered = value - average
    spread = lax.optimization_barrier(jnp.mean(centered * centered, axis=-1, keepdims=True))
    return centered * lax.rsqrt(spread + norm_eps) * gain_row + bias_row

def attend_sequence(bundle):
    queries, keys, values, segment = bundle
    slopes = jnp.exp2(-8.0 * (jnp.arange(HEADS).astype(jnp.float32) + 1.0) / HEADS)
    places = jnp.arange(L).astype(jnp.float32)
    distance = jnp.abs(places[:, None] - places[None, :])
    same_doc = segment[:, None] == segment[None, :]
    raw_score = jnp.einsum('qhe,khe->hqk', queries, keys, precision=precision_highest) * HEAD_DIM ** (-0.5)
    scores = jnp.where(same_doc[None], raw_score - slopes[:, None, None] * distance[None], -1e+30)
    scores = reduced_precision_reverse(scores)
    probs = reduced_precision(jax.nn.softmax(scores, axis=-1))
    return jnp.einsum('hqk,khe->qhe', probs, values, precision=precision_highest)

def block_forward(input_rows, query_key_value_weight, w_out, input_weight, w_down, gains, biases, segment):
    mixed_rows = jnp.einsum('ynk,okq->oynq', input_rows, query_key_value_weight, precision=precision_highest)
    mixed_rows = both_round(mixed_rows).reshape(3, SEQ_DEV, L, HEADS, HEAD_DIM)
    attended_rows = lax.map(jax.checkpoint(attend_sequence), (mixed_rows[0], mixed_rows[1], mixed_rows[2], segment))
    attended_rows = both_round(attended_rows.reshape(SEQ_DEV, L, N_TP, D // N_TP))
    partial_attn = jnp.einsum('slgh,ghd->gsld', attended_rows, w_out.reshape(N_TP, D // N_TP, D), precision=precision_highest)
    attn = reduced_precision_reverse(lax.optimization_barrier(jnp.sum(reduced_precision(partial_attn), axis=0)))
    resid_one = input_rows + attn
    hidden_state_first = layer_norm(resid_one, gains[0], biases[0])
    projected_rows = reduced_precision_reverse(jnp.einsum('hki,iet->hket', reduced_precision(hidden_state_first), input_weight, precision=precision_highest))
    hidden_state = reduced_precision(jax.nn.gelu(projected_rows[:, :, 0], approximate=False) * projected_rows[:, :, 1])
    partial_ffn = jnp.einsum('slgf,gfd->gsld', hidden_state.reshape(SEQ_DEV, L, N_TP, FF // N_TP), w_down.reshape(N_TP, FF // N_TP, D), precision=precision_highest)
    ffn = reduced_precision_reverse(lax.optimization_barrier(jnp.sum(reduced_precision(partial_ffn), axis=0)))
    resid_two = hidden_state_first + ffn
    outputs = layer_norm(resid_two, gains[1], biases[1])
    squares = jnp.stack([jnp.sum(attn * attn), jnp.sum(resid_one * resid_one), jnp.sum(ffn * ffn), jnp.sum(resid_two * resid_two)])
    return (outputs, squares)

def reference(tokens, segment_ids, query_key_value_weight, w_out, input_weight, w_down, norm_gains, norm_biases, cotangent):
    params = tuple((weight_arr.astype(jnp.float32) for weight_arr in (query_key_value_weight, w_out, input_weight, w_down, norm_gains, norm_biases)))
    token_blocks = tokens.astype(jnp.float32).reshape(N_FSDP, SEQ_DEV, L, D)
    grad_blocks = cotangent.astype(jnp.float32).reshape(N_FSDP, SEQ_DEV, L, D)
    seg_blocks = segment_ids.reshape(N_FSDP, SEQ_DEV, L)

    def scan_step(running, bundle):
        token_blk, seg_blk, grad_blk = bundle

        def bound_layer(input_rows, *weights):
            return block_forward(input_rows, *weights, seg_blk)
        outputs, puller, squares = jax.vjp(bound_layer, token_blk, *params, has_aux=True)
        pulled = puller(grad_blk)
        running = tuple((total_val + new_val for total_val, new_val in zip(running, tuple(pulled[1:]) + (squares,))))
        return (running, (outputs.astype(jnp.bfloat16), pulled[0].astype(jnp.bfloat16)))
    start_vals = tuple((jnp.zeros_like(weight_arr) for weight_arr in params)) + (jnp.zeros((4,), jnp.float32),)
    running, (out_blocks, back_blocks) = lax.scan(scan_step, start_vals, (token_blocks, seg_blocks, grad_blocks))
    layer_out = out_blocks.reshape(SEQUENCES, L, D)
    grad_tokens = back_blocks.reshape(SEQUENCES, L, D)
    stream_rms = jnp.sqrt(running[6] / (SEQUENCES * L * D))
    return (layer_out, grad_tokens, running[0], running[1], running[2], running[3], running[4], running[5], stream_rms)
```

```python
from functools import partial

import jax
import jax.numpy as jnp
from jax import lax
from jax.experimental import pallas as pl
from jax.experimental.pallas import tpu as pltpu
from jax.sharding import PartitionSpec as P

HEADS = 12
HEAD_DIM = 64
MESH = pl.DeviceIdType.MESH
VMEM_LIMIT = 63 << 20
norm_eps = 1e-05
SIZE = {"x": 2, "y": 2, "z": 4}
PORTIONS = ((0, 16, "yzx"), (16, 16, "xzy"), (32, 32, "zxy"), (64, 32, "zyx"))


class Place:
    def __init__(self, span):
        index = lax.axis_index("fsdp")
        shard = lax.axis_index("tp")
        self.span = span
        self.j = index % span
        block = index // span
        self.z = block // 2
        self.y = block % 2
        self.x = shard // 2
        self.k = shard % 2

    def shifted(self, dx=0, dy=0, dz=0, dk=0):
        x = 1 - self.x if dx else self.x
        y = 1 - self.y if dy else self.y
        z = (self.z + dz) % 4 if dz else self.z
        k = 1 - self.k if dk else self.k
        return x, y, z, k

    def device(self, dx=0, dy=0, dz=0, dk=0):
        x, y, z, k = self.shifted(dx, dy, dz, dk)
        return ((z * 2 + y) * self.span + self.j, x * 2 + k)

    def greet(self, offsets):
        barrier = pltpu.get_barrier_semaphore()
        for offset in offsets:
            pl.semaphore_signal(
                barrier, inc=1, device_id=self.device(**offset), device_id_type=MESH
            )
        pl.semaphore_wait(barrier, len(offsets))


ALL_PEERS = ({"dx": 1}, {"dy": 1}, {"dz": 1}, {"dz": 2}, {"dz": 3}, {"dk": 1})
PARTNER = ({"dk": 1},)


def offsets_of(order):
    found = []
    for dx in range(2):
        for dy in range(2):
            for dz in range(4):
                off = {"x": dx, "y": dy, "z": dz}
                stage = max([i + 1 for i, axis in enumerate(order) if off[axis]] or [0])
                found.append((stage, dz, dy, dx))
    return sorted(found)


def remote(src, dst, send, recv, device):
    return pltpu.make_async_remote_copy(
        src_ref=src, dst_ref=dst, send_sem=send, recv_sem=recv, device_id=device, device_id_type=MESH
    )


class Gather:
    def __init__(self, place, own, out, portions, sems):
        self.place, self.own, self.out, self.portions, self.sems = place, own, out, portions, sems

    def slot(self, dx, dy, dz, start, rows, dk=0):
        x, y, z, k = self.place.shifted(dx, dy, dz, dk)
        return self.out.at[x, k, z, y, pl.ds(start, rows), :]

    def index(self, dx, dy, dz):
        return (dx * 2 + dy) * 4 + dz

    def forward(self, number, stage, dx, dy, dz):
        start, rows, order = self.portions[number]
        send, recv = self.sems[2 * number], self.sems[2 * number + 1]
        place = self.place
        own = dx == 0 and dy == 0 and dz == 0
        src = self.own.at[pl.ds(start, rows), :] if own else self.slot(dx, dy, dz, start, rows)
        dst = self.slot(dx, dy, dz, start, rows)
        copies = []
        for later in range(stage, 3):
            axis = order[later]
            for step in range(1, SIZE[axis]):
                seen = {"x": dx, "y": dy, "z": dz}
                seen[axis] = step if axis != "z" else (4 - step)
                where = self.index(seen["x"], seen["y"], seen["z"])
                to = place.device(**{"d" + axis: step})
                copies.append(remote(src, dst, send.at[where], recv.at[where], to))
        where = 16 + self.index(dx, dy, dz)
        copies.append(remote(src, dst, send.at[where], recv.at[where], place.device(dk=1)))
        for copy in copies:
            copy.start()
        return copies

    def arrive(self, number, dx, dy, dz, dk=0):
        start, rows, order = self.portions[number]
        send, recv = self.sems[2 * number], self.sems[2 * number + 1]
        where = self.index(dx, dy, dz) + (16 if dk else 0)
        ref = self.slot(dx, dy, dz, start, rows, dk)
        remote(ref, ref, send.at[where], recv.at[where], self.place.device(dk=1)).wait_recv()

    def begin(self):
        self.started = []
        for number in range(len(self.portions)):
            self.started += self.forward(number, 0, 0, 0, 0)

    def relay(self, stage):
        for number, (start, rows, order) in enumerate(self.portions):
            for at, dz, dy, dx in offsets_of(order):
                if at == stage:
                    self.arrive(number, dx, dy, dz)
                    self.started += self.forward(number, stage, dx, dy, dz)

    def finish(self):
        for number, (start, rows, order) in enumerate(self.portions):
            for at, dz, dy, dx in offsets_of(order):
                self.arrive(number, dx, dy, dz, 1)
        for copy in self.started:
            copy.wait_send()


def gather_sems(portions):
    return [pltpu.SemaphoreType.DMA((32,)) for _ in portions for _ in range(2)]


def gather_kernel(span, wa, wf, ws, tok, cot, ga, gf, gs, xs, cs, *scratch):
    place = Place(span)
    sems_a, sems_f, sems_s = scratch[0:8], scratch[8:16], scratch[16:18]
    local_sems, send, recv = scratch[18:21]
    place.greet(ALL_PEERS)
    other = 1 - place.x
    peer = place.device(dx=1)
    swaps = []
    for n, (src, dst) in enumerate(((tok, xs), (cot, cs))):
        swaps.append(remote(src.at[other], dst.at[place.x], send.at[n], recv.at[n], peer))
    gathers = [
        Gather(place, ws, gs, ((0, 16, "zyx"),), sems_s),
        Gather(place, wa, ga, PORTIONS, sems_a),
        Gather(place, wf, gf, PORTIONS, sems_f),
    ]
    swaps[0].start()
    for gather in gathers:
        gather.begin()
    x, y, z, k = place.shifted()
    locals_ = [
        pltpu.make_async_copy(src, dst, local_sems.at[n])
        for n, (src, dst) in enumerate(
            (
                (wa, ga.at[x, k, z, y]),
                (wf, gf.at[x, k, z, y]),
                (ws, gs.at[x, k, z, y]),
                (tok.at[x], xs.at[x]),
                (cot.at[x], cs.at[x]),
            )
        )
    ]
    for copy in locals_:
        copy.start()
    for gather in gathers:
        for stage in (1, 2, 3):
            gather.relay(stage)
    swaps[1].start()
    for gather in gathers:
        gather.finish()
    for copy in locals_:
        copy.wait()
    for n, copy in enumerate(swaps):
        copy.wait()


def gather_all(span, wa, wf, ws, tok, cot):
    any_space = pl.BlockSpec(memory_space=pl.ANY)
    vmem = pl.BlockSpec(memory_space=pltpu.VMEM)
    shape = lambda a: jax.ShapeDtypeStruct((2, 2, 4, 2) + a.shape, a.dtype)
    return pl.pallas_call(
        partial(gather_kernel, span),
        out_shape=(
            shape(wa),
            shape(wf),
            shape(ws),
            jax.ShapeDtypeStruct(tok.shape, tok.dtype),
            jax.ShapeDtypeStruct(cot.shape, cot.dtype),
        ),
        in_specs=[vmem] * 5,
        out_specs=(any_space,) * 5,
        scratch_shapes=gather_sems(PORTIONS)
        + gather_sems(PORTIONS)
        + gather_sems((0,))
        + [
            pltpu.SemaphoreType.DMA((5,)),
            pltpu.SemaphoreType.DMA((2,)),
            pltpu.SemaphoreType.DMA((2,)),
        ],
        compiler_params=pltpu.CompilerParams(
            collective_id=0, has_side_effects=True, vmem_limit_bytes=VMEM_LIMIT
        ),
        name="gather_weights",
    )(wa, wf, ws, tok, cot)


def keys_kernel(span, kv, out, local_sem, send, recv):
    place = Place(span)
    place.greet(PARTNER)
    push = remote(kv, out.at[:, place.k], send, recv, place.device(dk=1))
    push.start()
    keep = pltpu.make_async_copy(kv, out.at[:, place.k], local_sem)
    keep.start()
    keep.wait()
    push.wait()


def share_keys(span, kv):
    return pl.pallas_call(
        partial(keys_kernel, span),
        out_shape=jax.ShapeDtypeStruct((2, 2) + kv.shape[1:], kv.dtype),
        in_specs=[pl.BlockSpec(memory_space=pltpu.VMEM)],
        out_specs=pl.BlockSpec(memory_space=pltpu.VMEM),
        scratch_shapes=[pltpu.SemaphoreType.DMA] * 3,
        compiler_params=pltpu.CompilerParams(
            collective_id=1, has_side_effects=True, vmem_limit_bytes=VMEM_LIMIT
        ),
        name="share_keys",
    )(kv)


def key_grads_kernel(span, part, out, held, send, recv):
    place = Place(span)
    place.greet(PARTNER)
    push = remote(part.at[:, 1 - place.k], held, send, recv, place.device(dk=1))
    push.start()
    push.wait()
    out[...] = (
        part[:, place.k].astype(jnp.float32) + held[...].astype(jnp.float32)
    ).astype(jnp.bfloat16)


def share_key_grads(span, part):
    shape = part.shape[:1] + part.shape[2:]
    return pl.pallas_call(
        partial(key_grads_kernel, span),
        out_shape=jax.ShapeDtypeStruct(shape, part.dtype),
        in_specs=[pl.BlockSpec(memory_space=pltpu.VMEM)],
        out_specs=pl.BlockSpec(memory_space=pltpu.VMEM),
        scratch_shapes=[pltpu.VMEM(shape, part.dtype)] + [pltpu.SemaphoreType.DMA] * 2,
        compiler_params=pltpu.CompilerParams(
            collective_id=2, has_side_effects=True, vmem_limit_bytes=VMEM_LIMIT
        ),
        name="share_key_grads",
    )(part)


class Scatter:
    def __init__(self, place, part, held, twin, landing, portions, sems, pair_sems):
        self.place, self.part, self.held, self.twin = place, part, held, twin
        self.landing, self.portions, self.sems, self.pair_sems = landing, portions, sems, pair_sems
        self.started = []

    def units(self):
        return [(dx, dz, dy) for dz in (2, 1, 3, 0) for dx in (1, 0) for dy in (1, 0)]

    def begin(self):
        self.loads = {}
        for n, (dx, dz, dy) in enumerate(self.units()):
            x, y, z, k = self.place.shifted(dx, dy, dz)
            load = pltpu.make_async_copy(
                self.part.at[x, k, z, y], self.held.at[dx, dz, dy], self.pair_sems[0].at[n]
            )
            push = remote(
                self.part.at[x, 1 - k, z, y],
                self.twin.at[dx, dz, dy],
                self.pair_sems[1].at[n],
                self.pair_sems[2].at[n],
                self.place.device(dk=1),
            )
            load.start()
            push.start()
            self.loads[dx, dz, dy] = (load, push)

    def hops(self, order):
        found = []
        done = []
        for stage, axis in enumerate(reversed(order)):
            rest = [a for a in "xyz" if a != axis and a not in done]
            for step in range(1, SIZE[axis]):
                for first in range(SIZE[rest[0]] if rest else 1):
                    for second in range(SIZE[rest[1]] if len(rest) > 1 else 1):
                        off = {"x": 0, "y": 0, "z": 0}
                        if rest:
                            off[rest[0]] = first
                        if len(rest) > 1:
                            off[rest[1]] = second
                        base = (off["x"], off["z"], off["y"])
                        off[axis] = step
                        sent = (off["x"], off["z"], off["y"])
                        found.append((stage, axis, step, sent, base, len(found)))
            done.append(axis)
        return found

    def send_unit(self, unit, stage):
        for number, (start, rows, order) in enumerate(self.portions):
            for at, axis, step, sent, base, slot in self.hops(order):
                if at == stage and sent == unit:
                    copy = remote(
                        self.held.at[sent + (pl.ds(start, rows), slice(None))],
                        self.landing[number].at[slot],
                        self.sems[2 * number].at[slot],
                        self.sems[2 * number + 1].at[slot],
                        self.place.device(**{"d" + axis: step}),
                    )
                    copy.start()
                    self.started.append(copy)

    def pair_sum(self):
        for unit in self.units():
            load, push = self.loads[unit]
            load.wait()
            push.wait_recv()
            self.held[unit] = (
                self.held[unit].astype(jnp.float32) + self.twin[unit].astype(jnp.float32)
            ).astype(jnp.bfloat16)
            self.send_unit(unit, 0)

    def reduce(self, stage, number, out=None):
        start, rows, order = self.portions[number]
        hops = [hop for hop in self.hops(order) if hop[0] == stage]
        bases = []
        for hop in hops:
            if hop[4] not in bases:
                bases.append(hop[4])
        for base in bases:
            window = base + (pl.ds(start, rows), slice(None))
            total = self.held[window].astype(jnp.float32)
            for at, axis, step, sent, of, slot in hops:
                if of == base:
                    ref = self.landing[number].at[slot]
                    remote(
                        ref,
                        ref,
                        self.sems[2 * number].at[slot],
                        self.sems[2 * number + 1].at[slot],
                        self.place.device(dk=1),
                    ).wait_recv()
                    total = total + self.landing[number][slot].astype(jnp.float32)
            if stage == 2:
                out[pl.ds(start, rows), :] = total
            else:
                self.held[window] = total.astype(jnp.bfloat16)
                for at, axis, step, sent, of, slot in self.hops(order):
                    if at == stage + 1 and sent == base:
                        copy = remote(
                            self.held.at[window],
                            self.landing[number].at[slot],
                            self.sems[2 * number].at[slot],
                            self.sems[2 * number + 1].at[slot],
                            self.place.device(**{"d" + axis: step}),
                        )
                        copy.start()
                        self.started.append(copy)

    def finish(self):
        for copy in self.started:
            copy.wait_send()
        for load, push in self.loads.values():
            push.wait_send()


def scatter_scratch(width, portions):
    buffers = [
        pltpu.VMEM((2, 4, 2, 96, width), jnp.bfloat16),
        pltpu.VMEM((2, 4, 2, 96, width), jnp.bfloat16),
    ]
    buffers += [pltpu.VMEM((15, rows, width), jnp.bfloat16) for start, rows, order in portions]
    buffers += [pltpu.SemaphoreType.DMA((15,)) for _ in portions for _ in range(2)]
    buffers += [pltpu.SemaphoreType.DMA((16,)) for _ in range(3)]
    return buffers


def scatter_kernel(span, part_a, part_f, small, lo, gt, out_a, out_f, out_s, olo, ogt, *scratch):
    place = Place(span)
    per = 2 + len(PORTIONS) * 3 + 3
    groups = scratch[:per], scratch[per : 2 * per]
    s_own, s_land, s_send, s_recv, t_sems = scratch[2 * per :]
    place.greet(ALL_PEERS)
    scatters = []
    for part, group in zip((part_f, part_a), groups):
        n = len(PORTIONS)
        scatters.append(
            Scatter(
                place,
                part,
                group[0],
                group[1],
                group[2 : 2 + n],
                PORTIONS,
                group[2 + n : 2 + 3 * n],
                group[2 + 3 * n :],
            )
        )
    for scatter in scatters:
        scatter.begin()
    x = place.x
    swaps, keeps = [], []
    for n, (src, dst) in enumerate(((lo, olo), (gt, ogt))):
        swaps.append(
            remote(src.at[1 - x], dst.at[x], t_sems.at[3 * n], t_sems.at[3 * n + 1], place.device(dx=1))
        )
        keeps.append(pltpu.make_async_copy(src.at[x], dst.at[x], t_sems.at[3 * n + 2]))
    for copy in swaps + keeps:
        copy.start()
    for scatter in scatters:
        scatter.pair_sum()
    s_own[...] = small[...]
    sends = []
    for n, to in enumerate(({"dk": 1}, {"dx": 1}, {"dy": 1})):
        copy = remote(s_own.at[...], s_land.at[n], s_send.at[n], s_recv.at[n], place.device(**to))
        copy.start()
        copy.wait()
        s_own[...] = s_own[...] + s_land[n]
    for step in (1, 2, 3):
        sends.append(
            remote(s_own, s_land.at[2 + step], s_send.at[2 + step], s_recv.at[2 + step], place.device(dz=step))
        )
        sends[-1].start()
    for scatter, out in zip(scatters, (out_f, out_a)):
        for stage in range(3):
            for number in (2, 3, 0, 1):
                scatter.reduce(stage, number, out)
    for copy in sends:
        copy.wait()
    total = jnp.zeros_like(s_own)
    for at in range(4):
        step = (place.z - at) % 4
        term = jnp.where(
            step == 0,
            s_own[...],
            jnp.where(step == 1, s_land[3], jnp.where(step == 2, s_land[4], s_land[5])),
        )
        total = total + term
    out_s[...] = total
    for scatter in scatters:
        scatter.finish()
    for copy in swaps + keeps:
        copy.wait()


def scatter_all(span, part_a, part_f, small, lo, gt):
    any_space = pl.BlockSpec(memory_space=pl.ANY)
    vmem = pl.BlockSpec(memory_space=pltpu.VMEM)
    return pl.pallas_call(
        partial(scatter_kernel, span),
        out_shape=(
            jax.ShapeDtypeStruct((96, part_a.shape[-1]), jnp.float32),
            jax.ShapeDtypeStruct((96, part_f.shape[-1]), jnp.float32),
            jax.ShapeDtypeStruct(small.shape, jnp.float32),
            jax.ShapeDtypeStruct(lo.shape, lo.dtype),
            jax.ShapeDtypeStruct(gt.shape, gt.dtype),
        ),
        in_specs=[any_space, any_space, vmem, vmem, vmem],
        out_specs=(vmem,) * 5,
        scratch_shapes=scatter_scratch(part_f.shape[-1], PORTIONS)
        + scatter_scratch(part_a.shape[-1], PORTIONS)
        + [
            pltpu.VMEM(small.shape, jnp.float32),
            pltpu.VMEM((6,) + small.shape, jnp.float32),
            pltpu.SemaphoreType.DMA((6,)),
            pltpu.SemaphoreType.DMA((6,)),
            pltpu.SemaphoreType.DMA((6,)),
        ],
        compiler_params=pltpu.CompilerParams(
            collective_id=3, has_side_effects=True, vmem_limit_bytes=VMEM_LIMIT
        ),
        name="scatter_gradients",
    )(part_a, part_f, small, lo, gt)


def lane_half(tile, half):
    lane = lax.broadcasted_iota(jnp.int32, tile.shape, 1)
    keep = (lane < HEAD_DIM) if half == 0 else (lane >= HEAD_DIM)
    return jnp.where(keep, tile, jnp.zeros_like(tile))


def fill_distance(dist, seg_col, seg_row, pos_row):
    keys, queries = dist.shape
    key_pos = lax.broadcasted_iota(jnp.int32, (keys, queries), 0).astype(jnp.float32)
    gap = jnp.abs(key_pos - pos_row)
    dist[...] = jnp.where(seg_col == seg_row, gap, 1e30)


NT = (((1,), (1,)), ((), ()))
NN = (((1,), (0,)), ((), ()))
CHUNK = 256


def dot(a, b, dims=NN):
    return lax.dot_general(a, b, dims, preferred_element_type=jnp.float32)


def attend_kernel(slopes, q, k, v, seg_col, seg_row, pos_row, ctx, lse, dist, out_t):
    step = pl.program_id(0)

    @pl.when(step == 0)
    def _():
        fill_distance(dist, seg_col[...], seg_row[...], pos_row[...])

    v_t = v[...].astype(jnp.float32).T.astype(jnp.bfloat16)
    for half in range(2):
        slope = slopes[2 * step + half]
        for start in range(0, q.shape[0], CHUNK):
            cols = pl.ds(start, CHUNK)
            part = lane_half(q[cols, :], half)
            scores = dot(k[...], part, NT) - slope * dist[:, cols]
            peak = jnp.max(scores, axis=0, keepdims=True)
            expo = jnp.exp(scores - peak)
            total = jnp.sum(expo, axis=0, keepdims=True)
            rows = slice(half * HEAD_DIM, (half + 1) * HEAD_DIM)
            mixed = dot(v_t[rows, :], expo.astype(jnp.bfloat16)) / total
            out_t[rows, cols] = mixed
            lse[0, pl.ds(half, 1), cols] = peak + jnp.log(total)
    ctx[...] = out_t[...].T.astype(jnp.bfloat16)


def attend(slopes, q, kv, seg_col, seg_row, pos_row):
    rows, keys = q.shape[0], kv.shape[0]
    whole = lambda a: pl.BlockSpec(a.shape, lambda i: (0, 0))
    return pl.pallas_call(
        attend_kernel,
        grid=(6,),
        out_shape=(
            jax.ShapeDtypeStruct((rows, 768), jnp.bfloat16),
            jax.ShapeDtypeStruct((6, 8, rows), jnp.float32),
        ),
        in_specs=[
            pl.BlockSpec(memory_space=pltpu.SMEM),
            pl.BlockSpec((rows, 128), lambda i: (0, i)),
            pl.BlockSpec((keys, 128), lambda i: (0, i)),
            pl.BlockSpec((keys, 128), lambda i: (0, 6 + i)),
            whole(seg_col),
            whole(seg_row),
            whole(pos_row),
        ],
        out_specs=(
            pl.BlockSpec((rows, 128), lambda i: (0, i)),
            pl.BlockSpec((1, 8, rows), lambda i: (i, 0, 0)),
        ),
        scratch_shapes=[
            pltpu.VMEM((keys, rows), jnp.float32),
            pltpu.VMEM((128, rows), jnp.float32),
        ],
        compiler_params=pltpu.CompilerParams(vmem_limit_bytes=VMEM_LIMIT),
        name="attend",
    )(slopes, q, kv, kv, seg_col, seg_row, pos_row)


def attend_grad_kernel(
    slopes, q, k, v, ctx, d_ctx, lse, seg_col, seg_row, pos_row, dq, dk, dv, dist, dq_t, dk_acc, dv_acc
):
    step = pl.program_id(0)

    @pl.when(step == 0)
    def _():
        fill_distance(dist, seg_col[...], seg_row[...], pos_row[...])

    k_t = k[...].astype(jnp.float32).T.astype(jnp.bfloat16)
    delta_t = (ctx[...].astype(jnp.float32) * d_ctx[...].astype(jnp.float32)).T
    for half in range(2):
        slope = slopes[2 * step + half]
        rows = slice(half * HEAD_DIM, (half + 1) * HEAD_DIM)
        delta = jnp.sum(delta_t[rows, :], axis=0, keepdims=True)
        for start in range(0, q.shape[0], CHUNK):
            cols = pl.ds(start, CHUNK)
            part = lane_half(q[cols, :], half)
            grad = lane_half(d_ctx[cols, :], half)
            scores = dot(k[...], part, NT) - slope * dist[:, cols]
            probs = jnp.exp(scores - lse[0, pl.ds(half, 1), cols])
            grad_probs = dot(v[...], grad, NT)
            term_v = dot(probs.astype(jnp.bfloat16), grad)
            grad_scores = (probs * (grad_probs - delta[:, start : start + CHUNK])).astype(jnp.bfloat16)
            term_k = dot(grad_scores, part)
            if half == 0 and start == 0:
                dv_acc[...] = term_v
                dk_acc[...] = term_k
            else:
                dv_acc[...] += term_v
                dk_acc[...] += term_k
            dq_t[rows, cols] = dot(k_t[rows, :], grad_scores)
    dq[...] = (dq_t[...].T * HEAD_DIM**-0.5).astype(jnp.bfloat16)
    dk[...] = dk_acc[...].astype(jnp.bfloat16)
    dv[...] = dv_acc[...].astype(jnp.bfloat16)


def attend_grad(slopes, q, kv, ctx, d_ctx, lse, seg_col, seg_row, pos_row):
    rows, keys = q.shape[0], kv.shape[0]
    whole = lambda a: pl.BlockSpec(a.shape, lambda i: (0, 0))
    row_block = pl.BlockSpec((rows, 128), lambda i: (0, i))
    key_block = pl.BlockSpec((keys, 128), lambda i: (0, i))
    return pl.pallas_call(
        attend_grad_kernel,
        grid=(6,),
        out_shape=(
            jax.ShapeDtypeStruct((rows, 768), jnp.bfloat16),
            jax.ShapeDtypeStruct((keys, 768), jnp.bfloat16),
            jax.ShapeDtypeStruct((keys, 768), jnp.bfloat16),
        ),
        in_specs=[
            pl.BlockSpec(memory_space=pltpu.SMEM),
            row_block,
            key_block,
            pl.BlockSpec((keys, 128), lambda i: (0, 6 + i)),
            row_block,
            row_block,
            pl.BlockSpec((1, 8, rows), lambda i: (i, 0, 0)),
            whole(seg_col),
            whole(seg_row),
            whole(pos_row),
        ],
        out_specs=(row_block, key_block, key_block),
        scratch_shapes=[
            pltpu.VMEM((keys, rows), jnp.float32),
            pltpu.VMEM((128, rows), jnp.float32),
            pltpu.VMEM((keys, 128), jnp.float32),
            pltpu.VMEM((keys, 128), jnp.float32),
        ],
        compiler_params=pltpu.CompilerParams(vmem_limit_bytes=VMEM_LIMIT),
        name="attend_grad",
    )(slopes, q, kv, kv, ctx, d_ctx, lse, seg_col, seg_row, pos_row)


def norm_forward(value, gain_row, bias_row):
    average = jnp.mean(value, axis=-1, keepdims=True)
    centered = value - average
    inv_std = lax.rsqrt(jnp.mean(centered * centered, axis=-1, keepdims=True) + norm_eps)
    normed = centered * inv_std
    return (normed * gain_row + bias_row, normed, inv_std)


def norm_backward(grad_val, normed, inv_std, gain_row):
    grad_norm = grad_val * gain_row
    return inv_std * (
        grad_norm
        - jnp.mean(grad_norm, axis=-1, keepdims=True)
        - normed * jnp.mean(grad_norm * normed, axis=-1, keepdims=True)
    )


def local(
    tokens,
    segment_ids,
    query_key_value_weight,
    w_out,
    input_weight,
    w_down,
    norm_gains,
    norm_biases,
    cotangent,
):
    bf16, f32 = jnp.bfloat16, jnp.float32
    shard_rows = query_key_value_weight.shape[1]
    span = 96 // shard_rows
    groups = None
    if span > 1:
        count = lax.axis_size("fsdp")
        groups = [list(range(i, i + span)) for i in range(0, count, span)]
    place_x = lax.axis_index("tp") // 2
    place_k = lax.axis_index("tp") % 2

    heads = query_key_value_weight.transpose(1, 0, 2).reshape(shard_rows, 3, 3, HEAD_DIM)
    w_out_t = w_out.T.reshape(shard_rows, 3, 1, HEAD_DIM)
    wa = jnp.concatenate([heads, w_out_t], axis=2).reshape(shard_rows, 768)
    wf = jnp.concatenate([input_weight.reshape(shard_rows, 1536), w_down.T], axis=1)
    norms = jnp.concatenate([norm_gains, norm_biases], axis=0)
    if span > 1:
        wa = lax.all_gather(wa, "fsdp", axis=0, tiled=True, axis_index_groups=groups)
        wf = lax.all_gather(wf, "fsdp", axis=0, tiled=True, axis_index_groups=groups)
        norms = lax.all_gather(norms, "fsdp", axis=1, tiled=True, axis_index_groups=groups)
    ws = jnp.pad(norms, ((0, 12), (0, 32)))
    ga, gf, gs, xs, cs = gather_all(span, wa, wf, ws, tokens, cotangent)

    norms = gs[0, 0, :, :, :4, :96].reshape(8, 4, 96).transpose(1, 0, 2).reshape(4, 768).astype(f32)
    gains, biases = norms[:2], norms[2:]
    ga = ga.reshape(4, 768, 3, 4, HEAD_DIM)
    w_qkv = ga[:, :, :, :3].transpose(1, 2, 0, 3, 4).reshape(768, 3 * 768)
    w_out_full_t = ga[:, :, :, 3].transpose(1, 0, 2, 3).reshape(768, 768)
    gf = gf.reshape(4, 768, 2304)

    x_rows = xs.reshape(512, 768)
    qkv = jnp.dot(x_rows, w_qkv, preferred_element_type=f32).astype(bf16)
    q = qkv[:, :768] * jnp.bfloat16(HEAD_DIM**-0.5)
    kv = share_keys(span, qkv[:, 768:].reshape(2, 256, 1536)).reshape(1024, 1536)

    segment = lax.dynamic_index_in_dim(segment_ids, place_x, 0, keepdims=False)
    seg_col = segment.reshape(1024, 1)
    seg_row = lax.dynamic_index_in_dim(segment.reshape(2, 2, 256), place_k, 1, keepdims=False)
    seg_row = seg_row.reshape(1, 512)
    pos_row = (
        lax.broadcasted_iota(jnp.int32, (2, 256), 0) * 512
        + place_k * 256
        + lax.broadcasted_iota(jnp.int32, (2, 256), 1)
    )
    pos_row = pos_row.reshape(1, 512).astype(f32)
    slopes = jnp.exp2(-8.0 * (jnp.arange(HEADS).astype(f32) + 1.0) / HEADS)
    ctx, lse = attend(slopes, q, kv, seg_col, seg_row, pos_row)

    attn = lax.dot_general(ctx, w_out_full_t, NT, preferred_element_type=f32)
    resid_one = x_rows.astype(f32) + attn
    h1, normed_one, inv_one = norm_forward(resid_one, gains[0], biases[0])
    h1b = h1.astype(bf16)
    ffn = jnp.zeros_like(h1)
    kept = []
    for t in range(4):
        projected = jnp.dot(h1b, gf[t, :, :1536], preferred_element_type=f32)
        gate, up = projected[:, :768], projected[:, 768:]
        cdf = 0.5 * (1.0 + lax.erf(gate * (0.5**0.5)))
        pdf = jnp.exp(-0.5 * gate * gate) * 0.3989422804014327
        act = gate * cdf
        hidden = (act * up).astype(bf16)
        slope = ((cdf + gate * pdf) * up).astype(bf16)
        kept.append((hidden, act.astype(bf16), slope))
        ffn = ffn + lax.dot_general(hidden, gf[t, :, 1536:], NT, preferred_element_type=f32)
    resid_two = h1 + ffn
    layer_out, normed_two, inv_two = norm_forward(resid_two, gains[1], biases[1])
    grad_layer = cs.reshape(512, 768).astype(f32)
    grad_two = norm_backward(grad_layer, normed_two, inv_two, gains[1])
    d_ffn = grad_two.astype(bf16)
    d_ffn_t = d_ffn.T
    h1b_t = h1b.T
    d_h1 = grad_two
    grads_f = []
    for t in range(4):
        hidden, act, slope = kept[t]
        d_hidden = jnp.dot(d_ffn, gf[t, :, 1536:], preferred_element_type=f32)
        d_gate = (d_hidden * slope.astype(f32)).astype(bf16)
        d_up = (d_hidden * act.astype(f32)).astype(bf16)
        d_proj = jnp.concatenate([d_gate, d_up], axis=1)
        d_win = jnp.dot(h1b_t, d_proj, preferred_element_type=f32).astype(bf16)
        d_down = jnp.dot(d_ffn_t, hidden, preferred_element_type=f32).astype(bf16)
        grads_f.append(jnp.concatenate([d_win, d_down], axis=1))
        d_h1 = d_h1 + lax.dot_general(d_proj, gf[t, :, :1536], NT, preferred_element_type=f32)
    part_f = jnp.stack(grads_f).reshape(2, 2, 4, 2, 96, 2304)
    grad_one = norm_backward(d_h1, normed_one, inv_one, gains[0])
    d_attn = grad_one.astype(bf16)
    d_ctx = jnp.dot(d_attn, w_out_full_t, preferred_element_type=f32).astype(bf16)
    d_wout_t = jnp.dot(d_attn.T, ctx, preferred_element_type=f32).astype(bf16)
    dq, dk, dv = attend_grad(slopes, q, kv, ctx, d_ctx, lse, seg_col, seg_row, pos_row)
    d_kv = share_key_grads(span, jnp.concatenate([dk, dv], axis=1).reshape(2, 2, 256, 1536))
    d_qkv = jnp.concatenate([dq, d_kv.reshape(512, 1536)], axis=1)
    d_wqkv = jnp.dot(x_rows.T, d_qkv, preferred_element_type=f32).astype(bf16)
    d_x = lax.dot_general(d_qkv, w_qkv, NT, preferred_element_type=f32)
    part_a = jnp.concatenate(
        [
            d_wqkv.reshape(768, 3, 4, 3, HEAD_DIM).transpose(2, 0, 1, 3, 4),
            d_wout_t.reshape(768, 4, 3, 1, HEAD_DIM).transpose(1, 0, 2, 3, 4),
        ],
        axis=3,
    ).reshape(2, 2, 4, 2, 96, 768)
    grad_tokens = (grad_one + d_x).astype(bf16).reshape(2, 256, 768)

    sums = jnp.stack(
        [
            jnp.sum(d_h1 * normed_one, axis=0),
            jnp.sum(grad_layer * normed_two, axis=0),
            jnp.sum(d_h1, axis=0),
            jnp.sum(grad_layer, axis=0),
        ]
    )
    squares = jnp.stack([jnp.sum(v * v) for v in (attn, resid_one, ffn, resid_two)])
    small = jnp.concatenate(
        [sums, jnp.pad(squares[None], ((0, 0), (0, 764))), jnp.zeros((3, 768), f32)], axis=0
    )
    out_a, out_f, out_s, lo, gt = scatter_all(
        span, part_a, part_f, small, layer_out.astype(bf16).reshape(2, 256, 768), grad_tokens
    )
    if span > 1:
        out_a = lax.psum_scatter(
            out_a, "fsdp", scatter_dimension=0, tiled=True, axis_index_groups=groups
        )
        out_f = lax.psum_scatter(
            out_f, "fsdp", scatter_dimension=0, tiled=True, axis_index_groups=groups
        )
        out_s = lax.psum(out_s, "fsdp", axis_index_groups=groups)
    out_a = out_a.reshape(shard_rows, 3, 4, HEAD_DIM)
    shard_start = lax.axis_index("fsdp") * shard_rows
    mine = lax.dynamic_slice_in_dim(out_s[:4], shard_start, shard_rows, 1)
    cells = float(lax.axis_size("fsdp") * 2 * 1024 * 768)
    return (
        lo,
        gt,
        out_a[:, :, :3].transpose(1, 0, 2, 3).reshape(3, shard_rows, 192),
        out_a[:, :, 3].reshape(shard_rows, 192).T,
        out_f[:, :1536].reshape(shard_rows, 2, 768),
        out_f[:, 1536:].T,
        mine[:2],
        mine[2:],
        jnp.sqrt(out_s[4, :4] / cells),
    )


def solution(mesh):
    placed = (
        P("fsdp", "tp", None),
        P("fsdp", None),
        P(None, "fsdp", "tp"),
        P("tp", "fsdp"),
        P("fsdp", None, "tp"),
        P("tp", "fsdp"),
        P(None, "fsdp"),
        P(None, "fsdp"),
        P("fsdp", "tp", None),
    )
    return jax.shard_map(
        local,
        mesh=mesh,
        in_specs=placed,
        out_specs=(
            P("fsdp", "tp", None),
            P("fsdp", "tp", None),
            P(None, "fsdp", "tp"),
            P("tp", "fsdp"),
            P("fsdp", None, "tp"),
            P("tp", "fsdp"),
            P(None, "fsdp"),
            P(None, "fsdp"),
            P(),
        ),
        check_vma=False,
    )
```

```python
from functools import partial

import jax
import jax.numpy as jnp
from jax import lax
from jax.experimental import pallas as pl
from jax.experimental.pallas import tpu as pltpu
from jax.sharding import PartitionSpec as P

HEADS = 12
HEAD_DIM = 64
MESH = pl.DeviceIdType.MESH
VMEM_LIMIT = 63 << 20
norm_eps = 1e-05
ROUNDS = 4
CUT = 48
NT = (((1,), (1,)), ((), ()))
NN = (((1,), (0,)), ((), ()))
CHUNK = 256


class Place:
    def __init__(self, span):
        index = lax.axis_index("fsdp")
        shard = lax.axis_index("tp")
        self.span = span
        self.j = index % span
        block = index // span
        self.z = block // 2
        self.y = block % 2
        self.x = shard // 2
        self.k = shard % 2

    def shifted(self, dx=0, dy=0, dz=0, dk=0):
        x = 1 - self.x if dx else self.x
        y = 1 - self.y if dy else self.y
        z = (self.z + dz) % 4 if dz else self.z
        k = 1 - self.k if dk else self.k
        return x, y, z, k

    def device(self, dx=0, dy=0, dz=0, dk=0):
        x, y, z, k = self.shifted(dx, dy, dz, dk)
        return ((z * 2 + y) * self.span + self.j, x * 2 + k)

    def greet(self, offsets):
        barrier = pltpu.get_barrier_semaphore()
        for offset in offsets:
            pl.semaphore_signal(
                barrier, inc=1, device_id=self.device(**offset), device_id_type=MESH
            )
        pl.semaphore_wait(barrier, len(offsets))


ALL_PEERS = ({"dx": 1}, {"dy": 1}, {"dz": 1}, {"dz": 2}, {"dz": 3}, {"dk": 1})


def remote(src, dst, send, recv, device):
    return pltpu.make_async_remote_copy(
        src_ref=src, dst_ref=dst, send_sem=send, recv_sem=recv, device_id=device, device_id_type=MESH
    )


def dot(a, b, dims=NN):
    return lax.dot_general(a, b, dims, preferred_element_type=jnp.float32)


class Copies:
    names = ()

    def start(self, *names):
        for name in names:
            self.copy(name).start()

    def wait(self, *names):
        for name in names:
            self.copy(name).wait_recv()

    def finish(self):
        for name in self.names:
            self.copy(name).wait_send()


class GatherRound(Copies):
    names = ("z1", "z2", "z3", "ax", "by", "ay0", "bx0", "ay1", "bx1") + tuple(
        "d%d" % i for i in range(7)
    )
    lines = {
        "ax": ((0, 0, "a"), {"dx": 1}),
        "by": ((0, 0, "b"), {"dy": 1}),
        "ay0": ((0, 0, "a"), {"dy": 1}),
        "bx0": ((0, 0, "b"), {"dx": 1}),
        "ay1": ((1, 0, "a"), {"dy": 1}),
        "bx1": ((0, 1, "b"), {"dx": 1}),
        "d0": ((0, 0, ""), {"dk": 1}),
        "d1": ((1, 0, "a"), {"dk": 1}),
        "d2": ((0, 1, "b"), {"dk": 1}),
        "d3": ((0, 1, "a"), {"dk": 1}),
        "d4": ((1, 0, "b"), {"dk": 1}),
        "d5": ((1, 1, "a"), {"dk": 1}),
        "d6": ((1, 1, "b"), {"dk": 1}),
    }
    steps = {
        2: ("ax", "ay1", "d1"),
        3: ("by", "bx1", "d2"),
        4: ("ay0", "d3"),
        5: ("bx0", "d4"),
        6: ("ay1", "d5"),
        7: ("bx1", "d6"),
    }

    def __init__(self, place, own, out, send, recv, keep):
        self.place, self.own, self.out = place, own, out
        self.send, self.recv, self.keep = send, recv, keep

    def line(self, dx, dy, part):
        x, y, z, k = self.place.shifted(dx, dy)
        rows = {"a": pl.ds(0, CUT), "b": pl.ds(CUT, 96 - CUT), "": pl.ds(0, 96)}[part]
        return self.out.at[x, k, :, y, rows, :]

    def copy(self, name):
        place = self.place
        at = self.names.index(name)
        send, recv = self.send.at[at], self.recv.at[at]
        if name[0] == "z":
            x, y, z, k = place.shifted()
            return remote(
                self.own, self.out.at[x, k, z, y], send, recv, place.device(dz=int(name[1]))
            )
        where, to = self.lines[name]
        ref = self.line(*where)
        return remote(ref, ref, send, recv, place.device(**to))

    def kept(self):
        x, y, z, k = self.place.shifted()
        return pltpu.make_async_copy(self.own, self.out.at[x, k, z, y], self.keep)

    def event(self, n):
        if n == 0:
            self.kept().start()
            self.start("z1", "z2", "z3")
        elif n == 1:
            self.kept().wait()
            self.wait("z1", "z2", "z3")
            self.start("ax", "by", "ay0", "bx0", "d0")
        elif n == 8:
            self.wait(*self.names[9:])
        else:
            self.wait(self.steps[n][0])
            self.start(*self.steps[n][1:])


class NormGather(Copies):
    names = ("z1", "z2", "z3", "y")

    def __init__(self, place, own, out, send, recv, keep):
        self.place, self.own, self.out = place, own, out
        self.send, self.recv, self.keep = send, recv, keep

    def copy(self, name):
        place = self.place
        at = self.names.index(name)
        send, recv = self.send.at[at], self.recv.at[at]
        if name == "y":
            ref = self.out.at[:, place.y]
            return remote(ref, ref, send, recv, place.device(dy=1))
        return remote(
            self.own, self.out.at[place.z, place.y], send, recv, place.device(dz=int(name[1]))
        )

    def kept(self):
        return pltpu.make_async_copy(self.own, self.out.at[self.place.z, self.place.y], self.keep)


class Events:
    def __init__(self, steps):
        self.steps = list(steps)

    def run(self, count):
        for step in self.steps[:count]:
            step()
        del self.steps[:count]

    def spread(self, trips, points, count):
        total = trips * points
        return self.place(trips, points, {n * total // max(count, 1): 1 for n in range(count)})

    def place(self, trips, points, counts):
        total = trips * points
        slots = [[] for _ in range(total)]
        for number in sorted(counts):
            slots[number] += self.steps[: counts[number]]
            del self.steps[: counts[number]]

        def stop(i, point):
            for trip in range(trips):
                todo = slots[trip * points + point]
                if todo:

                    @pl.when(i == trip)
                    def _():
                        for step in todo:
                            step()

        return stop


def lane_half(tile, half):
    lane = lax.broadcasted_iota(jnp.int32, tile.shape, 1)
    keep = (lane < HEAD_DIM) if half == 0 else (lane >= HEAD_DIM)
    return jnp.where(keep, tile, jnp.zeros_like(tile))


def swap_halves(tile):
    return pltpu.roll(tile.astype(jnp.float32), HEAD_DIM, 1)


def fill_distance(dist, seg_col, seg_row, pos_row):
    keys, queries = dist.shape
    key_pos = lax.broadcasted_iota(jnp.int32, (keys, queries), 0).astype(jnp.float32)
    gap = jnp.abs(key_pos - pos_row[...])
    dist[...] = jnp.where(seg_col[...] == seg_row[...], gap, 1e30)


def out_weights(w):
    first = lax.broadcasted_iota(jnp.int32, (768, 128), 1) < HEAD_DIM
    left = jnp.where(first, swap_halves(w[:, 128:256]), w[:, 384:512].astype(jnp.float32))
    right = jnp.where(first, swap_halves(w[:, 640:768]), 0.0)
    return left.astype(jnp.bfloat16), right.astype(jnp.bfloat16)


def whole(ref):
    value = ref[...]
    return value.reshape(768, value.shape[-1])


HEAD_SPOTS = ((0, 0), (0, 1), (1, 0))


def norm_stats(value):
    average = jnp.mean(value, axis=-1, keepdims=True)
    centered = value - average
    inv_std = lax.rsqrt(jnp.mean(centered * centered, axis=-1, keepdims=True) + norm_eps)
    return centered * inv_std, inv_std


def norm_backward(grad_val, normed, inv_std, gain_row):
    grad_norm = grad_val * gain_row
    return inv_std * (
        grad_norm
        - jnp.mean(grad_norm, axis=-1, keepdims=True)
        - normed * jnp.mean(grad_norm * normed, axis=-1, keepdims=True)
    )


ROWS = 128


def row_blocks(body):
    def step(i, carry):
        body(pl.ds(pl.multiple_of(i * ROWS, ROWS), ROWS), i)
        return carry

    lax.fori_loop(0, 512 // ROWS, step, 0)


def columns(value):
    return jnp.sum(value.reshape(value.shape[0] // 8, 8, value.shape[1]), axis=0)


def forward_kernel(
    span,
    slopes,
    shard,
    norm_rows,
    tok,
    cot,
    seg_col,
    seg_row,
    pos_row,
    o_weights,
    o_norms,
    o_x,
    o_cot,
    o_q,
    o_k,
    o_v,
    o_ctx,
    o_lse,
    o_kept,
    o_h1b,
    o_n1,
    o_i1,
    o_n2,
    o_i2,
    o_out,
    o_squares,
    weights,
    norms,
    xs,
    keys,
    values,
    dist,
    out_t,
    acc,
    h1,
    kept,
    g_send,
    g_recv,
    g_keep,
    n_send,
    n_recv,
    n_keep,
    t_sems,
    kv_send,
    kv_recv,
    store_sems,
    kept_sems,
):
    f32, bf16 = jnp.float32, jnp.bfloat16
    place = Place(span)
    x, y, z, k = place.shifted()
    rounds = [
        GatherRound(place, shard.at[r], weights.at[r], g_send.at[r], g_recv.at[r], g_keep.at[r])
        for r in range(ROUNDS)
    ]
    norm_gather = NormGather(place, norm_rows, norms, n_send, n_recv, n_keep)

    def swap(n):
        src, dst = ((tok, xs), (cot, o_cot))[n]
        return remote(
            src.at[1 - place.x],
            dst.at[place.x],
            t_sems.at[3 * n],
            t_sems.at[3 * n + 1],
            place.device(dx=1),
        )

    def stay(n):
        src, dst = ((tok, xs), (cot, o_cot))[n]
        return pltpu.make_async_copy(src.at[place.x], dst.at[place.x], t_sems.at[3 * n + 2])

    def store(n):
        src, dst = (
            (weights.at[0], o_weights.at[0]),
            (weights.at[1], o_weights.at[1]),
            (weights.at[2], o_weights.at[2]),
            (weights.at[3], o_weights.at[3]),
            (xs, o_x),
            (keys, o_k),
            (values, o_v),
        )[n]
        return pltpu.make_async_copy(src, dst, store_sems.at[n])

    place.greet(ALL_PEERS)
    swap(0).start()
    stay(0).start()
    stay(1).start()
    norm_gather.kept().start()
    norm_gather.start("z1", "z2", "z3")

    def step(r, n):
        def go():
            rounds[r].event(n)
            if n == 8:
                store(r).start()

        return go

    order = [(0, 0), (0, 1), (1, 0), (0, 2), (0, 3), (1, 1), (2, 0), (0, 4), (0, 5), (0, 6), (0, 7), (0, 8)]
    order += [(1, 2), (1, 3), (2, 1), (3, 0), (1, 4), (1, 5), (1, 6), (1, 7), (2, 2), (2, 3), (3, 1), (1, 8)]
    order += [(2, 4), (2, 5), (2, 6), (2, 7), (3, 2), (3, 3), (2, 8)]
    order += [(3, 4), (3, 5), (3, 6), (3, 7), (3, 8)]
    events = Events(step(*at) for at in order)
    events.steps.insert(-5, lambda: swap(1).start())

    events.run(2)
    fill_distance(dist, seg_col, seg_row, pos_row)
    norm_gather.kept().wait()
    norm_gather.wait("z1", "z2", "z3")
    norm_gather.start("y")
    events.run(10)
    swap(0).wait_recv()
    stay(0).wait()
    store(4).start()

    def share(t, n):
        ref = (keys, values)[n].at[pl.ds(2 * t, 2), :, place.k]
        return remote(ref, ref, kv_send.at[t, n], kv_recv.at[t, n], place.device(dk=1))

    def project(t, carry):
        w = whole(weights.at[0, t // 2, t % 2])
        for s in range(2):
            out = dot(xs[s], w).astype(bf16)
            for i in range(2):
                cols = slice(i * 128, i * 128 + 128)
                o_q[2 * t + i, pl.ds(s * 256, 256), :] = out[:, cols] * bf16(HEAD_DIM**-0.5)
                keys[2 * t + i, s, k] = out[:, 256 + i * 128 : 384 + i * 128]
                values[2 * t + i, s, k] = out[:, 512 + i * 128 : 640 + i * 128]
        share(t, 0).start()
        share(t, 1).start()
        return carry

    lax.fori_loop(0, 4, project, 0)
    out_t[1, pl.ds(HEAD_DIM, HEAD_DIM), :] = jnp.zeros((HEAD_DIM, 512), f32)
    stop = events.spread(4, 7, 12)

    def attend(t, carry):
        share(t, 0).wait_recv()
        share(t, 1).wait_recv()
        point = 0
        for spot, (tile, half) in enumerate(HEAD_SPOTS):
            slope = slopes[3 * t + spot]
            key = keys[2 * t + tile].reshape(1024, 128)
            rows = slice(half * HEAD_DIM, (half + 1) * HEAD_DIM)
            value_t = values[2 * t + tile].reshape(1024, 128).astype(f32).T.astype(bf16)[rows]
            for start in range(0, 512, CHUNK):
                cols = pl.ds(start, CHUNK)
                part = lane_half(o_q[2 * t + tile, cols, :], half)
                scores = dot(key, part, NT) - slope * dist[:, cols]
                peak = jnp.max(scores, axis=0, keepdims=True)
                expo = jnp.exp(scores - peak)
                total = jnp.sum(expo, axis=0, keepdims=True)
                out_t[tile, rows, cols] = dot(value_t, expo.astype(bf16)) / total
                o_lse[t, pl.ds(spot, 1), cols] = peak + jnp.log(total)
                stop(t, point)
                point += 1
        for tile in range(2):
            o_ctx[2 * t + tile] = out_t[tile].T.astype(bf16)
        left, right = out_weights(whole(weights.at[0, t // 2, t % 2]))
        mixed = dot(o_ctx[2 * t], left, NT) + dot(o_ctx[2 * t + 1], right, NT)

        @pl.when(t == 0)
        def _():
            acc[...] = mixed

        @pl.when(t > 0)
        def _():
            acc[...] += mixed

        stop(t, point)
        return carry

    lax.fori_loop(0, 4, attend, 0)
    store(5).start()
    store(6).start()
    norm_gather.wait("y")
    norm_sum = jnp.sum(norms[...].reshape(8, 8, 768), axis=0)
    o_norms[...] = norm_sum

    def first_norm(rows, i):
        attn = acc[rows, :]
        half = i // 2
        resid = xs[half, pl.ds(pl.multiple_of((i % 2) * ROWS, ROWS), ROWS), :].astype(f32) + attn
        normed, inv = norm_stats(resid)
        value = normed * norm_sum[0:1] + norm_sum[2:3]
        h1[rows, :] = value
        o_h1b[rows, :] = value.astype(bf16)
        o_n1[rows, :] = normed
        o_i1[rows, :] = inv
        acc[rows, :] = jnp.zeros_like(attn)
        if_first = jnp.where(i == 0, 0.0, 1.0)
        o_squares[0] = o_squares[0] * if_first + columns(attn * attn)
        o_squares[1] = o_squares[1] * if_first + columns(resid * resid)

    o_squares[...] = jnp.zeros_like(o_squares)
    row_blocks(first_norm)

    stop_f = events.place(
        12, 2, {1: 1, 2: 1, 3: 1, 4: 1, 5: 1, 6: 1, 8: 1, 9: 1, 11: 1, 12: 1, 13: 1, 14: 1, 16: 1}
    )
    assert not events.steps

    def keep_copy(n):
        return pltpu.make_async_copy(kept.at[n % 2], o_kept.at[n], kept_sems.at[n % 2])

    def feed(n, carry):
        r, t = 1 + n // 4, n % 4
        stop_f(n, 0)

        @pl.when(n >= 2)
        def _():
            keep_copy(n - 2).wait()

        ref = weights.at[r, t // 2, t % 2]
        for start in range(0, 512, CHUNK):
            rows = pl.ds(start, CHUNK)
            w = whole(ref)
            projected = dot(o_h1b[rows, :], w[:, :512])
            gate, up = projected[:, :256], projected[:, 256:]
            cdf = 0.5 + 0.5 * lax.erf(gate * (0.5**0.5))
            pdf = jnp.exp(-0.5 * gate * gate) * 0.3989422804014327
            act = gate * cdf
            hidden = (act * up).astype(bf16)
            kept[n % 2, 0, rows, :] = hidden
            kept[n % 2, 1, rows, :] = act.astype(bf16)
            kept[n % 2, 2, rows, :] = ((cdf + gate * pdf) * up).astype(bf16)
            acc[rows, :] += dot(hidden, w[:, 512:], NT)
        keep_copy(n).start()
        stop_f(n, 1)
        return carry

    lax.fori_loop(0, 12, feed, 0)

    def second_norm(rows, i):
        ffn = acc[rows, :]
        resid = h1[rows, :] + ffn
        normed, inv = norm_stats(resid)
        o_out[rows, :] = (normed * norm_sum[1:2] + norm_sum[3:4]).astype(bf16)
        o_n2[rows, :] = normed
        o_i2[rows, :] = inv
        o_squares[2] += columns(ffn * ffn)
        o_squares[3] += columns(resid * resid)

    row_blocks(second_norm)
    for n in (10, 11):
        keep_copy(n).wait()
    for r in rounds:
        r.finish()
    norm_gather.finish()
    for n in range(2):
        swap(n).wait_send()
    swap(1).wait_recv()
    stay(1).wait()
    for t in range(4):
        for n in range(2):
            share(t, n).wait_send()
    for n in range(7):
        store(n).wait()


def forward(span, slopes, shard, norm_rows, tok, cot, seg_col, seg_row, pos_row):
    f32, bf16 = jnp.float32, jnp.bfloat16
    any_space = pl.BlockSpec(memory_space=pl.ANY)
    vmem = pl.BlockSpec(memory_space=pltpu.VMEM)
    outs = (
        ((ROUNDS, 2, 2, 4, 2, 96, 768), bf16, any_space),
        ((8, 768), f32, vmem),
        ((2, 256, 768), bf16, any_space),
        ((2, 256, 768), bf16, any_space),
        ((8, 512, 128), bf16, vmem),
        ((8, 2, 2, 256, 128), bf16, any_space),
        ((8, 2, 2, 256, 128), bf16, any_space),
        ((8, 512, 128), bf16, vmem),
        ((4, 8, 512), f32, vmem),
        ((12, 3, 512, 256), bf16, any_space),
        ((512, 768), bf16, vmem),
        ((512, 768), f32, vmem),
        ((512, 1), f32, vmem),
        ((512, 768), f32, vmem),
        ((512, 1), f32, vmem),
        ((512, 768), bf16, vmem),
        ((4, 8, 768), f32, vmem),
    )
    dma = pltpu.SemaphoreType.DMA
    return pl.pallas_call(
        partial(forward_kernel, span),
        out_shape=tuple(jax.ShapeDtypeStruct(s, d) for s, d, _ in outs),
        in_specs=[pl.BlockSpec(memory_space=pltpu.SMEM)] + [vmem] * 7,
        out_specs=tuple(spec for _, _, spec in outs),
        scratch_shapes=[
            pltpu.VMEM((ROUNDS, 2, 2, 4, 2, 96, 768), bf16),
            pltpu.VMEM((4, 2, 8, 768), f32),
            pltpu.VMEM((2, 256, 768), bf16),
            pltpu.VMEM((8, 2, 2, 256, 128), bf16),
            pltpu.VMEM((8, 2, 2, 256, 128), bf16),
            pltpu.VMEM((1024, 512), f32),
            pltpu.VMEM((2, 128, 512), f32),
            pltpu.VMEM((512, 768), f32),
            pltpu.VMEM((512, 768), f32),
            pltpu.VMEM((2, 3, 512, 256), bf16),
            dma((ROUNDS, 16)),
            dma((ROUNDS, 16)),
            dma((ROUNDS,)),
            dma((4,)),
            dma((4,)),
            dma,
            dma((6,)),
            dma((4, 2)),
            dma((4, 2)),
            dma((7,)),
            dma((2,)),
        ],
        compiler_params=pltpu.CompilerParams(
            collective_id=0, has_side_effects=True, vmem_limit_bytes=VMEM_LIMIT
        ),
        name="forward",
    )(slopes, shard, norm_rows, tok, cot, seg_col, seg_row, pos_row)


class ScatterRound(Copies):
    names = ("ay1", "bx", "ay0", "ax", "by", "az1", "az2", "az3", "bz1", "bz2", "bz3")

    def __init__(self, place, held, twin, stage, land_ay, land_bx, land_ax, land_by, land_z, send, recv, pair):
        self.place, self.held, self.twin, self.stage = place, held, twin, stage
        self.land_ay, self.land_bx, self.land_ax = land_ay, land_bx, land_ax
        self.land_by, self.land_z = land_by, land_z
        self.send, self.recv, self.pair = send, recv, pair

    def copy(self, name):
        p = self.place
        at = self.names.index(name)
        send, recv = self.send.at[at], self.recv.at[at]
        a, b = pl.ds(0, CUT), pl.ds(CUT, 96 - CUT)
        if name in ("ay1", "ay0"):
            dx = int(name[2])
            return remote(
                self.held.at[dx, :, 1 - p.y, a, :], self.land_ay.at[dx], send, recv, p.device(dy=1)
            )
        if name == "bx":
            return remote(self.held.at[1, :, :, b, :], self.land_bx, send, recv, p.device(dx=1))
        if name == "ax":
            return remote(self.held.at[1, :, p.y, a, :], self.land_ax, send, recv, p.device(dx=1))
        if name == "by":
            return remote(self.held.at[0, :, 1 - p.y, b, :], self.land_by, send, recv, p.device(dy=1))
        step = int(name[2])
        rows = a if name[0] == "a" else b
        return remote(
            self.held.at[0, (p.z + step) % 4, p.y, rows, :],
            self.land_z.at[step - 1, rows, :],
            send,
            recv,
            p.device(dz=step),
        )

    def push(self, dx):
        return remote(
            self.stage.at[dx], self.twin.at[dx], self.pair.at[0, dx], self.pair.at[1, dx], self.place.device(dk=1)
        )

    def add(self, ref, other):
        ref[...] = (ref[...].astype(jnp.float32) + other[...].astype(jnp.float32)).astype(jnp.bfloat16)

    def pair_sum(self, dx):
        self.push(dx).wait_recv()

        def body(i, carry):
            self.add(self.held.at[dx, i], self.twin.at[dx, i])
            return carry

        lax.fori_loop(0, 4, body, 0)
        if dx:
            self.start("bx", "ay1")
        else:
            self.start("ay0")

    def event(self, n, out=None):
        p = self.place
        a, b = pl.ds(0, CUT), pl.ds(CUT, 96 - CUT)
        if n == 0:
            self.wait("ay1")
            self.add(self.held.at[1, :, p.y, a, :], self.land_ay.at[1])
            self.start("ax")
        elif n == 1:
            self.wait("bx")
            self.add(self.held.at[0, :, 1 - p.y, b, :], self.land_bx.at[:, 1 - p.y])
            self.start("by")
            self.add(self.held.at[0, :, p.y, b, :], self.land_bx.at[:, p.y])
        elif n == 2:
            self.wait("ay0")
            self.add(self.held.at[0, :, p.y, a, :], self.land_ay.at[0])
        elif n == 3:
            self.wait("ax")
            self.add(self.held.at[0, :, p.y, a, :], self.land_ax)
            self.start("az1", "az2", "az3")
        elif n == 4:
            self.wait("by")
            self.add(self.held.at[0, :, p.y, b, :], self.land_by)
            self.start("bz1", "bz2", "bz3")
        else:
            self.wait("az1", "az2", "az3", "bz1", "bz2", "bz3")
            total = self.held[0, p.z, p.y].astype(jnp.float32)
            for step in range(3):
                total = total + self.land_z[step].astype(jnp.float32)
            out[...] = total


def backward_kernel(
    span,
    slopes,
    i_weights,
    norms,
    i_x,
    i_cot,
    i_q,
    i_k,
    i_v,
    i_ctx,
    i_lse,
    i_kept,
    i_h1b,
    i_n1,
    i_i1,
    i_n2,
    i_i2,
    i_out,
    squares,
    seg_col,
    seg_row,
    pos_row,
    o_out,
    o_tokens,
    o_grads,
    o_small,
    w_buf,
    kept,
    h1_t,
    f_t,
    d_rows,
    n_buf,
    d_h1,
    q,
    keys,
    values,
    ctx,
    lse,
    dist,
    d_ctx,
    d_kv,
    d_kv_in,
    dq_t,
    acc_k,
    acc_v,
    held,
    twin,
    stage,
    land_ay,
    land_bx,
    land_ax,
    land_by,
    land_z,
    small,
    small_in,
    load_sems,
    step_sems,
    r_send,
    r_recv,
    r_pair,
    t_sems,
    kv_send,
    kv_recv,
    s_send,
    s_recv,
):
    f32, bf16 = jnp.float32, jnp.bfloat16
    place = Place(span)
    x, y, z, k = place.shifted()
    rounds = [
        ScatterRound(
            place,
            held.at[n],
            twin.at[n % 3],
            stage,
            land_ay.at[n],
            land_bx.at[n],
            land_ax.at[n],
            land_by.at[n],
            land_z.at[n],
            r_send.at[n],
            r_recv.at[n],
            r_pair.at[n],
        )
        for n in range(ROUNDS)
    ]

    def load(n):
        src, dst = (
            (i_cot, d_rows.at[2]),
            (i_n2, n_buf),
            (i_h1b, d_rows.at[1]),
            (i_x, d_rows.at[2]),
            (i_q, q),
            (i_k, keys),
            (i_v, values),
            (i_ctx, ctx),
            (i_lse, lse),
            (i_n1, n_buf),
        )[n]
        return pltpu.make_async_copy(src, dst, load_sems.at[n])

    def where(n):
        return x ^ (1 - n % 2), jnp.where(n < 2, 1 - k, k)

    def fetch(n, part):
        r = 3 - n // 4
        wx, wk = where(n % 4)
        if part == 0:
            return pltpu.make_async_copy(i_weights.at[r, wx, wk], w_buf.at[n % 2], step_sems.at[n % 2, 0])
        return pltpu.make_async_copy(
            i_kept.at[(r - 1) * 4 + wx * 2 + wk], kept.at[n % 2], step_sems.at[n % 2, 1]
        )

    for n in (0, 1, 2, 4, 5, 6, 7, 8):
        load(n).start()
    fetch(0, 0).start()
    fetch(0, 1).start()
    place.greet(ALL_PEERS)

    def swap(n):
        src, dst = ((i_out, o_out), (d_rows.at[0], o_tokens))[n]
        return remote(
            src.at[1 - place.x],
            dst.at[place.x],
            t_sems.at[3 * n],
            t_sems.at[3 * n + 1],
            place.device(dx=1),
        )

    def stay(n):
        src, dst = ((i_out, o_out), (d_rows.at[0], o_tokens))[n]
        return pltpu.make_async_copy(src.at[place.x], dst.at[place.x], t_sems.at[3 * n + 2])

    swap(0).start()
    stay(0).start()
    load(0).wait()
    load(1).wait()
    small[...] = jnp.zeros_like(small)

    def halves(ref, i):
        return ref.at[i // 2, pl.ds(pl.multiple_of((i % 2) * ROWS, ROWS), ROWS), :]

    sums = [jnp.zeros((8, 768), f32)] * 2
    for i in range(512 // ROWS):
        rows = pl.ds(i * ROWS, ROWS)
        grad = halves(d_rows.at[2], i)[...].astype(f32)
        normed = n_buf[rows, :]
        out = norm_backward(grad, normed, i_i2[rows, :], norms[1:2])
        d_h1[rows, :] = out
        halves(d_rows.at[0], i)[...] = out.astype(bf16)
        f_t[:, rows] = out.T.astype(bf16)
        sums[0] = sums[0] + columns(grad * normed)
        sums[1] = sums[1] + columns(grad)
    small[1] = sums[0]
    small[3] = sums[1]
    load(9).start()
    load(3).start()
    load(2).wait()
    for i in range(512 // ROWS):
        rows = pl.ds(i * ROWS, ROWS)
        h1_t[:, rows] = halves(d_rows.at[1], i)[...].astype(f32).T.astype(bf16)
    fill_distance(dist, seg_col, seg_row, pos_row)

    def pair(n, dx):
        return lambda: rounds[n].pair_sum(dx)

    def step(n, at):
        return lambda: rounds[n].event(at, o_grads.at[3 - n])

    def put(n, dx, value, cols):
        block = value.astype(bf16).reshape(4, 2, 96, value.shape[-1])

        @pl.when(n % 4 < 2)
        def _():
            stage[dx, :, :, :, cols] = block

        @pl.when(n % 4 >= 2)
        def _():
            held[n // 4, dx, :, :, :, cols] = block

    def push(n, dx):
        return remote(
            stage.at[dx], twin.at[n % 3, dx], r_pair.at[n, 0, dx], r_pair.at[n, 1, dx], place.device(dk=1)
        )

    plan = {
        2: [pair(0, 1)],
        3: [pair(0, 0)],
        5: [step(0, 0), step(0, 1)],
        6: [step(0, 2), pair(1, 1)],
        7: [pair(1, 0), step(0, 3), step(0, 4)],
        9: [step(1, 0), step(1, 1), step(0, 5)],
        10: [step(1, 2), pair(2, 1)],
        11: [pair(2, 0), step(1, 3), step(1, 4)],
    }

    def feed(n, carry):
        dx = 1 - n % 2

        @pl.when(n < 11)
        def _():
            fetch(n + 1, 0).start()
            fetch(n + 1, 1).start()

        @pl.when(n % 4 < 2)
        def _():
            @pl.when(n >= 4)
            def _():
                push(n // 4 - 1, dx).wait_send()

        fetch(n, 0).wait()
        fetch(n, 1).wait()
        w = whole(w_buf.at[n % 2])
        hold = kept.at[n % 2]
        d_ffn = d_rows[0].reshape(512, 768)
        put(n, dx, dot(f_t[...], hold[0]), slice(512, 768))
        d_hidden = dot(d_ffn, w[:, 512:])
        d_gate = (d_hidden * hold[2].astype(f32)).astype(bf16)
        d_up = (d_hidden * hold[1].astype(f32)).astype(bf16)
        put(n, dx, dot(h1_t[...], d_gate), slice(0, 256))
        put(n, dx, dot(h1_t[...], d_up), slice(256, 512))

        @pl.when(n % 4 < 2)
        def _():
            push(n // 4, dx).start()

        d_h1[...] += dot(d_gate, w[:, :256], NT) + dot(d_up, w[:, 256:512], NT)
        for at, todo in plan.items():

            @pl.when(n == at)
            def _():
                for item in todo:
                    item()

        return carry

    lax.fori_loop(0, 12, feed, 0)
    load(9).wait()
    load(3).wait()
    for i in range(512 // ROWS):
        rows = pl.ds(i * ROWS, ROWS)
        h1_t[:, rows] = halves(d_rows.at[2], i)[...].astype(f32).T.astype(bf16)
    sums = [jnp.zeros((8, 768), f32)] * 2
    for i in range(512 // ROWS):
        rows = pl.ds(i * ROWS, ROWS)
        grad = d_h1[rows, :]
        normed = n_buf[rows, :]
        out = norm_backward(grad, normed, i_i1[rows, :], norms[0:1])
        d_h1[rows, :] = out
        halves(d_rows.at[1], i)[...] = out.astype(bf16)
        f_t[:, rows] = out.T.astype(bf16)
        sums[0] = sums[0] + columns(grad * normed)
        sums[1] = sums[1] + columns(grad)
    small[0] = sums[0]
    small[2] = sums[1]
    for n in range(4, 9):
        load(n).wait()

    def fetch_a(n):
        wx, wk = where(n)
        return pltpu.make_async_copy(i_weights.at[0, wx, wk], w_buf.at[n % 2], step_sems.at[n % 2, 0])

    def fetch_b(t):
        return pltpu.make_async_copy(
            i_weights.at[0, t // 2, t % 2], w_buf.at[t % 2], step_sems.at[t % 2, 0]
        )

    fetch_b(0).start()
    dq_t[1, pl.ds(HEAD_DIM, HEAD_DIM), :] = jnp.zeros((HEAD_DIM, 512), f32)

    def share(t):
        return remote(
            d_kv.at[t, :, :, :, 1 - place.k], d_kv_in.at[t], kv_send.at[t], kv_recv.at[t], place.device(dk=1)
        )

    events = Events(
        [
            step(1, 5),
            step(2, 0),
            step(2, 1),
            step(2, 2),
            step(2, 3),
            step(2, 4),
        ]
    )
    stop = events.spread(4, 6, 6)

    def attend(t, carry):
        @pl.when(t < 3)
        def _():
            fetch_b(t + 1).start()

        fetch_b(t).wait()
        left, right = out_weights(whole(w_buf.at[t % 2]))
        d_attn = d_rows[1].reshape(512, 768)
        d_ctx[0] = dot(d_attn, left).astype(bf16)
        d_ctx[1] = dot(d_attn, right).astype(bf16)
        point = 0
        for spot, (tile, half) in enumerate(HEAD_SPOTS):
            slope = slopes[3 * t + spot]
            key = keys[2 * t + tile].reshape(1024, 128)
            value = values[2 * t + tile].reshape(1024, 128)
            rows = slice(half * HEAD_DIM, (half + 1) * HEAD_DIM)
            key_t = key.astype(f32).T.astype(bf16)[rows]
            product = ctx[2 * t + tile].astype(f32) * d_ctx[tile].astype(f32)
            delta = jnp.sum(product.T[rows], axis=0, keepdims=True)
            for start in range(0, 512, CHUNK):
                cols = pl.ds(start, CHUNK)
                part = lane_half(q[2 * t + tile, cols, :], half)
                grad = lane_half(d_ctx[tile, cols, :], half)
                scores = dot(key, part, NT) - slope * dist[:, cols]
                probs = jnp.exp(scores - lse[t, pl.ds(spot, 1), cols])
                grad_probs = dot(value, grad, NT)
                term_v = dot(probs.astype(bf16), grad)
                grad_scores = (probs * (grad_probs - delta[:, start : start + CHUNK])).astype(bf16)
                term_k = dot(grad_scores, part)
                if half == 0 and start == 0:
                    acc_v[...] = term_v
                    acc_k[...] = term_k
                else:
                    acc_v[...] += term_v
                    acc_k[...] += term_k
                dq_t[tile, rows, cols] = dot(key_t, grad_scores)
                stop(t, point)
                point += 1
            if half == 1 or tile == 1:
                d_kv[t, 0, tile] = acc_k[...].astype(bf16).reshape(2, 2, 256, 128)
                d_kv[t, 1, tile] = acc_v[...].astype(bf16).reshape(2, 2, 256, 128)
        share(t).start()
        for tile in range(2):
            q[2 * t + tile] = (dq_t[tile].T * HEAD_DIM**-0.5).astype(bf16)
        return carry

    lax.fori_loop(0, 4, attend, 0)
    fetch_a(0).start()
    first = lax.broadcasted_iota(jnp.int32, (768, 128), 1) < HEAD_DIM

    def project(n, carry):
        dx = 1 - n % 2
        wx, wk = where(n)
        t = wx * 2 + wk

        @pl.when(n < 3)
        def _():
            fetch_a(n + 1).start()

        @pl.when(n < 2)
        def _():
            push(2, dx).wait_send()

        share(t).wait_recv()
        parts = [q[2 * t], q[2 * t + 1]]
        for kind in range(2):
            for tile in range(2):
                mine = d_kv[t, kind, tile, :, k].reshape(512, 128).astype(f32)
                mine = mine + d_kv_in[t, kind, tile].reshape(512, 128).astype(f32)
                parts.append(mine.astype(bf16))
        d_qkv = jnp.concatenate(parts, axis=1)
        d_w = dot(h1_t[...], d_qkv)
        left = dot(f_t[...], ctx[2 * t])
        right = swap_halves(dot(f_t[...], ctx[2 * t + 1]))
        tiles = [
            d_w[:, 0:128],
            jnp.where(first, d_w[:, 128:256], pltpu.roll(left, HEAD_DIM, 1)),
            d_w[:, 256:384],
            jnp.where(first, d_w[:, 384:512], left),
            d_w[:, 512:640],
            jnp.where(first, d_w[:, 640:768], right),
        ]
        put(12 + n, dx, jnp.concatenate(tiles, axis=1), slice(0, 768))

        @pl.when(n < 2)
        def _():
            push(3, dx).start()

        fetch_a(n).wait()
        d_h1[...] += dot(d_qkv, whole(w_buf.at[n % 2]), NT)
        for at in (2, 3):

            @pl.when(n == at)
            def _():
                rounds[3].pair_sum(3 - at)

        return carry

    lax.fori_loop(0, 4, project, 0)
    for i in range(512 // ROWS):
        rows = pl.ds(i * ROWS, ROWS)
        halves(d_rows.at[0], i)[...] = d_h1[rows, :].astype(bf16)
    swap(1).start()
    stay(1).start()
    total = jnp.concatenate(
        [jnp.sum(small[i], axis=0, keepdims=True) for i in range(4)]
        + [jnp.sum(squares[i], axis=0, keepdims=True) for i in range(4)],
        axis=0,
    )

    def spread(n):
        to = ({"dk": 1}, {"dx": 1}, {"dy": 1}, {"dz": 1}, {"dz": 2}, {"dz": 3})[n]
        src = small.at[min(n, 3)]
        return remote(src, small_in.at[n], s_send.at[n], s_recv.at[n], place.device(**to))

    small[0] = total
    for n in range(3):
        spread(n).start()
        spread(n).wait_recv()
        total = total + small_in[n]
        small[n + 1] = total
    for n in range(3, 6):
        spread(n).start()
    rounds[3].event(0)
    rounds[3].event(1)
    rounds[2].event(5, o_grads.at[1])
    for at in range(2, 6):
        rounds[3].event(at, o_grads.at[0])
    for n in range(3, 6):
        spread(n).wait_recv()
    result = jnp.zeros_like(total)
    for at in range(4):
        step_of = (place.z - at) % 4
        term = jnp.where(
            step_of == 0,
            total,
            jnp.where(step_of == 1, small_in[3], jnp.where(step_of == 2, small_in[4], small_in[5])),
        )
        result = result + term
    o_small[...] = result
    for n in range(6):
        spread(n).wait_send()
    for r in rounds:
        r.finish()
    for dx in range(2):
        push(3, dx).wait_send()
    for t in range(4):
        share(t).wait_send()
    for n in range(2):
        swap(n).wait()
        stay(n).wait()


def backward(span, slopes, saved, seg_col, seg_row, pos_row):
    f32, bf16 = jnp.float32, jnp.bfloat16
    any_space = pl.BlockSpec(memory_space=pl.ANY)
    vmem = pl.BlockSpec(memory_space=pltpu.VMEM)
    dma = pltpu.SemaphoreType.DMA
    (weights, norms, xs, cot, q, keys, values, ctx, lse, kept, h1b, n1, i1, n2, i2, out, squares) = saved
    h1b = h1b.reshape(2, 256, 768)
    out = out.reshape(2, 256, 768)
    in_specs = [pl.BlockSpec(memory_space=pltpu.SMEM), any_space, vmem] + [any_space] * 10
    in_specs += [vmem, any_space, vmem, any_space, vmem, vmem, vmem, vmem]
    rest = 96 - CUT
    return pl.pallas_call(
        partial(backward_kernel, span),
        out_shape=(
            jax.ShapeDtypeStruct((2, 256, 768), bf16),
            jax.ShapeDtypeStruct((2, 256, 768), bf16),
            jax.ShapeDtypeStruct((ROUNDS, 96, 768), f32),
            jax.ShapeDtypeStruct((8, 768), f32),
        ),
        in_specs=in_specs,
        out_specs=(any_space, any_space, vmem, vmem),
        scratch_shapes=[
            pltpu.VMEM((2, 4, 2, 96, 768), bf16),
            pltpu.VMEM((2, 3, 512, 256), bf16),
            pltpu.VMEM((768, 512), bf16),
            pltpu.VMEM((768, 512), bf16),
            pltpu.VMEM((3, 2, 256, 768), bf16),
            pltpu.VMEM((512, 768), f32),
            pltpu.VMEM((512, 768), f32),
            pltpu.VMEM((8, 512, 128), bf16),
            pltpu.VMEM((8, 2, 2, 256, 128), bf16),
            pltpu.VMEM((8, 2, 2, 256, 128), bf16),
            pltpu.VMEM((8, 512, 128), bf16),
            pltpu.VMEM((4, 8, 512), f32),
            pltpu.VMEM((1024, 512), f32),
            pltpu.VMEM((2, 512, 128), bf16),
            pltpu.VMEM((4, 2, 2, 2, 2, 256, 128), bf16),
            pltpu.VMEM((4, 2, 2, 2, 256, 128), bf16),
            pltpu.VMEM((2, 128, 512), f32),
            pltpu.VMEM((1024, 128), f32),
            pltpu.VMEM((1024, 128), f32),
            pltpu.VMEM((ROUNDS, 2, 4, 2, 96, 768), bf16),
            pltpu.VMEM((3, 2, 4, 2, 96, 768), bf16),
            pltpu.VMEM((2, 4, 2, 96, 768), bf16),
            pltpu.VMEM((ROUNDS, 2, 4, CUT, 768), bf16),
            pltpu.VMEM((ROUNDS, 4, 2, rest, 768), bf16),
            pltpu.VMEM((ROUNDS, 4, CUT, 768), bf16),
            pltpu.VMEM((ROUNDS, 4, rest, 768), bf16),
            pltpu.VMEM((ROUNDS, 3, 96, 768), bf16),
            pltpu.VMEM((4, 8, 768), f32),
            pltpu.VMEM((6, 8, 768), f32),
            dma((10,)),
            dma((2, 2)),
            dma((ROUNDS, 11)),
            dma((ROUNDS, 11)),
            dma((ROUNDS, 2, 2)),
            dma((6,)),
            dma((4,)),
            dma((4,)),
            dma((6,)),
            dma((6,)),
        ],
        compiler_params=pltpu.CompilerParams(
            collective_id=1, has_side_effects=True, vmem_limit_bytes=VMEM_LIMIT
        ),
        name="backward",
    )(
        slopes,
        weights,
        norms,
        xs,
        cot,
        q,
        keys,
        values,
        ctx,
        lse,
        kept,
        h1b,
        n1,
        i1,
        n2,
        i2,
        out,
        squares,
        seg_col,
        seg_row,
        pos_row,
    )


def local(
    tokens,
    segment_ids,
    query_key_value_weight,
    w_out,
    input_weight,
    w_down,
    norm_gains,
    norm_biases,
    cotangent,
):
    f32 = jnp.float32
    shard_rows = query_key_value_weight.shape[1]
    span = 96 // shard_rows
    groups = None
    if span > 1:
        count = lax.axis_size("fsdp")
        groups = [list(range(i, i + span)) for i in range(0, count, span)]
    place_x = lax.axis_index("tp") // 2
    place_k = lax.axis_index("tp") % 2
    block = lax.axis_index("fsdp") // span

    heads = query_key_value_weight.transpose(1, 0, 2).reshape(shard_rows, 3, 3, HEAD_DIM)
    w_out_t = w_out.T.reshape(shard_rows, 3, 1, HEAD_DIM)
    wa = jnp.concatenate([heads, w_out_t], axis=2).reshape(shard_rows, 1, 768)
    gate_up = input_weight.reshape(shard_rows, 2, 3, 256).transpose(0, 2, 1, 3)
    down = w_down.T.reshape(shard_rows, 3, 1, 256)
    wf = jnp.concatenate([gate_up, down], axis=2).reshape(shard_rows, 3, 768)
    shard = jnp.concatenate([wa, wf], axis=1).transpose(1, 0, 2)
    norms = jnp.concatenate([norm_gains, norm_biases], axis=0).astype(f32)
    if span > 1:
        shard = lax.all_gather(shard, "fsdp", axis=1, tiled=True, axis_index_groups=groups)
        norms = lax.all_gather(norms, "fsdp", axis=1, tiled=True, axis_index_groups=groups)
    norm_rows = lax.dynamic_update_slice(jnp.zeros((8, 768), f32), norms, (0, block * 96))

    segment = lax.dynamic_index_in_dim(segment_ids, place_x, 0, keepdims=False)
    seg_col = segment.reshape(1024, 1)
    seg_row = lax.dynamic_index_in_dim(segment.reshape(2, 2, 256), place_k, 1, keepdims=False)
    seg_row = seg_row.reshape(1, 512)
    pos_row = (
        lax.broadcasted_iota(jnp.int32, (2, 256), 0) * 512
        + place_k * 256
        + lax.broadcasted_iota(jnp.int32, (2, 256), 1)
    )
    pos_row = pos_row.reshape(1, 512).astype(f32)
    slopes = jnp.exp2(-8.0 * (jnp.arange(HEADS).astype(f32) + 1.0) / HEADS)

    saved = forward(span, slopes, shard, norm_rows, tokens, cotangent, seg_col, seg_row, pos_row)
    layer_out, grad_tokens, grads, small = backward(span, slopes, saved, seg_col, seg_row, pos_row)

    if span > 1:
        grads = lax.psum_scatter(
            grads, "fsdp", scatter_dimension=1, tiled=True, axis_index_groups=groups
        )
        small = lax.psum(small, "fsdp", axis_index_groups=groups)
    grads_a = grads[0].reshape(shard_rows, 3, 4, HEAD_DIM)
    grads_f = grads[1:].reshape(3, shard_rows, 3, 256)
    shard_start = lax.axis_index("fsdp") * shard_rows
    mine = lax.dynamic_slice_in_dim(small[:4], shard_start, shard_rows, 1)
    cells = float(lax.axis_size("fsdp") * 2 * 1024 * 768)
    return (
        layer_out,
        grad_tokens,
        grads_a[:, :, :3].transpose(1, 0, 2, 3).reshape(3, shard_rows, 192),
        grads_a[:, :, 3].reshape(shard_rows, 192).T,
        grads_f[:, :, :2].transpose(1, 2, 0, 3).reshape(shard_rows, 2, 768),
        grads_f[:, :, 2].transpose(0, 2, 1).reshape(768, shard_rows),
        mine[:2],
        mine[2:],
        jnp.sqrt(jnp.sum(small[4:], axis=1) / cells),
    )


def solution(mesh):
    placed = (
        P("fsdp", "tp", None),
        P("fsdp", None),
        P(None, "fsdp", "tp"),
        P("tp", "fsdp"),
        P("fsdp", None, "tp"),
        P("tp", "fsdp"),
        P(None, "fsdp"),
        P(None, "fsdp"),
        P("fsdp", "tp", None),
    )
    return jax.shard_map(
        local,
        mesh=mesh,
        in_specs=placed,
        out_specs=(
            P("fsdp", "tp", None),
            P("fsdp", "tp", None),
            P(None, "fsdp", "tp"),
            P("tp", "fsdp"),
            P("fsdp", None, "tp"),
            P("tp", "fsdp"),
            P(None, "fsdp"),
            P(None, "fsdp"),
            P(),
        ),
        check_vma=False,
    )
```

```python
from functools import partial

import jax
import jax.numpy as jnp
from jax import lax
from jax.experimental import pallas as pl
from jax.experimental.pallas import tpu as pltpu
from jax.sharding import PartitionSpec as P

HEADS = 12
HEAD_DIM = 64
MESH = pl.DeviceIdType.MESH
VMEM_LIMIT = 63 << 20
norm_eps = 1e-05
ROUNDS = 4
NT = (((1,), (1,)), ((), ()))
NN = (((1,), (0,)), ((), ()))
CHUNK = 256


class Place:
    def __init__(self, span):
        index = lax.axis_index("fsdp")
        shard = lax.axis_index("tp")
        self.span = span
        self.j = index % span
        block = index // span
        self.z = block // 2
        self.y = block % 2
        self.x = shard // 2
        self.k = shard % 2

    def shifted(self, dx=0, dy=0, dz=0, dk=0):
        x = 1 - self.x if dx else self.x
        y = 1 - self.y if dy else self.y
        z = (self.z + dz) % 4 if dz else self.z
        k = 1 - self.k if dk else self.k
        return x, y, z, k

    def device(self, dx=0, dy=0, dz=0, dk=0):
        x, y, z, k = self.shifted(dx, dy, dz, dk)
        return ((z * 2 + y) * self.span + self.j, x * 2 + k)

    def greet(self, offsets):
        barrier = pltpu.get_barrier_semaphore()
        for offset in offsets:
            pl.semaphore_signal(
                barrier, inc=1, device_id=self.device(**offset), device_id_type=MESH
            )
        pl.semaphore_wait(barrier, len(offsets))


ALL_PEERS = ({"dx": 1}, {"dy": 1}, {"dz": 1}, {"dz": 2}, {"dz": 3}, {"dk": 1})


def remote(src, dst, send, recv, device):
    return pltpu.make_async_remote_copy(
        src_ref=src, dst_ref=dst, send_sem=send, recv_sem=recv, device_id=device, device_id_type=MESH
    )


PARTS = {
    "a": pl.ds(0, 32),
    "c": pl.ds(32, 16),
    "ac": pl.ds(0, 48),
    "b": pl.ds(48, 32),
    "d": pl.ds(80, 16),
    "bd": pl.ds(48, 48),
    "": pl.ds(0, 96),
}


def dot(a, b, dims=NN):
    return lax.dot_general(a, b, dims, preferred_element_type=jnp.float32)


class Copies:
    names = ()

    def start(self, *names):
        for name in names:
            self.copy(name).start()

    def wait(self, *names):
        for name in names:
            self.copy(name).wait_recv()

    def finish(self):
        for name in self.names:
            self.copy(name).wait_send()


class GatherRound(Copies):
    names = ("z1", "z2", "z3", "ax", "by", "ay0", "bx0", "ay1", "bx1") + tuple(
        "d%d" % i for i in range(7)
    )
    names += ("cx", "cz1", "cz2", "cz3", "dy", "dz1", "dz2", "dz3")
    lines = {
        "ax": ((0, 0, "a"), {"dx": 1}),
        "by": ((0, 0, "b"), {"dy": 1}),
        "ay0": ((0, 0, "ac"), {"dy": 1}),
        "bx0": ((0, 0, "bd"), {"dx": 1}),
        "ay1": ((1, 0, "ac"), {"dy": 1}),
        "bx1": ((0, 1, "bd"), {"dx": 1}),
        "d0": ((0, 0, ""), {"dk": 1}),
        "d1": ((1, 0, "ac"), {"dk": 1}),
        "d2": ((0, 1, "bd"), {"dk": 1}),
        "d3": ((0, 1, "ac"), {"dk": 1}),
        "d4": ((1, 0, "bd"), {"dk": 1}),
        "d5": ((1, 1, "ac"), {"dk": 1}),
        "d6": ((1, 1, "bd"), {"dk": 1}),
    }
    steps = {
        3: (("ax", "cz1", "cz2", "cz3"), ("ay1", "d1")),
        4: (("by", "dz1", "dz2", "dz3"), ("bx1", "d2")),
        5: (("ay0",), ("d3",)),
        6: (("bx0",), ("d4",)),
        7: (("ay1",), ("d5",)),
        8: (("bx1",), ("d6",)),
    }
    last = 9

    def __init__(self, place, own, out, send, recv, keep):
        self.place, self.own, self.out = place, own, out
        self.send, self.recv, self.keep = send, recv, keep

    def line(self, dx, dy, part):
        x, y, z, k = self.place.shifted(dx, dy)
        return self.out.at[x, k, :, y, PARTS[part], :]

    def copy(self, name):
        place = self.place
        at = self.names.index(name)
        send, recv = self.send.at[at], self.recv.at[at]
        x, y, z, k = place.shifted()
        if name[0] == "z":
            return remote(
                self.own, self.out.at[x, k, z, y], send, recv, place.device(dz=int(name[1]))
            )
        if name in ("cx", "dy"):
            rows = PARTS[name[0]]
            return remote(
                self.own.at[rows, :],
                self.out.at[x, k, z, y, rows, :],
                send,
                recv,
                place.device(**{"d" + name[1]: 1}),
            )
        if name[:2] in ("cz", "dz"):
            x, y, z, k = place.shifted(dx=1) if name[0] == "c" else place.shifted(dy=1)
            ref = self.out.at[x, k, z, y, PARTS[name[0]], :]
            return remote(ref, ref, send, recv, place.device(dz=int(name[2])))
        where, to = self.lines[name]
        ref = self.line(*where)
        return remote(ref, ref, send, recv, place.device(**to))

    def kept(self):
        x, y, z, k = self.place.shifted()
        return pltpu.make_async_copy(self.own, self.out.at[x, k, z, y], self.keep)

    def event(self, n):
        if n == 0:
            self.kept().start()
            self.start("cx", "dy", "z1", "z2", "z3")
        elif n == 1:
            self.wait("cx", "dy")
            self.start("cz1", "cz2", "cz3", "dz1", "dz2", "dz3")
        elif n == 2:
            self.kept().wait()
            self.wait("z1", "z2", "z3")
            self.start("ax", "by", "ay0", "bx0", "d0")
        elif n == 9:
            self.wait(*["d%d" % i for i in range(7)])
        else:
            self.wait(*self.steps[n][0])
            self.start(*self.steps[n][1])


class NormGather(Copies):
    names = ("z1", "z2", "z3", "y")

    def __init__(self, place, own, out, send, recv, keep):
        self.place, self.own, self.out = place, own, out
        self.send, self.recv, self.keep = send, recv, keep

    def copy(self, name):
        place = self.place
        at = self.names.index(name)
        send, recv = self.send.at[at], self.recv.at[at]
        if name == "y":
            ref = self.out.at[:, place.y]
            return remote(ref, ref, send, recv, place.device(dy=1))
        return remote(
            self.own, self.out.at[place.z, place.y], send, recv, place.device(dz=int(name[1]))
        )

    def kept(self):
        return pltpu.make_async_copy(self.own, self.out.at[self.place.z, self.place.y], self.keep)


class Events:
    def __init__(self, steps):
        self.steps = list(steps)

    def run(self, count):
        for step in self.steps[:count]:
            step()
        del self.steps[:count]

    def spread(self, trips, points, count):
        total = trips * points
        return self.place(trips, points, {n * total // max(count, 1): 1 for n in range(count)})

    def place(self, trips, points, counts):
        total = trips * points
        slots = [[] for _ in range(total)]
        for number in sorted(counts):
            slots[number] += self.steps[: counts[number]]
            del self.steps[: counts[number]]

        def stop(i, point):
            for trip in range(trips):
                todo = slots[trip * points + point]
                if todo:

                    @pl.when(i == trip)
                    def _():
                        for step in todo:
                            step()

        return stop


def lane_half(tile, half):
    lane = lax.broadcasted_iota(jnp.int32, tile.shape, 1)
    keep = (lane < HEAD_DIM) if half == 0 else (lane >= HEAD_DIM)
    return jnp.where(keep, tile, jnp.zeros_like(tile))


def swap_halves(tile):
    return pltpu.roll(tile.astype(jnp.float32), HEAD_DIM, 1)


def fill_distance(dist, segments, place):
    row = segments[pl.ds(place.x, 1), :].astype(jnp.float32)
    column = jnp.broadcast_to(row, (8, 1024)).T[:, 0:1]
    for s in range(2):
        first = (2 * s + place.k) * 256
        mine = segments[pl.ds(place.x, 1), pl.ds(pl.multiple_of(first, 256), 256)].astype(jnp.float32)
        gap = lax.broadcasted_iota(jnp.int32, (1024, 256), 0) - (
            lax.broadcasted_iota(jnp.int32, (1024, 256), 1) + first
        )
        dist[:, s * 256 : (s + 1) * 256] = jnp.where(
            column == mine, jnp.abs(gap).astype(jnp.float32), 1e30
        )


def pack_attention(raw, shard):
    qkv, w_out = raw[0], raw[1]
    turned = w_out[...].astype(jnp.float32).T
    for c in range(3):
        shard[0, :, c * 256 : c * 256 + 128] = qkv[c, :, 0:128]
        shard[0, :, c * 256 + 128 : c * 256 + 256] = jnp.concatenate(
            [
                qkv[c, :, 128:192].astype(jnp.float32),
                turned[:, c * HEAD_DIM : (c + 1) * HEAD_DIM],
            ],
            axis=1,
        ).astype(jnp.bfloat16)


def pack_feed(raw, shard):
    w_in, w_down = raw[2], raw[3]
    turned = w_down[...].astype(jnp.float32).T.astype(jnp.bfloat16)
    for r in range(3):
        units = slice(r * 256, (r + 1) * 256)
        shard[1 + r, :, 0:256] = w_in[:, 0, units]
        shard[1 + r, :, 256:512] = w_in[:, 1, units]
        shard[1 + r, :, 512:768] = turned[:, units]


def out_weights(w):
    first = lax.broadcasted_iota(jnp.int32, (768, 128), 1) < HEAD_DIM
    left = jnp.where(first, swap_halves(w[:, 128:256]), w[:, 384:512].astype(jnp.float32))
    right = jnp.where(first, swap_halves(w[:, 640:768]), 0.0)
    return left.astype(jnp.bfloat16), right.astype(jnp.bfloat16)


def whole(ref):
    value = ref[...]
    return value.reshape(768, value.shape[-1])


HEAD_SPOTS = ((0, 0), (0, 1), (1, 0))


def norm_stats(value):
    average = jnp.mean(value, axis=-1, keepdims=True)
    centered = value - average
    inv_std = lax.rsqrt(jnp.mean(centered * centered, axis=-1, keepdims=True) + norm_eps)
    return centered * inv_std, inv_std


def norm_backward(grad_val, normed, inv_std, gain_row):
    grad_norm = grad_val * gain_row
    return inv_std * (
        grad_norm
        - jnp.mean(grad_norm, axis=-1, keepdims=True)
        - normed * jnp.mean(grad_norm * normed, axis=-1, keepdims=True)
    )


ROWS = 128


def row_blocks(body):
    def step(i, carry):
        body(pl.ds(pl.multiple_of(i * ROWS, ROWS), ROWS), i)
        return carry

    lax.fori_loop(0, 512 // ROWS, step, 0)


def columns(value):
    return jnp.sum(value.reshape(value.shape[0] // 8, 8, value.shape[1]), axis=0)


def forward_kernel(
    span,
    slopes,
    raw,
    gains,
    biases,
    tok,
    cot,
    segments,
    o_weights,
    o_norms,
    o_x,
    o_cot,
    o_q,
    o_k,
    o_v,
    o_ctx,
    o_lse,
    o_kept,
    o_h1b,
    o_n1,
    o_i1,
    o_n2,
    o_i2,
    o_out,
    o_squares,
    shard,
    norm_rows,
    weights,
    norms,
    xs,
    q,
    keys,
    values,
    ctx,
    h1b,
    n1,
    dist,
    out_t,
    acc,
    h1,
    kept,
    g_send,
    g_recv,
    g_keep,
    n_send,
    n_recv,
    n_keep,
    t_sems,
    kv_send,
    kv_recv,
    store_sems,
    kept_sems,
):
    f32, bf16 = jnp.float32, jnp.bfloat16
    place = Place(span)
    x, y, z, k = place.shifted()
    rounds = [
        GatherRound(place, shard.at[r], weights.at[r], g_send.at[r], g_recv.at[r], g_keep.at[r])
        for r in range(ROUNDS)
    ]
    norm_gather = NormGather(place, norm_rows, norms, n_send, n_recv, n_keep)

    def swap(n):
        src, dst = ((tok, xs), (cot, o_cot))[n]
        return remote(
            src.at[1 - place.x],
            dst.at[place.x],
            t_sems.at[3 * n],
            t_sems.at[3 * n + 1],
            place.device(dx=1),
        )

    def stay(n):
        src, dst = ((tok, xs), (cot, o_cot))[n]
        return pltpu.make_async_copy(src.at[place.x], dst.at[place.x], t_sems.at[3 * n + 2])

    def store(n):
        src, dst = (
            (weights.at[0], o_weights.at[0]),
            (weights.at[1], o_weights.at[1]),
            (weights.at[2], o_weights.at[2]),
            (weights.at[3], o_weights.at[3]),
            (xs, o_x),
            (keys, o_k),
            (values, o_v),
            (q, o_q),
            (ctx, o_ctx),
            (h1b, o_h1b),
            (n1, o_n1),
        )[n]
        return pltpu.make_async_copy(src, dst, store_sems.at[n])

    if len(raw) > 1:
        pack_attention(raw, shard)
    else:
        shard[...] = raw[0][...]
    place.greet(ALL_PEERS)
    rounds[0].event(0)
    for n in range(2):
        swap(n).start()
        stay(n).start()
    norm_rows[...] = jnp.zeros_like(norm_rows)
    norm_rows[0:2, 0:96] = gains[...].astype(f32)
    norm_rows[2:4, 0:96] = biases[...].astype(f32)
    block = place.z * 2 + place.y
    norm_rows[...] = pltpu.roll(norm_rows[...], block * 96, 1)
    norm_gather.kept().start()
    norm_gather.start("z1", "z2", "z3")
    if len(raw) > 1:
        pack_feed(raw, shard)

    def step(r, n):
        def go():
            rounds[r].event(n)
            if n == GatherRound.last:
                store(r).start()

        return go

    order = [(0, 1), (0, 2), (1, 0), (1, 1), (0, 3), (0, 4), (1, 2), (2, 0), (2, 1)]
    order += [(0, 5), (0, 6), (0, 7), (0, 8), (0, 9)]
    begun = len(order)
    order += [(1, 3), (1, 4), (2, 2), (3, 0), (3, 1), (1, 5), (1, 6), (1, 7), (1, 8), (2, 3), (2, 4), (3, 2), (1, 9)]
    order += [(2, 5), (2, 6), (2, 7), (2, 8), (3, 3), (3, 4), (2, 9)]
    order += [(3, 5), (3, 6), (3, 7), (3, 8), (3, 9)]
    events = Events(step(*at) for at in order)

    events.run(1)
    fill_distance(dist, segments, place)
    norm_gather.kept().wait()
    norm_gather.wait("z1", "z2", "z3")
    norm_gather.start("y")
    events.run(begun - 1)
    swap(0).wait_recv()
    stay(0).wait()
    store(4).start()

    def share(t, n):
        ref = (keys, values)[n].at[pl.ds(2 * t, 2), :, place.k]
        return remote(ref, ref, kv_send.at[t, n], kv_recv.at[t, n], place.device(dk=1))

    def project(t, carry):
        w = whole(weights.at[0, t // 2, t % 2])
        for s in range(2):
            out = dot(xs[s], w).astype(bf16)
            for i in range(2):
                cols = slice(i * 128, i * 128 + 128)
                q[2 * t + i, pl.ds(s * 256, 256), :] = out[:, cols] * bf16(HEAD_DIM**-0.5)
                keys[2 * t + i, s, k] = out[:, 256 + i * 128 : 384 + i * 128]
                values[2 * t + i, s, k] = out[:, 512 + i * 128 : 640 + i * 128]
        share(t, 0).start()
        share(t, 1).start()
        return carry

    lax.fori_loop(0, 4, project, 0)
    out_t[1, pl.ds(HEAD_DIM, HEAD_DIM), :] = jnp.zeros((HEAD_DIM, 512), f32)
    stop = events.spread(4, 7, 13)

    def attend(t, carry):
        share(t, 0).wait_recv()
        share(t, 1).wait_recv()
        point = 0
        for spot, (tile, half) in enumerate(HEAD_SPOTS):
            slope = slopes[3 * t + spot]
            key = keys[2 * t + tile].reshape(1024, 128)
            rows = slice(half * HEAD_DIM, (half + 1) * HEAD_DIM)
            value_t = values[2 * t + tile].reshape(1024, 128).astype(f32).T.astype(bf16)[rows]
            for start in range(0, 512, CHUNK):
                cols = pl.ds(start, CHUNK)
                part = lane_half(q[2 * t + tile, cols, :], half)
                scores = dot(key, part, NT) - slope * dist[:, cols]
                peak = jnp.max(scores, axis=0, keepdims=True)
                expo = jnp.exp(scores - peak)
                total = jnp.sum(expo, axis=0, keepdims=True)
                out_t[tile, rows, cols] = dot(value_t, expo.astype(bf16)) / total
                o_lse[t, pl.ds(spot, 1), cols] = peak + jnp.log(total)
                stop(t, point)
                point += 1
        for tile in range(2):
            ctx[2 * t + tile] = out_t[tile].T.astype(bf16)
        left, right = out_weights(whole(weights.at[0, t // 2, t % 2]))
        mixed = dot(ctx[2 * t], left, NT) + dot(ctx[2 * t + 1], right, NT)

        @pl.when(t == 0)
        def _():
            acc[...] = mixed

        @pl.when(t > 0)
        def _():
            acc[...] += mixed

        stop(t, point)
        return carry

    lax.fori_loop(0, 4, attend, 0)
    for n in range(5, 9):
        store(n).start()
    norm_gather.wait("y")
    norm_sum = jnp.sum(norms[...].reshape(8, 8, 768), axis=0)
    o_norms[...] = norm_sum

    def first_norm(rows, i):
        attn = acc[rows, :]
        half = i // 2
        resid = xs[half, pl.ds(pl.multiple_of((i % 2) * ROWS, ROWS), ROWS), :].astype(f32) + attn
        normed, inv = norm_stats(resid)
        value = normed * norm_sum[0:1] + norm_sum[2:3]
        h1[rows, :] = value
        h1b[rows, :] = value.astype(bf16)
        n1[rows, :] = normed
        o_i1[rows, :] = inv
        acc[rows, :] = jnp.zeros_like(attn)
        if_first = jnp.where(i == 0, 0.0, 1.0)
        o_squares[0] = o_squares[0] * if_first + columns(attn * attn)
        o_squares[1] = o_squares[1] * if_first + columns(resid * resid)

    o_squares[...] = jnp.zeros_like(o_squares)
    row_blocks(first_norm)
    store(9).start()
    store(10).start()

    stop_f = events.place(
        12, 2, {1: 1, 2: 1, 3: 1, 4: 1, 5: 1, 6: 1, 8: 1, 9: 1, 11: 1, 13: 1, 14: 1, 16: 1}
    )
    assert not events.steps

    def keep_copy(n):
        return pltpu.make_async_copy(kept.at[n % 2], o_kept.at[n], kept_sems.at[n % 2])

    def feed(n, carry):
        r, t = 1 + n // 4, n % 4
        stop_f(n, 0)

        @pl.when(n >= 2)
        def _():
            keep_copy(n - 2).wait()

        ref = weights.at[r, t // 2, t % 2]
        for start in range(0, 512, CHUNK):
            rows = pl.ds(start, CHUNK)
            w = whole(ref)
            projected = dot(h1b[rows, :], w[:, :512])
            gate, up = projected[:, :256], projected[:, 256:]
            cdf = 0.5 + 0.5 * lax.erf(gate * (0.5**0.5))
            pdf = jnp.exp(-0.5 * gate * gate) * 0.3989422804014327
            act = gate * cdf
            hidden = (act * up).astype(bf16)
            kept[n % 2, 0, rows, :] = hidden
            kept[n % 2, 1, rows, :] = act.astype(bf16)
            kept[n % 2, 2, rows, :] = ((cdf + gate * pdf) * up).astype(bf16)
            acc[rows, :] += dot(hidden, w[:, 512:], NT)
        keep_copy(n).start()
        stop_f(n, 1)
        return carry

    lax.fori_loop(0, 12, feed, 0)

    def second_norm(rows, i):
        ffn = acc[rows, :]
        resid = h1[rows, :] + ffn
        normed, inv = norm_stats(resid)
        o_out[rows, :] = (normed * norm_sum[1:2] + norm_sum[3:4]).astype(bf16)
        o_n2[rows, :] = normed
        o_i2[rows, :] = inv
        o_squares[2] += columns(ffn * ffn)
        o_squares[3] += columns(resid * resid)

    row_blocks(second_norm)
    for n in (10, 11):
        keep_copy(n).wait()
    for r in rounds:
        r.finish()
    norm_gather.finish()
    for n in range(2):
        swap(n).wait_send()
    swap(1).wait_recv()
    stay(1).wait()
    for t in range(4):
        for n in range(2):
            share(t, n).wait_send()
    for n in range(11):
        store(n).wait()


def forward_refs(span, count, *refs):
    forward_kernel(span, refs[0], refs[1 : 1 + count], *refs[1 + count :])


def forward(span, slopes, raw, gains, biases, tok, cot, segments):
    f32, bf16 = jnp.float32, jnp.bfloat16
    any_space = pl.BlockSpec(memory_space=pl.ANY)
    vmem = pl.BlockSpec(memory_space=pltpu.VMEM)
    outs = (
        ((ROUNDS, 2, 2, 4, 2, 96, 768), bf16, any_space),
        ((8, 768), f32, vmem),
        ((2, 256, 768), bf16, any_space),
        ((2, 256, 768), bf16, any_space),
        ((8, 512, 128), bf16, any_space),
        ((8, 2, 2, 256, 128), bf16, any_space),
        ((8, 2, 2, 256, 128), bf16, any_space),
        ((8, 512, 128), bf16, any_space),
        ((4, 8, 512), f32, vmem),
        ((12, 3, 512, 256), bf16, any_space),
        ((512, 768), bf16, any_space),
        ((512, 768), f32, any_space),
        ((512, 1), f32, vmem),
        ((512, 768), f32, vmem),
        ((512, 1), f32, vmem),
        ((512, 768), bf16, vmem),
        ((4, 8, 768), f32, vmem),
    )
    dma = pltpu.SemaphoreType.DMA
    copies = len(GatherRound.names)
    return pl.pallas_call(
        partial(forward_refs, span, len(raw)),
        out_shape=tuple(jax.ShapeDtypeStruct(s, d) for s, d, _ in outs),
        in_specs=[pl.BlockSpec(memory_space=pltpu.SMEM)] + [vmem] * (len(raw) + 5),
        out_specs=tuple(spec for _, _, spec in outs),
        scratch_shapes=[
            pltpu.VMEM((ROUNDS, 96, 768), bf16),
            pltpu.VMEM((8, 768), f32),
            pltpu.VMEM((ROUNDS, 2, 2, 4, 2, 96, 768), bf16),
            pltpu.VMEM((4, 2, 8, 768), f32),
            pltpu.VMEM((2, 256, 768), bf16),
            pltpu.VMEM((8, 512, 128), bf16),
            pltpu.VMEM((8, 2, 2, 256, 128), bf16),
            pltpu.VMEM((8, 2, 2, 256, 128), bf16),
            pltpu.VMEM((8, 512, 128), bf16),
            pltpu.VMEM((512, 768), bf16),
            pltpu.VMEM((512, 768), f32),
            pltpu.VMEM((1024, 512), f32),
            pltpu.VMEM((2, 128, 512), f32),
            pltpu.VMEM((512, 768), f32),
            pltpu.VMEM((512, 768), f32),
            pltpu.VMEM((2, 3, 512, 256), bf16),
            dma((ROUNDS, copies)),
            dma((ROUNDS, copies)),
            dma((ROUNDS,)),
            dma((4,)),
            dma((4,)),
            dma,
            dma((6,)),
            dma((4, 2)),
            dma((4, 2)),
            dma((11,)),
            dma((2,)),
        ],
        compiler_params=pltpu.CompilerParams(
            collective_id=0, has_side_effects=True, vmem_limit_bytes=VMEM_LIMIT
        ),
        name="forward",
    )(slopes, *raw, gains, biases, tok, cot, segments)


class ScatterRound(Copies):
    names = ("ay1", "bx", "ay0", "ax", "by", "cx", "dy") + tuple(
        part + "z%d" % step for part in "abcd" for step in (1, 2, 3)
    )

    def __init__(self, place, held, twin, stage, landing, send, recv, pair):
        self.place, self.held, self.twin, self.stage = place, held, twin, stage
        self.ay, self.bx, self.ax, self.by, self.z, self.cz, self.dz, self.last = landing
        self.send, self.recv, self.pair = send, recv, pair

    def copy(self, name):
        p, held = self.place, self.held
        at = self.names.index(name)
        a, b, c, d = (PARTS[part] for part in "abcd")
        step = int(name[2]) if name[1] == "z" else 0
        far = (p.z + step) % 4
        ac, bd = PARTS["ac"], PARTS["bd"]
        if name in ("ay1", "ay0"):
            dx = int(name[2])
            src, dst, to = held.at[dx, :, 1 - p.y, ac, :], self.ay.at[dx], {"dy": 1}
        elif name == "bx":
            src, dst, to = held.at[1, :, :, bd, :], self.bx, {"dx": 1}
        elif name == "ax":
            src, dst, to = held.at[1, :, p.y, a, :], self.ax, {"dx": 1}
        elif name == "by":
            src, dst, to = held.at[0, :, 1 - p.y, b, :], self.by, {"dy": 1}
        elif name == "cx":
            src, dst, to = held.at[1, p.z, p.y, c, :], self.last.at[0], {"dx": 1}
        elif name == "dy":
            src, dst, to = held.at[0, p.z, 1 - p.y, d, :], self.last.at[1], {"dy": 1}
        elif name[0] == "c":
            src, dst, to = held.at[:, far, p.y, c, :], self.cz.at[step - 1], {"dz": step}
        elif name[0] == "d":
            src, dst, to = held.at[0, far, :, d, :], self.dz.at[step - 1], {"dz": step}
        else:
            rows = PARTS[name[0]]
            into = pl.ds(0, 32) if name[0] == "a" else pl.ds(32, 32)
            src, dst, to = held.at[0, far, p.y, rows, :], self.z.at[step - 1, into, :], {"dz": step}
        return remote(src, dst, self.send.at[at], self.recv.at[at], p.device(**to))

    def push(self, dx):
        return remote(
            self.stage.at[dx], self.twin.at[dx], self.pair.at[0, dx], self.pair.at[1, dx], self.place.device(dk=1)
        )

    def add(self, ref, *others):
        total = ref[...].astype(jnp.float32)
        for other in others:
            total = total + other[...].astype(jnp.float32)
        ref[...] = total.astype(jnp.bfloat16)

    def pair_sum(self, dx):
        self.push(dx).wait_recv()

        def body(i, carry):
            self.add(self.held.at[dx, i], self.twin.at[dx, i])
            return carry

        lax.fori_loop(0, 4, body, 0)
        if dx:
            self.start("bx", "ay1")
        else:
            self.start("ay0")

    def event(self, n, out=None):
        p, held = self.place, self.held
        a, b, c, d = (PARTS[part] for part in "abcd")
        ac, bd = PARTS["ac"], PARTS["bd"]
        if n == 0:
            self.wait("ay1")
            self.add(held.at[1, :, p.y, ac, :], self.ay.at[1])
            self.start("ax")
        elif n == 1:
            self.wait("bx")
            self.add(held.at[0, :, 1 - p.y, bd, :], self.bx.at[:, 1 - p.y])
            self.start("by")
            self.add(held.at[0, :, p.y, bd, :], self.bx.at[:, p.y])
            self.start("dz1", "dz2", "dz3")
        elif n == 2:
            self.wait("ay0")
            self.add(held.at[0, :, p.y, ac, :], self.ay.at[0])
            self.start("cz1", "cz2", "cz3")
        elif n == 3:
            self.wait("ax")
            self.add(held.at[0, :, p.y, a, :], self.ax)
            self.start("az1", "az2", "az3")
        elif n == 4:
            self.wait("by")
            self.add(held.at[0, :, p.y, b, :], self.by)
            self.start("bz1", "bz2", "bz3")
        elif n == 5:
            self.wait("cz1", "cz2", "cz3", "dz1", "dz2", "dz3")
            self.add(held.at[1, p.z, p.y, c, :], *[self.cz.at[i, 1] for i in range(3)])
            self.start("cx")
            self.add(held.at[0, p.z, 1 - p.y, d, :], *[self.dz.at[i, 1 - p.y] for i in range(3)])
            self.start("dy")
            self.add(held.at[0, p.z, p.y, c, :], *[self.cz.at[i, 0] for i in range(3)])
            self.add(held.at[0, p.z, p.y, d, :], *[self.dz.at[i, p.y] for i in range(3)])
        else:
            self.wait("az1", "az2", "az3", "bz1", "bz2", "bz3", "cx", "dy")
            for rows, others in (
                (a, [self.z.at[i, pl.ds(0, 32), :] for i in range(3)]),
                (b, [self.z.at[i, pl.ds(32, 32), :] for i in range(3)]),
                (c, [self.last.at[0]]),
                (d, [self.last.at[1]]),
            ):
                total = held[0, p.z, p.y, rows, :].astype(jnp.float32)
                for other in others:
                    total = total + other[...].astype(jnp.float32)
                out[rows, :] = total


def backward_kernel(
    span,
    slopes,
    i_weights,
    norms,
    i_x,
    i_cot,
    i_q,
    i_k,
    i_v,
    i_ctx,
    i_lse,
    i_kept,
    i_h1b,
    i_n1,
    i_i1,
    i_n2,
    i_i2,
    i_out,
    squares,
    segments,
    o_out,
    o_tokens,
    o_grads,
    o_small,
    w_buf,
    kept,
    h1_t,
    f_t,
    d_rows,
    n_buf,
    d_h1,
    q,
    keys,
    values,
    ctx,
    lse,
    dist,
    d_ctx,
    d_kv,
    d_kv_in,
    dq_t,
    acc_k,
    acc_v,
    held,
    twin,
    stage,
    land_ay,
    land_bx,
    land_ax,
    land_by,
    land_z,
    land_cz,
    land_dz,
    land_last,
    small,
    small_in,
    load_sems,
    step_sems,
    r_send,
    r_recv,
    r_pair,
    t_sems,
    kv_send,
    kv_recv,
    s_send,
    s_recv,
):
    f32, bf16 = jnp.float32, jnp.bfloat16
    place = Place(span)
    x, y, z, k = place.shifted()
    rounds = [
        ScatterRound(
            place,
            held.at[n],
            twin.at[n % 3],
            stage,
            [
                ref.at[n]
                for ref in (land_ay, land_bx, land_ax, land_by, land_z, land_cz, land_dz, land_last)
            ],
            r_send.at[n],
            r_recv.at[n],
            r_pair.at[n],
        )
        for n in range(ROUNDS)
    ]

    def load(n):
        src, dst = (
            (i_cot, d_rows.at[2]),
            (i_n2, n_buf),
            (i_h1b, d_rows.at[1]),
            (i_x, d_rows.at[2]),
            (i_q, q),
            (i_k, keys),
            (i_v, values),
            (i_ctx, ctx),
            (i_lse, lse),
            (i_n1, n_buf),
        )[n]
        return pltpu.make_async_copy(src, dst, load_sems.at[n])

    def where(n):
        return x ^ (1 - n // 2), k ^ (1 - n % 2)

    def where_heads(n):
        return x ^ (1 - n // 2), n % 2

    def fetch(n, part):
        r = 3 - n // 4
        wx, wk = where(n % 4)
        if part == 0:
            return pltpu.make_async_copy(i_weights.at[r, wx, wk], w_buf.at[n % 2], step_sems.at[n % 2, 0])
        return pltpu.make_async_copy(
            i_kept.at[(r - 1) * 4 + wx * 2 + wk], kept.at[n % 2], step_sems.at[n % 2, 1]
        )

    for n in (0, 1, 2, 4, 5, 6, 7, 8):
        load(n).start()
    fetch(0, 0).start()
    fetch(0, 1).start()
    place.greet(ALL_PEERS)

    def swap(n):
        src, dst = ((i_out, o_out), (d_rows.at[0], o_tokens))[n]
        return remote(
            src.at[1 - place.x],
            dst.at[place.x],
            t_sems.at[3 * n],
            t_sems.at[3 * n + 1],
            place.device(dx=1),
        )

    def stay(n):
        src, dst = ((i_out, o_out), (d_rows.at[0], o_tokens))[n]
        return pltpu.make_async_copy(src.at[place.x], dst.at[place.x], t_sems.at[3 * n + 2])

    swap(0).start()
    stay(0).start()
    load(0).wait()
    load(1).wait()
    small[...] = jnp.zeros_like(small)

    def halves(ref, i):
        return ref.at[i // 2, pl.ds(pl.multiple_of((i % 2) * ROWS, ROWS), ROWS), :]

    sums = [jnp.zeros((8, 768), f32)] * 2
    for i in range(512 // ROWS):
        rows = pl.ds(i * ROWS, ROWS)
        grad = halves(d_rows.at[2], i)[...].astype(f32)
        normed = n_buf[rows, :]
        out = norm_backward(grad, normed, i_i2[rows, :], norms[1:2])
        d_h1[rows, :] = out
        halves(d_rows.at[0], i)[...] = out.astype(bf16)
        f_t[:, rows] = out.T.astype(bf16)
        sums[0] = sums[0] + columns(grad * normed)
        sums[1] = sums[1] + columns(grad)
    small[1] = sums[0]
    small[3] = sums[1]
    load(9).start()
    load(3).start()
    load(2).wait()
    for i in range(512 // ROWS):
        rows = pl.ds(i * ROWS, ROWS)
        h1_t[:, rows] = halves(d_rows.at[1], i)[...].astype(f32).T.astype(bf16)
    fill_distance(dist, segments, place)

    def pair(n, dx):
        return lambda: rounds[n].pair_sum(dx)

    def step(n, at):
        return lambda: rounds[n].event(at, o_grads.at[3 - n])

    def put(n, dx, theirs, value, cols):
        block = value.astype(bf16).reshape(4, 2, 96, value.shape[-1])

        @pl.when(theirs)
        def _():
            stage[dx, :, :, :, cols] = block

        @pl.when(jnp.logical_not(theirs))
        def _():
            held[n, dx, :, :, :, cols] = block

    def push(n, dx):
        return remote(
            stage.at[dx], twin.at[n % 3, dx], r_pair.at[n, 0, dx], r_pair.at[n, 1, dx], place.device(dk=1)
        )

    plan = {
        1: [pair(0, 1)],
        3: [pair(0, 0)],
        5: [step(0, 0), pair(1, 1)],
        7: [step(0, 2), pair(1, 0)],
        8: [step(0, 1)],
        9: [step(1, 0), pair(2, 1)],
        10: [step(0, 3)],
        11: [step(0, 4), step(1, 2), pair(2, 0)],
    }

    def feed(n, carry):
        dx = 1 - n % 4 // 2
        theirs = n % 2 == 0

        @pl.when(n < 11)
        def _():
            fetch(n + 1, 0).start()
            fetch(n + 1, 1).start()

        @pl.when(jnp.logical_and(theirs, n >= 4))
        def _():
            push(n // 4 - 1, dx).wait_send()

        fetch(n, 0).wait()
        fetch(n, 1).wait()
        w = whole(w_buf.at[n % 2])
        hold = kept.at[n % 2]
        d_ffn = d_rows[0].reshape(512, 768)
        put(n // 4, dx, theirs, dot(f_t[...], hold[0]), slice(512, 768))
        d_hidden = dot(d_ffn, w[:, 512:])
        d_gate = (d_hidden * hold[2].astype(f32)).astype(bf16)
        d_up = (d_hidden * hold[1].astype(f32)).astype(bf16)
        put(n // 4, dx, theirs, dot(h1_t[...], d_gate), slice(0, 256))
        put(n // 4, dx, theirs, dot(h1_t[...], d_up), slice(256, 512))

        @pl.when(theirs)
        def _():
            push(n // 4, dx).start()

        d_h1[...] += dot(d_gate, w[:, :256], NT) + dot(d_up, w[:, 256:512], NT)
        for at, todo in plan.items():

            @pl.when(n == at)
            def _():
                for item in todo:
                    item()

        return carry

    lax.fori_loop(0, 12, feed, 0)
    load(9).wait()
    load(3).wait()
    for i in range(512 // ROWS):
        rows = pl.ds(i * ROWS, ROWS)
        h1_t[:, rows] = halves(d_rows.at[2], i)[...].astype(f32).T.astype(bf16)
    sums = [jnp.zeros((8, 768), f32)] * 2
    for i in range(512 // ROWS):
        rows = pl.ds(i * ROWS, ROWS)
        grad = d_h1[rows, :]
        normed = n_buf[rows, :]
        out = norm_backward(grad, normed, i_i1[rows, :], norms[0:1])
        d_h1[rows, :] = out
        halves(d_rows.at[1], i)[...] = out.astype(bf16)
        f_t[:, rows] = out.T.astype(bf16)
        sums[0] = sums[0] + columns(grad * normed)
        sums[1] = sums[1] + columns(grad)
    small[0] = sums[0]
    small[2] = sums[1]
    for n in range(4, 9):
        load(n).wait()

    small[0] = jnp.concatenate(
        [jnp.sum(small[i], axis=0, keepdims=True) for i in range(4)]
        + [jnp.sum(squares[i], axis=0, keepdims=True) for i in range(4)],
        axis=0,
    )

    def spread(n):
        to = ({"dk": 1}, {"dx": 1}, {"dy": 1}, {"dz": 1}, {"dz": 2}, {"dz": 3})[n]
        return remote(
            small.at[min(n, 3)], small_in.at[n], s_send.at[n], s_recv.at[n], place.device(**to)
        )

    def small_step(n):
        def go():
            if 0 < n < 4:
                spread(n - 1).wait_recv()
                small[n] = small[n - 1] + small_in[n - 1]
            if n < 3:
                spread(n).start()
            if n == 3:
                for at in (3, 4, 5):
                    spread(at).start()
            if n == 4:
                for at in (3, 4, 5):
                    spread(at).wait_recv()
                total = small[3]
                result = jnp.zeros_like(total)
                for at in range(4):
                    back = (place.z - at) % 4
                    term = jnp.where(
                        back == 0,
                        total,
                        jnp.where(
                            back == 1, small_in[3], jnp.where(back == 2, small_in[4], small_in[5])
                        ),
                    )
                    result = result + term
                o_small[...] = result

        return go

    def fetch_heads(n):
        wx, wk = where_heads(n)
        return pltpu.make_async_copy(i_weights.at[0, wx, wk], w_buf.at[n % 2], step_sems.at[n % 2, 0])

    fetch_heads(0).start()
    dq_t[1, pl.ds(HEAD_DIM, HEAD_DIM), :] = jnp.zeros((HEAD_DIM, 512), f32)

    def share(t):
        return remote(
            d_kv.at[t, :, :, :, 1 - place.k], d_kv_in.at[t], kv_send.at[t], kv_recv.at[t], place.device(dk=1)
        )

    beside = {
        (0, 0): [small_step(0), step(0, 5)],
        (0, 2): [small_step(1), step(2, 0)],
        (0, 4): [small_step(2), step(1, 1)],
        (1, 0): [small_step(3), step(0, 6)],
        (1, 2): [step(1, 3)],
        (1, 4): [small_step(4), step(2, 2)],
        (2, 0): [step(1, 4)],
        (2, 2): [step(1, 5)],
        (2, 5): [step(2, 1)],
        (3, 0): [pair(3, 1)],
        (3, 1): [step(1, 6)],
        (3, 3): [step(2, 3)],
        (3, 5): [step(2, 4)],
    }
    first = lax.broadcasted_iota(jnp.int32, (768, 128), 1) < HEAD_DIM

    def stop(i, point):
        for (trip, at), todo in beside.items():
            if at == point:

                @pl.when(i == trip)
                def _():
                    for item in todo:
                        item()

    def attend(n):
        wx, wk = where_heads(n)
        t = wx * 2 + wk
        fetch_heads(n).wait()
        left, right = out_weights(whole(w_buf.at[n % 2]))
        d_attn = d_rows[1].reshape(512, 768)
        d_ctx[0] = dot(d_attn, left).astype(bf16)
        d_ctx[1] = dot(d_attn, right).astype(bf16)
        point = 0
        for spot, (tile, half) in enumerate(HEAD_SPOTS):
            slope = slopes[3 * t + spot]
            key = keys[2 * t + tile].reshape(1024, 128)
            value = values[2 * t + tile].reshape(1024, 128)
            rows = slice(half * HEAD_DIM, (half + 1) * HEAD_DIM)
            key_t = key.astype(f32).T.astype(bf16)[rows]
            product = ctx[2 * t + tile].astype(f32) * d_ctx[tile].astype(f32)
            delta = jnp.sum(product.T[rows], axis=0, keepdims=True)
            for start in range(0, 512, CHUNK):
                cols = pl.ds(start, CHUNK)
                part = lane_half(q[2 * t + tile, cols, :], half)
                grad = lane_half(d_ctx[tile, cols, :], half)
                scores = dot(key, part, NT) - slope * dist[:, cols]
                probs = jnp.exp(scores - lse[t, pl.ds(spot, 1), cols])
                grad_probs = dot(value, grad, NT)
                term_v = dot(probs.astype(bf16), grad)
                grad_scores = (probs * (grad_probs - delta[:, start : start + CHUNK])).astype(bf16)
                term_k = dot(grad_scores, part)
                if half == 0 and start == 0:
                    acc_v[...] = term_v
                    acc_k[...] = term_k
                else:
                    acc_v[...] += term_v
                    acc_k[...] += term_k
                dq_t[tile, rows, cols] = dot(key_t, grad_scores)
                stop(n, point)
                point += 1
            if half == 1 or tile == 1:
                d_kv[t, 0, tile] = acc_k[...].astype(bf16).reshape(2, 2, 256, 128)
                d_kv[t, 1, tile] = acc_v[...].astype(bf16).reshape(2, 2, 256, 128)
        share(t).start()
        for tile in range(2):
            q[2 * t + tile] = (dq_t[tile].T * HEAD_DIM**-0.5).astype(bf16)

    def project(n):
        wx, wk = where_heads(n)
        t = wx * 2 + wk
        dx = 1 - n // 2
        theirs = wk != k

        @pl.when(theirs)
        def _():
            push(2, dx).wait_send()

        share(t).wait_recv()
        parts = [q[2 * t], q[2 * t + 1]]
        for kind in range(2):
            for tile in range(2):
                mine = d_kv[t, kind, tile, :, k].reshape(512, 128).astype(f32)
                mine = mine + d_kv_in[t, kind, tile].reshape(512, 128).astype(f32)
                parts.append(mine.astype(bf16))
        d_qkv = jnp.concatenate(parts, axis=1)
        d_w = dot(h1_t[...], d_qkv)
        left = dot(f_t[...], ctx[2 * t])
        right = swap_halves(dot(f_t[...], ctx[2 * t + 1]))
        tiles = [
            d_w[:, 0:128],
            jnp.where(first, d_w[:, 128:256], pltpu.roll(left, HEAD_DIM, 1)),
            d_w[:, 256:384],
            jnp.where(first, d_w[:, 384:512], left),
            d_w[:, 512:640],
            jnp.where(first, d_w[:, 640:768], right),
        ]
        put(3, dx, theirs, jnp.concatenate(tiles, axis=1), slice(0, 768))

        @pl.when(theirs)
        def _():
            push(3, dx).start()

        d_h1[...] += dot(d_qkv, whole(w_buf.at[n % 2]), NT)

    def heads(n, carry):
        @pl.when(n < 4)
        def _():
            attend(n)

        @pl.when(n > 0)
        def _():
            project(n - 1)

        @pl.when(n < 3)
        def _():
            fetch_heads(n + 1).start()

        return carry

    lax.fori_loop(0, 5, heads, 0)
    for i in range(512 // ROWS):
        rows = pl.ds(i * ROWS, ROWS)
        halves(d_rows.at[0], i)[...] = d_h1[rows, :].astype(bf16)
    rounds[3].pair_sum(0)
    swap(1).start()
    stay(1).start()
    step(2, 5)()
    for at in (0, 1, 2):
        step(3, at)()
    step(2, 6)()
    for at in (3, 4, 5, 6):
        step(3, at)()
    for n in range(6):
        spread(n).wait_send()
    for r in rounds:
        r.finish()
    for dx in range(2):
        push(3, dx).wait_send()
    for t in range(4):
        share(t).wait_send()
    for n in range(2):
        swap(n).wait()
        stay(n).wait()


def backward(span, slopes, saved, segments):
    f32, bf16 = jnp.float32, jnp.bfloat16
    any_space = pl.BlockSpec(memory_space=pl.ANY)
    vmem = pl.BlockSpec(memory_space=pltpu.VMEM)
    dma = pltpu.SemaphoreType.DMA
    (weights, norms, xs, cot, q, keys, values, ctx, lse, kept, h1b, n1, i1, n2, i2, out, squares) = saved
    h1b = h1b.reshape(2, 256, 768)
    out = out.reshape(2, 256, 768)
    in_specs = [pl.BlockSpec(memory_space=pltpu.SMEM), any_space, vmem] + [any_space] * 10
    in_specs += [vmem, any_space, vmem, any_space, vmem, vmem]
    copies = len(ScatterRound.names)
    return pl.pallas_call(
        partial(backward_kernel, span),
        out_shape=(
            jax.ShapeDtypeStruct((2, 256, 768), bf16),
            jax.ShapeDtypeStruct((2, 256, 768), bf16),
            jax.ShapeDtypeStruct((ROUNDS, 96, 768), f32),
            jax.ShapeDtypeStruct((8, 768), f32),
        ),
        in_specs=in_specs,
        out_specs=(any_space, any_space, vmem, vmem),
        scratch_shapes=[
            pltpu.VMEM((2, 4, 2, 96, 768), bf16),
            pltpu.VMEM((2, 3, 512, 256), bf16),
            pltpu.VMEM((768, 512), bf16),
            pltpu.VMEM((768, 512), bf16),
            pltpu.VMEM((3, 2, 256, 768), bf16),
            pltpu.VMEM((512, 768), f32),
            pltpu.VMEM((512, 768), f32),
            pltpu.VMEM((8, 512, 128), bf16),
            pltpu.VMEM((8, 2, 2, 256, 128), bf16),
            pltpu.VMEM((8, 2, 2, 256, 128), bf16),
            pltpu.VMEM((8, 512, 128), bf16),
            pltpu.VMEM((4, 8, 512), f32),
            pltpu.VMEM((1024, 512), f32),
            pltpu.VMEM((2, 512, 128), bf16),
            pltpu.VMEM((4, 2, 2, 2, 2, 256, 128), bf16),
            pltpu.VMEM((4, 2, 2, 2, 256, 128), bf16),
            pltpu.VMEM((2, 128, 512), f32),
            pltpu.VMEM((1024, 128), f32),
            pltpu.VMEM((1024, 128), f32),
            pltpu.VMEM((ROUNDS, 2, 4, 2, 96, 768), bf16),
            pltpu.VMEM((3, 2, 4, 2, 96, 768), bf16),
            pltpu.VMEM((2, 4, 2, 96, 768), bf16),
            pltpu.VMEM((ROUNDS, 2, 4, 48, 768), bf16),
            pltpu.VMEM((ROUNDS, 4, 2, 48, 768), bf16),
            pltpu.VMEM((ROUNDS, 4, 32, 768), bf16),
            pltpu.VMEM((ROUNDS, 4, 32, 768), bf16),
            pltpu.VMEM((ROUNDS, 3, 64, 768), bf16),
            pltpu.VMEM((ROUNDS, 3, 2, 16, 768), bf16),
            pltpu.VMEM((ROUNDS, 3, 2, 16, 768), bf16),
            pltpu.VMEM((ROUNDS, 2, 16, 768), bf16),
            pltpu.VMEM((4, 8, 768), f32),
            pltpu.VMEM((6, 8, 768), f32),
            dma((10,)),
            dma((2, 2)),
            dma((ROUNDS, copies)),
            dma((ROUNDS, copies)),
            dma((ROUNDS, 2, 2)),
            dma((6,)),
            dma((4,)),
            dma((4,)),
            dma((6,)),
            dma((6,)),
        ],
        compiler_params=pltpu.CompilerParams(
            collective_id=1, has_side_effects=True, vmem_limit_bytes=VMEM_LIMIT
        ),
        name="backward",
    )(
        slopes,
        weights,
        norms,
        xs,
        cot,
        q,
        keys,
        values,
        ctx,
        lse,
        kept,
        h1b,
        n1,
        i1,
        n2,
        i2,
        out,
        squares,
        segments,
    )


def finish_kernel(
    block, grads, small, lo, gt, o_lo, o_gt, o_qkv, o_wout, o_win, o_down, o_gains, o_biases, rows, sems
):
    def move(n, src, dst):
        return pltpu.make_async_copy(src, dst, sems.at[n])

    move(0, lo, rows.at[0]).start()
    move(1, gt, rows.at[1]).start()
    turned = []
    for c in range(3):
        o_qkv[c] = grads[0, :, c * 256 : c * 256 + 192]
        turned.append(grads[0, :, c * 256 + 128 : c * 256 + 256].T[HEAD_DIM:])
    o_wout[...] = jnp.concatenate(turned, axis=0)
    move(0, lo, rows.at[0]).wait()
    move(2, rows.at[0], o_lo).start()
    move(1, gt, rows.at[1]).wait()
    move(3, rows.at[1], o_gt).start()
    for r in range(3):
        units = slice(r * 256, (r + 1) * 256)
        o_win[:, 0, units] = grads[1 + r, :, 0:256]
        o_win[:, 1, units] = grads[1 + r, :, 256:512]
        o_down[units, :] = grads[1 + r, :, 512:768].T
    mine = pltpu.roll(small[...], 768 - block[0] * 96, 1)
    o_gains[...] = mine[0:2, 0:96]
    o_biases[...] = mine[2:4, 0:96]
    move(2, rows.at[0], o_lo).wait()
    move(3, rows.at[1], o_gt).wait()


def finish(block, grads, small, lo, gt):
    any_space = pl.BlockSpec(memory_space=pl.ANY)
    vmem = pl.BlockSpec(memory_space=pltpu.VMEM)
    f32 = jnp.float32
    shape = jax.ShapeDtypeStruct
    return pl.pallas_call(
        finish_kernel,
        out_shape=(
            shape(lo.shape, lo.dtype),
            shape(gt.shape, gt.dtype),
            shape((3, 96, 192), f32),
            shape((192, 96), f32),
            shape((96, 2, 768), f32),
            shape((768, 96), f32),
            shape((2, 96), f32),
            shape((2, 96), f32),
        ),
        in_specs=[pl.BlockSpec(memory_space=pltpu.SMEM), vmem, vmem, any_space, any_space],
        out_specs=(any_space, any_space) + (vmem,) * 6,
        scratch_shapes=[pltpu.VMEM((2,) + lo.shape, lo.dtype), pltpu.SemaphoreType.DMA((4,))],
        compiler_params=pltpu.CompilerParams(vmem_limit_bytes=VMEM_LIMIT),
        name="finish",
    )(block, grads, small, lo, gt)


def local(
    tokens,
    segment_ids,
    query_key_value_weight,
    w_out,
    input_weight,
    w_down,
    norm_gains,
    norm_biases,
    cotangent,
):
    f32 = jnp.float32
    shard_rows = query_key_value_weight.shape[1]
    span = 96 // shard_rows
    slopes = jnp.exp2(-8.0 * (jnp.arange(HEADS).astype(f32) + 1.0) / HEADS)
    cells = float(lax.axis_size("fsdp") * 2 * 1024 * 768)
    if span == 1:
        raw = (query_key_value_weight, w_out, input_weight, w_down)
        gains, biases = norm_gains, norm_biases
    else:
        count = lax.axis_size("fsdp")
        groups = [list(range(i, i + span)) for i in range(0, count, span)]
        heads = query_key_value_weight.transpose(1, 0, 2).reshape(shard_rows, 3, 3, HEAD_DIM)
        w_out_t = w_out.T.reshape(shard_rows, 3, 1, HEAD_DIM)
        wa = jnp.concatenate([heads, w_out_t], axis=2).reshape(shard_rows, 1, 768)
        gate_up = input_weight.reshape(shard_rows, 2, 3, 256).transpose(0, 2, 1, 3)
        down = w_down.T.reshape(shard_rows, 3, 1, 256)
        wf = jnp.concatenate([gate_up, down], axis=2).reshape(shard_rows, 3, 768)
        shard = jnp.concatenate([wa, wf], axis=1).transpose(1, 0, 2)
        raw = (lax.all_gather(shard, "fsdp", axis=1, tiled=True, axis_index_groups=groups),)
        gains, biases = (
            lax.all_gather(rows, "fsdp", axis=1, tiled=True, axis_index_groups=groups)
            for rows in (norm_gains, norm_biases)
        )

    saved = forward(span, slopes, raw, gains, biases, tokens, cotangent, segment_ids)
    layer_out, grad_tokens, grads, small = backward(span, slopes, saved, segment_ids)

    if span == 1:
        block = lax.axis_index("fsdp").astype(jnp.int32).reshape(1)
        outs = finish(block, grads, small, layer_out, grad_tokens)
    else:
        grads = lax.psum_scatter(
            grads, "fsdp", scatter_dimension=1, tiled=True, axis_index_groups=groups
        )
        small = lax.psum(small, "fsdp", axis_index_groups=groups)
        grads_a = grads[0].reshape(shard_rows, 3, 4, HEAD_DIM)
        grads_f = grads[1:].reshape(3, shard_rows, 3, 256)
        shard_start = lax.axis_index("fsdp") * shard_rows
        mine = lax.dynamic_slice_in_dim(small[:4], shard_start, shard_rows, 1)
        outs = (
            layer_out,
            grad_tokens,
            grads_a[:, :, :3].transpose(1, 0, 2, 3).reshape(3, shard_rows, 192),
            grads_a[:, :, 3].reshape(shard_rows, 192).T,
            grads_f[:, :, :2].transpose(1, 2, 0, 3).reshape(shard_rows, 2, 768),
            grads_f[:, :, 2].transpose(0, 2, 1).reshape(768, shard_rows),
            mine[:2],
            mine[2:],
        )
    return outs + (jnp.sqrt(jnp.sum(small[4:], axis=1) / cells),)


def solution(mesh):
    placed = (
        P("fsdp", "tp", None),
        P("fsdp", None),
        P(None, "fsdp", "tp"),
        P("tp", "fsdp"),
        P("fsdp", None, "tp"),
        P("tp", "fsdp"),
        P(None, "fsdp"),
        P(None, "fsdp"),
        P("fsdp", "tp", None),
    )
    return jax.shard_map(
        local,
        mesh=mesh,
        in_specs=placed,
        out_specs=(
            P("fsdp", "tp", None),
            P("fsdp", "tp", None),
            P(None, "fsdp", "tp"),
            P("tp", "fsdp"),
            P("fsdp", None, "tp"),
            P("tp", "fsdp"),
            P(None, "fsdp"),
            P(None, "fsdp"),
            P(),
        ),
        check_vma=False,
    )
```

```python
from functools import partial

import jax
import jax.numpy as jnp
from jax import lax
from jax.experimental import pallas as pl
from jax.experimental.pallas import tpu as pltpu
from jax.sharding import PartitionSpec as P

HEADS = 12
HEAD_DIM = 64
MESH = pl.DeviceIdType.MESH
VMEM_LIMIT = 63 << 20
norm_eps = 1e-05
ROUNDS = 4
NT = (((1,), (1,)), ((), ()))
NN = (((1,), (0,)), ((), ()))
CHUNK = 256


class Place:
    def __init__(self, span):
        index = lax.axis_index("fsdp")
        shard = lax.axis_index("tp")
        self.span = span
        self.j = index % span
        block = index // span
        self.z = block // 2
        self.y = block % 2
        self.x = shard // 2
        self.k = shard % 2

    def shifted(self, dx=0, dy=0, dz=0, dk=0):
        x = 1 - self.x if dx else self.x
        y = 1 - self.y if dy else self.y
        z = (self.z + dz) % 4 if dz else self.z
        k = 1 - self.k if dk else self.k
        return x, y, z, k

    def device(self, dx=0, dy=0, dz=0, dk=0):
        x, y, z, k = self.shifted(dx, dy, dz, dk)
        return ((z * 2 + y) * self.span + self.j, x * 2 + k)

    def greet(self, offsets):
        barrier = pltpu.get_barrier_semaphore()
        for offset in offsets:
            pl.semaphore_signal(
                barrier, inc=1, device_id=self.device(**offset), device_id_type=MESH
            )
        pl.semaphore_wait(barrier, len(offsets))


ALL_PEERS = ({"dx": 1}, {"dy": 1}, {"dz": 1}, {"dz": 2}, {"dz": 3}, {"dk": 1})


def remote(src, dst, send, recv, device):
    return pltpu.make_async_remote_copy(
        src_ref=src, dst_ref=dst, send_sem=send, recv_sem=recv, device_id=device, device_id_type=MESH
    )


PARTS = {
    "a": pl.ds(0, 32),
    "c": pl.ds(32, 16),
    "ac": pl.ds(0, 48),
    "b": pl.ds(48, 32),
    "d": pl.ds(80, 16),
    "bd": pl.ds(48, 48),
    "": pl.ds(0, 96),
}


def dot(a, b, dims=NN):
    return lax.dot_general(a, b, dims, preferred_element_type=jnp.float32)


class Copies:
    names = ()

    def start(self, *names):
        for name in names:
            self.copy(name).start()

    def wait(self, *names):
        for name in names:
            self.copy(name).wait_recv()

    def finish(self):
        for name in self.names:
            self.copy(name).wait_send()


class GatherRound(Copies):
    names = ("z1", "z2", "z3", "ax", "by", "ay0", "bx0", "ay1", "bx1") + tuple(
        "d%d" % i for i in range(7)
    )
    names += ("cx", "cz1", "cz2", "cz3", "dy", "dz1", "dz2", "dz3")
    lines = {
        "ax": ((0, 0, "a"), {"dx": 1}),
        "by": ((0, 0, "b"), {"dy": 1}),
        "ay0": ((0, 0, "ac"), {"dy": 1}),
        "bx0": ((0, 0, "bd"), {"dx": 1}),
        "ay1": ((1, 0, "ac"), {"dy": 1}),
        "bx1": ((0, 1, "bd"), {"dx": 1}),
        "d0": ((0, 0, ""), {"dk": 1}),
        "d1": ((1, 0, "ac"), {"dk": 1}),
        "d2": ((0, 1, "bd"), {"dk": 1}),
        "d3": ((0, 1, "ac"), {"dk": 1}),
        "d4": ((1, 0, "bd"), {"dk": 1}),
        "d5": ((1, 1, "ac"), {"dk": 1}),
        "d6": ((1, 1, "bd"), {"dk": 1}),
    }
    steps = {
        3: (("ax", "cz1", "cz2", "cz3"), ("ay1", "d1")),
        4: (("by", "dz1", "dz2", "dz3"), ("bx1", "d2")),
        5: (("ay0",), ("d3",)),
        6: (("bx0",), ("d4",)),
        7: (("ay1",), ("d5",)),
        8: (("bx1",), ("d6",)),
    }
    last = 9

    def __init__(self, place, own, out, send, recv, keep):
        self.place, self.own, self.out = place, own, out
        self.send, self.recv, self.keep = send, recv, keep

    def line(self, dx, dy, part):
        x, y, z, k = self.place.shifted(dx, dy)
        return self.out.at[x, k, :, y, PARTS[part], :]

    def copy(self, name):
        place = self.place
        at = self.names.index(name)
        send, recv = self.send.at[at], self.recv.at[at]
        x, y, z, k = place.shifted()
        if name[0] == "z":
            return remote(
                self.own, self.out.at[x, k, z, y], send, recv, place.device(dz=int(name[1]))
            )
        if name in ("cx", "dy"):
            rows = PARTS[name[0]]
            return remote(
                self.own.at[rows, :],
                self.out.at[x, k, z, y, rows, :],
                send,
                recv,
                place.device(**{"d" + name[1]: 1}),
            )
        if name[:2] in ("cz", "dz"):
            x, y, z, k = place.shifted(dx=1) if name[0] == "c" else place.shifted(dy=1)
            ref = self.out.at[x, k, z, y, PARTS[name[0]], :]
            return remote(ref, ref, send, recv, place.device(dz=int(name[2])))
        where, to = self.lines[name]
        ref = self.line(*where)
        return remote(ref, ref, send, recv, place.device(**to))

    def kept(self):
        x, y, z, k = self.place.shifted()
        return pltpu.make_async_copy(self.own, self.out.at[x, k, z, y], self.keep)

    def event(self, n):
        if n == 0:
            self.kept().start()
            self.start("cx", "dy", "z1", "z2", "z3")
        elif n == 1:
            self.wait("cx", "dy")
            self.start("cz1", "cz2", "cz3", "dz1", "dz2", "dz3")
        elif n == 2:
            self.kept().wait()
            self.wait("z1", "z2", "z3")
            self.start("ax", "by", "ay0", "bx0", "d0")
        elif n == 9:
            self.wait(*["d%d" % i for i in range(7)])
        else:
            self.wait(*self.steps[n][0])
            self.start(*self.steps[n][1])


class NormGather(Copies):
    names = ("z1", "z2", "z3", "y")

    def __init__(self, place, own, out, send, recv, keep):
        self.place, self.own, self.out = place, own, out
        self.send, self.recv, self.keep = send, recv, keep

    def copy(self, name):
        place = self.place
        at = self.names.index(name)
        send, recv = self.send.at[at], self.recv.at[at]
        if name == "y":
            ref = self.out.at[:, place.y]
            return remote(ref, ref, send, recv, place.device(dy=1))
        return remote(
            self.own, self.out.at[place.z, place.y], send, recv, place.device(dz=int(name[1]))
        )

    def kept(self):
        return pltpu.make_async_copy(self.own, self.out.at[self.place.z, self.place.y], self.keep)


class Events:
    def __init__(self, steps):
        self.steps = list(steps)

    def run(self, count):
        for step in self.steps[:count]:
            step()
        del self.steps[:count]

    def spread(self, trips, points, count):
        total = trips * points
        return self.place(trips, points, {n * total // max(count, 1): 1 for n in range(count)})

    def place(self, trips, points, counts):
        total = trips * points
        slots = [[] for _ in range(total)]
        for number in sorted(counts):
            slots[number] += self.steps[: counts[number]]
            del self.steps[: counts[number]]

        def stop(i, point):
            for trip in range(trips):
                todo = slots[trip * points + point]
                if todo:

                    @pl.when(i == trip)
                    def _():
                        for step in todo:
                            step()

        return stop


def lane_half(tile, half):
    lane = lax.broadcasted_iota(jnp.int32, tile.shape, 1)
    keep = (lane < HEAD_DIM) if half == 0 else (lane >= HEAD_DIM)
    return jnp.where(keep, tile, jnp.zeros_like(tile))


def swap_halves(tile):
    return pltpu.roll(tile.astype(jnp.float32), HEAD_DIM, 1)


def fill_distance(dist, segments, place):
    row = segments[pl.ds(place.x, 1), :].astype(jnp.float32)
    column = jnp.broadcast_to(row, (8, 1024)).T[:, 0:1]
    for s in range(2):
        first = (2 * s + place.k) * 256
        mine = segments[pl.ds(place.x, 1), pl.ds(pl.multiple_of(first, 256), 256)].astype(jnp.float32)
        gap = lax.broadcasted_iota(jnp.int32, (1024, 256), 0) - (
            lax.broadcasted_iota(jnp.int32, (1024, 256), 1) + first
        )
        dist[:, s * 256 : (s + 1) * 256] = jnp.where(
            column == mine, jnp.abs(gap).astype(jnp.float32), 1e30
        )


def pack_attention(raw, shard):
    qkv, w_out = raw[0], raw[1]
    turned = w_out[...].astype(jnp.float32).T
    for c in range(3):
        tiles = (
            qkv[c, :, 0:128],
            jnp.concatenate(
                [
                    qkv[c, :, 128:192].astype(jnp.float32),
                    turned[:, c * HEAD_DIM : (c + 1) * HEAD_DIM],
                ],
                axis=1,
            ).astype(jnp.bfloat16),
        )
        for i in range(2):
            half, at = divmod(2 * c + i, 3)
            shard[half, :, at * 128 : at * 128 + 128] = tiles[i]


def pack_feed(raw, shard):
    w_in, w_down = raw[2], raw[3]
    turned = w_down[...].astype(jnp.float32).T.astype(jnp.bfloat16)
    for r in range(3):
        units = slice(r * 256, (r + 1) * 256)
        first = slice(r * 256, r * 256 + 128)
        second = slice(r * 256 + 128, r * 256 + 256)
        shard[2 + 2 * r, :, 0:256] = w_in[:, 0, units]
        shard[2 + 2 * r, :, 256:384] = w_in[:, 1, first]
        shard[3 + 2 * r, :, 0:128] = w_in[:, 1, second]
        shard[3 + 2 * r, :, 128:384] = turned[:, units]


def out_weights(w):
    first = lax.broadcasted_iota(jnp.int32, (768, 128), 1) < HEAD_DIM
    left = jnp.where(first, swap_halves(w[:, 128:256]), w[:, 384:512].astype(jnp.float32))
    right = jnp.where(first, swap_halves(w[:, 640:768]), 0.0)
    return left.astype(jnp.bfloat16), right.astype(jnp.bfloat16)


def whole(ref):
    return jnp.concatenate([ref[i].reshape(768, 384) for i in range(2)], axis=1)


HEAD_SPOTS = ((0, 0), (0, 1), (1, 0))


def norm_stats(value):
    average = jnp.mean(value, axis=-1, keepdims=True)
    centered = value - average
    inv_std = lax.rsqrt(jnp.mean(centered * centered, axis=-1, keepdims=True) + norm_eps)
    return centered * inv_std, inv_std


def norm_backward(grad_val, normed, inv_std, gain_row):
    grad_norm = grad_val * gain_row
    return inv_std * (
        grad_norm
        - jnp.mean(grad_norm, axis=-1, keepdims=True)
        - normed * jnp.mean(grad_norm * normed, axis=-1, keepdims=True)
    )


ROWS = 128


def row_blocks(body):
    def step(i, carry):
        body(pl.ds(pl.multiple_of(i * ROWS, ROWS), ROWS), i)
        return carry

    lax.fori_loop(0, 512 // ROWS, step, 0)


def columns(value):
    return jnp.sum(value.reshape(value.shape[0] // 8, 8, value.shape[1]), axis=0)


def forward_kernel(
    span,
    slopes,
    raw,
    gains,
    biases,
    tok,
    cot,
    segments,
    o_weights,
    o_norms,
    o_x,
    o_cot,
    o_q,
    o_k,
    o_v,
    o_ctx,
    o_lse,
    o_kept,
    o_h1b,
    o_n1,
    o_i1,
    o_n2,
    o_i2,
    o_out,
    o_squares,
    shard,
    norm_rows,
    weights,
    norms,
    xs,
    q,
    keys,
    values,
    ctx,
    h1b,
    n1,
    dist,
    out_t,
    acc,
    h1,
    kept,
    g_send,
    g_recv,
    g_keep,
    n_send,
    n_recv,
    n_keep,
    t_sems,
    kv_send,
    kv_recv,
    store_sems,
    kept_sems,
):
    f32, bf16 = jnp.float32, jnp.bfloat16
    place = Place(span)
    x, y, z, k = place.shifted()
    rounds = [
        GatherRound(place, shard.at[r], weights.at[r], g_send.at[r], g_recv.at[r], g_keep.at[r])
        for r in range(2 * ROUNDS)
    ]
    norm_gather = NormGather(place, norm_rows, norms, n_send, n_recv, n_keep)

    def swap(n):
        src, dst = ((tok, xs), (cot, o_cot))[n]
        return remote(
            src.at[1 - place.x],
            dst.at[place.x],
            t_sems.at[3 * n],
            t_sems.at[3 * n + 1],
            place.device(dx=1),
        )

    def stay(n):
        src, dst = ((tok, xs), (cot, o_cot))[n]
        return pltpu.make_async_copy(src.at[place.x], dst.at[place.x], t_sems.at[3 * n + 2])

    def store(n):
        src, dst = (
            (weights.at[0:2], o_weights.at[0:2]),
            (weights.at[2:4], o_weights.at[2:4]),
            (weights.at[4:6], o_weights.at[4:6]),
            (weights.at[6:8], o_weights.at[6:8]),
            (xs, o_x),
            (keys, o_k),
            (values, o_v),
            (q, o_q),
            (ctx, o_ctx),
            (h1b, o_h1b),
            (n1, o_n1),
        )[n]
        return pltpu.make_async_copy(src, dst, store_sems.at[n])

    if len(raw) > 1:
        pack_attention(raw, shard)
    else:
        shard[...] = raw[0][...]
    place.greet(ALL_PEERS)
    rounds[0].event(0)
    swap(0).start()
    for n in range(2):
        stay(n).start()
    norm_rows[...] = jnp.zeros_like(norm_rows)
    norm_rows[0:2, 0:96] = gains[...].astype(f32)
    norm_rows[2:4, 0:96] = biases[...].astype(f32)
    block = place.z * 2 + place.y
    norm_rows[...] = pltpu.roll(norm_rows[...], block * 96, 1)
    norm_gather.kept().start()
    norm_gather.start("z1", "z2", "z3")
    if len(raw) > 1:
        pack_feed(raw, shard)

    def step(r, n):
        def go():
            rounds[r].event(n)
            if n == GatherRound.last and r % 2:
                store(r // 2).start()

        return go

    stages = {0: 0, 1: 1, 2: 1, 3: 2, 4: 2, 5: 3, 6: 3, 7: 3, 8: 3, 9: 4}
    order = sorted((r + stages[n], r, n) for r in range(2 * ROUNDS) for n in range(10))
    order = [(r, n) for _, r, n in order][1:]
    begun = order.index((1, 9)) + 1
    beside_heads = order.index((3, 9)) + 1 - begun
    rest = len(order) - begun - beside_heads
    events = Events(step(*at) for at in order)
    events.steps.insert(order.index((7, 4)) + 1, lambda: swap(1).start())

    events.run(1)
    fill_distance(dist, segments, place)
    norm_gather.kept().wait()
    norm_gather.wait("z1", "z2", "z3")
    norm_gather.start("y")
    events.run(begun - 1)
    swap(0).wait_recv()
    stay(0).wait()
    store(4).start()

    def share(t, n):
        ref = (keys, values)[n].at[pl.ds(2 * t, 2), :, place.k]
        return remote(ref, ref, kv_send.at[t, n], kv_recv.at[t, n], place.device(dk=1))

    def project(t, carry):
        w = whole(weights.at[0:2, t // 2, t % 2])
        for s in range(2):
            out = dot(xs[s], w).astype(bf16)
            for i in range(2):
                cols = slice(i * 128, i * 128 + 128)
                q[2 * t + i, pl.ds(s * 256, 256), :] = out[:, cols] * bf16(HEAD_DIM**-0.5)
                keys[2 * t + i, s, k] = out[:, 256 + i * 128 : 384 + i * 128]
                values[2 * t + i, s, k] = out[:, 512 + i * 128 : 640 + i * 128]
        share(t, 0).start()
        share(t, 1).start()
        return carry

    lax.fori_loop(0, 4, project, 0)
    out_t[1, pl.ds(HEAD_DIM, HEAD_DIM), :] = jnp.zeros((HEAD_DIM, 512), f32)
    stop = events.spread(4, 7, beside_heads)

    def attend(t, carry):
        share(t, 0).wait_recv()
        share(t, 1).wait_recv()
        point = 0
        for spot, (tile, half) in enumerate(HEAD_SPOTS):
            slope = slopes[3 * t + spot]
            key = keys[2 * t + tile].reshape(1024, 128)
            rows = slice(half * HEAD_DIM, (half + 1) * HEAD_DIM)
            value_t = values[2 * t + tile].reshape(1024, 128).astype(f32).T.astype(bf16)[rows]
            for start in range(0, 512, CHUNK):
                cols = pl.ds(start, CHUNK)
                part = lane_half(q[2 * t + tile, cols, :], half)
                scores = dot(key, part, NT) - slope * dist[:, cols]
                peak = jnp.max(scores, axis=0, keepdims=True)
                expo = jnp.exp(scores - peak)
                total = jnp.sum(expo, axis=0, keepdims=True)
                out_t[tile, rows, cols] = dot(value_t, expo.astype(bf16)) / total
                o_lse[t, pl.ds(spot, 1), cols] = peak + jnp.log(total)
                stop(t, point)
                point += 1
        for tile in range(2):
            ctx[2 * t + tile] = out_t[tile].T.astype(bf16)
        left, right = out_weights(whole(weights.at[0:2, t // 2, t % 2]))
        mixed = dot(ctx[2 * t], left, NT) + dot(ctx[2 * t + 1], right, NT)

        @pl.when(t == 0)
        def _():
            acc[...] = mixed

        @pl.when(t > 0)
        def _():
            acc[...] += mixed

        stop(t, point)
        return carry

    lax.fori_loop(0, 4, attend, 0)
    for n in range(5, 9):
        store(n).start()
    norm_gather.wait("y")
    norm_sum = jnp.sum(norms[...].reshape(8, 8, 768), axis=0)
    o_norms[...] = norm_sum

    def first_norm(rows, i):
        attn = acc[rows, :]
        half = i // 2
        resid = xs[half, pl.ds(pl.multiple_of((i % 2) * ROWS, ROWS), ROWS), :].astype(f32) + attn
        normed, inv = norm_stats(resid)
        value = normed * norm_sum[0:1] + norm_sum[2:3]
        h1[rows, :] = value
        h1b[rows, :] = value.astype(bf16)
        n1[rows, :] = normed
        o_i1[rows, :] = inv
        acc[rows, :] = jnp.zeros_like(attn)
        if_first = jnp.where(i == 0, 0.0, 1.0)
        o_squares[0] = o_squares[0] * if_first + columns(attn * attn)
        o_squares[1] = o_squares[1] * if_first + columns(resid * resid)

    o_squares[...] = jnp.zeros_like(o_squares)
    row_blocks(first_norm)
    store(9).start()
    store(10).start()

    first_part = order.index((5, 9)) - begun - beside_heads
    last_part = len(order) - order.index((6, 9))
    counts = {}
    for n in range(first_part):
        at = n * 8 // first_part
        counts[at] = counts.get(at, 0) + 1
    counts[8] = 1
    middle = rest + 1 - first_part - last_part - 1
    for n in range(middle):
        at = 9 + n * 6 // middle
        counts[at] = counts.get(at, 0) + 1
    counts[16] = last_part
    stop_f = events.place(12, 2, counts)
    assert not events.steps

    def keep_copy(n):
        return pltpu.make_async_copy(kept.at[n % 2], o_kept.at[n], kept_sems.at[n % 2])

    def feed(n, carry):
        r, t = 1 + n // 4, n % 4
        stop_f(n, 0)

        @pl.when(n >= 2)
        def _():
            keep_copy(n - 2).wait()

        ref = weights.at[pl.ds(2 * r, 2), t // 2, t % 2]
        for start in range(0, 512, CHUNK):
            rows = pl.ds(start, CHUNK)
            w = whole(ref)
            projected = dot(h1b[rows, :], w[:, :512])
            gate, up = projected[:, :256], projected[:, 256:]
            cdf = 0.5 + 0.5 * lax.erf(gate * (0.5**0.5))
            pdf = jnp.exp(-0.5 * gate * gate) * 0.3989422804014327
            act = gate * cdf
            hidden = (act * up).astype(bf16)
            kept[n % 2, 0, rows, :] = hidden
            kept[n % 2, 1, rows, :] = act.astype(bf16)
            kept[n % 2, 2, rows, :] = ((cdf + gate * pdf) * up).astype(bf16)
            acc[rows, :] += dot(hidden, w[:, 512:], NT)
        keep_copy(n).start()
        stop_f(n, 1)
        return carry

    lax.fori_loop(0, 12, feed, 0)

    def second_norm(rows, i):
        ffn = acc[rows, :]
        resid = h1[rows, :] + ffn
        normed, inv = norm_stats(resid)
        o_out[rows, :] = (normed * norm_sum[1:2] + norm_sum[3:4]).astype(bf16)
        o_n2[rows, :] = normed
        o_i2[rows, :] = inv
        o_squares[2] += columns(ffn * ffn)
        o_squares[3] += columns(resid * resid)

    row_blocks(second_norm)
    for n in (10, 11):
        keep_copy(n).wait()
    for r in rounds:
        r.finish()
    norm_gather.finish()
    for n in range(2):
        swap(n).wait_send()
    swap(1).wait_recv()
    stay(1).wait()
    for t in range(4):
        for n in range(2):
            share(t, n).wait_send()
    for n in range(11):
        store(n).wait()


def forward_refs(span, count, *refs):
    forward_kernel(span, refs[0], refs[1 : 1 + count], *refs[1 + count :])


def forward(span, slopes, raw, gains, biases, tok, cot, segments):
    f32, bf16 = jnp.float32, jnp.bfloat16
    any_space = pl.BlockSpec(memory_space=pl.ANY)
    vmem = pl.BlockSpec(memory_space=pltpu.VMEM)
    outs = (
        ((2 * ROUNDS, 2, 2, 4, 2, 96, 384), bf16, any_space),
        ((8, 768), f32, vmem),
        ((2, 256, 768), bf16, any_space),
        ((2, 256, 768), bf16, any_space),
        ((8, 512, 128), bf16, any_space),
        ((8, 2, 2, 256, 128), bf16, any_space),
        ((8, 2, 2, 256, 128), bf16, any_space),
        ((8, 512, 128), bf16, any_space),
        ((4, 8, 512), f32, vmem),
        ((12, 3, 512, 256), bf16, any_space),
        ((512, 768), bf16, any_space),
        ((512, 768), f32, any_space),
        ((512, 1), f32, vmem),
        ((512, 768), f32, vmem),
        ((512, 1), f32, vmem),
        ((512, 768), bf16, vmem),
        ((4, 8, 768), f32, vmem),
    )
    dma = pltpu.SemaphoreType.DMA
    copies = len(GatherRound.names)
    return pl.pallas_call(
        partial(forward_refs, span, len(raw)),
        out_shape=tuple(jax.ShapeDtypeStruct(s, d) for s, d, _ in outs),
        in_specs=[pl.BlockSpec(memory_space=pltpu.SMEM)] + [vmem] * (len(raw) + 5),
        out_specs=tuple(spec for _, _, spec in outs),
        scratch_shapes=[
            pltpu.VMEM((2 * ROUNDS, 96, 384), bf16),
            pltpu.VMEM((8, 768), f32),
            pltpu.VMEM((2 * ROUNDS, 2, 2, 4, 2, 96, 384), bf16),
            pltpu.VMEM((4, 2, 8, 768), f32),
            pltpu.VMEM((2, 256, 768), bf16),
            pltpu.VMEM((8, 512, 128), bf16),
            pltpu.VMEM((8, 2, 2, 256, 128), bf16),
            pltpu.VMEM((8, 2, 2, 256, 128), bf16),
            pltpu.VMEM((8, 512, 128), bf16),
            pltpu.VMEM((512, 768), bf16),
            pltpu.VMEM((512, 768), f32),
            pltpu.VMEM((1024, 512), f32),
            pltpu.VMEM((2, 128, 512), f32),
            pltpu.VMEM((512, 768), f32),
            pltpu.VMEM((512, 768), f32),
            pltpu.VMEM((2, 3, 512, 256), bf16),
            dma((2 * ROUNDS, copies)),
            dma((2 * ROUNDS, copies)),
            dma((2 * ROUNDS,)),
            dma((4,)),
            dma((4,)),
            dma,
            dma((6,)),
            dma((4, 2)),
            dma((4, 2)),
            dma((11,)),
            dma((2,)),
        ],
        compiler_params=pltpu.CompilerParams(
            collective_id=0, has_side_effects=True, vmem_limit_bytes=VMEM_LIMIT
        ),
        name="forward",
    )(slopes, *raw, gains, biases, tok, cot, segments)


class ScatterRound(Copies):
    names = ("ay1", "bx", "ay0", "ax", "by", "cx", "dy") + tuple(
        part + "z%d" % step for part in "abcd" for step in (1, 2, 3)
    )

    def __init__(self, place, held, twin, stage, landing, send, recv, pair):
        self.place, self.held, self.twin, self.stage = place, held, twin, stage
        self.ay, self.bx, self.ax, self.by, self.z, self.cz, self.dz, self.last = landing
        self.send, self.recv, self.pair = send, recv, pair

    def copy(self, name):
        p, held = self.place, self.held
        at = self.names.index(name)
        a, b, c, d = (PARTS[part] for part in "abcd")
        step = int(name[2]) if name[1] == "z" else 0
        far = (p.z + step) % 4
        ac, bd = PARTS["ac"], PARTS["bd"]
        if name in ("ay1", "ay0"):
            dx = int(name[2])
            src, dst, to = held.at[dx, :, 1 - p.y, ac, :], self.ay.at[dx], {"dy": 1}
        elif name == "bx":
            src, dst, to = held.at[1, :, :, bd, :], self.bx, {"dx": 1}
        elif name == "ax":
            src, dst, to = held.at[1, :, p.y, a, :], self.ax, {"dx": 1}
        elif name == "by":
            src, dst, to = held.at[0, :, 1 - p.y, b, :], self.by, {"dy": 1}
        elif name == "cx":
            src, dst, to = held.at[1, p.z, p.y, c, :], self.last.at[0], {"dx": 1}
        elif name == "dy":
            src, dst, to = held.at[0, p.z, 1 - p.y, d, :], self.last.at[1], {"dy": 1}
        elif name[0] == "c":
            src, dst, to = held.at[:, far, p.y, c, :], self.cz.at[step - 1], {"dz": step}
        elif name[0] == "d":
            src, dst, to = held.at[0, far, :, d, :], self.dz.at[step - 1], {"dz": step}
        else:
            rows = PARTS[name[0]]
            into = pl.ds(0, 32) if name[0] == "a" else pl.ds(32, 32)
            src, dst, to = held.at[0, far, p.y, rows, :], self.z.at[step - 1, into, :], {"dz": step}
        return remote(src, dst, self.send.at[at], self.recv.at[at], p.device(**to))

    def push(self, dx):
        return remote(
            self.stage.at[dx], self.twin.at[dx], self.pair.at[0, dx], self.pair.at[1, dx], self.place.device(dk=1)
        )

    def add(self, ref, *others):
        total = ref[...].astype(jnp.float32)
        for other in others:
            total = total + other[...].astype(jnp.float32)
        ref[...] = total.astype(jnp.bfloat16)

    def pair_sum(self, dx):
        self.push(dx).wait_recv()

        def body(i, carry):
            self.add(self.held.at[dx, i], self.twin.at[dx, i])
            return carry

        lax.fori_loop(0, 4, body, 0)
        if dx:
            self.start("bx", "ay1")
        else:
            self.start("ay0")

    def event(self, n, out=None):
        p, held = self.place, self.held
        a, b, c, d = (PARTS[part] for part in "abcd")
        ac, bd = PARTS["ac"], PARTS["bd"]
        if n == 0:
            self.wait("ay1")
            self.add(held.at[1, :, p.y, ac, :], self.ay.at[1])
            self.start("ax")
        elif n == 1:
            self.wait("bx")
            self.add(held.at[0, :, 1 - p.y, bd, :], self.bx.at[:, 1 - p.y])
            self.start("by")
            self.add(held.at[0, :, p.y, bd, :], self.bx.at[:, p.y])
            self.start("dz1", "dz2", "dz3")
        elif n == 2:
            self.wait("ay0")
            self.add(held.at[0, :, p.y, ac, :], self.ay.at[0])
            self.start("cz1", "cz2", "cz3")
        elif n == 3:
            self.wait("ax")
            self.add(held.at[0, :, p.y, a, :], self.ax)
            self.start("az1", "az2", "az3")
        elif n == 4:
            self.wait("by")
            self.add(held.at[0, :, p.y, b, :], self.by)
            self.start("bz1", "bz2", "bz3")
        elif n == 5:
            self.wait("cz1", "cz2", "cz3", "dz1", "dz2", "dz3")
            self.add(held.at[1, p.z, p.y, c, :], *[self.cz.at[i, 1] for i in range(3)])
            self.start("cx")
            self.add(held.at[0, p.z, 1 - p.y, d, :], *[self.dz.at[i, 1 - p.y] for i in range(3)])
            self.start("dy")
            self.add(held.at[0, p.z, p.y, c, :], *[self.cz.at[i, 0] for i in range(3)])
            self.add(held.at[0, p.z, p.y, d, :], *[self.dz.at[i, p.y] for i in range(3)])
        else:
            self.wait("az1", "az2", "az3", "bz1", "bz2", "bz3", "cx", "dy")
            for rows, others in (
                (a, [self.z.at[i, pl.ds(0, 32), :] for i in range(3)]),
                (b, [self.z.at[i, pl.ds(32, 32), :] for i in range(3)]),
                (c, [self.last.at[0]]),
                (d, [self.last.at[1]]),
            ):
                total = held[0, p.z, p.y, rows, :].astype(jnp.float32)
                for other in others:
                    total = total + other[...].astype(jnp.float32)
                out[rows, :] = total


def backward_kernel(
    span,
    slopes,
    i_weights,
    norms,
    i_x,
    i_cot,
    i_q,
    i_k,
    i_v,
    i_ctx,
    i_lse,
    i_kept,
    i_h1b,
    i_n1,
    i_i1,
    i_n2,
    i_i2,
    i_out,
    squares,
    segments,
    o_out,
    o_tokens,
    o_grads,
    o_small,
    w_buf,
    kept,
    h1_t,
    f_t,
    d_rows,
    n_buf,
    d_h1,
    q,
    keys,
    values,
    ctx,
    lse,
    dist,
    d_ctx,
    d_kv,
    d_kv_in,
    dq_t,
    acc_k,
    acc_v,
    held,
    twin,
    stage,
    land_ay,
    land_bx,
    land_ax,
    land_by,
    land_z,
    land_cz,
    land_dz,
    land_last,
    small,
    small_in,
    load_sems,
    step_sems,
    r_send,
    r_recv,
    r_pair,
    t_sems,
    kv_send,
    kv_recv,
    s_send,
    s_recv,
):
    f32, bf16 = jnp.float32, jnp.bfloat16
    place = Place(span)
    x, y, z, k = place.shifted()
    rounds = [
        ScatterRound(
            place,
            held.at[n],
            twin.at[n % 3],
            stage,
            [
                ref.at[n]
                for ref in (land_ay, land_bx, land_ax, land_by, land_z, land_cz, land_dz, land_last)
            ],
            r_send.at[n],
            r_recv.at[n],
            r_pair.at[n],
        )
        for n in range(ROUNDS)
    ]

    def load(n):
        src, dst = (
            (i_cot, d_rows.at[2]),
            (i_n2, n_buf),
            (i_h1b, d_rows.at[1]),
            (i_x, d_rows.at[2]),
            (i_q, q),
            (i_k, keys),
            (i_v, values),
            (i_ctx, ctx),
            (i_lse, lse),
            (i_n1, n_buf),
        )[n]
        return pltpu.make_async_copy(src, dst, load_sems.at[n])

    def where(n):
        return x ^ (1 - n // 2), k ^ (1 - n % 2)

    def where_heads(n):
        return x ^ (1 - n // 2), n % 2

    def fetch(n, part):
        r = 3 - n // 4
        wx, wk = where(n % 4)
        if part == 0:
            return pltpu.make_async_copy(i_weights.at[pl.ds(2 * r, 2), wx, wk], w_buf.at[n % 2], step_sems.at[n % 2, 0])
        return pltpu.make_async_copy(
            i_kept.at[(r - 1) * 4 + wx * 2 + wk], kept.at[n % 2], step_sems.at[n % 2, 1]
        )

    for n in (0, 1, 2, 4, 5, 6, 7, 8):
        load(n).start()
    fetch(0, 0).start()
    fetch(0, 1).start()
    place.greet(ALL_PEERS)

    def swap(n):
        src, dst = ((i_out, o_out), (d_rows.at[0], o_tokens))[n]
        return remote(
            src.at[1 - place.x],
            dst.at[place.x],
            t_sems.at[3 * n],
            t_sems.at[3 * n + 1],
            place.device(dx=1),
        )

    def stay(n):
        src, dst = ((i_out, o_out), (d_rows.at[0], o_tokens))[n]
        return pltpu.make_async_copy(src.at[place.x], dst.at[place.x], t_sems.at[3 * n + 2])

    swap(0).start()
    stay(0).start()
    load(0).wait()
    load(1).wait()
    small[...] = jnp.zeros_like(small)

    def halves(ref, i):
        return ref.at[i // 2, pl.ds(pl.multiple_of((i % 2) * ROWS, ROWS), ROWS), :]

    sums = [jnp.zeros((8, 768), f32)] * 2
    for i in range(512 // ROWS):
        rows = pl.ds(i * ROWS, ROWS)
        grad = halves(d_rows.at[2], i)[...].astype(f32)
        normed = n_buf[rows, :]
        out = norm_backward(grad, normed, i_i2[rows, :], norms[1:2])
        d_h1[rows, :] = out
        halves(d_rows.at[0], i)[...] = out.astype(bf16)
        f_t[:, rows] = out.T.astype(bf16)
        sums[0] = sums[0] + columns(grad * normed)
        sums[1] = sums[1] + columns(grad)
    small[1] = sums[0]
    small[3] = sums[1]
    load(9).start()
    load(3).start()
    load(2).wait()
    for i in range(512 // ROWS):
        rows = pl.ds(i * ROWS, ROWS)
        h1_t[:, rows] = halves(d_rows.at[1], i)[...].astype(f32).T.astype(bf16)
    fill_distance(dist, segments, place)

    def pair(n, dx):
        return lambda: rounds[n].pair_sum(dx)

    def step(n, at):
        return lambda: rounds[n].event(at, o_grads.at[3 - n])

    def put(n, dx, theirs, value, cols):
        block = value.astype(bf16).reshape(4, 2, 96, value.shape[-1])

        @pl.when(theirs)
        def _():
            stage[dx, :, :, :, cols] = block

        @pl.when(jnp.logical_not(theirs))
        def _():
            held[n, dx, :, :, :, cols] = block

    def push(n, dx):
        return remote(
            stage.at[dx], twin.at[n % 3, dx], r_pair.at[n, 0, dx], r_pair.at[n, 1, dx], place.device(dk=1)
        )

    plan = {
        1: [pair(0, 1)],
        3: [pair(0, 0)],
        5: [step(0, 0), pair(1, 1)],
        7: [step(0, 2), pair(1, 0)],
        8: [step(0, 1)],
        9: [step(1, 0), pair(2, 1)],
        10: [step(0, 3)],
        11: [step(0, 4), step(1, 2), pair(2, 0)],
    }

    def feed(n, carry):
        dx = 1 - n % 4 // 2
        theirs = n % 2 == 0

        @pl.when(n < 11)
        def _():
            fetch(n + 1, 0).start()
            fetch(n + 1, 1).start()

        @pl.when(jnp.logical_and(theirs, n >= 4))
        def _():
            push(n // 4 - 1, dx).wait_send()

        fetch(n, 0).wait()
        fetch(n, 1).wait()
        w = whole(w_buf.at[n % 2])
        hold = kept.at[n % 2]
        d_ffn = d_rows[0].reshape(512, 768)
        put(n // 4, dx, theirs, dot(f_t[...], hold[0]), slice(512, 768))
        d_hidden = dot(d_ffn, w[:, 512:])
        d_gate = (d_hidden * hold[2].astype(f32)).astype(bf16)
        d_up = (d_hidden * hold[1].astype(f32)).astype(bf16)
        put(n // 4, dx, theirs, dot(h1_t[...], d_gate), slice(0, 256))
        put(n // 4, dx, theirs, dot(h1_t[...], d_up), slice(256, 512))

        @pl.when(theirs)
        def _():
            push(n // 4, dx).start()

        d_h1[...] += dot(d_gate, w[:, :256], NT) + dot(d_up, w[:, 256:512], NT)
        for at, todo in plan.items():

            @pl.when(n == at)
            def _():
                for item in todo:
                    item()

        return carry

    lax.fori_loop(0, 12, feed, 0)
    load(9).wait()
    load(3).wait()
    for i in range(512 // ROWS):
        rows = pl.ds(i * ROWS, ROWS)
        h1_t[:, rows] = halves(d_rows.at[2], i)[...].astype(f32).T.astype(bf16)
    sums = [jnp.zeros((8, 768), f32)] * 2
    for i in range(512 // ROWS):
        rows = pl.ds(i * ROWS, ROWS)
        grad = d_h1[rows, :]
        normed = n_buf[rows, :]
        out = norm_backward(grad, normed, i_i1[rows, :], norms[0:1])
        d_h1[rows, :] = out
        halves(d_rows.at[1], i)[...] = out.astype(bf16)
        f_t[:, rows] = out.T.astype(bf16)
        sums[0] = sums[0] + columns(grad * normed)
        sums[1] = sums[1] + columns(grad)
    small[0] = sums[0]
    small[2] = sums[1]
    for n in range(4, 9):
        load(n).wait()

    small[0] = jnp.concatenate(
        [jnp.sum(small[i], axis=0, keepdims=True) for i in range(4)]
        + [jnp.sum(squares[i], axis=0, keepdims=True) for i in range(4)],
        axis=0,
    )

    def spread(n):
        to = ({"dk": 1}, {"dx": 1}, {"dy": 1}, {"dz": 1}, {"dz": 2}, {"dz": 3})[n]
        return remote(
            small.at[min(n, 3)], small_in.at[n], s_send.at[n], s_recv.at[n], place.device(**to)
        )

    def small_step(n):
        def go():
            if 0 < n < 4:
                spread(n - 1).wait_recv()
                small[n] = small[n - 1] + small_in[n - 1]
            if n < 3:
                spread(n).start()
            if n == 3:
                for at in (3, 4, 5):
                    spread(at).start()
            if n == 4:
                for at in (3, 4, 5):
                    spread(at).wait_recv()
                total = small[3]
                result = jnp.zeros_like(total)
                for at in range(4):
                    back = (place.z - at) % 4
                    term = jnp.where(
                        back == 0,
                        total,
                        jnp.where(
                            back == 1, small_in[3], jnp.where(back == 2, small_in[4], small_in[5])
                        ),
                    )
                    result = result + term
                o_small[...] = result

        return go

    def fetch_heads(n):
        wx, wk = where_heads(n)
        return pltpu.make_async_copy(i_weights.at[0:2, wx, wk], w_buf.at[n % 2], step_sems.at[n % 2, 0])

    fetch_heads(0).start()
    dq_t[1, pl.ds(HEAD_DIM, HEAD_DIM), :] = jnp.zeros((HEAD_DIM, 512), f32)

    def share(t):
        return remote(
            d_kv.at[t, :, :, :, 1 - place.k], d_kv_in.at[t], kv_send.at[t], kv_recv.at[t], place.device(dk=1)
        )

    beside = {
        (0, 0): [small_step(0), step(0, 5)],
        (0, 2): [small_step(1), step(2, 0)],
        (0, 4): [small_step(2), step(1, 1)],
        (1, 0): [small_step(3), step(0, 6)],
        (1, 2): [step(1, 3)],
        (1, 4): [small_step(4), step(2, 2)],
        (2, 0): [step(1, 4)],
        (2, 2): [step(1, 5)],
        (2, 5): [step(2, 1)],
        (3, 0): [pair(3, 1)],
        (3, 1): [step(1, 6)],
        (3, 3): [step(2, 3)],
        (3, 5): [step(2, 4)],
    }
    first = lax.broadcasted_iota(jnp.int32, (768, 128), 1) < HEAD_DIM

    def stop(i, point):
        for (trip, at), todo in beside.items():
            if at == point:

                @pl.when(i == trip)
                def _():
                    for item in todo:
                        item()

    def attend(n):
        wx, wk = where_heads(n)
        t = wx * 2 + wk
        fetch_heads(n).wait()
        left, right = out_weights(whole(w_buf.at[n % 2]))
        d_attn = d_rows[1].reshape(512, 768)
        d_ctx[0] = dot(d_attn, left).astype(bf16)
        d_ctx[1] = dot(d_attn, right).astype(bf16)
        point = 0
        for spot, (tile, half) in enumerate(HEAD_SPOTS):
            slope = slopes[3 * t + spot]
            key = keys[2 * t + tile].reshape(1024, 128)
            value = values[2 * t + tile].reshape(1024, 128)
            rows = slice(half * HEAD_DIM, (half + 1) * HEAD_DIM)
            key_t = key.astype(f32).T.astype(bf16)[rows]
            product = ctx[2 * t + tile].astype(f32) * d_ctx[tile].astype(f32)
            delta = jnp.sum(product.T[rows], axis=0, keepdims=True)
            for start in range(0, 512, CHUNK):
                cols = pl.ds(start, CHUNK)
                part = lane_half(q[2 * t + tile, cols, :], half)
                grad = lane_half(d_ctx[tile, cols, :], half)
                scores = dot(key, part, NT) - slope * dist[:, cols]
                probs = jnp.exp(scores - lse[t, pl.ds(spot, 1), cols])
                grad_probs = dot(value, grad, NT)
                term_v = dot(probs.astype(bf16), grad)
                grad_scores = (probs * (grad_probs - delta[:, start : start + CHUNK])).astype(bf16)
                term_k = dot(grad_scores, part)
                if half == 0 and start == 0:
                    acc_v[...] = term_v
                    acc_k[...] = term_k
                else:
                    acc_v[...] += term_v
                    acc_k[...] += term_k
                dq_t[tile, rows, cols] = dot(key_t, grad_scores)
                stop(n, point)
                point += 1
            if half == 1 or tile == 1:
                d_kv[t, 0, tile] = acc_k[...].astype(bf16).reshape(2, 2, 256, 128)
                d_kv[t, 1, tile] = acc_v[...].astype(bf16).reshape(2, 2, 256, 128)
        share(t).start()
        for tile in range(2):
            q[2 * t + tile] = (dq_t[tile].T * HEAD_DIM**-0.5).astype(bf16)

    def project(n):
        wx, wk = where_heads(n)
        t = wx * 2 + wk
        dx = 1 - n // 2
        theirs = wk != k

        @pl.when(theirs)
        def _():
            push(2, dx).wait_send()

        share(t).wait_recv()
        parts = [q[2 * t], q[2 * t + 1]]
        for kind in range(2):
            for tile in range(2):
                mine = d_kv[t, kind, tile, :, k].reshape(512, 128).astype(f32)
                mine = mine + d_kv_in[t, kind, tile].reshape(512, 128).astype(f32)
                parts.append(mine.astype(bf16))
        d_qkv = jnp.concatenate(parts, axis=1)
        d_w = dot(h1_t[...], d_qkv)
        left = dot(f_t[...], ctx[2 * t])
        right = swap_halves(dot(f_t[...], ctx[2 * t + 1]))
        tiles = [
            d_w[:, 0:128],
            jnp.where(first, d_w[:, 128:256], pltpu.roll(left, HEAD_DIM, 1)),
            d_w[:, 256:384],
            jnp.where(first, d_w[:, 384:512], left),
            d_w[:, 512:640],
            jnp.where(first, d_w[:, 640:768], right),
        ]
        put(3, dx, theirs, jnp.concatenate(tiles, axis=1), slice(0, 768))

        @pl.when(theirs)
        def _():
            push(3, dx).start()

        d_h1[...] += dot(d_qkv, whole(w_buf.at[n % 2]), NT)

    def heads(n, carry):
        @pl.when(n < 4)
        def _():
            attend(n)

        @pl.when(n > 0)
        def _():
            project(n - 1)

        @pl.when(n < 3)
        def _():
            fetch_heads(n + 1).start()

        return carry

    lax.fori_loop(0, 5, heads, 0)
    for i in range(512 // ROWS):
        rows = pl.ds(i * ROWS, ROWS)
        halves(d_rows.at[0], i)[...] = d_h1[rows, :].astype(bf16)
    rounds[3].pair_sum(0)
    swap(1).start()
    stay(1).start()
    step(2, 5)()
    for at in (0, 1, 2):
        step(3, at)()
    step(2, 6)()
    for at in (3, 4, 5, 6):
        step(3, at)()
    for n in range(6):
        spread(n).wait_send()
    for r in rounds:
        r.finish()
    for dx in range(2):
        push(3, dx).wait_send()
    for t in range(4):
        share(t).wait_send()
    for n in range(2):
        swap(n).wait()
        stay(n).wait()


def backward(span, slopes, saved, segments):
    f32, bf16 = jnp.float32, jnp.bfloat16
    any_space = pl.BlockSpec(memory_space=pl.ANY)
    vmem = pl.BlockSpec(memory_space=pltpu.VMEM)
    dma = pltpu.SemaphoreType.DMA
    (weights, norms, xs, cot, q, keys, values, ctx, lse, kept, h1b, n1, i1, n2, i2, out, squares) = saved
    h1b = h1b.reshape(2, 256, 768)
    out = out.reshape(2, 256, 768)
    in_specs = [pl.BlockSpec(memory_space=pltpu.SMEM), any_space, vmem] + [any_space] * 10
    in_specs += [vmem, any_space, vmem, any_space, vmem, vmem]
    copies = len(ScatterRound.names)
    return pl.pallas_call(
        partial(backward_kernel, span),
        out_shape=(
            jax.ShapeDtypeStruct((2, 256, 768), bf16),
            jax.ShapeDtypeStruct((2, 256, 768), bf16),
            jax.ShapeDtypeStruct((ROUNDS, 96, 768), f32),
            jax.ShapeDtypeStruct((8, 768), f32),
        ),
        in_specs=in_specs,
        out_specs=(any_space, any_space, vmem, vmem),
        scratch_shapes=[
            pltpu.VMEM((2, 2, 4, 2, 96, 384), bf16),
            pltpu.VMEM((2, 3, 512, 256), bf16),
            pltpu.VMEM((768, 512), bf16),
            pltpu.VMEM((768, 512), bf16),
            pltpu.VMEM((3, 2, 256, 768), bf16),
            pltpu.VMEM((512, 768), f32),
            pltpu.VMEM((512, 768), f32),
            pltpu.VMEM((8, 512, 128), bf16),
            pltpu.VMEM((8, 2, 2, 256, 128), bf16),
            pltpu.VMEM((8, 2, 2, 256, 128), bf16),
            pltpu.VMEM((8, 512, 128), bf16),
            pltpu.VMEM((4, 8, 512), f32),
            pltpu.VMEM((1024, 512), f32),
            pltpu.VMEM((2, 512, 128), bf16),
            pltpu.VMEM((4, 2, 2, 2, 2, 256, 128), bf16),
            pltpu.VMEM((4, 2, 2, 2, 256, 128), bf16),
            pltpu.VMEM((2, 128, 512), f32),
            pltpu.VMEM((1024, 128), f32),
            pltpu.VMEM((1024, 128), f32),
            pltpu.VMEM((ROUNDS, 2, 4, 2, 96, 768), bf16),
            pltpu.VMEM((3, 2, 4, 2, 96, 768), bf16),
            pltpu.VMEM((2, 4, 2, 96, 768), bf16),
            pltpu.VMEM((ROUNDS, 2, 4, 48, 768), bf16),
            pltpu.VMEM((ROUNDS, 4, 2, 48, 768), bf16),
            pltpu.VMEM((ROUNDS, 4, 32, 768), bf16),
            pltpu.VMEM((ROUNDS, 4, 32, 768), bf16),
            pltpu.VMEM((ROUNDS, 3, 64, 768), bf16),
            pltpu.VMEM((ROUNDS, 3, 2, 16, 768), bf16),
            pltpu.VMEM((ROUNDS, 3, 2, 16, 768), bf16),
            pltpu.VMEM((ROUNDS, 2, 16, 768), bf16),
            pltpu.VMEM((4, 8, 768), f32),
            pltpu.VMEM((6, 8, 768), f32),
            dma((10,)),
            dma((2, 2)),
            dma((ROUNDS, copies)),
            dma((ROUNDS, copies)),
            dma((ROUNDS, 2, 2)),
            dma((6,)),
            dma((4,)),
            dma((4,)),
            dma((6,)),
            dma((6,)),
        ],
        compiler_params=pltpu.CompilerParams(
            collective_id=1, has_side_effects=True, vmem_limit_bytes=VMEM_LIMIT
        ),
        name="backward",
    )(
        slopes,
        weights,
        norms,
        xs,
        cot,
        q,
        keys,
        values,
        ctx,
        lse,
        kept,
        h1b,
        n1,
        i1,
        n2,
        i2,
        out,
        squares,
        segments,
    )


def finish_kernel(
    block, grads, small, lo, gt, o_lo, o_gt, o_qkv, o_wout, o_win, o_down, o_gains, o_biases, rows, sems
):
    def move(n, src, dst):
        return pltpu.make_async_copy(src, dst, sems.at[n])

    move(0, lo, rows.at[0]).start()
    move(1, gt, rows.at[1]).start()
    turned = []
    for c in range(3):
        o_qkv[c] = grads[0, :, c * 256 : c * 256 + 192]
        turned.append(grads[0, :, c * 256 + 128 : c * 256 + 256].T[HEAD_DIM:])
    o_wout[...] = jnp.concatenate(turned, axis=0)
    move(0, lo, rows.at[0]).wait()
    move(2, rows.at[0], o_lo).start()
    move(1, gt, rows.at[1]).wait()
    move(3, rows.at[1], o_gt).start()
    for r in range(3):
        units = slice(r * 256, (r + 1) * 256)
        o_win[:, 0, units] = grads[1 + r, :, 0:256]
        o_win[:, 1, units] = grads[1 + r, :, 256:512]
        o_down[units, :] = grads[1 + r, :, 512:768].T
    mine = pltpu.roll(small[...], 768 - block[0] * 96, 1)
    o_gains[...] = mine[0:2, 0:96]
    o_biases[...] = mine[2:4, 0:96]
    move(2, rows.at[0], o_lo).wait()
    move(3, rows.at[1], o_gt).wait()


def finish(block, grads, small, lo, gt):
    any_space = pl.BlockSpec(memory_space=pl.ANY)
    vmem = pl.BlockSpec(memory_space=pltpu.VMEM)
    f32 = jnp.float32
    shape = jax.ShapeDtypeStruct
    return pl.pallas_call(
        finish_kernel,
        out_shape=(
            shape(lo.shape, lo.dtype),
            shape(gt.shape, gt.dtype),
            shape((3, 96, 192), f32),
            shape((192, 96), f32),
            shape((96, 2, 768), f32),
            shape((768, 96), f32),
            shape((2, 96), f32),
            shape((2, 96), f32),
        ),
        in_specs=[pl.BlockSpec(memory_space=pltpu.SMEM), vmem, vmem, any_space, any_space],
        out_specs=(any_space, any_space) + (vmem,) * 6,
        scratch_shapes=[pltpu.VMEM((2,) + lo.shape, lo.dtype), pltpu.SemaphoreType.DMA((4,))],
        compiler_params=pltpu.CompilerParams(vmem_limit_bytes=VMEM_LIMIT),
        name="finish",
    )(block, grads, small, lo, gt)


def local(
    tokens,
    segment_ids,
    query_key_value_weight,
    w_out,
    input_weight,
    w_down,
    norm_gains,
    norm_biases,
    cotangent,
):
    f32 = jnp.float32
    shard_rows = query_key_value_weight.shape[1]
    span = 96 // shard_rows
    slopes = jnp.exp2(-8.0 * (jnp.arange(HEADS).astype(f32) + 1.0) / HEADS)
    cells = float(lax.axis_size("fsdp") * 2 * 1024 * 768)
    if span == 1:
        raw = (query_key_value_weight, w_out, input_weight, w_down)
        gains, biases = norm_gains, norm_biases
    else:
        count = lax.axis_size("fsdp")
        groups = [list(range(i, i + span)) for i in range(0, count, span)]
        heads = query_key_value_weight.transpose(1, 0, 2).reshape(shard_rows, 3, 3, HEAD_DIM)
        w_out_t = w_out.T.reshape(shard_rows, 3, 1, HEAD_DIM)
        wa = jnp.concatenate([heads, w_out_t], axis=2).reshape(shard_rows, 1, 768)
        gate_up = input_weight.reshape(shard_rows, 2, 3, 256).transpose(0, 2, 1, 3)
        down = w_down.T.reshape(shard_rows, 3, 1, 256)
        wf = jnp.concatenate([gate_up, down], axis=2).reshape(shard_rows, 3, 768)
        shard = jnp.concatenate([wa, wf], axis=1).reshape(shard_rows, 8, 384).transpose(1, 0, 2)
        raw = (lax.all_gather(shard, "fsdp", axis=1, tiled=True, axis_index_groups=groups),)
        gains, biases = (
            lax.all_gather(rows, "fsdp", axis=1, tiled=True, axis_index_groups=groups)
            for rows in (norm_gains, norm_biases)
        )

    saved = forward(span, slopes, raw, gains, biases, tokens, cotangent, segment_ids)
    layer_out, grad_tokens, grads, small = backward(span, slopes, saved, segment_ids)

    if span == 1:
        block = lax.axis_index("fsdp").astype(jnp.int32).reshape(1)
        outs = finish(block, grads, small, layer_out, grad_tokens)
    else:
        grads = lax.psum_scatter(
            grads, "fsdp", scatter_dimension=1, tiled=True, axis_index_groups=groups
        )
        small = lax.psum(small, "fsdp", axis_index_groups=groups)
        grads_a = grads[0].reshape(shard_rows, 3, 4, HEAD_DIM)
        grads_f = grads[1:].reshape(3, shard_rows, 3, 256)
        shard_start = lax.axis_index("fsdp") * shard_rows
        mine = lax.dynamic_slice_in_dim(small[:4], shard_start, shard_rows, 1)
        outs = (
            layer_out,
            grad_tokens,
            grads_a[:, :, :3].transpose(1, 0, 2, 3).reshape(3, shard_rows, 192),
            grads_a[:, :, 3].reshape(shard_rows, 192).T,
            grads_f[:, :, :2].transpose(1, 2, 0, 3).reshape(shard_rows, 2, 768),
            grads_f[:, :, 2].transpose(0, 2, 1).reshape(768, shard_rows),
            mine[:2],
            mine[2:],
        )
    return outs + (jnp.sqrt(jnp.sum(small[4:], axis=1) / cells),)


def solution(mesh):
    placed = (
        P("fsdp", "tp", None),
        P("fsdp", None),
        P(None, "fsdp", "tp"),
        P("tp", "fsdp"),
        P("fsdp", None, "tp"),
        P("tp", "fsdp"),
        P(None, "fsdp"),
        P(None, "fsdp"),
        P("fsdp", "tp", None),
    )
    return jax.shard_map(
        local,
        mesh=mesh,
        in_specs=placed,
        out_specs=(
            P("fsdp", "tp", None),
            P("fsdp", "tp", None),
            P(None, "fsdp", "tp"),
            P("tp", "fsdp"),
            P("fsdp", None, "tp"),
            P("tp", "fsdp"),
            P(None, "fsdp"),
            P(None, "fsdp"),
            P(),
        ),
        check_vma=False,
    )
```

```python
from functools import partial

import jax
import jax.numpy as jnp
from jax import lax
from jax.experimental import pallas as pl
from jax.experimental.pallas import tpu as pltpu
from jax.sharding import PartitionSpec as P

HEADS = 12
HEAD_DIM = 64
MESH = pl.DeviceIdType.MESH
VMEM_LIMIT = 63 << 20
norm_eps = 1e-05
ROUNDS = 4
NT = (((1,), (1,)), ((), ()))
NN = (((1,), (0,)), ((), ()))
CHUNK = 256


class Place:
    def __init__(self, span):
        index = lax.axis_index("fsdp")
        shard = lax.axis_index("tp")
        self.span = span
        self.j = index % span
        block = index // span
        self.z = block // 2
        self.y = block % 2
        self.x = shard // 2
        self.k = shard % 2

    def shifted(self, dx=0, dy=0, dz=0, dk=0):
        x = 1 - self.x if dx else self.x
        y = 1 - self.y if dy else self.y
        z = (self.z + dz) % 4 if dz else self.z
        k = 1 - self.k if dk else self.k
        return x, y, z, k

    def device(self, dx=0, dy=0, dz=0, dk=0):
        x, y, z, k = self.shifted(dx, dy, dz, dk)
        return ((z * 2 + y) * self.span + self.j, x * 2 + k)

    def greet(self, offsets):
        barrier = pltpu.get_barrier_semaphore()
        for offset in offsets:
            pl.semaphore_signal(
                barrier, inc=1, device_id=self.device(**offset), device_id_type=MESH
            )
        pl.semaphore_wait(barrier, len(offsets))


ALL_PEERS = ({"dx": 1}, {"dy": 1}, {"dz": 1}, {"dz": 2}, {"dz": 3}, {"dk": 1})


def remote(src, dst, send, recv, device):
    return pltpu.make_async_remote_copy(
        src_ref=src, dst_ref=dst, send_sem=send, recv_sem=recv, device_id=device, device_id_type=MESH
    )


PARTS = {
    "a": pl.ds(0, 32),
    "c": pl.ds(32, 16),
    "ac": pl.ds(0, 48),
    "b": pl.ds(48, 32),
    "d": pl.ds(80, 16),
    "bd": pl.ds(48, 48),
    "": pl.ds(0, 96),
}


def dot(a, b, dims=NN):
    return lax.dot_general(a, b, dims, preferred_element_type=jnp.float32)


class Copies:
    names = ()

    def start(self, *names):
        for name in names:
            self.copy(name).start()

    def wait(self, *names):
        for name in names:
            self.copy(name).wait_recv()

    def finish(self):
        for name in self.names:
            self.copy(name).wait_send()


class GatherRound(Copies):
    names = ("z1", "z2", "z3", "ax", "by", "ay0", "bx0", "ay1", "bx1") + tuple(
        "d%d" % i for i in range(7)
    )
    names += ("cx", "cz1", "cz2", "cz3", "dy", "dz1", "dz2", "dz3")
    lines = {
        "ax": ((0, 0, "a"), {"dx": 1}),
        "by": ((0, 0, "b"), {"dy": 1}),
        "ay0": ((0, 0, "ac"), {"dy": 1}),
        "bx0": ((0, 0, "bd"), {"dx": 1}),
        "ay1": ((1, 0, "ac"), {"dy": 1}),
        "bx1": ((0, 1, "bd"), {"dx": 1}),
        "d0": ((0, 0, ""), {"dk": 1}),
        "d1": ((1, 0, "ac"), {"dk": 1}),
        "d2": ((0, 1, "bd"), {"dk": 1}),
        "d3": ((0, 1, "ac"), {"dk": 1}),
        "d4": ((1, 0, "bd"), {"dk": 1}),
        "d5": ((1, 1, "ac"), {"dk": 1}),
        "d6": ((1, 1, "bd"), {"dk": 1}),
    }
    steps = {
        3: (("ax", "cz1", "cz2", "cz3"), ("ay1", "d1")),
        4: (("by", "dz1", "dz2", "dz3"), ("bx1", "d2")),
        5: (("ay0",), ("d3",)),
        6: (("bx0",), ("d4",)),
        7: (("ay1",), ("d5",)),
        8: (("bx1",), ("d6",)),
    }
    last = 10

    def __init__(self, place, own, out, send, recv, keep):
        self.place, self.own, self.out = place, own, out
        self.send, self.recv, self.keep = send, recv, keep

    def line(self, dx, dy, part):
        x, y, z, k = self.place.shifted(dx, dy)
        return self.out.at[x, k, :, y, PARTS[part], :]

    def copy(self, name):
        place = self.place
        at = self.names.index(name)
        send, recv = self.send.at[at], self.recv.at[at]
        x, y, z, k = place.shifted()
        if name[0] == "z":
            return remote(
                self.own, self.out.at[x, k, z, y], send, recv, place.device(dz=int(name[1]))
            )
        if name in ("cx", "dy"):
            rows = PARTS[name[0]]
            return remote(
                self.own.at[rows, :],
                self.out.at[x, k, z, y, rows, :],
                send,
                recv,
                place.device(**{"d" + name[1]: 1}),
            )
        if name[:2] in ("cz", "dz"):
            x, y, z, k = place.shifted(dx=1) if name[0] == "c" else place.shifted(dy=1)
            ref = self.out.at[x, k, z, y, PARTS[name[0]], :]
            return remote(ref, ref, send, recv, place.device(dz=int(name[2])))
        where, to = self.lines[name]
        ref = self.line(*where)
        return remote(ref, ref, send, recv, place.device(**to))

    def kept(self):
        x, y, z, k = self.place.shifted()
        return pltpu.make_async_copy(self.own, self.out.at[x, k, z, y], self.keep)

    def event(self, n):
        if n == 0:
            self.kept().start()
            self.start("cx", "dy", "z1", "z2", "z3")
        elif n == 1:
            self.wait("cx", "dy")
            self.start("cz1", "cz2", "cz3", "dz1", "dz2", "dz3")
        elif n == 2:
            self.kept().wait()
            self.wait("z1", "z2", "z3")
            self.start("ax", "by", "ay0", "bx0", "d0")
        elif n == 9:
            self.wait("d0", "d2", "d3")
        elif n == 10:
            self.wait("d1", "d4", "d5", "d6")
        else:
            self.wait(*self.steps[n][0])
            self.start(*self.steps[n][1])


class NormGather(Copies):
    names = ("z1", "z2", "z3", "y")

    def __init__(self, place, own, out, send, recv, keep):
        self.place, self.own, self.out = place, own, out
        self.send, self.recv, self.keep = send, recv, keep

    def copy(self, name):
        place = self.place
        at = self.names.index(name)
        send, recv = self.send.at[at], self.recv.at[at]
        if name == "y":
            ref = self.out.at[:, place.y]
            return remote(ref, ref, send, recv, place.device(dy=1))
        return remote(
            self.own, self.out.at[place.z, place.y], send, recv, place.device(dz=int(name[1]))
        )

    def kept(self):
        return pltpu.make_async_copy(self.own, self.out.at[self.place.z, self.place.y], self.keep)


class Events:
    def __init__(self, steps):
        self.steps = list(steps)

    def run(self, count):
        for step in self.steps[:count]:
            step()
        del self.steps[:count]

    def spread(self, trips, points, count):
        total = trips * points
        return self.place(trips, points, {n * total // max(count, 1): 1 for n in range(count)})

    def place(self, trips, points, counts):
        total = trips * points
        slots = [[] for _ in range(total)]
        for number in sorted(counts):
            slots[number] += self.steps[: counts[number]]
            del self.steps[: counts[number]]

        def stop(i, point):
            for trip in range(trips):
                todo = slots[trip * points + point]
                if todo:

                    @pl.when(i == trip)
                    def _():
                        for step in todo:
                            step()

        return stop


def lane_half(tile, half):
    lane = lax.broadcasted_iota(jnp.int32, tile.shape, 1)
    keep = (lane < HEAD_DIM) if half == 0 else (lane >= HEAD_DIM)
    return jnp.where(keep, tile, jnp.zeros_like(tile))


def swap_halves(tile):
    return pltpu.roll(tile.astype(jnp.float32), HEAD_DIM, 1)


def fill_distance(dist, segments, place):
    row = segments[pl.ds(place.x, 1), :].astype(jnp.float32)
    column = jnp.broadcast_to(row, (8, 1024)).T[:, 0:1]
    for s in range(2):
        first = (2 * s + place.k) * 256
        mine = segments[pl.ds(place.x, 1), pl.ds(pl.multiple_of(first, 256), 256)].astype(jnp.float32)
        gap = lax.broadcasted_iota(jnp.int32, (1024, 256), 0) - (
            lax.broadcasted_iota(jnp.int32, (1024, 256), 1) + first
        )
        dist[:, s * 256 : (s + 1) * 256] = jnp.where(
            column == mine, jnp.abs(gap).astype(jnp.float32), 1e30
        )


def pack_attention(raw, shard):
    qkv, w_out = raw[0], raw[1]
    turned = w_out[...].astype(jnp.float32).T
    for c in range(3):
        tiles = (
            qkv[c, :, 0:128],
            jnp.concatenate(
                [
                    qkv[c, :, 128:192].astype(jnp.float32),
                    turned[:, c * HEAD_DIM : (c + 1) * HEAD_DIM],
                ],
                axis=1,
            ).astype(jnp.bfloat16),
        )
        for i in range(2):
            half, at = divmod(2 * c + i, 3)
            shard[half, :, at * 128 : at * 128 + 128] = tiles[i]


def pack_feed(raw, shard):
    w_in, w_down = raw[2:]
    turned = w_down[...].astype(jnp.float32).T.astype(jnp.bfloat16)
    for r in range(3):
        units = slice(r * 256, (r + 1) * 256)
        first = slice(r * 256, r * 256 + 128)
        second = slice(r * 256 + 128, r * 256 + 256)
        shard[2 + 2 * r, :, 0:256] = w_in[:, 0, units]
        shard[2 + 2 * r, :, 256:384] = w_in[:, 1, first]
        shard[3 + 2 * r, :, 0:128] = w_in[:, 1, second]
        shard[3 + 2 * r, :, 128:384] = turned[:, units]


def out_weights(w):
    first = lax.broadcasted_iota(jnp.int32, (768, 128), 1) < HEAD_DIM
    left = jnp.where(first, swap_halves(w[:, 128:256]), w[:, 384:512].astype(jnp.float32))
    right = jnp.where(first, swap_halves(w[:, 640:768]), 0.0)
    return left.astype(jnp.bfloat16), right.astype(jnp.bfloat16)


def whole(ref):
    return jnp.concatenate([ref[i].reshape(768, 384) for i in range(2)], axis=1)


HEAD_SPOTS = ((0, 0), (0, 1), (1, 0))


def norm_stats(value):
    average = jnp.mean(value, axis=-1, keepdims=True)
    centered = value - average
    inv_std = lax.rsqrt(jnp.mean(centered * centered, axis=-1, keepdims=True) + norm_eps)
    return centered * inv_std, inv_std


def norm_backward(grad_val, normed, inv_std, gain_row):
    grad_norm = grad_val * gain_row
    return inv_std * (
        grad_norm
        - jnp.mean(grad_norm, axis=-1, keepdims=True)
        - normed * jnp.mean(grad_norm * normed, axis=-1, keepdims=True)
    )


ROWS = 128


def row_blocks(body):
    def step(i, carry):
        body(pl.ds(pl.multiple_of(i * ROWS, ROWS), ROWS), i)
        return carry

    lax.fori_loop(0, 512 // ROWS, step, 0)


def columns(value):
    return jnp.sum(value.reshape(value.shape[0] // 8, 8, value.shape[1]), axis=0)


def forward_kernel(
    span,
    slopes,
    raw,
    gains,
    biases,
    tok,
    cot,
    segments,
    o_weights,
    o_norms,
    o_x,
    o_cot,
    o_q,
    o_k,
    o_v,
    o_ctx,
    o_lse,
    o_kept,
    o_n1,
    o_i1,
    o_n2,
    o_i2,
    o_out,
    o_squares,
    o_h1_t,
    o_x_t,
    o_dist,
    o_wo,
    shard,
    norm_rows,
    weights,
    norms,
    xs,
    q,
    keys,
    values,
    ctx,
    h1b,
    n1,
    h1_t,
    x_t,
    wo,
    dist,
    out_t,
    acc,
    h1,
    kept,
    g_send,
    g_recv,
    g_keep,
    n_send,
    n_recv,
    n_keep,
    t_sems,
    kv_send,
    kv_recv,
    store_sems,
    kept_sems,
):
    f32, bf16 = jnp.float32, jnp.bfloat16
    place = Place(span)
    x, y, z, k = place.shifted()
    rounds = [
        GatherRound(place, shard.at[r], weights.at[r], g_send.at[r], g_recv.at[r], g_keep.at[r])
        for r in range(2 * ROUNDS)
    ]
    norm_gather = NormGather(place, norm_rows, norms, n_send, n_recv, n_keep)

    def swap(n):
        src, dst = ((tok, xs), (cot, o_cot))[n]
        return remote(
            src.at[1 - place.x],
            dst.at[place.x],
            t_sems.at[3 * n],
            t_sems.at[3 * n + 1],
            place.device(dx=1),
        )

    def stay(n):
        src, dst = ((tok, xs), (cot, o_cot))[n]
        return pltpu.make_async_copy(src.at[place.x], dst.at[place.x], t_sems.at[3 * n + 2])

    def store(n):
        src, dst = (
            (weights.at[0:2], o_weights.at[0:2]),
            (weights.at[2:4], o_weights.at[2:4]),
            (weights.at[4:6], o_weights.at[4:6]),
            (weights.at[6:8], o_weights.at[6:8]),
            (xs, o_x),
            (keys, o_k),
            (values, o_v),
            (q, o_q),
            (ctx, o_ctx),
            (n1, o_n1),
            (h1_t, o_h1_t),
            (x_t, o_x_t),
            (dist, o_dist),
            (wo, o_wo),
        )[n]
        return pltpu.make_async_copy(src, dst, store_sems.at[n])

    if len(raw) > 1:
        pack_attention(raw, shard)
    else:
        shard[...] = raw[0][...]
    place.greet(ALL_PEERS)
    rounds[0].event(0)
    swap(0).start()
    for n in range(2):
        stay(n).start()
    norm_rows[...] = jnp.zeros_like(norm_rows)
    norm_rows[0:2, 0:96] = gains[...].astype(f32)
    norm_rows[2:4, 0:96] = biases[...].astype(f32)
    block = place.z * 2 + place.y
    norm_rows[...] = pltpu.roll(norm_rows[...], block * 96, 1)
    norm_gather.kept().start()
    norm_gather.start("z1", "z2", "z3")
    if len(raw) > 1:
        pack_feed(raw, shard)

    def step(r, n):
        def go():
            rounds[r].event(n)
            if n == GatherRound.last and r % 2:
                store(r // 2).start()

        return go

    stages = {0: 0, 1: 1, 2: 1, 3: 2, 4: 2, 5: 3, 6: 3, 7: 3, 8: 3, 9: 4, 10: 4}
    order = sorted((r + stages[n], r, n) for r in range(2 * ROUNDS) for n in range(11))
    order = [(r, n) for _, r, n in order][1:]
    order = order[: order.index((7, 4)) + 1]
    order += [(7, 5), (6, 9), (7, 9), (7, 6), (7, 7), (7, 8), (6, 10), (7, 10)]
    begun = order.index((1, 10)) + 1
    beside_heads = order.index((3, 10)) + 1 - begun
    events = Events(step(*at) for at in order)
    events.steps.insert(order.index((7, 4)) + 1, lambda: swap(1).start())

    events.run(1)
    fill_distance(dist, segments, place)
    norm_gather.kept().wait()
    norm_gather.wait("z1", "z2", "z3")
    norm_gather.start("y")
    events.run(begun - 1)
    swap(0).wait_recv()
    stay(0).wait()
    store(4).start()
    for i in range(512 // ROWS):
        rows = pl.ds((i % 2) * ROWS, ROWS)
        x_t[:, i * ROWS : (i + 1) * ROWS] = xs[i // 2, rows, :].astype(f32).T.astype(bf16)
    store(11).start()
    store(12).start()

    def share(t, n):
        ref = (keys, values)[n].at[pl.ds(2 * t, 2), :, place.k]
        return remote(ref, ref, kv_send.at[t, n], kv_recv.at[t, n], place.device(dk=1))

    def project(t, carry):
        w = whole(weights.at[0:2, t // 2, t % 2])
        for s in range(2):
            out = dot(xs[s], w).astype(bf16)
            for i in range(2):
                cols = slice(i * 128, i * 128 + 128)
                q[2 * t + i, pl.ds(s * 256, 256), :] = out[:, cols] * bf16(HEAD_DIM**-0.5)
                keys[2 * t + i, s, k] = out[:, 256 + i * 128 : 384 + i * 128]
                values[2 * t + i, s, k] = out[:, 512 + i * 128 : 640 + i * 128]
        share(t, 0).start()
        share(t, 1).start()
        return carry

    lax.fori_loop(0, 4, project, 0)
    out_t[1, pl.ds(HEAD_DIM, HEAD_DIM), :] = jnp.zeros((HEAD_DIM, 512), f32)
    stop = events.spread(4, 7, beside_heads)

    def attend(t, carry):
        share(t, 0).wait_recv()
        share(t, 1).wait_recv()
        point = 0
        for spot, (tile, half) in enumerate(HEAD_SPOTS):
            slope = slopes[3 * t + spot]
            key = keys[2 * t + tile].reshape(1024, 128)
            rows = slice(half * HEAD_DIM, (half + 1) * HEAD_DIM)
            value_t = values[2 * t + tile].reshape(1024, 128).astype(f32).T.astype(bf16)[rows]
            for start in range(0, 512, CHUNK):
                cols = pl.ds(start, CHUNK)
                part = lane_half(q[2 * t + tile, cols, :], half)
                scores = dot(key, part, NT) - slope * dist[:, cols]
                peak = jnp.max(scores, axis=0, keepdims=True)
                expo = jnp.exp(scores - peak)
                total = jnp.sum(expo, axis=0, keepdims=True)
                out_t[tile, rows, cols] = dot(value_t, expo.astype(bf16)) / total
                o_lse[t, pl.ds(spot, 1), cols] = peak + jnp.log(total)
                stop(t, point)
                point += 1
        for tile in range(2):
            ctx[2 * t + tile] = out_t[tile].T.astype(bf16)
        left, right = out_weights(whole(weights.at[0:2, t // 2, t % 2]))
        wo[t, 0] = left
        wo[t, 1] = right
        mixed = dot(ctx[2 * t], left, NT) + dot(ctx[2 * t + 1], right, NT)

        @pl.when(t == 0)
        def _():
            acc[...] = mixed

        @pl.when(t > 0)
        def _():
            acc[...] += mixed

        stop(t, point)
        return carry

    lax.fori_loop(0, 4, attend, 0)
    for n in (5, 6, 7, 8, 13):
        store(n).start()
    norm_gather.wait("y")
    norm_sum = jnp.sum(norms[...].reshape(8, 8, 768), axis=0)
    o_norms[...] = norm_sum

    def first_norm(rows, i):
        attn = acc[rows, :]
        half = i // 2
        resid = xs[half, pl.ds(pl.multiple_of((i % 2) * ROWS, ROWS), ROWS), :].astype(f32) + attn
        normed, inv = norm_stats(resid)
        value = normed * norm_sum[0:1] + norm_sum[2:3]
        h1[rows, :] = value
        h1b[rows, :] = value.astype(bf16)
        h1_t[:, rows] = value.T.astype(bf16)
        n1[rows, :] = normed
        o_i1[rows, :] = inv
        acc[rows, :] = jnp.zeros_like(attn)
        if_first = jnp.where(i == 0, 0.0, 1.0)
        o_squares[0] = o_squares[0] * if_first + columns(attn * attn)
        o_squares[1] = o_squares[1] * if_first + columns(resid * resid)

    o_squares[...] = jnp.zeros_like(o_squares)
    row_blocks(first_norm)
    store(9).start()
    store(10).start()

    first_part = order.index((5, 10)) - begun - beside_heads
    middle = len(order) - 7 - order.index((5, 10)) - 1
    counts = {}
    for n in range(first_part):
        at = n * 8 // first_part
        counts[at] = counts.get(at, 0) + 1
    counts[8] = 1
    for n in range(middle):
        at = 9 + n * 6 // middle
        counts[at] = counts.get(at, 0) + 1
    counts[16] = 1
    counts[18] = counts[22] = 2
    counts[20] = 3
    stop_f = events.place(12, 2, counts)
    assert not events.steps

    def keep_copy(n):
        at = n // 4 * 4 + (x ^ (n % 4 // 2)) * 2 + (k ^ (n % 2))
        return pltpu.make_async_copy(kept.at[n % 2], o_kept.at[at], kept_sems.at[n % 2])

    def feed(n, carry):
        r = 1 + n // 4
        wx, wk = x ^ (n % 4 // 2), k ^ (n % 2)
        stop_f(n, 0)

        @pl.when(n >= 2)
        def _():
            keep_copy(n - 2).wait()

        ref = weights.at[pl.ds(2 * r, 2), wx, wk]
        for start in range(0, 512, CHUNK):
            rows = pl.ds(start, CHUNK)
            w = whole(ref)
            projected = dot(h1b[rows, :], w[:, :512])
            gate, up = projected[:, :256], projected[:, 256:]
            cdf = 0.5 + 0.5 * lax.erf(gate * (0.5**0.5))
            pdf = jnp.exp(-0.5 * gate * gate) * 0.3989422804014327
            act = gate * cdf
            hidden = (act * up).astype(bf16)
            kept[n % 2, 0, rows, :] = hidden
            kept[n % 2, 1, rows, :] = act.astype(bf16)
            kept[n % 2, 2, rows, :] = ((cdf + gate * pdf) * up).astype(bf16)
            acc[rows, :] += dot(hidden, w[:, 512:], NT)
        keep_copy(n).start()
        stop_f(n, 1)
        return carry

    lax.fori_loop(0, 12, feed, 0)

    def second_norm(rows, i):
        ffn = acc[rows, :]
        resid = h1[rows, :] + ffn
        normed, inv = norm_stats(resid)
        o_out[rows, :] = (normed * norm_sum[1:2] + norm_sum[3:4]).astype(bf16)
        o_n2[rows, :] = normed
        o_i2[rows, :] = inv
        o_squares[2] += columns(ffn * ffn)
        o_squares[3] += columns(resid * resid)

    row_blocks(second_norm)
    for n in (10, 11):
        keep_copy(n).wait()
    for r in rounds:
        r.finish()
    norm_gather.finish()
    for n in range(2):
        swap(n).wait_send()
    swap(1).wait_recv()
    stay(1).wait()
    for t in range(4):
        for n in range(2):
            share(t, n).wait_send()
    for n in range(14):
        store(n).wait()


def forward_refs(span, count, *refs):
    forward_kernel(span, refs[0], refs[1 : 1 + count], *refs[1 + count :])


def forward(span, slopes, raw, gains, biases, tok, cot, segments):
    f32, bf16 = jnp.float32, jnp.bfloat16
    any_space = pl.BlockSpec(memory_space=pl.ANY)
    vmem = pl.BlockSpec(memory_space=pltpu.VMEM)
    outs = (
        ((2 * ROUNDS, 2, 2, 4, 2, 96, 384), bf16, any_space),
        ((8, 768), f32, vmem),
        ((2, 256, 768), bf16, any_space),
        ((2, 256, 768), bf16, any_space),
        ((8, 512, 128), bf16, any_space),
        ((8, 2, 2, 256, 128), bf16, any_space),
        ((8, 2, 2, 256, 128), bf16, any_space),
        ((8, 512, 128), bf16, any_space),
        ((4, 8, 512), f32, vmem),
        ((12, 3, 512, 256), bf16, any_space),
        ((512, 768), f32, any_space),
        ((512, 1), f32, vmem),
        ((512, 768), f32, vmem),
        ((512, 1), f32, vmem),
        ((512, 768), bf16, vmem),
        ((4, 8, 768), f32, vmem),
        ((768, 512), bf16, any_space),
        ((768, 512), bf16, any_space),
        ((1024, 512), f32, any_space),
        ((4, 2, 768, 128), bf16, any_space),
    )
    dma = pltpu.SemaphoreType.DMA
    copies = len(GatherRound.names)
    return pl.pallas_call(
        partial(forward_refs, span, len(raw)),
        out_shape=tuple(jax.ShapeDtypeStruct(s, d) for s, d, _ in outs),
        in_specs=[pl.BlockSpec(memory_space=pltpu.SMEM)]
        + [vmem] * (len(raw) + 2)
        + [any_space, any_space, vmem],
        out_specs=tuple(spec for _, _, spec in outs),
        scratch_shapes=[
            pltpu.VMEM((2 * ROUNDS, 96, 384), bf16),
            pltpu.VMEM((8, 768), f32),
            pltpu.VMEM((2 * ROUNDS, 2, 2, 4, 2, 96, 384), bf16),
            pltpu.VMEM((4, 2, 8, 768), f32),
            pltpu.VMEM((2, 256, 768), bf16),
            pltpu.VMEM((8, 512, 128), bf16),
            pltpu.VMEM((8, 2, 2, 256, 128), bf16),
            pltpu.VMEM((8, 2, 2, 256, 128), bf16),
            pltpu.VMEM((8, 512, 128), bf16),
            pltpu.VMEM((512, 768), bf16),
            pltpu.VMEM((512, 768), f32),
            pltpu.VMEM((768, 512), bf16),
            pltpu.VMEM((768, 512), bf16),
            pltpu.VMEM((4, 2, 768, 128), bf16),
            pltpu.VMEM((1024, 512), f32),
            pltpu.VMEM((2, 128, 512), f32),
            pltpu.VMEM((512, 768), f32),
            pltpu.VMEM((512, 768), f32),
            pltpu.VMEM((2, 3, 512, 256), bf16),
            dma((2 * ROUNDS, copies)),
            dma((2 * ROUNDS, copies)),
            dma((2 * ROUNDS,)),
            dma((4,)),
            dma((4,)),
            dma,
            dma((6,)),
            dma((4, 2)),
            dma((4, 2)),
            dma((14,)),
            dma((2,)),
        ],
        compiler_params=pltpu.CompilerParams(
            collective_id=0, has_side_effects=True, vmem_limit_bytes=VMEM_LIMIT
        ),
        name="forward",
    )(slopes, *raw, gains, biases, tok, cot, segments)


class ScatterRound(Copies):
    names = ("ay1", "bx", "ay0", "ax", "by", "cx", "dy") + tuple(
        part + "z%d" % step for part in "abcd" for step in (1, 2, 3)
    )

    def __init__(self, place, held, twin, stage, landing, send, recv, pair):
        self.place, self.held, self.twin, self.stage = place, held, twin, stage
        self.ay, self.bx, self.ax, self.by, self.z, self.cz, self.dz, self.last = landing
        self.send, self.recv, self.pair = send, recv, pair

    def copy(self, name):
        p, held = self.place, self.held
        at = self.names.index(name)
        a, b, c, d = (PARTS[part] for part in "abcd")
        step = int(name[2]) if name[1] == "z" else 0
        far = (p.z + step) % 4
        ac, bd = PARTS["ac"], PARTS["bd"]
        if name in ("ay1", "ay0"):
            dx = int(name[2])
            src, dst, to = held.at[dx, :, 1 - p.y, ac, :], self.ay.at[dx], {"dy": 1}
        elif name == "bx":
            src, dst, to = held.at[1, :, :, bd, :], self.bx, {"dx": 1}
        elif name == "ax":
            src, dst, to = held.at[1, :, p.y, a, :], self.ax, {"dx": 1}
        elif name == "by":
            src, dst, to = held.at[0, :, 1 - p.y, b, :], self.by, {"dy": 1}
        elif name == "cx":
            src, dst, to = held.at[1, p.z, p.y, c, :], self.last.at[0], {"dx": 1}
        elif name == "dy":
            src, dst, to = held.at[0, p.z, 1 - p.y, d, :], self.last.at[1], {"dy": 1}
        elif name[0] == "c":
            src, dst, to = held.at[:, far, p.y, c, :], self.cz.at[step - 1], {"dz": step}
        elif name[0] == "d":
            src, dst, to = held.at[0, far, :, d, :], self.dz.at[step - 1], {"dz": step}
        else:
            rows = PARTS[name[0]]
            into = pl.ds(0, 32) if name[0] == "a" else pl.ds(32, 32)
            src, dst, to = held.at[0, far, p.y, rows, :], self.z.at[step - 1, into, :], {"dz": step}
        return remote(src, dst, self.send.at[at], self.recv.at[at], p.device(**to))

    def push(self, dx):
        return remote(
            self.stage.at[dx], self.twin.at[dx], self.pair.at[0, dx], self.pair.at[1, dx], self.place.device(dk=1)
        )

    def add(self, ref, *others):
        total = ref[...].astype(jnp.float32)
        for other in others:
            total = total + other[...].astype(jnp.float32)
        ref[...] = total.astype(jnp.bfloat16)

    def pair_sum(self, dx):
        self.push(dx).wait_recv()

        def body(i, carry):
            self.add(self.held.at[dx, i], self.twin.at[dx, i])
            return carry

        lax.fori_loop(0, 4, body, 0)
        if dx:
            self.start("bx", "ay1")
        else:
            self.start("ay0")

    def event(self, n, out=None):
        p, held = self.place, self.held
        a, b, c, d = (PARTS[part] for part in "abcd")
        ac, bd = PARTS["ac"], PARTS["bd"]
        if n == 0:
            self.wait("ay1")
            self.add(held.at[1, :, p.y, ac, :], self.ay.at[1])
            self.start("ax")
        elif n == 1:
            self.wait("bx")
            self.add(held.at[0, :, 1 - p.y, bd, :], self.bx.at[:, 1 - p.y])
            self.start("by")
            self.add(held.at[0, :, p.y, bd, :], self.bx.at[:, p.y])
            self.start("dz1", "dz2", "dz3")
        elif n == 2:
            self.wait("ay0")
            self.add(held.at[0, :, p.y, ac, :], self.ay.at[0])
            self.start("cz1", "cz2", "cz3")
        elif n == 3:
            self.wait("ax")
            self.add(held.at[0, :, p.y, a, :], self.ax)
            self.start("az1", "az2", "az3")
        elif n == 4:
            self.wait("by")
            self.add(held.at[0, :, p.y, b, :], self.by)
            self.start("bz1", "bz2", "bz3")
        elif n == 5:
            self.wait("cz1", "cz2", "cz3", "dz1", "dz2", "dz3")
            self.add(held.at[1, p.z, p.y, c, :], *[self.cz.at[i, 1] for i in range(3)])
            self.start("cx")
            self.add(held.at[0, p.z, 1 - p.y, d, :], *[self.dz.at[i, 1 - p.y] for i in range(3)])
            self.start("dy")
            self.add(held.at[0, p.z, p.y, c, :], *[self.cz.at[i, 0] for i in range(3)])
            self.add(held.at[0, p.z, p.y, d, :], *[self.dz.at[i, p.y] for i in range(3)])
        else:
            self.wait("az1", "az2", "az3", "bz1", "bz2", "bz3", "cx", "dy")
            for rows, others in (
                (a, [self.z.at[i, pl.ds(0, 32), :] for i in range(3)]),
                (b, [self.z.at[i, pl.ds(32, 32), :] for i in range(3)]),
                (c, [self.last.at[0]]),
                (d, [self.last.at[1]]),
            ):
                total = held[0, p.z, p.y, rows, :].astype(jnp.float32)
                for other in others:
                    total = total + other[...].astype(jnp.float32)
                out[rows, :] = total


def backward_kernel(
    span,
    slopes,
    i_weights,
    norms,
    i_cot,
    i_q,
    i_k,
    i_v,
    i_ctx,
    i_lse,
    i_kept,
    i_n1,
    i_i1,
    i_n2,
    i_i2,
    i_out,
    squares,
    i_h1_t,
    i_x_t,
    i_dist,
    i_wo,
    o_out,
    o_tokens,
    o_grads,
    o_small,
    w_buf,
    wo,
    kept,
    h1_t,
    f_t,
    d_rows,
    n_buf,
    d_h1,
    q,
    keys,
    values,
    ctx,
    lse,
    dist,
    d_ctx,
    d_kv,
    d_kv_in,
    dq_t,
    acc_k,
    acc_v,
    held,
    twin,
    stage,
    land_ay,
    land_bx,
    land_ax,
    land_by,
    land_z,
    land_cz,
    land_dz,
    land_last,
    small,
    small_in,
    load_sems,
    step_sems,
    r_send,
    r_recv,
    r_pair,
    t_sems,
    kv_send,
    kv_recv,
    s_send,
    s_recv,
):
    f32, bf16 = jnp.float32, jnp.bfloat16
    place = Place(span)
    x, y, z, k = place.shifted()
    rounds = [
        ScatterRound(
            place,
            held.at[n],
            twin.at[n % 6],
            stage.at[n % 2],
            [
                ref.at[n]
                for ref in (land_ay, land_bx, land_ax, land_by, land_z, land_cz, land_dz, land_last)
            ],
            r_send.at[n],
            r_recv.at[n],
            r_pair.at[n],
        )
        for n in range(2 * ROUNDS)
    ]

    def load(n):
        src, dst = (
            (i_cot, d_rows.at[1]),
            (i_n2, n_buf),
            (i_h1_t, h1_t),
            (i_x_t, h1_t),
            (i_q, q),
            (i_k, keys),
            (i_v, values),
            (i_ctx, ctx),
            (i_lse, lse),
            (i_n1, n_buf),
            (i_dist, dist),
        )[n]
        return pltpu.make_async_copy(src, dst, load_sems.at[n])

    def where(n):
        return x ^ (1 - n // 2), k ^ (1 - n % 2)

    def where_heads(n):
        return x ^ (1 - n // 2), n % 2

    def fetch(n, part):
        r = 3 - n // 4
        wx, wk = where(n % 4)
        if part == 0:
            return pltpu.make_async_copy(i_weights.at[pl.ds(2 * r, 2), wx, wk], w_buf.at[n % 2], step_sems.at[n % 2, 0])
        return pltpu.make_async_copy(
            i_kept.at[(r - 1) * 4 + wx * 2 + wk], kept.at[n % 2], step_sems.at[n % 2, 1]
        )

    for n in (0, 1):
        load(n).start()
    fetch(0, 0).start()
    fetch(0, 1).start()
    for n in (2, 4, 5, 6, 7, 8, 10):
        load(n).start()
    place.greet(ALL_PEERS)

    def swap(n):
        src, dst = ((i_out, o_out), (d_rows.at[0], o_tokens))[n]
        return remote(
            src.at[1 - place.x],
            dst.at[place.x],
            t_sems.at[3 * n],
            t_sems.at[3 * n + 1],
            place.device(dx=1),
        )

    def stay(n):
        src, dst = ((i_out, o_out), (d_rows.at[0], o_tokens))[n]
        return pltpu.make_async_copy(src.at[place.x], dst.at[place.x], t_sems.at[3 * n + 2])

    swap(0).start()
    stay(0).start()
    load(0).wait()
    load(1).wait()
    small[...] = jnp.zeros_like(small)

    def halves(ref, i):
        return ref.at[i // 2, pl.ds(pl.multiple_of((i % 2) * ROWS, ROWS), ROWS), :]

    sums = [jnp.zeros((8, 768), f32)] * 2
    for i in range(512 // ROWS):
        rows = pl.ds(i * ROWS, ROWS)
        grad = halves(d_rows.at[1], i)[...].astype(f32)
        normed = n_buf[rows, :]
        out = norm_backward(grad, normed, i_i2[rows, :], norms[1:2])
        d_h1[rows, :] = out
        halves(d_rows.at[0], i)[...] = out.astype(bf16)
        f_t[:, rows] = out.T.astype(bf16)
        sums[0] = sums[0] + columns(grad * normed)
        sums[1] = sums[1] + columns(grad)
    small[1] = sums[0]
    small[3] = sums[1]
    load(9).start()
    load(2).wait()

    def pair(n, dx):
        return lambda: rounds[n].pair_sum(dx)

    def step(n, at):
        chunk = 3 - n // 2
        return lambda: rounds[n].event(at, o_grads.at[2 * chunk + n % 2])

    def put(n, dx, theirs, value, start):
        block = value.astype(bf16).reshape(4, 2, 96, value.shape[-1])
        stop_at = start + value.shape[-1]

        def store(ref_of):
            for half in range(2):
                low, high = max(start, 384 * half), min(stop_at, 384 * half + 384)
                if low < high:
                    ref_of(half)[:, :, :, low - 384 * half : high - 384 * half] = block[
                        :, :, :, low - start : high - start
                    ]

        @pl.when(theirs)
        def _():
            store(lambda half: stage.at[half, dx])

        @pl.when(jnp.logical_not(theirs))
        def _():
            store(lambda half: held.at[2 * n + half, dx])

    def pushes(n, dx):
        return [
            remote(
                stage.at[half, dx],
                twin.at[(2 * n + half) % 6, dx],
                r_pair.at[2 * n + half, 0, dx],
                r_pair.at[2 * n + half, 1, dx],
                place.device(dk=1),
            )
            for half in range(2)
        ]

    def push(n, dx):
        for copy in pushes(n, dx):
            copy.start()

    def pushed(n, dx):
        for copy in pushes(n, dx):
            copy.wait_send()

    plan = {
        1: [pair(0, 1), pair(1, 1)],
        3: [pair(0, 0), pair(1, 0)],
        5: [step(0, 0), step(1, 0), pair(2, 1), pair(3, 1)],
        6: [step(0, 1), step(0, 2), step(1, 2)],
        7: [pair(2, 0), pair(3, 0), step(1, 1)],
        8: [step(0, 3), step(1, 3)],
        9: [step(0, 5), step(2, 0), step(3, 0), pair(4, 1), pair(5, 1)],
        10: [step(0, 4), step(2, 2), step(3, 2), step(2, 1)],
        11: [step(1, 4), step(1, 5), pair(4, 0), pair(5, 0)],
    }

    def feed(n, carry):
        dx = 1 - n % 4 // 2
        theirs = n % 2 == 0

        @pl.when(n < 11)
        def _():
            fetch(n + 1, 0).start()
            fetch(n + 1, 1).start()

        @pl.when(jnp.logical_and(theirs, n >= 4))
        def _():
            pushed(n // 4 - 1, dx)

        fetch(n, 0).wait()
        fetch(n, 1).wait()
        w = whole(w_buf.at[n % 2])
        hold = kept.at[n % 2]
        d_ffn = d_rows[0].reshape(512, 768)
        put(n // 4, dx, theirs, dot(f_t[...], hold[0]), 512)
        d_hidden = dot(d_ffn, w[:, 512:])
        d_gate = (d_hidden * hold[2].astype(f32)).astype(bf16)
        d_up = (d_hidden * hold[1].astype(f32)).astype(bf16)
        put(n // 4, dx, theirs, dot(h1_t[...], d_gate), 0)
        put(n // 4, dx, theirs, dot(h1_t[...], d_up), 256)

        @pl.when(theirs)
        def _():
            push(n // 4, dx)

        d_h1[...] += dot(d_gate, w[:, :256], NT) + dot(d_up, w[:, 256:512], NT)
        for at, todo in plan.items():

            @pl.when(n == at)
            def _():
                for item in todo:
                    item()

        return carry

    lax.fori_loop(0, 12, feed, 0)
    load(9).wait()
    load(3).start()
    sums = [jnp.zeros((8, 768), f32)] * 2
    for i in range(512 // ROWS):
        rows = pl.ds(i * ROWS, ROWS)
        grad = d_h1[rows, :]
        normed = n_buf[rows, :]
        out = norm_backward(grad, normed, i_i1[rows, :], norms[0:1])
        d_h1[rows, :] = out
        halves(d_rows.at[1], i)[...] = out.astype(bf16)
        f_t[:, rows] = out.T.astype(bf16)
        sums[0] = sums[0] + columns(grad * normed)
        sums[1] = sums[1] + columns(grad)
    small[0] = sums[0]
    small[2] = sums[1]
    for n in (3, 4, 5, 6, 7, 8, 10):
        load(n).wait()

    small[0] = jnp.concatenate(
        [jnp.sum(small[i], axis=0, keepdims=True) for i in range(4)]
        + [jnp.sum(squares[i], axis=0, keepdims=True) for i in range(4)],
        axis=0,
    )

    def spread(n):
        to = ({"dk": 1}, {"dx": 1}, {"dy": 1}, {"dz": 1}, {"dz": 2}, {"dz": 3})[n]
        return remote(
            small.at[min(n, 3)], small_in.at[n], s_send.at[n], s_recv.at[n], place.device(**to)
        )

    def small_step(n):
        def go():
            if 0 < n < 4:
                spread(n - 1).wait_recv()
                small[n] = small[n - 1] + small_in[n - 1]
            if n < 3:
                spread(n).start()
            if n == 3:
                for at in (3, 4, 5):
                    spread(at).start()
            if n == 4:
                for at in (3, 4, 5):
                    spread(at).wait_recv()
                total = small[3]
                result = jnp.zeros_like(total)
                for at in range(4):
                    back = (place.z - at) % 4
                    term = jnp.where(
                        back == 0,
                        total,
                        jnp.where(
                            back == 1, small_in[3], jnp.where(back == 2, small_in[4], small_in[5])
                        ),
                    )
                    result = result + term
                o_small[...] = result

        return go

    def fetch_heads(n):
        wx, wk = where_heads(n)
        return pltpu.make_async_copy(i_weights.at[0:2, wx, wk], w_buf.at[n % 2], step_sems.at[n % 2, 0])

    def fetch_wo(n):
        wx, wk = where_heads(n)
        return pltpu.make_async_copy(i_wo.at[wx * 2 + wk], wo.at[n % 2], step_sems.at[n % 2, 1])

    fetch_heads(0).start()
    fetch_wo(0).start()
    dq_t[1, pl.ds(HEAD_DIM, HEAD_DIM), :] = jnp.zeros((HEAD_DIM, 512), f32)

    def share(t):
        return remote(
            d_kv.at[t, :, :, :, 1 - place.k], d_kv_in.at[t], kv_send.at[t], kv_recv.at[t], place.device(dk=1)
        )

    beside = {
        (0, 0): [small_step(0), step(0, 6)],
        (0, 1): [step(3, 1)],
        (0, 2): [small_step(1), step(2, 3)],
        (0, 3): [step(3, 3)],
        (0, 4): [small_step(2), step(4, 0), step(5, 0)],
        (1, 0): [small_step(3), step(1, 6)],
        (1, 1): [step(2, 5)],
        (1, 2): [step(2, 4)],
        (1, 3): [small_step(4), step(4, 2), step(5, 2)],
        (1, 5): [step(4, 1)],
        (2, 0): [step(3, 4), step(3, 5)],
        (2, 1): [step(2, 6)],
        (2, 2): [step(5, 1)],
        (2, 4): [step(4, 3), step(5, 3)],
        (3, 0): [pair(6, 1), pair(7, 1)],
        (3, 1): [step(3, 6)],
        (3, 3): [step(4, 4), step(4, 5)],
        (3, 5): [step(6, 0), step(7, 0)],
        (4, 6): [step(5, 4), step(5, 5)],
    }
    first = lax.broadcasted_iota(jnp.int32, (768, 128), 1) < HEAD_DIM

    def stop(i, point):
        for (trip, at), todo in beside.items():
            if at == point:

                @pl.when(i == trip)
                def _():
                    for item in todo:
                        item()

    def attend(n):
        wx, wk = where_heads(n)
        t = wx * 2 + wk
        fetch_heads(n).wait()
        fetch_wo(n).wait()
        left, right = wo[n % 2, 0], wo[n % 2, 1]
        d_attn = d_rows[1].reshape(512, 768)
        d_ctx[0] = dot(d_attn, left).astype(bf16)
        d_ctx[1] = dot(d_attn, right).astype(bf16)
        point = 0
        for spot, (tile, half) in enumerate(HEAD_SPOTS):
            slope = slopes[3 * t + spot]
            key = keys[2 * t + tile].reshape(1024, 128)
            value = values[2 * t + tile].reshape(1024, 128)
            rows = slice(half * HEAD_DIM, (half + 1) * HEAD_DIM)
            key_t = key.astype(f32).T.astype(bf16)[rows]
            product = ctx[2 * t + tile].astype(f32) * d_ctx[tile].astype(f32)
            delta = jnp.sum(product.T[rows], axis=0, keepdims=True)
            for start in range(0, 512, CHUNK):
                cols = pl.ds(start, CHUNK)
                part = lane_half(q[2 * t + tile, cols, :], half)
                grad = lane_half(d_ctx[tile, cols, :], half)
                scores = dot(key, part, NT) - slope * dist[:, cols]
                probs = jnp.exp(scores - lse[t, pl.ds(spot, 1), cols])
                grad_probs = dot(value, grad, NT)
                term_v = dot(probs.astype(bf16), grad)
                grad_scores = (probs * (grad_probs - delta[:, start : start + CHUNK])).astype(bf16)
                term_k = dot(grad_scores, part)
                if half == 0 and start == 0:
                    acc_v[...] = term_v
                    acc_k[...] = term_k
                else:
                    acc_v[...] += term_v
                    acc_k[...] += term_k
                dq_t[tile, rows, cols] = dot(key_t, grad_scores)
                stop(n, point)
                point += 1
            if half == 1 or tile == 1:
                d_kv[t, 0, tile] = acc_k[...].astype(bf16).reshape(2, 2, 256, 128)
                d_kv[t, 1, tile] = acc_v[...].astype(bf16).reshape(2, 2, 256, 128)
        share(t).start()
        for tile in range(2):
            q[2 * t + tile] = (dq_t[tile].T * HEAD_DIM**-0.5).astype(bf16)

    def project(n):
        wx, wk = where_heads(n)
        t = wx * 2 + wk
        dx = 1 - n // 2
        theirs = wk != k

        @pl.when(theirs)
        def _():
            pushed(2, dx)

        share(t).wait_recv()
        parts = [q[2 * t], q[2 * t + 1]]
        for kind in range(2):
            for tile in range(2):
                mine = d_kv[t, kind, tile, :, k].reshape(512, 128).astype(f32)
                mine = mine + d_kv_in[t, kind, tile].reshape(512, 128).astype(f32)
                parts.append(mine.astype(bf16))
        d_qkv = jnp.concatenate(parts, axis=1)
        d_w = dot(h1_t[...], d_qkv)
        left = dot(f_t[...], ctx[2 * t])
        right = swap_halves(dot(f_t[...], ctx[2 * t + 1]))
        tiles = [
            d_w[:, 0:128],
            jnp.where(first, d_w[:, 128:256], pltpu.roll(left, HEAD_DIM, 1)),
            d_w[:, 256:384],
            jnp.where(first, d_w[:, 384:512], left),
            d_w[:, 512:640],
            jnp.where(first, d_w[:, 640:768], right),
        ]
        put(3, dx, theirs, jnp.concatenate(tiles, axis=1), 0)

        @pl.when(theirs)
        def _():
            push(3, dx)

        d_h1[...] += dot(d_qkv, whole(w_buf.at[n % 2]), NT)

    def heads(n, carry):
        @pl.when(n < 4)
        def _():
            attend(n)

        @pl.when(n > 0)
        def _():
            project(n - 1)

        stop(n, 6)

        @pl.when(n < 3)
        def _():
            fetch_heads(n + 1).start()
            fetch_wo(n + 1).start()

        return carry

    lax.fori_loop(0, 5, heads, 0)
    for i in range(512 // ROWS):
        rows = pl.ds(i * ROWS, ROWS)
        halves(d_rows.at[0], i)[...] = d_h1[rows, :].astype(bf16)
    for n, at in (
        [(6, -1), (7, -1)]
        + [(4, 6), (6, 2), (7, 2), (5, 6), (6, 1), (7, 1), (6, 3), (7, 3)]
        + [(6, 5), (6, 4), (7, 5), (7, 4), (6, 6), (7, 6)]
    ):
        if at < 0:
            rounds[n].pair_sum(0)
        else:
            step(n, at)()
        if (n, at) == (7, -1):
            swap(1).start()
            stay(1).start()
    for n in range(6):
        spread(n).wait_send()
    for r in rounds:
        r.finish()
    for dx in range(2):
        pushed(3, dx)
    for t in range(4):
        share(t).wait_send()
    for n in range(2):
        swap(n).wait()
        stay(n).wait()


def backward(span, slopes, saved):
    f32, bf16 = jnp.float32, jnp.bfloat16
    any_space = pl.BlockSpec(memory_space=pl.ANY)
    vmem = pl.BlockSpec(memory_space=pltpu.VMEM)
    dma = pltpu.SemaphoreType.DMA
    (weights, norms, xs, cot, q, keys, values, ctx, lse, kept, n1, i1, n2, i2, out, squares) = saved[:16]
    h1_t, x_t, dist, wo = saved[16:]
    out = out.reshape(2, 256, 768)
    in_specs = [pl.BlockSpec(memory_space=pltpu.SMEM), any_space, vmem] + [any_space] * 8
    in_specs += [vmem, any_space, vmem, any_space, vmem] + [any_space] * 4
    copies = len(ScatterRound.names)
    return pl.pallas_call(
        partial(backward_kernel, span),
        out_shape=(
            jax.ShapeDtypeStruct((2, 256, 768), bf16),
            jax.ShapeDtypeStruct((2, 256, 768), bf16),
            jax.ShapeDtypeStruct((2 * ROUNDS, 96, 384), f32),
            jax.ShapeDtypeStruct((8, 768), f32),
        ),
        in_specs=in_specs,
        out_specs=(any_space, any_space, vmem, vmem),
        scratch_shapes=[
            pltpu.VMEM((2, 2, 4, 2, 96, 384), bf16),
            pltpu.VMEM((2, 2, 768, 128), bf16),
            pltpu.VMEM((2, 3, 512, 256), bf16),
            pltpu.VMEM((768, 512), bf16),
            pltpu.VMEM((768, 512), bf16),
            pltpu.VMEM((2, 2, 256, 768), bf16),
            pltpu.VMEM((512, 768), f32),
            pltpu.VMEM((512, 768), f32),
            pltpu.VMEM((8, 512, 128), bf16),
            pltpu.VMEM((8, 2, 2, 256, 128), bf16),
            pltpu.VMEM((8, 2, 2, 256, 128), bf16),
            pltpu.VMEM((8, 512, 128), bf16),
            pltpu.VMEM((4, 8, 512), f32),
            pltpu.VMEM((1024, 512), f32),
            pltpu.VMEM((2, 512, 128), bf16),
            pltpu.VMEM((4, 2, 2, 2, 2, 256, 128), bf16),
            pltpu.VMEM((4, 2, 2, 2, 256, 128), bf16),
            pltpu.VMEM((2, 128, 512), f32),
            pltpu.VMEM((1024, 128), f32),
            pltpu.VMEM((1024, 128), f32),
            pltpu.VMEM((2 * ROUNDS, 2, 4, 2, 96, 384), bf16),
            pltpu.VMEM((6, 2, 4, 2, 96, 384), bf16),
            pltpu.VMEM((2, 2, 4, 2, 96, 384), bf16),
            pltpu.VMEM((2 * ROUNDS, 2, 4, 48, 384), bf16),
            pltpu.VMEM((2 * ROUNDS, 4, 2, 48, 384), bf16),
            pltpu.VMEM((2 * ROUNDS, 4, 32, 384), bf16),
            pltpu.VMEM((2 * ROUNDS, 4, 32, 384), bf16),
            pltpu.VMEM((2 * ROUNDS, 3, 64, 384), bf16),
            pltpu.VMEM((2 * ROUNDS, 3, 2, 16, 384), bf16),
            pltpu.VMEM((2 * ROUNDS, 3, 2, 16, 384), bf16),
            pltpu.VMEM((2 * ROUNDS, 2, 16, 384), bf16),
            pltpu.VMEM((4, 8, 768), f32),
            pltpu.VMEM((6, 8, 768), f32),
            dma((11,)),
            dma((2, 2)),
            dma((2 * ROUNDS, copies)),
            dma((2 * ROUNDS, copies)),
            dma((2 * ROUNDS, 2, 2)),
            dma((6,)),
            dma((4,)),
            dma((4,)),
            dma((6,)),
            dma((6,)),
        ],
        compiler_params=pltpu.CompilerParams(
            collective_id=1, has_side_effects=True, vmem_limit_bytes=VMEM_LIMIT
        ),
        name="backward",
    )(
        slopes,
        weights,
        norms,
        cot,
        q,
        keys,
        values,
        ctx,
        lse,
        kept,
        n1,
        i1,
        n2,
        i2,
        out,
        squares,
        h1_t,
        x_t,
        dist,
        wo,
    )


def finish_kernel(
    block, grads, small, lo, gt, o_lo, o_gt, o_qkv, o_wout, o_win, o_down, o_gains, o_biases, rows, sems
):
    def move(n, src, dst):
        return pltpu.make_async_copy(src, dst, sems.at[n])

    move(0, lo, rows.at[0]).start()
    move(1, gt, rows.at[1]).start()
    turned = []

    def tile(i):
        return grads[i // 3, :, i % 3 * 128 : i % 3 * 128 + 128]

    for c in range(3):
        o_qkv[c, :, 0:128] = tile(2 * c)
        o_qkv[c, :, 128:192] = tile(2 * c + 1)[:, :HEAD_DIM]
        turned.append(tile(2 * c + 1).T[HEAD_DIM:])
    o_wout[...] = jnp.concatenate(turned, axis=0)
    move(0, lo, rows.at[0]).wait()
    move(2, rows.at[0], o_lo).start()
    move(1, gt, rows.at[1]).wait()
    move(3, rows.at[1], o_gt).start()
    for r in range(3):
        units = slice(r * 256, (r + 1) * 256)
        o_win[:, 0, units] = grads[2 + 2 * r, :, 0:256]
        o_win[:, 1, r * 256 : r * 256 + 128] = grads[2 + 2 * r, :, 256:384]
        o_win[:, 1, r * 256 + 128 : r * 256 + 256] = grads[3 + 2 * r, :, 0:128]
        o_down[units, :] = grads[3 + 2 * r, :, 128:384].T
    mine = pltpu.roll(small[...], 768 - block[0] * 96, 1)
    o_gains[...] = mine[0:2, 0:96]
    o_biases[...] = mine[2:4, 0:96]
    move(2, rows.at[0], o_lo).wait()
    move(3, rows.at[1], o_gt).wait()


def finish(block, grads, small, lo, gt):
    any_space = pl.BlockSpec(memory_space=pl.ANY)
    vmem = pl.BlockSpec(memory_space=pltpu.VMEM)
    f32 = jnp.float32
    shape = jax.ShapeDtypeStruct
    return pl.pallas_call(
        finish_kernel,
        out_shape=(
            shape(lo.shape, lo.dtype),
            shape(gt.shape, gt.dtype),
            shape((3, 96, 192), f32),
            shape((192, 96), f32),
            shape((96, 2, 768), f32),
            shape((768, 96), f32),
            shape((2, 96), f32),
            shape((2, 96), f32),
        ),
        in_specs=[pl.BlockSpec(memory_space=pltpu.SMEM), vmem, vmem, any_space, any_space],
        out_specs=(any_space, any_space) + (vmem,) * 6,
        scratch_shapes=[pltpu.VMEM((2,) + lo.shape, lo.dtype), pltpu.SemaphoreType.DMA((4,))],
        compiler_params=pltpu.CompilerParams(vmem_limit_bytes=VMEM_LIMIT),
        name="finish",
    )(block, grads, small, lo, gt)


def local(
    tokens,
    segment_ids,
    query_key_value_weight,
    w_out,
    input_weight,
    w_down,
    norm_gains,
    norm_biases,
    cotangent,
):
    f32 = jnp.float32
    shard_rows = query_key_value_weight.shape[1]
    span = 96 // shard_rows
    slopes = jnp.asarray([2.0 ** (-8.0 * (h + 1) / HEADS) for h in range(HEADS)], f32)
    cells = float(lax.axis_size("fsdp") * 2 * 1024 * 768)
    if span == 1:
        raw = (query_key_value_weight, w_out, input_weight, w_down)
        gains, biases = norm_gains, norm_biases
    else:
        count = lax.axis_size("fsdp")
        groups = [list(range(i, i + span)) for i in range(0, count, span)]
        heads = query_key_value_weight.transpose(1, 0, 2).reshape(shard_rows, 3, 3, HEAD_DIM)
        w_out_t = w_out.T.reshape(shard_rows, 3, 1, HEAD_DIM)
        wa = jnp.concatenate([heads, w_out_t], axis=2).reshape(shard_rows, 1, 768)
        gate_up = input_weight.reshape(shard_rows, 2, 3, 256).transpose(0, 2, 1, 3)
        down = w_down.T.reshape(shard_rows, 3, 1, 256)
        wf = jnp.concatenate([gate_up, down], axis=2).reshape(shard_rows, 3, 768)
        shard = jnp.concatenate([wa, wf], axis=1).reshape(shard_rows, 8, 384).transpose(1, 0, 2)
        raw = (lax.all_gather(shard, "fsdp", axis=1, tiled=True, axis_index_groups=groups),)
        gains, biases = (
            lax.all_gather(rows, "fsdp", axis=1, tiled=True, axis_index_groups=groups)
            for rows in (norm_gains, norm_biases)
        )

    saved = forward(span, slopes, raw, gains, biases, tokens, cotangent, segment_ids)
    layer_out, grad_tokens, grads, small = backward(span, slopes, saved)

    if span == 1:
        block = lax.axis_index("fsdp").astype(jnp.int32).reshape(1)
        outs = finish(block, grads, small, layer_out, grad_tokens)
    else:
        grads = lax.psum_scatter(
            grads, "fsdp", scatter_dimension=1, tiled=True, axis_index_groups=groups
        )
        small = lax.psum(small, "fsdp", axis_index_groups=groups)
        grads = grads.reshape(4, 2, shard_rows, 384).transpose(0, 2, 1, 3)
        grads_a = grads[0].reshape(shard_rows, 3, 4, HEAD_DIM)
        grads_f = grads[1:].reshape(3, shard_rows, 3, 256)
        shard_start = lax.axis_index("fsdp") * shard_rows
        mine = lax.dynamic_slice_in_dim(small[:4], shard_start, shard_rows, 1)
        outs = (
            layer_out,
            grad_tokens,
            grads_a[:, :, :3].transpose(1, 0, 2, 3).reshape(3, shard_rows, 192),
            grads_a[:, :, 3].reshape(shard_rows, 192).T,
            grads_f[:, :, :2].transpose(1, 2, 0, 3).reshape(shard_rows, 2, 768),
            grads_f[:, :, 2].transpose(0, 2, 1).reshape(768, shard_rows),
            mine[:2],
            mine[2:],
        )
    return outs + (jnp.sqrt(jnp.sum(small[4:], axis=1) / cells),)


def solution(mesh):
    placed = (
        P("fsdp", "tp", None),
        P("fsdp", None),
        P(None, "fsdp", "tp"),
        P("tp", "fsdp"),
        P("fsdp", None, "tp"),
        P("tp", "fsdp"),
        P(None, "fsdp"),
        P(None, "fsdp"),
        P("fsdp", "tp", None),
    )
    return jax.shard_map(
        local,
        mesh=mesh,
        in_specs=placed,
        out_specs=(
            P("fsdp", "tp", None),
            P("fsdp", "tp", None),
            P(None, "fsdp", "tp"),
            P("tp", "fsdp"),
            P("fsdp", None, "tp"),
            P("tp", "fsdp"),
            P(None, "fsdp"),
            P(None, "fsdp"),
            P(),
        ),
        check_vma=False,
    )
```

```python
from functools import partial

import jax
import jax.numpy as jnp
from jax import lax
from jax.experimental import pallas as pl
from jax.experimental.pallas import tpu as pltpu
from jax.sharding import PartitionSpec as P

HEADS = 12
HEAD_DIM = 64
MESH = pl.DeviceIdType.MESH
VMEM_LIMIT = 63 << 20
norm_eps = 1e-05
ROUNDS = 4
NT = (((1,), (1,)), ((), ()))
NN = (((1,), (0,)), ((), ()))
CHUNK = 256


class Place:
    def __init__(self, span):
        index = lax.axis_index("fsdp")
        shard = lax.axis_index("tp")
        self.span = span
        self.j = index % span
        block = index // span
        self.z = block // 2
        self.y = block % 2
        self.x = shard // 2
        self.k = shard % 2

    def shifted(self, dx=0, dy=0, dz=0, dk=0):
        x = 1 - self.x if dx else self.x
        y = 1 - self.y if dy else self.y
        z = (self.z + dz) % 4 if dz else self.z
        k = 1 - self.k if dk else self.k
        return x, y, z, k

    def device(self, dx=0, dy=0, dz=0, dk=0):
        x, y, z, k = self.shifted(dx, dy, dz, dk)
        return ((z * 2 + y) * self.span + self.j, x * 2 + k)

    def greet(self, offsets):
        barrier = pltpu.get_barrier_semaphore()
        for offset in offsets:
            pl.semaphore_signal(
                barrier, inc=1, device_id=self.device(**offset), device_id_type=MESH
            )
        pl.semaphore_wait(barrier, len(offsets))


ALL_PEERS = ({"dx": 1}, {"dy": 1}, {"dz": 1}, {"dz": 2}, {"dz": 3}, {"dk": 1})


def remote(src, dst, send, recv, device):
    return pltpu.make_async_remote_copy(
        src_ref=src, dst_ref=dst, send_sem=send, recv_sem=recv, device_id=device, device_id_type=MESH
    )


PARTS = {
    "a": pl.ds(0, 32),
    "c": pl.ds(32, 16),
    "ac": pl.ds(0, 48),
    "b": pl.ds(48, 32),
    "d": pl.ds(80, 16),
    "bd": pl.ds(48, 48),
    "": pl.ds(0, 96),
}


def dot(a, b, dims=NN):
    return lax.dot_general(a, b, dims, preferred_element_type=jnp.float32)


class Copies:
    names = ()

    def start(self, *names):
        for name in names:
            self.copy(name).start()

    def wait(self, *names):
        for name in names:
            self.copy(name).wait_recv()

    def finish(self):
        for name in self.names:
            self.copy(name).wait_send()


class GatherRound(Copies):
    names = ("z1", "z2", "z3", "ax", "by", "ay0", "bx0", "ay1", "bx1") + tuple(
        "d%d" % i for i in range(7)
    )
    names += ("cx", "cz1", "cz2", "cz3", "dy", "dz1", "dz2", "dz3")
    lines = {
        "ax": ((0, 0, "a"), {"dx": 1}),
        "by": ((0, 0, "b"), {"dy": 1}),
        "ay0": ((0, 0, "ac"), {"dy": 1}),
        "bx0": ((0, 0, "bd"), {"dx": 1}),
        "ay1": ((1, 0, "ac"), {"dy": 1}),
        "bx1": ((0, 1, "bd"), {"dx": 1}),
        "d0": ((0, 0, ""), {"dk": 1}),
        "d1": ((1, 0, "ac"), {"dk": 1}),
        "d2": ((0, 1, "bd"), {"dk": 1}),
        "d3": ((0, 1, "ac"), {"dk": 1}),
        "d4": ((1, 0, "bd"), {"dk": 1}),
        "d5": ((1, 1, "ac"), {"dk": 1}),
        "d6": ((1, 1, "bd"), {"dk": 1}),
    }
    steps = {
        3: (("ax", "cz1", "cz2", "cz3"), ("ay1", "d1")),
        4: (("by", "dz1", "dz2", "dz3"), ("bx1", "d2")),
        5: (("ay0",), ("d3",)),
        6: (("bx0",), ("d4",)),
        7: (("ay1",), ("d5",)),
        8: (("bx1",), ("d6",)),
    }
    last = 10

    def __init__(self, place, own, out, send, recv, keep):
        self.place, self.own, self.out = place, own, out
        self.send, self.recv, self.keep = send, recv, keep

    def line(self, dx, dy, part):
        x, y, z, k = self.place.shifted(dx, dy)
        return self.out.at[x, k, :, y, PARTS[part], :]

    def copy(self, name):
        place = self.place
        at = self.names.index(name)
        send, recv = self.send.at[at], self.recv.at[at]
        x, y, z, k = place.shifted()
        if name[0] == "z":
            return remote(
                self.own, self.out.at[x, k, z, y], send, recv, place.device(dz=int(name[1]))
            )
        if name in ("cx", "dy"):
            rows = PARTS[name[0]]
            return remote(
                self.own.at[rows, :],
                self.out.at[x, k, z, y, rows, :],
                send,
                recv,
                place.device(**{"d" + name[1]: 1}),
            )
        if name[:2] in ("cz", "dz"):
            x, y, z, k = place.shifted(dx=1) if name[0] == "c" else place.shifted(dy=1)
            ref = self.out.at[x, k, z, y, PARTS[name[0]], :]
            return remote(ref, ref, send, recv, place.device(dz=int(name[2])))
        where, to = self.lines[name]
        ref = self.line(*where)
        return remote(ref, ref, send, recv, place.device(**to))

    def kept(self):
        x, y, z, k = self.place.shifted()
        return pltpu.make_async_copy(self.own, self.out.at[x, k, z, y], self.keep)

    def event(self, n):
        if n == 0:
            self.kept().start()
            self.start("cx", "dy", "z1", "z2", "z3")
        elif n == 1:
            self.wait("cx", "dy")
            self.start("cz1", "cz2", "cz3", "dz1", "dz2", "dz3")
        elif n == 2:
            self.kept().wait()
            self.wait("z1", "z2", "z3")
            self.start("ax", "by", "ay0", "bx0", "d0")
        elif n == 9:
            self.wait("d0", "d2", "d3")
        elif n == 10:
            self.wait("d1", "d4", "d5", "d6")
        else:
            self.wait(*self.steps[n][0])
            self.start(*self.steps[n][1])


class NormGather(Copies):
    names = ("z1", "z2", "z3", "y")

    def __init__(self, place, own, out, send, recv, keep):
        self.place, self.own, self.out = place, own, out
        self.send, self.recv, self.keep = send, recv, keep

    def copy(self, name):
        place = self.place
        at = self.names.index(name)
        send, recv = self.send.at[at], self.recv.at[at]
        if name == "y":
            ref = self.out.at[:, place.y]
            return remote(ref, ref, send, recv, place.device(dy=1))
        return remote(
            self.own, self.out.at[place.z, place.y], send, recv, place.device(dz=int(name[1]))
        )

    def kept(self):
        return pltpu.make_async_copy(self.own, self.out.at[self.place.z, self.place.y], self.keep)


class Events:
    def __init__(self, steps):
        self.steps = list(steps)

    def run(self, count):
        for step in self.steps[:count]:
            step()
        del self.steps[:count]

    def spread(self, trips, points, count):
        total = trips * points
        return self.place(trips, points, {n * total // max(count, 1): 1 for n in range(count)})

    def place(self, trips, points, counts):
        total = trips * points
        slots = [[] for _ in range(total)]
        for number in sorted(counts):
            slots[number] += self.steps[: counts[number]]
            del self.steps[: counts[number]]

        def stop(i, point):
            for trip in range(trips):
                todo = slots[trip * points + point]
                if todo:

                    @pl.when(i == trip)
                    def _():
                        for step in todo:
                            step()

        return stop


def lane_half(tile, half):
    lane = lax.broadcasted_iota(jnp.int32, tile.shape, 1)
    keep = (lane < HEAD_DIM) if half == 0 else (lane >= HEAD_DIM)
    return jnp.where(keep, tile, jnp.zeros_like(tile))


def swap_halves(tile):
    return pltpu.roll(tile.astype(jnp.float32), HEAD_DIM, 1)


def fill_distance(dist, segments, place):
    row = segments[pl.ds(place.x, 1), :].astype(jnp.float32)
    column = jnp.broadcast_to(row, (8, 1024)).T[:, 0:1]
    for s in range(2):
        first = (2 * s + place.k) * 256
        mine = segments[pl.ds(place.x, 1), pl.ds(pl.multiple_of(first, 256), 256)].astype(jnp.float32)
        gap = lax.broadcasted_iota(jnp.int32, (1024, 256), 0) - (
            lax.broadcasted_iota(jnp.int32, (1024, 256), 1) + first
        )
        dist[:, s * 256 : (s + 1) * 256] = jnp.where(
            column == mine, jnp.abs(gap).astype(jnp.float32), 1e30
        )


def pack_attention(raw, shard):
    qkv, w_out = raw[0], raw[1]
    turned = w_out[...].astype(jnp.float32).T
    for c in range(3):
        tiles = (
            qkv[c, :, 0:128],
            jnp.concatenate(
                [
                    qkv[c, :, 128:192].astype(jnp.float32),
                    turned[:, c * HEAD_DIM : (c + 1) * HEAD_DIM],
                ],
                axis=1,
            ).astype(jnp.bfloat16),
        )
        for i in range(2):
            half, at = divmod(2 * c + i, 3)
            shard[half, :, at * 128 : at * 128 + 128] = tiles[i]


def pack_feed(raw, shard):
    w_in, w_down = raw[2:]
    turned = w_down[...].astype(jnp.float32).T.astype(jnp.bfloat16)
    for r in range(3):
        units = slice(r * 256, (r + 1) * 256)
        first = slice(r * 256, r * 256 + 128)
        second = slice(r * 256 + 128, r * 256 + 256)
        shard[2 + 2 * r, :, 0:256] = w_in[:, 0, units]
        shard[2 + 2 * r, :, 256:384] = w_in[:, 1, first]
        shard[3 + 2 * r, :, 0:128] = w_in[:, 1, second]
        shard[3 + 2 * r, :, 128:384] = turned[:, units]


def out_weights(w):
    first = lax.broadcasted_iota(jnp.int32, (768, 128), 1) < HEAD_DIM
    left = jnp.where(first, swap_halves(w[:, 128:256]), w[:, 384:512].astype(jnp.float32))
    right = jnp.where(first, swap_halves(w[:, 640:768]), 0.0)
    return left.astype(jnp.bfloat16), right.astype(jnp.bfloat16)


def whole(ref):
    return jnp.concatenate([ref[i].reshape(768, 384) for i in range(2)], axis=1)


HEAD_SPOTS = ((0, 0), (0, 1), (1, 0))


def norm_stats(value):
    average = jnp.mean(value, axis=-1, keepdims=True)
    centered = value - average
    inv_std = lax.rsqrt(jnp.mean(centered * centered, axis=-1, keepdims=True) + norm_eps)
    return centered * inv_std, inv_std


def norm_backward(grad_val, normed, inv_std, gain_row):
    grad_norm = grad_val * gain_row
    return inv_std * (
        grad_norm
        - jnp.mean(grad_norm, axis=-1, keepdims=True)
        - normed * jnp.mean(grad_norm * normed, axis=-1, keepdims=True)
    )


ROWS = 128


def row_blocks(body):
    def step(i, carry):
        body(pl.ds(pl.multiple_of(i * ROWS, ROWS), ROWS), i)
        return carry

    lax.fori_loop(0, 512 // ROWS, step, 0)


def columns(value):
    return jnp.sum(value.reshape(value.shape[0] // 8, 8, value.shape[1]), axis=0)


def forward_kernel(
    span,
    slopes,
    raw,
    gains,
    biases,
    tok,
    cot,
    segments,
    o_weights,
    o_norms,
    o_x,
    o_cot,
    o_q,
    o_k,
    o_v,
    o_ctx,
    o_lse,
    o_kept,
    o_n1,
    o_i1,
    o_n2,
    o_i2,
    o_out,
    o_squares,
    o_h1_t,
    o_x_t,
    o_dist,
    o_wo,
    shard,
    norm_rows,
    weights,
    norms,
    xs,
    q,
    keys,
    values,
    ctx,
    h1b,
    n1,
    h1_t,
    x_t,
    wo,
    dist,
    out_t,
    acc,
    h1,
    kept,
    g_send,
    g_recv,
    g_keep,
    n_send,
    n_recv,
    n_keep,
    t_sems,
    kv_send,
    kv_recv,
    store_sems,
    kept_sems,
):
    f32, bf16 = jnp.float32, jnp.bfloat16
    place = Place(span)
    x, y, z, k = place.shifted()
    rounds = [
        GatherRound(place, shard.at[r], weights.at[r], g_send.at[r], g_recv.at[r], g_keep.at[r])
        for r in range(2 * ROUNDS)
    ]
    norm_gather = NormGather(place, norm_rows, norms, n_send, n_recv, n_keep)

    def swap(n):
        src, dst = ((tok, xs), (cot, o_cot))[n]
        return remote(
            src.at[1 - place.x],
            dst.at[place.x],
            t_sems.at[3 * n],
            t_sems.at[3 * n + 1],
            place.device(dx=1),
        )

    def stay(n):
        src, dst = ((tok, xs), (cot, o_cot))[n]
        return pltpu.make_async_copy(src.at[place.x], dst.at[place.x], t_sems.at[3 * n + 2])

    def store(n):
        src, dst = (
            (weights.at[0:2], o_weights.at[0:2]),
            (weights.at[2:4], o_weights.at[2:4]),
            (weights.at[4:6], o_weights.at[4:6]),
            (weights.at[6:8], o_weights.at[6:8]),
            (xs, o_x),
            (keys, o_k),
            (values, o_v),
            (q, o_q),
            (ctx, o_ctx),
            (n1, o_n1),
            (h1_t, o_h1_t),
            (x_t, o_x_t),
            (dist, o_dist),
            (wo, o_wo),
        )[n]
        return pltpu.make_async_copy(src, dst, store_sems.at[n])

    if len(raw) > 1:
        pack_attention(raw, shard)
    else:
        shard[...] = raw[0][...]
    place.greet(ALL_PEERS)
    rounds[0].event(0)
    swap(0).start()
    for n in range(2):
        stay(n).start()
    norm_rows[...] = jnp.zeros_like(norm_rows)
    norm_rows[0:2, 0:96] = gains[...].astype(f32)
    norm_rows[2:4, 0:96] = biases[...].astype(f32)
    block = place.z * 2 + place.y
    norm_rows[...] = pltpu.roll(norm_rows[...], block * 96, 1)
    norm_gather.kept().start()
    norm_gather.start("z1", "z2", "z3")
    if len(raw) > 1:
        pack_feed(raw, shard)

    def step(r, n):
        def go():
            rounds[r].event(n)
            if n == GatherRound.last and r % 2:
                store(r // 2).start()

        return go

    stages = {0: 0, 1: 1, 2: 1, 3: 2, 4: 2, 5: 3, 6: 3, 7: 3, 8: 3, 9: 4, 10: 4}
    order = sorted((r + stages[n], r, n) for r in range(2 * ROUNDS) for n in range(11))
    order = [(r, n) for _, r, n in order][1:]
    order = order[: order.index((7, 4)) + 1]
    order += [(7, 5), (6, 9), (7, 9), (7, 6), (7, 7), (7, 8), (6, 10), (7, 10)]
    begun = order.index((1, 10)) + 1
    beside_heads = order.index((3, 10)) + 1 - begun
    events = Events(step(*at) for at in order)
    events.steps.insert(order.index((7, 4)) + 1, lambda: swap(1).start())

    events.run(1)
    fill_distance(dist, segments, place)
    norm_gather.kept().wait()
    norm_gather.wait("z1", "z2", "z3")
    norm_gather.start("y")
    events.run(begun - 1)
    swap(0).wait_recv()
    stay(0).wait()
    store(4).start()
    for i in range(512 // ROWS):
        rows = pl.ds((i % 2) * ROWS, ROWS)
        x_t[:, i * ROWS : (i + 1) * ROWS] = xs[i // 2, rows, :].astype(f32).T.astype(bf16)
    store(11).start()
    store(12).start()

    def share(t, n):
        ref = (keys, values)[n].at[pl.ds(2 * t, 2), :, place.k]
        return remote(ref, ref, kv_send.at[t, n], kv_recv.at[t, n], place.device(dk=1))

    def project(t, carry):
        w = whole(weights.at[0:2, t // 2, t % 2])
        for s in range(2):
            out = dot(xs[s], w).astype(bf16)
            for i in range(2):
                cols = slice(i * 128, i * 128 + 128)
                q[2 * t + i, pl.ds(s * 256, 256), :] = out[:, cols] * bf16(HEAD_DIM**-0.5)
                keys[2 * t + i, s, k] = out[:, 256 + i * 128 : 384 + i * 128]
                values[2 * t + i, s, k] = out[:, 512 + i * 128 : 640 + i * 128]
        share(t, 0).start()
        share(t, 1).start()
        return carry

    lax.fori_loop(0, 4, project, 0)
    out_t[1, pl.ds(HEAD_DIM, HEAD_DIM), :] = jnp.zeros((HEAD_DIM, 512), f32)
    stop = events.spread(4, 7, beside_heads)

    def attend(t, carry):
        share(t, 0).wait_recv()
        share(t, 1).wait_recv()
        point = 0
        for spot, (tile, half) in enumerate(HEAD_SPOTS):
            slope = slopes[3 * t + spot]
            key = keys[2 * t + tile].reshape(1024, 128)
            rows = slice(half * HEAD_DIM, (half + 1) * HEAD_DIM)
            value_t = values[2 * t + tile].reshape(1024, 128).astype(f32).T.astype(bf16)[rows]
            for start in range(0, 512, CHUNK):
                cols = pl.ds(start, CHUNK)
                part = lane_half(q[2 * t + tile, cols, :], half)
                scores = dot(key, part, NT) - slope * dist[:, cols]
                peak = jnp.max(scores, axis=0, keepdims=True)
                expo = jnp.exp(scores - peak)
                total = jnp.sum(expo, axis=0, keepdims=True)
                out_t[tile, rows, cols] = dot(value_t, expo.astype(bf16)) / total
                o_lse[t, pl.ds(spot, 1), cols] = peak + jnp.log(total)
                stop(t, point)
                point += 1
        for tile in range(2):
            ctx[2 * t + tile] = out_t[tile].T.astype(bf16)
        left, right = out_weights(whole(weights.at[0:2, t // 2, t % 2]))
        wo[t, 0] = left
        wo[t, 1] = right
        mixed = dot(ctx[2 * t], left, NT) + dot(ctx[2 * t + 1], right, NT)

        @pl.when(t == 0)
        def _():
            acc[...] = mixed

        @pl.when(t > 0)
        def _():
            acc[...] += mixed

        stop(t, point)
        return carry

    lax.fori_loop(0, 4, attend, 0)
    for n in (5, 6, 7, 8, 13):
        store(n).start()
    norm_gather.wait("y")
    norm_sum = jnp.sum(norms[...].reshape(8, 8, 768), axis=0)
    o_norms[...] = norm_sum

    def first_norm(rows, i):
        attn = acc[rows, :]
        half = i // 2
        resid = xs[half, pl.ds(pl.multiple_of((i % 2) * ROWS, ROWS), ROWS), :].astype(f32) + attn
        normed, inv = norm_stats(resid)
        value = normed * norm_sum[0:1] + norm_sum[2:3]
        h1[rows, :] = value
        h1b[rows, :] = value.astype(bf16)
        h1_t[:, rows] = value.T.astype(bf16)
        n1[rows, :] = normed
        o_i1[rows, :] = inv
        acc[rows, :] = jnp.zeros_like(attn)
        if_first = jnp.where(i == 0, 0.0, 1.0)
        o_squares[0] = o_squares[0] * if_first + columns(attn * attn)
        o_squares[1] = o_squares[1] * if_first + columns(resid * resid)

    o_squares[...] = jnp.zeros_like(o_squares)
    row_blocks(first_norm)
    store(9).start()
    store(10).start()

    first_part = order.index((5, 10)) - begun - beside_heads
    middle = len(order) - 7 - order.index((5, 10)) - 1
    counts = {}
    for n in range(first_part):
        at = n * 8 // first_part
        counts[at] = counts.get(at, 0) + 1
    counts[8] = 1
    for n in range(middle):
        at = 9 + n * 6 // middle
        counts[at] = counts.get(at, 0) + 1
    counts[16] = 1
    counts[18] = counts[22] = 2
    counts[20] = 3
    stop_f = events.place(12, 2, counts)
    assert not events.steps

    def keep_copy(n):
        at = n // 4 * 4 + (x ^ (n % 4 // 2)) * 2 + (k ^ (n % 2))
        return pltpu.make_async_copy(kept.at[n % 2], o_kept.at[at], kept_sems.at[n % 2])

    def feed(n, carry):
        r = 1 + n // 4
        wx, wk = x ^ (n % 4 // 2), k ^ (n % 2)
        stop_f(n, 0)

        @pl.when(n >= 2)
        def _():
            keep_copy(n - 2).wait()

        ref = weights.at[pl.ds(2 * r, 2), wx, wk]
        for start in range(0, 512, CHUNK):
            rows = pl.ds(start, CHUNK)
            w = whole(ref)
            projected = dot(h1b[rows, :], w[:, :512])
            gate, up = projected[:, :256], projected[:, 256:]
            cdf = 0.5 + 0.5 * lax.erf(gate * (0.5**0.5))
            pdf = jnp.exp(-0.5 * gate * gate) * 0.3989422804014327
            act = gate * cdf
            hidden = (act * up).astype(bf16)
            kept[n % 2, 0, rows, :] = hidden
            kept[n % 2, 1, rows, :] = act.astype(bf16)
            kept[n % 2, 2, rows, :] = ((cdf + gate * pdf) * up).astype(bf16)
            acc[rows, :] += dot(hidden, w[:, 512:], NT)
        keep_copy(n).start()
        stop_f(n, 1)
        return carry

    lax.fori_loop(0, 12, feed, 0)

    def second_norm(rows, i):
        ffn = acc[rows, :]
        resid = h1[rows, :] + ffn
        normed, inv = norm_stats(resid)
        o_out[rows, :] = (normed * norm_sum[1:2] + norm_sum[3:4]).astype(bf16)
        o_n2[rows, :] = normed
        o_i2[rows, :] = inv
        o_squares[2] += columns(ffn * ffn)
        o_squares[3] += columns(resid * resid)

    row_blocks(second_norm)
    for n in (10, 11):
        keep_copy(n).wait()
    for r in rounds:
        r.finish()
    norm_gather.finish()
    for n in range(2):
        swap(n).wait_send()
    swap(1).wait_recv()
    stay(1).wait()
    for t in range(4):
        for n in range(2):
            share(t, n).wait_send()
    for n in range(14):
        store(n).wait()


def forward_refs(span, count, *refs):
    forward_kernel(span, refs[0], refs[1 : 1 + count], *refs[1 + count :])


def forward(span, slopes, raw, gains, biases, tok, cot, segments):
    f32, bf16 = jnp.float32, jnp.bfloat16
    any_space = pl.BlockSpec(memory_space=pl.ANY)
    vmem = pl.BlockSpec(memory_space=pltpu.VMEM)
    outs = (
        ((2 * ROUNDS, 2, 2, 4, 2, 96, 384), bf16, any_space),
        ((8, 768), f32, vmem),
        ((2, 256, 768), bf16, any_space),
        ((2, 256, 768), bf16, any_space),
        ((8, 512, 128), bf16, any_space),
        ((8, 2, 2, 256, 128), bf16, any_space),
        ((8, 2, 2, 256, 128), bf16, any_space),
        ((8, 512, 128), bf16, any_space),
        ((4, 8, 512), f32, vmem),
        ((12, 3, 512, 256), bf16, any_space),
        ((512, 768), f32, any_space),
        ((512, 1), f32, vmem),
        ((512, 768), f32, vmem),
        ((512, 1), f32, vmem),
        ((512, 768), bf16, vmem),
        ((4, 8, 768), f32, vmem),
        ((768, 512), bf16, any_space),
        ((768, 512), bf16, any_space),
        ((1024, 512), f32, any_space),
        ((4, 2, 768, 128), bf16, any_space),
    )
    dma = pltpu.SemaphoreType.DMA
    copies = len(GatherRound.names)
    return pl.pallas_call(
        partial(forward_refs, span, len(raw)),
        out_shape=tuple(jax.ShapeDtypeStruct(s, d) for s, d, _ in outs),
        in_specs=[pl.BlockSpec(memory_space=pltpu.SMEM)]
        + [vmem] * (len(raw) + 2)
        + [any_space, any_space, vmem],
        out_specs=tuple(spec for _, _, spec in outs),
        scratch_shapes=[
            pltpu.VMEM((2 * ROUNDS, 96, 384), bf16),
            pltpu.VMEM((8, 768), f32),
            pltpu.VMEM((2 * ROUNDS, 2, 2, 4, 2, 96, 384), bf16),
            pltpu.VMEM((4, 2, 8, 768), f32),
            pltpu.VMEM((2, 256, 768), bf16),
            pltpu.VMEM((8, 512, 128), bf16),
            pltpu.VMEM((8, 2, 2, 256, 128), bf16),
            pltpu.VMEM((8, 2, 2, 256, 128), bf16),
            pltpu.VMEM((8, 512, 128), bf16),
            pltpu.VMEM((512, 768), bf16),
            pltpu.VMEM((512, 768), f32),
            pltpu.VMEM((768, 512), bf16),
            pltpu.VMEM((768, 512), bf16),
            pltpu.VMEM((4, 2, 768, 128), bf16),
            pltpu.VMEM((1024, 512), f32),
            pltpu.VMEM((2, 128, 512), f32),
            pltpu.VMEM((512, 768), f32),
            pltpu.VMEM((512, 768), f32),
            pltpu.VMEM((2, 3, 512, 256), bf16),
            dma((2 * ROUNDS, copies)),
            dma((2 * ROUNDS, copies)),
            dma((2 * ROUNDS,)),
            dma((4,)),
            dma((4,)),
            dma,
            dma((6,)),
            dma((4, 2)),
            dma((4, 2)),
            dma((14,)),
            dma((2,)),
        ],
        compiler_params=pltpu.CompilerParams(
            collective_id=0, has_side_effects=True, vmem_limit_bytes=VMEM_LIMIT
        ),
        name="forward",
    )(slopes, *raw, gains, biases, tok, cot, segments)


class ScatterRound(Copies):
    names = ("ay1", "bx", "ay0", "ax", "by", "cx", "dy") + tuple(
        part + "z%d" % step for part in "abcd" for step in (1, 2, 3)
    )

    def __init__(self, place, held, twin, stage, landing, send, recv, pair):
        self.place, self.held, self.twin, self.stage = place, held, twin, stage
        self.ay, self.bx, self.ax, self.by, self.z, self.cz, self.dz, self.last = landing
        self.send, self.recv, self.pair = send, recv, pair

    def copy(self, name):
        p, held = self.place, self.held
        at = self.names.index(name)
        a, b, c, d = (PARTS[part] for part in "abcd")
        step = int(name[2]) if name[1] == "z" else 0
        far = (p.z + step) % 4
        ac, bd = PARTS["ac"], PARTS["bd"]
        if name in ("ay1", "ay0"):
            dx = int(name[2])
            src, dst, to = held.at[dx, :, 1 - p.y, ac, :], self.ay.at[dx], {"dy": 1}
        elif name == "bx":
            src, dst, to = held.at[1, :, :, bd, :], self.bx, {"dx": 1}
        elif name == "ax":
            src, dst, to = held.at[1, :, p.y, a, :], self.ax, {"dx": 1}
        elif name == "by":
            src, dst, to = held.at[0, :, 1 - p.y, b, :], self.by, {"dy": 1}
        elif name == "cx":
            src, dst, to = held.at[1, p.z, p.y, c, :], self.last.at[0], {"dx": 1}
        elif name == "dy":
            src, dst, to = held.at[0, p.z, 1 - p.y, d, :], self.last.at[1], {"dy": 1}
        elif name[0] == "c":
            src, dst, to = held.at[:, far, p.y, c, :], self.cz.at[step - 1], {"dz": step}
        elif name[0] == "d":
            src, dst, to = held.at[0, far, :, d, :], self.dz.at[step - 1], {"dz": step}
        else:
            rows = PARTS[name[0]]
            into = pl.ds(0, 32) if name[0] == "a" else pl.ds(32, 32)
            src, dst, to = held.at[0, far, p.y, rows, :], self.z.at[step - 1, into, :], {"dz": step}
        return remote(src, dst, self.send.at[at], self.recv.at[at], p.device(**to))

    def push(self, dx):
        return remote(
            self.stage.at[dx], self.twin.at[dx], self.pair.at[0, dx], self.pair.at[1, dx], self.place.device(dk=1)
        )

    def add(self, ref, *others):
        total = ref[...].astype(jnp.float32)
        for other in others:
            total = total + other[...].astype(jnp.float32)
        ref[...] = total.astype(jnp.bfloat16)

    def pair_sum(self, dx):
        self.push(dx).wait_recv()

        def body(i, carry):
            self.add(self.held.at[dx, i], self.twin.at[dx, i])
            return carry

        lax.fori_loop(0, 4, body, 0)
        if dx:
            self.start("bx", "ay1")
        else:
            self.start("ay0")

    def event(self, n, out=None):
        p, held = self.place, self.held
        a, b, c, d = (PARTS[part] for part in "abcd")
        ac, bd = PARTS["ac"], PARTS["bd"]
        if n == 0:
            self.wait("ay1")
            self.add(held.at[1, :, p.y, ac, :], self.ay.at[1])
            self.start("ax")
        elif n == 1:
            self.wait("bx")
            self.add(held.at[0, :, 1 - p.y, bd, :], self.bx.at[:, 1 - p.y])
            self.start("by")
            self.add(held.at[0, :, p.y, bd, :], self.bx.at[:, p.y])
            self.start("dz1", "dz2", "dz3")
        elif n == 2:
            self.wait("ay0")
            self.add(held.at[0, :, p.y, ac, :], self.ay.at[0])
            self.start("cz1", "cz2", "cz3")
        elif n == 3:
            self.wait("ax")
            self.add(held.at[0, :, p.y, a, :], self.ax)
            self.start("az1", "az2", "az3")
        elif n == 4:
            self.wait("by")
            self.add(held.at[0, :, p.y, b, :], self.by)
            self.start("bz1", "bz2", "bz3")
        elif n == 5:
            self.wait("cz1", "cz2", "cz3", "dz1", "dz2", "dz3")
            self.add(held.at[1, p.z, p.y, c, :], *[self.cz.at[i, 1] for i in range(3)])
            self.start("cx")
            self.add(held.at[0, p.z, 1 - p.y, d, :], *[self.dz.at[i, 1 - p.y] for i in range(3)])
            self.start("dy")
            self.add(held.at[0, p.z, p.y, c, :], *[self.cz.at[i, 0] for i in range(3)])
            self.add(held.at[0, p.z, p.y, d, :], *[self.dz.at[i, p.y] for i in range(3)])
        else:
            self.wait("az1", "az2", "az3", "bz1", "bz2", "bz3", "cx", "dy")
            for rows, others in (
                (a, [self.z.at[i, pl.ds(0, 32), :] for i in range(3)]),
                (b, [self.z.at[i, pl.ds(32, 32), :] for i in range(3)]),
                (c, [self.last.at[0]]),
                (d, [self.last.at[1]]),
            ):
                total = held[0, p.z, p.y, rows, :].astype(jnp.float32)
                for other in others:
                    total = total + other[...].astype(jnp.float32)
                out[rows, :] = total


def backward_kernel(
    span,
    slopes,
    i_weights,
    norms,
    i_cot,
    i_q,
    i_k,
    i_v,
    i_ctx,
    i_lse,
    i_kept,
    i_n1,
    i_i1,
    i_n2,
    i_i2,
    i_out,
    squares,
    i_h1_t,
    i_x_t,
    i_dist,
    i_wo,
    o_out,
    o_tokens,
    o_grads,
    o_small,
    w_buf,
    wo,
    kept,
    h1_t,
    f_t,
    d_rows,
    n_buf,
    d_h1,
    q,
    keys,
    values,
    ctx,
    lse,
    dist,
    d_ctx,
    d_kv,
    d_kv_in,
    dq_t,
    acc_k,
    acc_v,
    held,
    twin,
    land_ay,
    land_bx,
    land_ax,
    land_by,
    land_z,
    land_cz,
    land_dz,
    land_last,
    small,
    small_in,
    load_sems,
    step_sems,
    r_send,
    r_recv,
    r_pair,
    t_sems,
    kv_send,
    kv_recv,
    s_send,
    s_recv,
):
    f32, bf16 = jnp.float32, jnp.bfloat16
    place = Place(span)
    x, y, z, k = place.shifted()
    rounds = [
        ScatterRound(
            place,
            held.at[n],
            twin.at[n % 6],
            held.at[2 * ROUNDS + n % 2],
            [
                ref.at[n]
                for ref in (land_ay, land_bx, land_ax, land_by, land_z, land_cz, land_dz, land_last)
            ],
            r_send.at[n],
            r_recv.at[n],
            r_pair.at[n],
        )
        for n in range(2 * ROUNDS)
    ]

    def load(n):
        src, dst = (
            (i_cot, d_rows.at[1]),
            (i_n2, n_buf),
            (i_h1_t, h1_t),
            (i_x_t, h1_t),
            (i_q, q),
            (i_k, keys),
            (i_v, values),
            (i_ctx, ctx),
            (i_lse, lse),
            (i_n1, n_buf),
            (i_dist, dist),
        )[n]
        return pltpu.make_async_copy(src, dst, load_sems.at[n])

    def where(n):
        return x ^ (1 - n // 2), k ^ (1 - n % 2)

    def where_heads(n):
        return x ^ (1 - n // 2), n % 2

    def fetch(n, part):
        r = 3 - n // 4
        wx, wk = where(n % 4)
        if part == 0:
            return pltpu.make_async_copy(i_weights.at[pl.ds(2 * r, 2), wx, wk], w_buf.at[n % 2], step_sems.at[n % 2, 0])
        return pltpu.make_async_copy(
            i_kept.at[(r - 1) * 4 + wx * 2 + wk], kept.at[n % 2], step_sems.at[n % 2, 1]
        )

    for n in (0, 1):
        load(n).start()
    fetch(0, 0).start()
    fetch(0, 1).start()
    for n in (2, 4, 5, 6, 7, 8, 10):
        load(n).start()
    place.greet(ALL_PEERS)

    def swap(n):
        src, dst = ((i_out, o_out), (d_rows.at[0], o_tokens))[n]
        return remote(
            src.at[1 - place.x],
            dst.at[place.x],
            t_sems.at[3 * n],
            t_sems.at[3 * n + 1],
            place.device(dx=1),
        )

    def stay(n):
        src, dst = ((i_out, o_out), (d_rows.at[0], o_tokens))[n]
        return pltpu.make_async_copy(src.at[place.x], dst.at[place.x], t_sems.at[3 * n + 2])

    swap(0).start()
    stay(0).start()
    load(0).wait()
    load(1).wait()
    small[...] = jnp.zeros_like(small)

    def halves(ref, i):
        return ref.at[i // 2, pl.ds(pl.multiple_of((i % 2) * ROWS, ROWS), ROWS), :]

    sums = [jnp.zeros((8, 768), f32)] * 2
    for i in range(512 // ROWS):
        rows = pl.ds(i * ROWS, ROWS)
        grad = halves(d_rows.at[1], i)[...].astype(f32)
        normed = n_buf[rows, :]
        out = norm_backward(grad, normed, i_i2[rows, :], norms[1:2])
        d_h1[rows, :] = out
        halves(d_rows.at[0], i)[...] = out.astype(bf16)
        f_t[:, rows] = out.T.astype(bf16)
        sums[0] = sums[0] + columns(grad * normed)
        sums[1] = sums[1] + columns(grad)
    small[1] = sums[0]
    small[3] = sums[1]
    load(9).start()
    load(2).wait()

    def pair(n, dx):
        return lambda: rounds[n].pair_sum(dx)

    def step(n, at):
        chunk = 3 - n // 2
        return lambda: rounds[n].event(at, o_grads.at[2 * chunk + n % 2])

    def put(n, dx, theirs, value, start):
        block = value.astype(bf16).reshape(4, 2, 96, value.shape[-1])
        stop_at = start + value.shape[-1]
        for half in range(2):
            low, high = max(start, 384 * half), min(stop_at, 384 * half + 384)
            if low < high:
                slot = theirs * (2 * ROUNDS + half) + (1 - theirs) * (2 * n + half)
                held[slot, dx, :, :, :, low - 384 * half : high - 384 * half] = block[
                    :, :, :, low - start : high - start
                ]

    def pushes(n, dx):
        return [
            remote(
                held.at[2 * ROUNDS + half, dx],
                twin.at[(2 * n + half) % 6, dx],
                r_pair.at[2 * n + half, 0, dx],
                r_pair.at[2 * n + half, 1, dx],
                place.device(dk=1),
            )
            for half in range(2)
        ]

    def push(n, dx):
        for copy in pushes(n, dx):
            copy.start()

    def pushed(n, dx):
        for copy in pushes(n, dx):
            copy.wait_send()

    between = {
        5: [step(0, 0), step(1, 0)],
        6: [step(0, 1)],
        8: [step(0, 2), step(1, 1)],
        9: [step(1, 2)],
        10: [step(0, 3), step(1, 3)],
        11: [step(0, 5), step(2, 0), step(3, 0)],
    }
    after = {
        1: [pair(0, 1), pair(1, 1)],
        3: [pair(0, 0), pair(1, 0)],
        5: [pair(2, 1), pair(3, 1)],
        7: [pair(2, 0), pair(3, 0)],
        11: [pair(4, 1), pair(5, 1), pair(4, 0), pair(5, 0)],
    }

    def go(n, plan):
        for at, todo in plan.items():

            @pl.when(n == at)
            def _():
                for item in todo:
                    item()

    def feed(n, carry):
        dx = 1 - n % 4 // 2
        theirs = 1 - n % 2

        @pl.when(n < 11)
        def _():
            fetch(n + 1, 0).start()
            fetch(n + 1, 1).start()

        @pl.when(jnp.logical_and(theirs == 1, n >= 4))
        def _():
            pushed(n // 4 - 1, dx)

        fetch(n, 0).wait()
        fetch(n, 1).wait()
        w = whole(w_buf.at[n % 2])
        hold = kept.at[n % 2]
        d_ffn = d_rows[0].reshape(512, 768)
        d_hidden = dot(d_ffn, w[:, 512:])
        d_gate = (d_hidden * hold[2].astype(f32)).astype(bf16)
        d_up = (d_hidden * hold[1].astype(f32)).astype(bf16)
        d_projected = jnp.concatenate([d_gate, d_up], axis=1)
        put(n // 4, dx, theirs, dot(f_t[...], hold[0]), 512)
        go(n, between)
        put(n // 4, dx, theirs, dot(h1_t[...], d_projected), 0)

        @pl.when(theirs == 1)
        def _():
            push(n // 4, dx)

        go(n, after)
        d_h1[...] += dot(d_projected, w[:, :512], NT)
        return carry

    lax.fori_loop(0, 12, feed, 0)
    load(9).wait()
    load(3).start()
    sums = [jnp.zeros((8, 768), f32)] * 2
    for i in range(512 // ROWS):
        rows = pl.ds(i * ROWS, ROWS)
        grad = d_h1[rows, :]
        normed = n_buf[rows, :]
        out = norm_backward(grad, normed, i_i1[rows, :], norms[0:1])
        d_h1[rows, :] = out
        halves(d_rows.at[1], i)[...] = out.astype(bf16)
        f_t[:, rows] = out.T.astype(bf16)
        sums[0] = sums[0] + columns(grad * normed)
        sums[1] = sums[1] + columns(grad)
    small[0] = sums[0]
    small[2] = sums[1]
    for n in (3, 4, 5, 6, 7, 8, 10):
        load(n).wait()

    small[0] = jnp.concatenate(
        [jnp.sum(small[i], axis=0, keepdims=True) for i in range(4)]
        + [jnp.sum(squares[i], axis=0, keepdims=True) for i in range(4)],
        axis=0,
    )

    def spread(n):
        to = ({"dk": 1}, {"dx": 1}, {"dy": 1}, {"dz": 1}, {"dz": 2}, {"dz": 3})[n]
        return remote(
            small.at[min(n, 3)], small_in.at[n], s_send.at[n], s_recv.at[n], place.device(**to)
        )

    def small_step(n):
        def go():
            if 0 < n < 4:
                spread(n - 1).wait_recv()
                small[n] = small[n - 1] + small_in[n - 1]
            if n < 3:
                spread(n).start()
            if n == 3:
                for at in (3, 4, 5):
                    spread(at).start()
            if n == 4:
                for at in (3, 4, 5):
                    spread(at).wait_recv()
                total = small[3]
                result = jnp.zeros_like(total)
                for at in range(4):
                    back = (place.z - at) % 4
                    term = jnp.where(
                        back == 0,
                        total,
                        jnp.where(
                            back == 1, small_in[3], jnp.where(back == 2, small_in[4], small_in[5])
                        ),
                    )
                    result = result + term
                o_small[...] = result

        return go

    def fetch_heads(n):
        wx, wk = where_heads(n)
        return pltpu.make_async_copy(i_weights.at[0:2, wx, wk], w_buf.at[n % 2], step_sems.at[n % 2, 0])

    def fetch_wo(n):
        wx, wk = where_heads(n)
        return pltpu.make_async_copy(i_wo.at[wx * 2 + wk], wo.at[n % 2], step_sems.at[n % 2, 1])

    fetch_heads(0).start()
    fetch_wo(0).start()
    dq_t[1, pl.ds(HEAD_DIM, HEAD_DIM), :] = jnp.zeros((HEAD_DIM, 512), f32)

    def share(t):
        return remote(
            d_kv.at[t, :, :, :, 1 - place.k], d_kv_in.at[t], kv_send.at[t], kv_recv.at[t], place.device(dk=1)
        )

    beside = {
        (0, 0): [small_step(0), step(0, 4)],
        (0, 1): [step(2, 1)],
        (0, 2): [small_step(1), step(1, 5)],
        (0, 3): [step(2, 2)],
        (0, 4): [small_step(2)],
        (0, 5): [step(3, 2)],
        (1, 0): [small_step(3), step(1, 4), step(3, 1), step(0, 6)],
        (1, 2): [step(2, 3), step(3, 3)],
        (1, 3): [small_step(4), step(2, 5)],
        (1, 5): [step(2, 4), step(1, 6)],
        (2, 0): [step(3, 5), step(3, 4), step(4, 0), step(5, 0)],
        (2, 2): [step(4, 1), step(4, 2), step(5, 2)],
        (2, 4): [step(2, 6)],
        (2, 5): [step(3, 6)],
        (3, 0): [pair(6, 1), pair(7, 1)],
        (3, 1): [step(5, 1)],
        (3, 3): [step(4, 3), step(5, 3)],
        (3, 5): [step(4, 5), step(4, 4)],
        (4, 6): [step(6, 0), step(7, 0), step(5, 5), step(5, 4)],
    }
    first = lax.broadcasted_iota(jnp.int32, (768, 128), 1) < HEAD_DIM

    def stop(i, point):
        for (trip, at), todo in beside.items():
            if at == point:

                @pl.when(i == trip)
                def _():
                    for item in todo:
                        item()

    def attend(n):
        wx, wk = where_heads(n)
        t = wx * 2 + wk
        fetch_heads(n).wait()
        fetch_wo(n).wait()
        left, right = wo[n % 2, 0], wo[n % 2, 1]
        d_attn = d_rows[1].reshape(512, 768)
        d_ctx[0] = dot(d_attn, left).astype(bf16)
        d_ctx[1] = dot(d_attn, right).astype(bf16)
        point = 0
        for spot, (tile, half) in enumerate(HEAD_SPOTS):
            slope = slopes[3 * t + spot]
            key = keys[2 * t + tile].reshape(1024, 128)
            value = values[2 * t + tile].reshape(1024, 128)
            rows = slice(half * HEAD_DIM, (half + 1) * HEAD_DIM)
            key_t = key.astype(f32).T.astype(bf16)[rows]
            product = ctx[2 * t + tile].astype(f32) * d_ctx[tile].astype(f32)
            delta = jnp.sum(product.T[rows], axis=0, keepdims=True)
            for start in range(0, 512, CHUNK):
                cols = pl.ds(start, CHUNK)
                part = lane_half(q[2 * t + tile, cols, :], half)
                grad = lane_half(d_ctx[tile, cols, :], half)
                scores = dot(key, part, NT) - slope * dist[:, cols]
                probs = jnp.exp(scores - lse[t, pl.ds(spot, 1), cols])
                grad_probs = dot(value, grad, NT)
                term_v = dot(probs.astype(bf16), grad)
                grad_scores = (probs * (grad_probs - delta[:, start : start + CHUNK])).astype(bf16)
                term_k = dot(grad_scores, part)
                if half == 0 and start == 0:
                    acc_v[...] = term_v
                    acc_k[...] = term_k
                else:
                    acc_v[...] += term_v
                    acc_k[...] += term_k
                dq_t[tile, rows, cols] = dot(key_t, grad_scores)
                stop(n, point)
                point += 1
            if half == 1 or tile == 1:
                d_kv[t, 0, tile] = acc_k[...].astype(bf16).reshape(2, 2, 256, 128)
                d_kv[t, 1, tile] = acc_v[...].astype(bf16).reshape(2, 2, 256, 128)
        share(t).start()
        for tile in range(2):
            q[2 * t + tile] = (dq_t[tile].T * HEAD_DIM**-0.5).astype(bf16)

    def project(n):
        wx, wk = where_heads(n)
        t = wx * 2 + wk
        dx = 1 - n // 2
        theirs = wk ^ k

        @pl.when(theirs == 1)
        def _():
            pushed(2, dx)

        share(t).wait_recv()
        parts = [q[2 * t], q[2 * t + 1]]
        for kind in range(2):
            for tile in range(2):
                mine = d_kv[t, kind, tile, :, k].reshape(512, 128).astype(f32)
                mine = mine + d_kv_in[t, kind, tile].reshape(512, 128).astype(f32)
                parts.append(mine.astype(bf16))
        d_qkv = jnp.concatenate(parts, axis=1)
        d_wo = dot(f_t[...], jnp.concatenate([ctx[2 * t], ctx[2 * t + 1]], axis=1))
        turned = (swap_halves(d_wo[:, :128]), d_wo[:, :128], swap_halves(d_wo[:, 128:]))
        for kind in range(3):
            d_w = dot(h1_t[...], d_qkv[:, 256 * kind : 256 * kind + 256])
            put(3, dx, theirs, d_w[:, :128], 256 * kind)
            put(3, dx, theirs, jnp.where(first, d_w[:, 128:], turned[kind]), 256 * kind + 128)

        @pl.when(theirs == 1)
        def _():
            push(3, dx)

        d_h1[...] += dot(d_qkv, whole(w_buf.at[n % 2]), NT)

    def heads(n, carry):
        @pl.when(n < 4)
        def _():
            attend(n)

        @pl.when(n > 0)
        def _():
            project(n - 1)

        stop(n, 6)

        @pl.when(n < 3)
        def _():
            fetch_heads(n + 1).start()
            fetch_wo(n + 1).start()

        return carry

    lax.fori_loop(0, 5, heads, 0)
    for i in range(512 // ROWS):
        rows = pl.ds(i * ROWS, ROWS)
        halves(d_rows.at[0], i)[...] = d_h1[rows, :].astype(bf16)
    for n, at in (
        [(6, -1), (7, -1)]
        + [(6, 1), (4, 6), (7, 1), (6, 2), (7, 2), (5, 6), (6, 3), (7, 3)]
        + [(6, 5), (6, 4), (7, 5), (7, 4), (6, 6), (7, 6)]
    ):
        if at < 0:
            rounds[n].pair_sum(0)
        else:
            step(n, at)()
        if (n, at) == (7, -1):
            swap(1).start()
            stay(1).start()
    for n in range(6):
        spread(n).wait_send()
    for r in rounds:
        r.finish()
    for dx in range(2):
        pushed(3, dx)
    for t in range(4):
        share(t).wait_send()
    for n in range(2):
        swap(n).wait()
        stay(n).wait()


def backward(span, slopes, saved):
    f32, bf16 = jnp.float32, jnp.bfloat16
    any_space = pl.BlockSpec(memory_space=pl.ANY)
    vmem = pl.BlockSpec(memory_space=pltpu.VMEM)
    dma = pltpu.SemaphoreType.DMA
    (weights, norms, xs, cot, q, keys, values, ctx, lse, kept, n1, i1, n2, i2, out, squares) = saved[:16]
    h1_t, x_t, dist, wo = saved[16:]
    out = out.reshape(2, 256, 768)
    in_specs = [pl.BlockSpec(memory_space=pltpu.SMEM), any_space, vmem] + [any_space] * 8
    in_specs += [vmem, any_space, vmem, any_space, vmem] + [any_space] * 4
    copies = len(ScatterRound.names)
    return pl.pallas_call(
        partial(backward_kernel, span),
        out_shape=(
            jax.ShapeDtypeStruct((2, 256, 768), bf16),
            jax.ShapeDtypeStruct((2, 256, 768), bf16),
            jax.ShapeDtypeStruct((2 * ROUNDS, 96, 384), f32),
            jax.ShapeDtypeStruct((8, 768), f32),
        ),
        in_specs=in_specs,
        out_specs=(any_space, any_space, vmem, vmem),
        scratch_shapes=[
            pltpu.VMEM((2, 2, 4, 2, 96, 384), bf16),
            pltpu.VMEM((2, 2, 768, 128), bf16),
            pltpu.VMEM((2, 3, 512, 256), bf16),
            pltpu.VMEM((768, 512), bf16),
            pltpu.VMEM((768, 512), bf16),
            pltpu.VMEM((2, 2, 256, 768), bf16),
            pltpu.VMEM((512, 768), f32),
            pltpu.VMEM((512, 768), f32),
            pltpu.VMEM((8, 512, 128), bf16),
            pltpu.VMEM((8, 2, 2, 256, 128), bf16),
            pltpu.VMEM((8, 2, 2, 256, 128), bf16),
            pltpu.VMEM((8, 512, 128), bf16),
            pltpu.VMEM((4, 8, 512), f32),
            pltpu.VMEM((1024, 512), f32),
            pltpu.VMEM((2, 512, 128), bf16),
            pltpu.VMEM((4, 2, 2, 2, 2, 256, 128), bf16),
            pltpu.VMEM((4, 2, 2, 2, 256, 128), bf16),
            pltpu.VMEM((2, 128, 512), f32),
            pltpu.VMEM((1024, 128), f32),
            pltpu.VMEM((1024, 128), f32),
            pltpu.VMEM((2 * ROUNDS + 2, 2, 4, 2, 96, 384), bf16),
            pltpu.VMEM((6, 2, 4, 2, 96, 384), bf16),
            pltpu.VMEM((2 * ROUNDS, 2, 4, 48, 384), bf16),
            pltpu.VMEM((2 * ROUNDS, 4, 2, 48, 384), bf16),
            pltpu.VMEM((2 * ROUNDS, 4, 32, 384), bf16),
            pltpu.VMEM((2 * ROUNDS, 4, 32, 384), bf16),
            pltpu.VMEM((2 * ROUNDS, 3, 64, 384), bf16),
            pltpu.VMEM((2 * ROUNDS, 3, 2, 16, 384), bf16),
            pltpu.VMEM((2 * ROUNDS, 3, 2, 16, 384), bf16),
            pltpu.VMEM((2 * ROUNDS, 2, 16, 384), bf16),
            pltpu.VMEM((4, 8, 768), f32),
            pltpu.VMEM((6, 8, 768), f32),
            dma((11,)),
            dma((2, 2)),
            dma((2 * ROUNDS, copies)),
            dma((2 * ROUNDS, copies)),
            dma((2 * ROUNDS, 2, 2)),
            dma((6,)),
            dma((4,)),
            dma((4,)),
            dma((6,)),
            dma((6,)),
        ],
        compiler_params=pltpu.CompilerParams(
            collective_id=1, has_side_effects=True, vmem_limit_bytes=VMEM_LIMIT
        ),
        name="backward",
    )(
        slopes,
        weights,
        norms,
        cot,
        q,
        keys,
        values,
        ctx,
        lse,
        kept,
        n1,
        i1,
        n2,
        i2,
        out,
        squares,
        h1_t,
        x_t,
        dist,
        wo,
    )


def finish_kernel(
    block, grads, small, lo, gt, o_lo, o_gt, o_qkv, o_wout, o_win, o_down, o_gains, o_biases, rows, sems
):
    def move(n, src, dst):
        return pltpu.make_async_copy(src, dst, sems.at[n])

    move(0, lo, rows.at[0]).start()
    move(1, gt, rows.at[1]).start()
    turned = []

    def tile(i):
        return grads[i // 3, :, i % 3 * 128 : i % 3 * 128 + 128]

    for c in range(3):
        o_qkv[c, :, 0:128] = tile(2 * c)
        o_qkv[c, :, 128:192] = tile(2 * c + 1)[:, :HEAD_DIM]
        turned.append(tile(2 * c + 1).T[HEAD_DIM:])
    o_wout[...] = jnp.concatenate(turned, axis=0)
    move(0, lo, rows.at[0]).wait()
    move(2, rows.at[0], o_lo).start()
    move(1, gt, rows.at[1]).wait()
    move(3, rows.at[1], o_gt).start()
    for r in range(3):
        units = slice(r * 256, (r + 1) * 256)
        o_win[:, 0, units] = grads[2 + 2 * r, :, 0:256]
        o_win[:, 1, r * 256 : r * 256 + 128] = grads[2 + 2 * r, :, 256:384]
        o_win[:, 1, r * 256 + 128 : r * 256 + 256] = grads[3 + 2 * r, :, 0:128]
        o_down[units, :] = grads[3 + 2 * r, :, 128:384].T
    mine = pltpu.roll(small[...], 768 - block[0] * 96, 1)
    o_gains[...] = mine[0:2, 0:96]
    o_biases[...] = mine[2:4, 0:96]
    move(2, rows.at[0], o_lo).wait()
    move(3, rows.at[1], o_gt).wait()


def finish(block, grads, small, lo, gt):
    any_space = pl.BlockSpec(memory_space=pl.ANY)
    vmem = pl.BlockSpec(memory_space=pltpu.VMEM)
    f32 = jnp.float32
    shape = jax.ShapeDtypeStruct
    return pl.pallas_call(
        finish_kernel,
        out_shape=(
            shape(lo.shape, lo.dtype),
            shape(gt.shape, gt.dtype),
            shape((3, 96, 192), f32),
            shape((192, 96), f32),
            shape((96, 2, 768), f32),
            shape((768, 96), f32),
            shape((2, 96), f32),
            shape((2, 96), f32),
        ),
        in_specs=[pl.BlockSpec(memory_space=pltpu.SMEM), vmem, vmem, any_space, any_space],
        out_specs=(any_space, any_space) + (vmem,) * 6,
        scratch_shapes=[pltpu.VMEM((2,) + lo.shape, lo.dtype), pltpu.SemaphoreType.DMA((4,))],
        compiler_params=pltpu.CompilerParams(vmem_limit_bytes=VMEM_LIMIT),
        name="finish",
    )(block, grads, small, lo, gt)


def local(
    tokens,
    segment_ids,
    query_key_value_weight,
    w_out,
    input_weight,
    w_down,
    norm_gains,
    norm_biases,
    cotangent,
):
    f32 = jnp.float32
    shard_rows = query_key_value_weight.shape[1]
    span = 96 // shard_rows
    slopes = jnp.asarray([2.0 ** (-8.0 * (h + 1) / HEADS) for h in range(HEADS)], f32)
    cells = float(lax.axis_size("fsdp") * 2 * 1024 * 768)
    if span == 1:
        raw = (query_key_value_weight, w_out, input_weight, w_down)
        gains, biases = norm_gains, norm_biases
    else:
        count = lax.axis_size("fsdp")
        groups = [list(range(i, i + span)) for i in range(0, count, span)]
        heads = query_key_value_weight.transpose(1, 0, 2).reshape(shard_rows, 3, 3, HEAD_DIM)
        w_out_t = w_out.T.reshape(shard_rows, 3, 1, HEAD_DIM)
        wa = jnp.concatenate([heads, w_out_t], axis=2).reshape(shard_rows, 1, 768)
        gate_up = input_weight.reshape(shard_rows, 2, 3, 256).transpose(0, 2, 1, 3)
        down = w_down.T.reshape(shard_rows, 3, 1, 256)
        wf = jnp.concatenate([gate_up, down], axis=2).reshape(shard_rows, 3, 768)
        shard = jnp.concatenate([wa, wf], axis=1).reshape(shard_rows, 8, 384).transpose(1, 0, 2)
        raw = (lax.all_gather(shard, "fsdp", axis=1, tiled=True, axis_index_groups=groups),)
        gains, biases = (
            lax.all_gather(rows, "fsdp", axis=1, tiled=True, axis_index_groups=groups)
            for rows in (norm_gains, norm_biases)
        )

    saved = forward(span, slopes, raw, gains, biases, tokens, cotangent, segment_ids)
    layer_out, grad_tokens, grads, small = backward(span, slopes, saved)

    if span == 1:
        block = lax.axis_index("fsdp").astype(jnp.int32).reshape(1)
        outs = finish(block, grads, small, layer_out, grad_tokens)
    else:
        grads = lax.psum_scatter(
            grads, "fsdp", scatter_dimension=1, tiled=True, axis_index_groups=groups
        )
        small = lax.psum(small, "fsdp", axis_index_groups=groups)
        grads = grads.reshape(4, 2, shard_rows, 384).transpose(0, 2, 1, 3)
        grads_a = grads[0].reshape(shard_rows, 3, 4, HEAD_DIM)
        grads_f = grads[1:].reshape(3, shard_rows, 3, 256)
        shard_start = lax.axis_index("fsdp") * shard_rows
        mine = lax.dynamic_slice_in_dim(small[:4], shard_start, shard_rows, 1)
        outs = (
            layer_out,
            grad_tokens,
            grads_a[:, :, :3].transpose(1, 0, 2, 3).reshape(3, shard_rows, 192),
            grads_a[:, :, 3].reshape(shard_rows, 192).T,
            grads_f[:, :, :2].transpose(1, 2, 0, 3).reshape(shard_rows, 2, 768),
            grads_f[:, :, 2].transpose(0, 2, 1).reshape(768, shard_rows),
            mine[:2],
            mine[2:],
        )
    return outs + (jnp.sqrt(jnp.sum(small[4:], axis=1) / cells),)


def solution(mesh):
    placed = (
        P("fsdp", "tp", None),
        P("fsdp", None),
        P(None, "fsdp", "tp"),
        P("tp", "fsdp"),
        P("fsdp", None, "tp"),
        P("tp", "fsdp"),
        P(None, "fsdp"),
        P(None, "fsdp"),
        P("fsdp", "tp", None),
    )
    return jax.shard_map(
        local,
        mesh=mesh,
        in_specs=placed,
        out_specs=(
            P("fsdp", "tp", None),
            P("fsdp", "tp", None),
            P(None, "fsdp", "tp"),
            P("tp", "fsdp"),
            P("fsdp", None, "tp"),
            P("tp", "fsdp"),
            P(None, "fsdp"),
            P(None, "fsdp"),
            P(),
        ),
        check_vma=False,
    )
```

```python
from functools import partial

import jax
import jax.numpy as jnp
from jax import lax
from jax.experimental import pallas as pl
from jax.experimental.pallas import tpu as pltpu
from jax.sharding import PartitionSpec as P

HEADS = 12
HEAD_DIM = 64
MESH = pl.DeviceIdType.MESH
VMEM_LIMIT = 63 << 20
norm_eps = 1e-05
ROUNDS = 4
NT = (((1,), (1,)), ((), ()))
NN = (((1,), (0,)), ((), ()))
CHUNK = 256


class Place:
    def __init__(self, span):
        index = lax.axis_index("fsdp")
        shard = lax.axis_index("tp")
        self.span = span
        self.j = index % span
        block = index // span
        self.z = block // 2
        self.y = block % 2
        self.x = shard // 2
        self.k = shard % 2

    def shifted(self, dx=0, dy=0, dz=0, dk=0):
        x = 1 - self.x if dx else self.x
        y = 1 - self.y if dy else self.y
        z = (self.z + dz) % 4 if dz else self.z
        k = 1 - self.k if dk else self.k
        return x, y, z, k

    def device(self, dx=0, dy=0, dz=0, dk=0):
        x, y, z, k = self.shifted(dx, dy, dz, dk)
        return ((z * 2 + y) * self.span + self.j, x * 2 + k)

    def greet(self, offsets):
        barrier = pltpu.get_barrier_semaphore()
        for offset in offsets:
            pl.semaphore_signal(
                barrier, inc=1, device_id=self.device(**offset), device_id_type=MESH
            )
        pl.semaphore_wait(barrier, len(offsets))


ALL_PEERS = ({"dx": 1}, {"dy": 1}, {"dz": 1}, {"dz": 2}, {"dz": 3}, {"dk": 1})


def remote(src, dst, send, recv, device):
    return pltpu.make_async_remote_copy(
        src_ref=src, dst_ref=dst, send_sem=send, recv_sem=recv, device_id=device, device_id_type=MESH
    )


PARTS = {
    "a": pl.ds(0, 32),
    "c": pl.ds(32, 16),
    "ac": pl.ds(0, 48),
    "b": pl.ds(48, 32),
    "d": pl.ds(80, 16),
    "bd": pl.ds(48, 48),
    "": pl.ds(0, 96),
}


def dot(a, b, dims=NN):
    return lax.dot_general(a, b, dims, preferred_element_type=jnp.float32)


class Copies:
    names = ()

    def start(self, *names):
        for name in names:
            self.copy(name).start()

    def wait(self, *names):
        for name in names:
            self.copy(name).wait_recv()

    def finish(self):
        for name in self.names:
            self.copy(name).wait_send()


class GatherRound(Copies):
    names = ("z1", "z2", "z3", "ax", "by", "ay0", "bx0", "ay1", "bx1") + tuple(
        "d%d" % i for i in range(7)
    )
    names += ("cx", "cz1", "cz2", "cz3", "dy", "dz1", "dz2", "dz3")
    lines = {
        "ax": ((0, 0, "a"), {"dx": 1}),
        "by": ((0, 0, "b"), {"dy": 1}),
        "ay0": ((0, 0, "ac"), {"dy": 1}),
        "bx0": ((0, 0, "bd"), {"dx": 1}),
        "ay1": ((1, 0, "ac"), {"dy": 1}),
        "bx1": ((0, 1, "bd"), {"dx": 1}),
        "d0": ((0, 0, ""), {"dk": 1}),
        "d1": ((1, 0, "ac"), {"dk": 1}),
        "d2": ((0, 1, "bd"), {"dk": 1}),
        "d3": ((0, 1, "ac"), {"dk": 1}),
        "d4": ((1, 0, "bd"), {"dk": 1}),
        "d5": ((1, 1, "ac"), {"dk": 1}),
        "d6": ((1, 1, "bd"), {"dk": 1}),
    }
    steps = {
        3: (("ax", "cz1", "cz2", "cz3"), ("ay1", "d1")),
        4: (("by", "dz1", "dz2", "dz3"), ("bx1", "d2")),
        5: (("ay0",), ("d3",)),
        6: (("bx0",), ("d4",)),
        7: (("ay1",), ("d5",)),
        8: (("bx1",), ("d6",)),
    }
    last = 10

    def __init__(self, place, own, out, send, recv, keep):
        self.place, self.own, self.out = place, own, out
        self.send, self.recv, self.keep = send, recv, keep

    def line(self, dx, dy, part):
        x, y, z, k = self.place.shifted(dx, dy)
        return self.out.at[x, k, :, y, PARTS[part], :]

    def copy(self, name):
        place = self.place
        at = self.names.index(name)
        send, recv = self.send.at[at], self.recv.at[at]
        x, y, z, k = place.shifted()
        if name[0] == "z":
            return remote(
                self.own, self.out.at[x, k, z, y], send, recv, place.device(dz=int(name[1]))
            )
        if name in ("cx", "dy"):
            rows = PARTS[name[0]]
            return remote(
                self.own.at[rows, :],
                self.out.at[x, k, z, y, rows, :],
                send,
                recv,
                place.device(**{"d" + name[1]: 1}),
            )
        if name[:2] in ("cz", "dz"):
            x, y, z, k = place.shifted(dx=1) if name[0] == "c" else place.shifted(dy=1)
            ref = self.out.at[x, k, z, y, PARTS[name[0]], :]
            return remote(ref, ref, send, recv, place.device(dz=int(name[2])))
        where, to = self.lines[name]
        ref = self.line(*where)
        return remote(ref, ref, send, recv, place.device(**to))

    def kept(self):
        x, y, z, k = self.place.shifted()
        return pltpu.make_async_copy(self.own, self.out.at[x, k, z, y], self.keep)

    def event(self, n):
        if n == 0:
            self.kept().start()
            self.start("cx", "dy", "z1", "z2", "z3")
        elif n == 1:
            self.wait("cx", "dy")
            self.start("cz1", "cz2", "cz3", "dz1", "dz2", "dz3")
        elif n == 2:
            self.kept().wait()
            self.wait("z1", "z2", "z3")
            self.start("ax", "by", "ay0", "bx0", "d0")
        elif n == 9:
            self.wait("d0", "d2", "d3")
        elif n == 10:
            self.wait("d1", "d4", "d5", "d6")
        else:
            self.wait(*self.steps[n][0])
            self.start(*self.steps[n][1])


class NormGather(Copies):
    names = ("z1", "z2", "z3", "y")

    def __init__(self, place, own, out, send, recv, keep):
        self.place, self.own, self.out = place, own, out
        self.send, self.recv, self.keep = send, recv, keep

    def copy(self, name):
        place = self.place
        at = self.names.index(name)
        send, recv = self.send.at[at], self.recv.at[at]
        if name == "y":
            ref = self.out.at[:, place.y]
            return remote(ref, ref, send, recv, place.device(dy=1))
        return remote(
            self.own, self.out.at[place.z, place.y], send, recv, place.device(dz=int(name[1]))
        )

    def kept(self):
        return pltpu.make_async_copy(self.own, self.out.at[self.place.z, self.place.y], self.keep)


class Events:
    def __init__(self, steps):
        self.steps = list(steps)

    def run(self, count):
        for step in self.steps[:count]:
            step()
        del self.steps[:count]

    def spread(self, trips, points, count):
        total = trips * points
        return self.place(trips, points, {n * total // max(count, 1): 1 for n in range(count)})

    def place(self, trips, points, counts):
        total = trips * points
        slots = [[] for _ in range(total)]
        for number in sorted(counts):
            slots[number] += self.steps[: counts[number]]
            del self.steps[: counts[number]]

        def stop(i, point):
            for trip in range(trips):
                todo = slots[trip * points + point]
                if todo:

                    @pl.when(i == trip)
                    def _():
                        for step in todo:
                            step()

        return stop


def lane_half(tile, half):
    lane = lax.broadcasted_iota(jnp.int32, tile.shape, 1)
    keep = (lane < HEAD_DIM) if half == 0 else (lane >= HEAD_DIM)
    return jnp.where(keep, tile, jnp.zeros_like(tile))


def swap_halves(tile):
    return pltpu.roll(tile.astype(jnp.float32), HEAD_DIM, 1)


def fill_distance(dist, segments, place):
    row = segments[pl.ds(place.x, 1), :].astype(jnp.float32)
    column = jnp.broadcast_to(row, (8, 1024)).T[:, 0:1]
    for s in range(2):
        first = (2 * s + place.k) * 256
        mine = segments[pl.ds(place.x, 1), pl.ds(pl.multiple_of(first, 256), 256)].astype(jnp.float32)
        gap = lax.broadcasted_iota(jnp.int32, (1024, 256), 0) - (
            lax.broadcasted_iota(jnp.int32, (1024, 256), 1) + first
        )
        dist[:, s * 256 : (s + 1) * 256] = jnp.where(
            column == mine, jnp.abs(gap).astype(jnp.float32), 1e30
        )


def pack_attention(raw, shard):
    qkv, w_out = raw[0], raw[1]
    turned = w_out[...].astype(jnp.float32).T
    for c in range(3):
        tiles = (
            qkv[c, :, 0:128],
            jnp.concatenate(
                [
                    qkv[c, :, 128:192].astype(jnp.float32),
                    turned[:, c * HEAD_DIM : (c + 1) * HEAD_DIM],
                ],
                axis=1,
            ).astype(jnp.bfloat16),
        )
        for i in range(2):
            half, at = divmod(2 * c + i, 3)
            shard[half, :, at * 128 : at * 128 + 128] = tiles[i]


def pack_feed(raw, shard):
    w_in, w_down = raw[2:]
    turned = w_down[...].astype(jnp.float32).T.astype(jnp.bfloat16)
    for r in range(3):
        units = slice(r * 256, (r + 1) * 256)
        first = slice(r * 256, r * 256 + 128)
        second = slice(r * 256 + 128, r * 256 + 256)
        shard[2 + 2 * r, :, 0:256] = w_in[:, 0, units]
        shard[2 + 2 * r, :, 256:384] = w_in[:, 1, first]
        shard[3 + 2 * r, :, 0:128] = w_in[:, 1, second]
        shard[3 + 2 * r, :, 128:384] = turned[:, units]


def out_weights(w):
    first = lax.broadcasted_iota(jnp.int32, (768, 128), 1) < HEAD_DIM
    left = jnp.where(first, swap_halves(w[:, 128:256]), w[:, 384:512].astype(jnp.float32))
    right = jnp.where(first, swap_halves(w[:, 640:768]), 0.0)
    return left.astype(jnp.bfloat16), right.astype(jnp.bfloat16)


def whole(ref):
    return jnp.concatenate([ref[i].reshape(768, 384) for i in range(2)], axis=1)


HEAD_SPOTS = ((0, 0), (0, 1), (1, 0))


def norm_stats(value):
    average = jnp.mean(value, axis=-1, keepdims=True)
    centered = value - average
    inv_std = lax.rsqrt(jnp.mean(centered * centered, axis=-1, keepdims=True) + norm_eps)
    return centered * inv_std, inv_std


def norm_backward(grad_val, normed, inv_std, gain_row):
    grad_norm = grad_val * gain_row
    return inv_std * (
        grad_norm
        - jnp.mean(grad_norm, axis=-1, keepdims=True)
        - normed * jnp.mean(grad_norm * normed, axis=-1, keepdims=True)
    )


ROWS = 128


def row_blocks(body):
    def step(i, carry):
        body(pl.ds(pl.multiple_of(i * ROWS, ROWS), ROWS), i)
        return carry

    lax.fori_loop(0, 512 // ROWS, step, 0)


def columns(value):
    return jnp.sum(value.reshape(value.shape[0] // 8, 8, value.shape[1]), axis=0)


def forward_kernel(
    span,
    slopes,
    raw,
    gains,
    biases,
    tok,
    cot,
    segments,
    o_weights,
    o_norms,
    o_x,
    o_cot,
    o_q,
    o_k,
    o_v,
    o_ctx,
    o_lse,
    o_kept,
    o_n1,
    o_i1,
    o_n2,
    o_i2,
    o_out,
    o_squares,
    o_h1_t,
    o_x_t,
    o_dist,
    o_wo,
    shard,
    norm_rows,
    weights,
    norms,
    xs,
    q,
    keys,
    values,
    ctx,
    h1b,
    n1,
    h1_t,
    x_t,
    wo,
    dist,
    out_t,
    acc,
    h1,
    kept,
    g_send,
    g_recv,
    g_keep,
    n_send,
    n_recv,
    n_keep,
    t_sems,
    kv_send,
    kv_recv,
    store_sems,
    kept_sems,
):
    f32, bf16 = jnp.float32, jnp.bfloat16
    place = Place(span)
    x, y, z, k = place.shifted()
    rounds = [
        GatherRound(place, shard.at[r], weights.at[r], g_send.at[r], g_recv.at[r], g_keep.at[r])
        for r in range(2 * ROUNDS)
    ]
    norm_gather = NormGather(place, norm_rows, norms, n_send, n_recv, n_keep)

    def swap(n):
        src, dst = ((tok, xs), (cot, o_cot))[n]
        return remote(
            src.at[1 - place.x],
            dst.at[place.x],
            t_sems.at[3 * n],
            t_sems.at[3 * n + 1],
            place.device(dx=1),
        )

    def stay(n):
        src, dst = ((tok, xs), (cot, o_cot))[n]
        return pltpu.make_async_copy(src.at[place.x], dst.at[place.x], t_sems.at[3 * n + 2])

    def store(n):
        src, dst = (
            (weights.at[0:2], o_weights.at[0:2]),
            (weights.at[2:4], o_weights.at[2:4]),
            (weights.at[4:6], o_weights.at[4:6]),
            (weights.at[6:8], o_weights.at[6:8]),
            (xs, o_x),
            (keys, o_k),
            (values, o_v),
            (q, o_q),
            (ctx, o_ctx),
            (n1, o_n1),
            (h1_t, o_h1_t),
            (x_t, o_x_t),
            (dist, o_dist),
            (wo, o_wo),
        )[n]
        return pltpu.make_async_copy(src, dst, store_sems.at[n])

    if len(raw) > 1:
        pack_attention(raw, shard)
    else:
        shard[...] = raw[0][...]
    place.greet(ALL_PEERS)
    rounds[0].event(0)
    swap(0).start()
    for n in range(2):
        stay(n).start()
    norm_rows[...] = jnp.zeros_like(norm_rows)
    norm_rows[0:2, 0:96] = gains[...].astype(f32)
    norm_rows[2:4, 0:96] = biases[...].astype(f32)
    block = place.z * 2 + place.y
    norm_rows[...] = pltpu.roll(norm_rows[...], block * 96, 1)
    norm_gather.kept().start()
    norm_gather.start("z1", "z2", "z3")
    if len(raw) > 1:
        pack_feed(raw, shard)

    def step(r, n):
        def go():
            rounds[r].event(n)
            if n == GatherRound.last and r % 2:
                store(r // 2).start()

        return go

    stages = {0: 0, 1: 1, 2: 1, 3: 2, 4: 2, 5: 3, 6: 3, 7: 3, 8: 3, 9: 4, 10: 4}
    order = sorted((r + stages[n], r, n) for r in range(2 * ROUNDS) for n in range(11))
    order = [(r, n) for _, r, n in order][1:]
    order = order[: order.index((7, 4)) + 1]
    order += [(7, 5), (6, 9), (7, 9), (7, 6), (7, 7), (7, 8), (6, 10), (7, 10)]
    head_part = order[: order.index((1, 10)) + 1]
    later = [at for at in head_part if at[0] >= 2 and at not in ((2, 0), (2, 1), (2, 2), (3, 0))]
    order = [at for at in head_part if at not in later] + later + order[len(head_part) :]
    begun = order.index((1, 10)) + 1
    beside_heads = order.index((3, 10)) + 1 - begun
    events = Events(step(*at) for at in order)
    events.steps.insert(order.index((7, 4)) + 1, lambda: swap(1).start())

    events.run(1)
    fill_distance(dist, segments, place)
    norm_gather.kept().wait()
    norm_gather.wait("z1", "z2", "z3")
    norm_gather.start("y")
    events.run(begun - 1)
    swap(0).wait_recv()
    stay(0).wait()
    store(4).start()
    for i in range(512 // ROWS):
        rows = pl.ds((i % 2) * ROWS, ROWS)
        x_t[:, i * ROWS : (i + 1) * ROWS] = xs[i // 2, rows, :].astype(f32).T.astype(bf16)
    store(11).start()
    store(12).start()

    def share(t, n):
        ref = (keys, values)[n].at[pl.ds(2 * t, 2), :, place.k]
        return remote(ref, ref, kv_send.at[t, n], kv_recv.at[t, n], place.device(dk=1))

    def project(t, carry):
        w = whole(weights.at[0:2, t // 2, t % 2])
        for s in range(2):
            out = dot(xs[s], w).astype(bf16)
            for i in range(2):
                cols = slice(i * 128, i * 128 + 128)
                q[2 * t + i, pl.ds(s * 256, 256), :] = out[:, cols] * bf16(HEAD_DIM**-0.5)
                keys[2 * t + i, s, k] = out[:, 256 + i * 128 : 384 + i * 128]
                values[2 * t + i, s, k] = out[:, 512 + i * 128 : 640 + i * 128]
        share(t, 0).start()
        share(t, 1).start()
        return carry

    lax.fori_loop(0, 4, project, 0)
    out_t[1, pl.ds(HEAD_DIM, HEAD_DIM), :] = jnp.zeros((HEAD_DIM, 512), f32)
    stop = events.spread(4, 7, beside_heads)

    def attend(t, carry):
        share(t, 0).wait_recv()
        share(t, 1).wait_recv()
        point = 0
        for spot, (tile, half) in enumerate(HEAD_SPOTS):
            slope = slopes[3 * t + spot]
            key = keys[2 * t + tile].reshape(1024, 128)
            rows = slice(half * HEAD_DIM, (half + 1) * HEAD_DIM)
            value_t = values[2 * t + tile].reshape(1024, 128).astype(f32).T.astype(bf16)[rows]
            for start in range(0, 512, CHUNK):
                cols = pl.ds(start, CHUNK)
                part = lane_half(q[2 * t + tile, cols, :], half)
                scores = dot(key, part, NT) - slope * dist[:, cols]
                peak = jnp.max(scores, axis=0, keepdims=True)
                expo = jnp.exp(scores - peak)
                total = jnp.sum(expo, axis=0, keepdims=True)
                out_t[tile, rows, cols] = dot(value_t, expo.astype(bf16)) / total
                o_lse[t, pl.ds(spot, 1), cols] = peak + jnp.log(total)
                stop(t, point)
                point += 1
        for tile in range(2):
            ctx[2 * t + tile] = out_t[tile].T.astype(bf16)
        left, right = out_weights(whole(weights.at[0:2, t // 2, t % 2]))
        wo[t, 0] = left
        wo[t, 1] = right
        mixed = dot(ctx[2 * t], left, NT) + dot(ctx[2 * t + 1], right, NT)

        @pl.when(t == 0)
        def _():
            acc[...] = mixed

        @pl.when(t > 0)
        def _():
            acc[...] += mixed

        stop(t, point)
        return carry

    lax.fori_loop(0, 4, attend, 0)
    for n in (5, 6, 7, 8, 13):
        store(n).start()
    norm_gather.wait("y")
    norm_sum = jnp.sum(norms[...].reshape(8, 8, 768), axis=0)
    o_norms[...] = norm_sum

    def first_norm(rows, i):
        attn = acc[rows, :]
        half = i // 2
        resid = xs[half, pl.ds(pl.multiple_of((i % 2) * ROWS, ROWS), ROWS), :].astype(f32) + attn
        normed, inv = norm_stats(resid)
        value = normed * norm_sum[0:1] + norm_sum[2:3]
        h1[rows, :] = value
        h1b[rows, :] = value.astype(bf16)
        h1_t[:, rows] = value.T.astype(bf16)
        n1[rows, :] = normed
        o_i1[rows, :] = inv
        acc[rows, :] = jnp.zeros_like(attn)
        if_first = jnp.where(i == 0, 0.0, 1.0)
        o_squares[0] = o_squares[0] * if_first + columns(attn * attn)
        o_squares[1] = o_squares[1] * if_first + columns(resid * resid)

    o_squares[...] = jnp.zeros_like(o_squares)
    row_blocks(first_norm)
    store(9).start()
    store(10).start()

    first_part = order.index((5, 10)) - begun - beside_heads
    middle = len(order) - 7 - order.index((5, 10)) - 1
    counts = {}
    for n in range(first_part):
        at = n * 8 // first_part
        counts[at] = counts.get(at, 0) + 1
    counts[8] = 1
    for n in range(middle):
        at = 9 + n * 6 // middle
        counts[at] = counts.get(at, 0) + 1
    counts[16] = 1
    counts[18] = counts[22] = 2
    counts[20] = 3
    stop_f = events.place(12, 2, counts)
    assert not events.steps

    def keep_copy(n):
        at = n // 4 * 4 + (x ^ (n % 4 // 2)) * 2 + (k ^ (n % 2))
        return pltpu.make_async_copy(kept.at[n % 2], o_kept.at[at], kept_sems.at[n % 2])

    def feed(n, carry):
        r = 1 + n // 4
        wx, wk = x ^ (n % 4 // 2), k ^ (n % 2)
        stop_f(n, 0)

        @pl.when(n >= 2)
        def _():
            keep_copy(n - 2).wait()

        ref = weights.at[pl.ds(2 * r, 2), wx, wk]
        for start in range(0, 512, CHUNK):
            rows = pl.ds(start, CHUNK)
            w = whole(ref)
            projected = dot(h1b[rows, :], w[:, :512])
            gate, up = projected[:, :256], projected[:, 256:]
            cdf = 0.5 + 0.5 * lax.erf(gate * (0.5**0.5))
            pdf = jnp.exp(-0.5 * gate * gate) * 0.3989422804014327
            act = gate * cdf
            hidden = (act * up).astype(bf16)
            kept[n % 2, 0, rows, :] = hidden
            kept[n % 2, 1, rows, :] = act.astype(bf16)
            kept[n % 2, 2, rows, :] = ((cdf + gate * pdf) * up).astype(bf16)
            acc[rows, :] += dot(hidden, w[:, 512:], NT)
        keep_copy(n).start()
        stop_f(n, 1)
        return carry

    lax.fori_loop(0, 12, feed, 0)

    def second_norm(rows, i):
        ffn = acc[rows, :]
        resid = h1[rows, :] + ffn
        normed, inv = norm_stats(resid)
        o_out[rows, :] = (normed * norm_sum[1:2] + norm_sum[3:4]).astype(bf16)
        o_n2[rows, :] = normed
        o_i2[rows, :] = inv
        o_squares[2] += columns(ffn * ffn)
        o_squares[3] += columns(resid * resid)

    row_blocks(second_norm)
    for n in (10, 11):
        keep_copy(n).wait()
    for r in rounds:
        r.finish()
    norm_gather.finish()
    for n in range(2):
        swap(n).wait_send()
    swap(1).wait_recv()
    stay(1).wait()
    for t in range(4):
        for n in range(2):
            share(t, n).wait_send()
    for n in range(14):
        store(n).wait()


def forward_refs(span, count, *refs):
    forward_kernel(span, refs[0], refs[1 : 1 + count], *refs[1 + count :])


def forward(span, slopes, raw, gains, biases, tok, cot, segments):
    f32, bf16 = jnp.float32, jnp.bfloat16
    any_space = pl.BlockSpec(memory_space=pl.ANY)
    vmem = pl.BlockSpec(memory_space=pltpu.VMEM)
    outs = (
        ((2 * ROUNDS, 2, 2, 4, 2, 96, 384), bf16, any_space),
        ((8, 768), f32, vmem),
        ((2, 256, 768), bf16, any_space),
        ((2, 256, 768), bf16, any_space),
        ((8, 512, 128), bf16, any_space),
        ((8, 2, 2, 256, 128), bf16, any_space),
        ((8, 2, 2, 256, 128), bf16, any_space),
        ((8, 512, 128), bf16, any_space),
        ((4, 8, 512), f32, vmem),
        ((12, 3, 512, 256), bf16, any_space),
        ((512, 768), f32, any_space),
        ((512, 1), f32, vmem),
        ((512, 768), f32, vmem),
        ((512, 1), f32, vmem),
        ((512, 768), bf16, vmem),
        ((4, 8, 768), f32, vmem),
        ((768, 512), bf16, any_space),
        ((768, 512), bf16, any_space),
        ((1024, 512), f32, any_space),
        ((4, 2, 768, 128), bf16, any_space),
    )
    dma = pltpu.SemaphoreType.DMA
    copies = len(GatherRound.names)
    return pl.pallas_call(
        partial(forward_refs, span, len(raw)),
        out_shape=tuple(jax.ShapeDtypeStruct(s, d) for s, d, _ in outs),
        in_specs=[pl.BlockSpec(memory_space=pltpu.SMEM)]
        + [vmem] * (len(raw) + 2)
        + [any_space, any_space, vmem],
        out_specs=tuple(spec for _, _, spec in outs),
        scratch_shapes=[
            pltpu.VMEM((2 * ROUNDS, 96, 384), bf16),
            pltpu.VMEM((8, 768), f32),
            pltpu.VMEM((2 * ROUNDS, 2, 2, 4, 2, 96, 384), bf16),
            pltpu.VMEM((4, 2, 8, 768), f32),
            pltpu.VMEM((2, 256, 768), bf16),
            pltpu.VMEM((8, 512, 128), bf16),
            pltpu.VMEM((8, 2, 2, 256, 128), bf16),
            pltpu.VMEM((8, 2, 2, 256, 128), bf16),
            pltpu.VMEM((8, 512, 128), bf16),
            pltpu.VMEM((512, 768), bf16),
            pltpu.VMEM((512, 768), f32),
            pltpu.VMEM((768, 512), bf16),
            pltpu.VMEM((768, 512), bf16),
            pltpu.VMEM((4, 2, 768, 128), bf16),
            pltpu.VMEM((1024, 512), f32),
            pltpu.VMEM((2, 128, 512), f32),
            pltpu.VMEM((512, 768), f32),
            pltpu.VMEM((512, 768), f32),
            pltpu.VMEM((2, 3, 512, 256), bf16),
            dma((2 * ROUNDS, copies)),
            dma((2 * ROUNDS, copies)),
            dma((2 * ROUNDS,)),
            dma((4,)),
            dma((4,)),
            dma,
            dma((6,)),
            dma((4, 2)),
            dma((4, 2)),
            dma((14,)),
            dma((2,)),
        ],
        compiler_params=pltpu.CompilerParams(
            collective_id=0, has_side_effects=True, vmem_limit_bytes=VMEM_LIMIT
        ),
        name="forward",
    )(slopes, *raw, gains, biases, tok, cot, segments)


class ScatterRound(Copies):
    names = ("ay1", "bx", "ay0", "ax", "by", "cx", "dy") + tuple(
        part + "z%d" % step for part in "abcd" for step in (1, 2, 3)
    )

    def __init__(self, place, held, twin, stage, landing, send, recv, pair):
        self.place, self.held, self.twin, self.stage = place, held, twin, stage
        self.ay, self.bx, self.ax, self.by, self.z, self.cz, self.dz, self.last = landing
        self.send, self.recv, self.pair = send, recv, pair

    def copy(self, name):
        p, held = self.place, self.held
        at = self.names.index(name)
        a, b, c, d = (PARTS[part] for part in "abcd")
        step = int(name[2]) if name[1] == "z" else 0
        far = (p.z + step) % 4
        ac, bd = PARTS["ac"], PARTS["bd"]
        if name in ("ay1", "ay0"):
            dx = int(name[2])
            src, dst, to = held.at[dx, :, 1 - p.y, ac, :], self.ay.at[dx], {"dy": 1}
        elif name == "bx":
            src, dst, to = held.at[1, :, :, bd, :], self.bx, {"dx": 1}
        elif name == "ax":
            src, dst, to = held.at[1, :, p.y, a, :], self.ax, {"dx": 1}
        elif name == "by":
            src, dst, to = held.at[0, :, 1 - p.y, b, :], self.by, {"dy": 1}
        elif name == "cx":
            src, dst, to = held.at[1, p.z, p.y, c, :], self.last.at[0], {"dx": 1}
        elif name == "dy":
            src, dst, to = held.at[0, p.z, 1 - p.y, d, :], self.last.at[1], {"dy": 1}
        elif name[0] == "c":
            src, dst, to = held.at[:, far, p.y, c, :], self.cz.at[step - 1], {"dz": step}
        elif name[0] == "d":
            src, dst, to = held.at[0, far, :, d, :], self.dz.at[step - 1], {"dz": step}
        else:
            rows = PARTS[name[0]]
            into = pl.ds(0, 32) if name[0] == "a" else pl.ds(32, 32)
            src, dst, to = held.at[0, far, p.y, rows, :], self.z.at[step - 1, into, :], {"dz": step}
        return remote(src, dst, self.send.at[at], self.recv.at[at], p.device(**to))

    def push(self, dx):
        return remote(
            self.stage.at[dx], self.twin.at[dx], self.pair.at[0, dx], self.pair.at[1, dx], self.place.device(dk=1)
        )

    def add(self, ref, *others):
        total = ref[...].astype(jnp.float32)
        for other in others:
            total = total + other[...].astype(jnp.float32)
        ref[...] = total.astype(jnp.bfloat16)

    def pair_sum(self, dx):
        self.push(dx).wait_recv()

        def body(i, carry):
            self.add(self.held.at[dx, i], self.twin.at[dx, i])
            return carry

        lax.fori_loop(0, 4, body, 0)
        if dx:
            self.start("bx", "ay1")
        else:
            self.start("ay0")

    def event(self, n, out=None):
        p, held = self.place, self.held
        a, b, c, d = (PARTS[part] for part in "abcd")
        ac, bd = PARTS["ac"], PARTS["bd"]
        if n == 0:
            self.wait("ay1")
            self.add(held.at[1, :, p.y, ac, :], self.ay.at[1])
            self.start("ax")
        elif n == 1:
            self.wait("bx")
            self.add(held.at[0, :, 1 - p.y, bd, :], self.bx.at[:, 1 - p.y])
            self.start("by")
            self.add(held.at[0, :, p.y, bd, :], self.bx.at[:, p.y])
            self.start("dz1", "dz2", "dz3")
        elif n == 2:
            self.wait("ay0")
            self.add(held.at[0, :, p.y, ac, :], self.ay.at[0])
            self.start("cz1", "cz2", "cz3")
        elif n == 3:
            self.wait("ax")
            self.add(held.at[0, :, p.y, a, :], self.ax)
            self.start("az1", "az2", "az3")
        elif n == 4:
            self.wait("by")
            self.add(held.at[0, :, p.y, b, :], self.by)
            self.start("bz1", "bz2", "bz3")
        elif n == 5:
            self.wait("cz1", "cz2", "cz3", "dz1", "dz2", "dz3")
            self.add(held.at[1, p.z, p.y, c, :], *[self.cz.at[i, 1] for i in range(3)])
            self.start("cx")
            self.add(held.at[0, p.z, 1 - p.y, d, :], *[self.dz.at[i, 1 - p.y] for i in range(3)])
            self.start("dy")
            self.add(held.at[0, p.z, p.y, c, :], *[self.cz.at[i, 0] for i in range(3)])
            self.add(held.at[0, p.z, p.y, d, :], *[self.dz.at[i, p.y] for i in range(3)])
        else:
            self.wait("az1", "az2", "az3", "bz1", "bz2", "bz3", "cx", "dy")
            for rows, others in (
                (a, [self.z.at[i, pl.ds(0, 32), :] for i in range(3)]),
                (b, [self.z.at[i, pl.ds(32, 32), :] for i in range(3)]),
                (c, [self.last.at[0]]),
                (d, [self.last.at[1]]),
            ):
                total = held[0, p.z, p.y, rows, :].astype(jnp.float32)
                for other in others:
                    total = total + other[...].astype(jnp.float32)
                out[rows, :] = total


def backward_kernel(
    span,
    slopes,
    i_weights,
    norms,
    i_cot,
    i_q,
    i_k,
    i_v,
    i_ctx,
    i_lse,
    i_kept,
    i_n1,
    i_i1,
    i_n2,
    i_i2,
    i_out,
    squares,
    i_h1_t,
    i_x_t,
    i_dist,
    i_wo,
    o_out,
    o_tokens,
    o_grads,
    o_small,
    w_buf,
    wo,
    kept,
    h1_t,
    f_t,
    d_rows,
    n_buf,
    d_h1,
    q,
    keys,
    values,
    ctx,
    lse,
    dist,
    d_ctx,
    d_kv,
    d_kv_in,
    dq_t,
    acc_k,
    acc_v,
    held,
    twin,
    land_ay,
    land_bx,
    land_ax,
    land_by,
    land_z,
    land_cz,
    land_dz,
    land_last,
    small,
    small_in,
    load_sems,
    step_sems,
    r_send,
    r_recv,
    r_pair,
    t_sems,
    kv_send,
    kv_recv,
    s_send,
    s_recv,
):
    f32, bf16 = jnp.float32, jnp.bfloat16
    place = Place(span)
    x, y, z, k = place.shifted()
    rounds = [
        ScatterRound(
            place,
            held.at[n],
            twin.at[n % 6],
            held.at[2 * ROUNDS + n % 2],
            [
                ref.at[n]
                for ref in (land_ay, land_bx, land_ax, land_by, land_z, land_cz, land_dz, land_last)
            ],
            r_send.at[n],
            r_recv.at[n],
            r_pair.at[n],
        )
        for n in range(2 * ROUNDS)
    ]

    def load(n):
        src, dst = (
            (i_cot, d_rows.at[1]),
            (i_n2, n_buf),
            (i_h1_t, h1_t),
            (i_x_t, h1_t),
            (i_q, q),
            (i_k, keys),
            (i_v, values),
            (i_ctx, ctx),
            (i_lse, lse),
            (i_n1, n_buf),
            (i_dist, dist),
        )[n]
        return pltpu.make_async_copy(src, dst, load_sems.at[n])

    def where(n):
        return x ^ (1 - n // 2), k ^ (1 - n % 2)

    def where_heads(n):
        return x ^ (1 - n // 2), n % 2

    def fetch(n, part):
        r = 3 - n // 4
        wx, wk = where(n % 4)
        if part == 0:
            return pltpu.make_async_copy(i_weights.at[pl.ds(2 * r, 2), wx, wk], w_buf.at[n % 2], step_sems.at[n % 2, 0])
        return pltpu.make_async_copy(
            i_kept.at[(r - 1) * 4 + wx * 2 + wk], kept.at[n % 2], step_sems.at[n % 2, 1]
        )

    for n in (0, 1):
        load(n).start()
    fetch(0, 0).start()
    fetch(0, 1).start()
    for n in (2, 4, 5, 6, 7, 8, 10):
        load(n).start()
    place.greet(ALL_PEERS)

    def swap(n):
        src, dst = ((i_out, o_out), (d_rows.at[0], o_tokens))[n]
        return remote(
            src.at[1 - place.x],
            dst.at[place.x],
            t_sems.at[3 * n],
            t_sems.at[3 * n + 1],
            place.device(dx=1),
        )

    def stay(n):
        src, dst = ((i_out, o_out), (d_rows.at[0], o_tokens))[n]
        return pltpu.make_async_copy(src.at[place.x], dst.at[place.x], t_sems.at[3 * n + 2])

    swap(0).start()
    stay(0).start()
    load(0).wait()
    load(1).wait()
    small[...] = jnp.zeros_like(small)

    def halves(ref, i):
        return ref.at[i // 2, pl.ds(pl.multiple_of((i % 2) * ROWS, ROWS), ROWS), :]

    sums = [jnp.zeros((8, 768), f32)] * 2
    for i in range(512 // ROWS):
        rows = pl.ds(i * ROWS, ROWS)
        grad = halves(d_rows.at[1], i)[...].astype(f32)
        normed = n_buf[rows, :]
        out = norm_backward(grad, normed, i_i2[rows, :], norms[1:2])
        d_h1[rows, :] = out
        halves(d_rows.at[0], i)[...] = out.astype(bf16)
        f_t[:, rows] = out.T.astype(bf16)
        sums[0] = sums[0] + columns(grad * normed)
        sums[1] = sums[1] + columns(grad)
    small[1] = sums[0]
    small[3] = sums[1]
    load(9).start()
    load(2).wait()

    def pair(n, dx):
        return lambda: rounds[n].pair_sum(dx)

    def step(n, at):
        chunk = 3 - n // 2
        return lambda: rounds[n].event(at, o_grads.at[2 * chunk + n % 2])

    def put(n, dx, theirs, value, start):
        block = value.astype(bf16).reshape(4, 2, 96, value.shape[-1])
        stop_at = start + value.shape[-1]
        for half in range(2):
            low, high = max(start, 384 * half), min(stop_at, 384 * half + 384)
            if low < high:
                slot = theirs * (2 * ROUNDS + half) + (1 - theirs) * (2 * n + half)
                held[slot, dx, :, :, :, low - 384 * half : high - 384 * half] = block[
                    :, :, :, low - start : high - start
                ]

    def pushes(n, dx):
        return [
            remote(
                held.at[2 * ROUNDS + half, dx],
                twin.at[(2 * n + half) % 6, dx],
                r_pair.at[2 * n + half, 0, dx],
                r_pair.at[2 * n + half, 1, dx],
                place.device(dk=1),
            )
            for half in range(2)
        ]

    def push(n, dx):
        for copy in pushes(n, dx):
            copy.start()

    def pushed(n, dx):
        for copy in pushes(n, dx):
            copy.wait_send()

    between = {
        5: [step(0, 0), step(1, 0)],
        6: [step(0, 1)],
        8: [step(0, 2), step(1, 1)],
        9: [step(1, 2)],
        10: [step(0, 3), step(1, 3)],
        11: [step(0, 5), step(2, 0), step(3, 0)],
    }
    after = {
        1: [pair(0, 1), pair(1, 1)],
        3: [pair(0, 0), pair(1, 0)],
        5: [pair(2, 1), pair(3, 1)],
        7: [pair(2, 0), pair(3, 0)],
        11: [pair(4, 1), pair(5, 1), pair(4, 0), pair(5, 0)],
    }

    def go(n, plan):
        for at, todo in plan.items():

            @pl.when(n == at)
            def _():
                for item in todo:
                    item()

    def feed(n, carry):
        dx = 1 - n % 4 // 2
        theirs = 1 - n % 2

        @pl.when(n < 11)
        def _():
            fetch(n + 1, 0).start()
            fetch(n + 1, 1).start()

        @pl.when(jnp.logical_and(theirs == 1, n >= 4))
        def _():
            pushed(n // 4 - 1, dx)

        fetch(n, 0).wait()
        fetch(n, 1).wait()
        w = whole(w_buf.at[n % 2])
        hold = kept.at[n % 2]
        d_ffn = d_rows[0].reshape(512, 768)
        d_hidden = dot(d_ffn, w[:, 512:])
        d_gate = (d_hidden * hold[2].astype(f32)).astype(bf16)
        d_up = (d_hidden * hold[1].astype(f32)).astype(bf16)
        d_projected = jnp.concatenate([d_gate, d_up], axis=1)
        put(n // 4, dx, theirs, dot(f_t[...], hold[0]), 512)
        go(n, between)
        put(n // 4, dx, theirs, dot(h1_t[...], d_projected), 0)

        @pl.when(theirs == 1)
        def _():
            push(n // 4, dx)

        go(n, after)
        d_h1[...] += dot(d_projected, w[:, :512], NT)
        return carry

    lax.fori_loop(0, 12, feed, 0)
    load(9).wait()
    load(3).start()
    sums = [jnp.zeros((8, 768), f32)] * 2
    for i in range(512 // ROWS):
        rows = pl.ds(i * ROWS, ROWS)
        grad = d_h1[rows, :]
        normed = n_buf[rows, :]
        out = norm_backward(grad, normed, i_i1[rows, :], norms[0:1])
        d_h1[rows, :] = out
        halves(d_rows.at[1], i)[...] = out.astype(bf16)
        f_t[:, rows] = out.T.astype(bf16)
        sums[0] = sums[0] + columns(grad * normed)
        sums[1] = sums[1] + columns(grad)
    small[0] = sums[0]
    small[2] = sums[1]
    for n in (3, 4, 5, 6, 7, 8, 10):
        load(n).wait()

    small[0] = jnp.concatenate(
        [jnp.sum(small[i], axis=0, keepdims=True) for i in range(4)]
        + [jnp.sum(squares[i], axis=0, keepdims=True) for i in range(4)],
        axis=0,
    )

    def spread(n):
        to = ({"dk": 1}, {"dx": 1}, {"dy": 1}, {"dz": 1}, {"dz": 2}, {"dz": 3})[n]
        return remote(
            small.at[min(n, 3)], small_in.at[n], s_send.at[n], s_recv.at[n], place.device(**to)
        )

    def small_step(n):
        def go():
            if 0 < n < 4:
                spread(n - 1).wait_recv()
                small[n] = small[n - 1] + small_in[n - 1]
            if n < 3:
                spread(n).start()
            if n == 3:
                for at in (3, 4, 5):
                    spread(at).start()
            if n == 4:
                for at in (3, 4, 5):
                    spread(at).wait_recv()
                total = small[3]
                result = jnp.zeros_like(total)
                for at in range(4):
                    back = (place.z - at) % 4
                    term = jnp.where(
                        back == 0,
                        total,
                        jnp.where(
                            back == 1, small_in[3], jnp.where(back == 2, small_in[4], small_in[5])
                        ),
                    )
                    result = result + term
                o_small[...] = result

        return go

    def fetch_heads(n):
        wx, wk = where_heads(n)
        return pltpu.make_async_copy(i_weights.at[0:2, wx, wk], w_buf.at[n % 2], step_sems.at[n % 2, 0])

    def fetch_wo(n):
        wx, wk = where_heads(n)
        return pltpu.make_async_copy(i_wo.at[wx * 2 + wk], wo.at[n % 2], step_sems.at[n % 2, 1])

    fetch_heads(0).start()
    fetch_wo(0).start()
    dq_t[1, pl.ds(HEAD_DIM, HEAD_DIM), :] = jnp.zeros((HEAD_DIM, 512), f32)

    def share(t):
        return remote(
            d_kv.at[t, :, :, :, 1 - place.k], d_kv_in.at[t], kv_send.at[t], kv_recv.at[t], place.device(dk=1)
        )

    beside = {
        (1, 6): [small_step(0), step(0, 4)],
        (2, 0): [step(2, 1)],
        (2, 1): [small_step(1), step(1, 5)],
        (2, 2): [step(2, 2)],
        (2, 3): [small_step(2)],
        (2, 4): [step(3, 2)],
        (2, 6): [
            small_step(3), step(1, 4), step(3, 1), step(0, 6), pair(6, 1),
            pair(7, 1),
        ],
        (3, 1): [step(2, 3), step(3, 3)],
        (3, 2): [small_step(4), step(2, 5)],
        (3, 4): [step(2, 4), step(1, 6)],
        (3, 6): [
            step(3, 5), step(3, 4), step(4, 0), step(5, 0), step(4, 1),
            step(4, 2), step(5, 2), step(2, 6), step(3, 6), step(5, 1),
            step(4, 3), step(5, 3), step(4, 5), step(4, 4),
        ],
        (4, 6): [step(6, 0), step(7, 0), step(5, 5), step(5, 4)],
    }
    first = lax.broadcasted_iota(jnp.int32, (768, 128), 1) < HEAD_DIM

    def stop(i, point):
        for (trip, at), todo in beside.items():
            if at == point:

                @pl.when(i == trip)
                def _():
                    for item in todo:
                        item()

    def attend(n):
        wx, wk = where_heads(n)
        t = wx * 2 + wk
        fetch_heads(n).wait()
        fetch_wo(n).wait()
        left, right = wo[n % 2, 0], wo[n % 2, 1]
        d_attn = d_rows[1].reshape(512, 768)
        d_ctx[0] = dot(d_attn, left).astype(bf16)
        d_ctx[1] = dot(d_attn, right).astype(bf16)
        point = 0
        for spot, (tile, half) in enumerate(HEAD_SPOTS):
            slope = slopes[3 * t + spot]
            key = keys[2 * t + tile].reshape(1024, 128)
            value = values[2 * t + tile].reshape(1024, 128)
            rows = slice(half * HEAD_DIM, (half + 1) * HEAD_DIM)
            key_t = key.astype(f32).T.astype(bf16)[rows]
            product = ctx[2 * t + tile].astype(f32) * d_ctx[tile].astype(f32)
            delta = jnp.sum(product.T[rows], axis=0, keepdims=True)
            for start in range(0, 512, CHUNK):
                cols = pl.ds(start, CHUNK)
                part = lane_half(q[2 * t + tile, cols, :], half)
                grad = lane_half(d_ctx[tile, cols, :], half)
                scores = dot(key, part, NT) - slope * dist[:, cols]
                probs = jnp.exp(scores - lse[t, pl.ds(spot, 1), cols])
                grad_probs = dot(value, grad, NT)
                term_v = dot(probs.astype(bf16), grad)
                grad_scores = (probs * (grad_probs - delta[:, start : start + CHUNK])).astype(bf16)
                term_k = dot(grad_scores, part)
                if half == 0 and start == 0:
                    acc_v[...] = term_v
                    acc_k[...] = term_k
                else:
                    acc_v[...] += term_v
                    acc_k[...] += term_k
                dq_t[tile, rows, cols] = dot(key_t, grad_scores)
                stop(n, point)
                point += 1
            if half == 1 or tile == 1:
                d_kv[t, 0, tile] = acc_k[...].astype(bf16).reshape(2, 2, 256, 128)
                d_kv[t, 1, tile] = acc_v[...].astype(bf16).reshape(2, 2, 256, 128)
        share(t).start()
        for tile in range(2):
            q[2 * t + tile] = (dq_t[tile].T * HEAD_DIM**-0.5).astype(bf16)

    def project(n):
        wx, wk = where_heads(n)
        t = wx * 2 + wk
        dx = 1 - n // 2
        theirs = wk ^ k

        @pl.when(theirs == 1)
        def _():
            pushed(2, dx)

        share(t).wait_recv()
        parts = [q[2 * t], q[2 * t + 1]]
        for kind in range(2):
            for tile in range(2):
                mine = d_kv[t, kind, tile, :, k].reshape(512, 128).astype(f32)
                mine = mine + d_kv_in[t, kind, tile].reshape(512, 128).astype(f32)
                parts.append(mine.astype(bf16))
        d_qkv = jnp.concatenate(parts, axis=1)
        d_wo = dot(f_t[...], jnp.concatenate([ctx[2 * t], ctx[2 * t + 1]], axis=1))
        turned = (swap_halves(d_wo[:, :128]), d_wo[:, :128], swap_halves(d_wo[:, 128:]))
        for kind in range(3):
            d_w = dot(h1_t[...], d_qkv[:, 256 * kind : 256 * kind + 256])
            put(3, dx, theirs, d_w[:, :128], 256 * kind)
            put(3, dx, theirs, jnp.where(first, d_w[:, 128:], turned[kind]), 256 * kind + 128)

        @pl.when(theirs == 1)
        def _():
            push(3, dx)

        d_h1[...] += dot(d_qkv, whole(w_buf.at[n % 2]), NT)

    def heads(n, carry):
        @pl.when(n < 4)
        def _():
            attend(n)

        @pl.when(n > 0)
        def _():
            project(n - 1)

        stop(n, 6)

        @pl.when(n < 3)
        def _():
            fetch_heads(n + 1).start()
            fetch_wo(n + 1).start()

        return carry

    lax.fori_loop(0, 5, heads, 0)
    for i in range(512 // ROWS):
        rows = pl.ds(i * ROWS, ROWS)
        halves(d_rows.at[0], i)[...] = d_h1[rows, :].astype(bf16)
    for n, at in (
        [(6, -1), (7, -1)]
        + [(6, 1), (4, 6), (7, 1), (6, 2), (7, 2), (5, 6), (6, 3), (7, 3)]
        + [(6, 5), (6, 4), (7, 5), (7, 4), (6, 6), (7, 6)]
    ):
        if at < 0:
            rounds[n].pair_sum(0)
        else:
            step(n, at)()
        if (n, at) == (7, -1):
            swap(1).start()
            stay(1).start()
    for n in range(6):
        spread(n).wait_send()
    for r in rounds:
        r.finish()
    for dx in range(2):
        pushed(3, dx)
    for t in range(4):
        share(t).wait_send()
    for n in range(2):
        swap(n).wait()
        stay(n).wait()


def backward(span, slopes, saved):
    f32, bf16 = jnp.float32, jnp.bfloat16
    any_space = pl.BlockSpec(memory_space=pl.ANY)
    vmem = pl.BlockSpec(memory_space=pltpu.VMEM)
    dma = pltpu.SemaphoreType.DMA
    (weights, norms, xs, cot, q, keys, values, ctx, lse, kept, n1, i1, n2, i2, out, squares) = saved[:16]
    h1_t, x_t, dist, wo = saved[16:]
    out = out.reshape(2, 256, 768)
    in_specs = [pl.BlockSpec(memory_space=pltpu.SMEM), any_space, vmem] + [any_space] * 8
    in_specs += [vmem, any_space, vmem, any_space, vmem] + [any_space] * 4
    copies = len(ScatterRound.names)
    return pl.pallas_call(
        partial(backward_kernel, span),
        out_shape=(
            jax.ShapeDtypeStruct((2, 256, 768), bf16),
            jax.ShapeDtypeStruct((2, 256, 768), bf16),
            jax.ShapeDtypeStruct((2 * ROUNDS, 96, 384), f32),
            jax.ShapeDtypeStruct((8, 768), f32),
        ),
        in_specs=in_specs,
        out_specs=(any_space, any_space, vmem, vmem),
        scratch_shapes=[
            pltpu.VMEM((2, 2, 4, 2, 96, 384), bf16),
            pltpu.VMEM((2, 2, 768, 128), bf16),
            pltpu.VMEM((2, 3, 512, 256), bf16),
            pltpu.VMEM((768, 512), bf16),
            pltpu.VMEM((768, 512), bf16),
            pltpu.VMEM((2, 2, 256, 768), bf16),
            pltpu.VMEM((512, 768), f32),
            pltpu.VMEM((512, 768), f32),
            pltpu.VMEM((8, 512, 128), bf16),
            pltpu.VMEM((8, 2, 2, 256, 128), bf16),
            pltpu.VMEM((8, 2, 2, 256, 128), bf16),
            pltpu.VMEM((8, 512, 128), bf16),
            pltpu.VMEM((4, 8, 512), f32),
            pltpu.VMEM((1024, 512), f32),
            pltpu.VMEM((2, 512, 128), bf16),
            pltpu.VMEM((4, 2, 2, 2, 2, 256, 128), bf16),
            pltpu.VMEM((4, 2, 2, 2, 256, 128), bf16),
            pltpu.VMEM((2, 128, 512), f32),
            pltpu.VMEM((1024, 128), f32),
            pltpu.VMEM((1024, 128), f32),
            pltpu.VMEM((2 * ROUNDS + 2, 2, 4, 2, 96, 384), bf16),
            pltpu.VMEM((6, 2, 4, 2, 96, 384), bf16),
            pltpu.VMEM((2 * ROUNDS, 2, 4, 48, 384), bf16),
            pltpu.VMEM((2 * ROUNDS, 4, 2, 48, 384), bf16),
            pltpu.VMEM((2 * ROUNDS, 4, 32, 384), bf16),
            pltpu.VMEM((2 * ROUNDS, 4, 32, 384), bf16),
            pltpu.VMEM((2 * ROUNDS, 3, 64, 384), bf16),
            pltpu.VMEM((2 * ROUNDS, 3, 2, 16, 384), bf16),
            pltpu.VMEM((2 * ROUNDS, 3, 2, 16, 384), bf16),
            pltpu.VMEM((2 * ROUNDS, 2, 16, 384), bf16),
            pltpu.VMEM((4, 8, 768), f32),
            pltpu.VMEM((6, 8, 768), f32),
            dma((11,)),
            dma((2, 2)),
            dma((2 * ROUNDS, copies)),
            dma((2 * ROUNDS, copies)),
            dma((2 * ROUNDS, 2, 2)),
            dma((6,)),
            dma((4,)),
            dma((4,)),
            dma((6,)),
            dma((6,)),
        ],
        compiler_params=pltpu.CompilerParams(
            collective_id=1, has_side_effects=True, vmem_limit_bytes=VMEM_LIMIT
        ),
        name="backward",
    )(
        slopes,
        weights,
        norms,
        cot,
        q,
        keys,
        values,
        ctx,
        lse,
        kept,
        n1,
        i1,
        n2,
        i2,
        out,
        squares,
        h1_t,
        x_t,
        dist,
        wo,
    )


def finish_kernel(
    block, grads, small, lo, gt, o_lo, o_gt, o_qkv, o_wout, o_win, o_down, o_gains, o_biases, rows, sems
):
    def move(n, src, dst):
        return pltpu.make_async_copy(src, dst, sems.at[n])

    move(0, lo, rows.at[0]).start()
    move(1, gt, rows.at[1]).start()
    turned = []

    def tile(i):
        return grads[i // 3, :, i % 3 * 128 : i % 3 * 128 + 128]

    for c in range(3):
        o_qkv[c, :, 0:128] = tile(2 * c)
        o_qkv[c, :, 128:192] = tile(2 * c + 1)[:, :HEAD_DIM]
        turned.append(tile(2 * c + 1).T[HEAD_DIM:])
    o_wout[...] = jnp.concatenate(turned, axis=0)
    move(0, lo, rows.at[0]).wait()
    move(2, rows.at[0], o_lo).start()
    move(1, gt, rows.at[1]).wait()
    move(3, rows.at[1], o_gt).start()
    for r in range(3):
        units = slice(r * 256, (r + 1) * 256)
        o_win[:, 0, units] = grads[2 + 2 * r, :, 0:256]
        o_win[:, 1, r * 256 : r * 256 + 128] = grads[2 + 2 * r, :, 256:384]
        o_win[:, 1, r * 256 + 128 : r * 256 + 256] = grads[3 + 2 * r, :, 0:128]
        o_down[units, :] = grads[3 + 2 * r, :, 128:384].T
    mine = pltpu.roll(small[...], 768 - block[0] * 96, 1)
    o_gains[...] = mine[0:2, 0:96]
    o_biases[...] = mine[2:4, 0:96]
    move(2, rows.at[0], o_lo).wait()
    move(3, rows.at[1], o_gt).wait()


def finish(block, grads, small, lo, gt):
    any_space = pl.BlockSpec(memory_space=pl.ANY)
    vmem = pl.BlockSpec(memory_space=pltpu.VMEM)
    f32 = jnp.float32
    shape = jax.ShapeDtypeStruct
    return pl.pallas_call(
        finish_kernel,
        out_shape=(
            shape(lo.shape, lo.dtype),
            shape(gt.shape, gt.dtype),
            shape((3, 96, 192), f32),
            shape((192, 96), f32),
            shape((96, 2, 768), f32),
            shape((768, 96), f32),
            shape((2, 96), f32),
            shape((2, 96), f32),
        ),
        in_specs=[pl.BlockSpec(memory_space=pltpu.SMEM), vmem, vmem, any_space, any_space],
        out_specs=(any_space, any_space) + (vmem,) * 6,
        scratch_shapes=[pltpu.VMEM((2,) + lo.shape, lo.dtype), pltpu.SemaphoreType.DMA((4,))],
        compiler_params=pltpu.CompilerParams(vmem_limit_bytes=VMEM_LIMIT),
        name="finish",
    )(block, grads, small, lo, gt)


def local(
    tokens,
    segment_ids,
    query_key_value_weight,
    w_out,
    input_weight,
    w_down,
    norm_gains,
    norm_biases,
    cotangent,
):
    f32 = jnp.float32
    shard_rows = query_key_value_weight.shape[1]
    span = 96 // shard_rows
    slopes = jnp.asarray([2.0 ** (-8.0 * (h + 1) / HEADS) for h in range(HEADS)], f32)
    cells = float(lax.axis_size("fsdp") * 2 * 1024 * 768)
    if span == 1:
        raw = (query_key_value_weight, w_out, input_weight, w_down)
        gains, biases = norm_gains, norm_biases
    else:
        count = lax.axis_size("fsdp")
        groups = [list(range(i, i + span)) for i in range(0, count, span)]
        heads = query_key_value_weight.transpose(1, 0, 2).reshape(shard_rows, 3, 3, HEAD_DIM)
        w_out_t = w_out.T.reshape(shard_rows, 3, 1, HEAD_DIM)
        wa = jnp.concatenate([heads, w_out_t], axis=2).reshape(shard_rows, 1, 768)
        gate_up = input_weight.reshape(shard_rows, 2, 3, 256).transpose(0, 2, 1, 3)
        down = w_down.T.reshape(shard_rows, 3, 1, 256)
        wf = jnp.concatenate([gate_up, down], axis=2).reshape(shard_rows, 3, 768)
        shard = jnp.concatenate([wa, wf], axis=1).reshape(shard_rows, 8, 384).transpose(1, 0, 2)
        raw = (lax.all_gather(shard, "fsdp", axis=1, tiled=True, axis_index_groups=groups),)
        gains, biases = (
            lax.all_gather(rows, "fsdp", axis=1, tiled=True, axis_index_groups=groups)
            for rows in (norm_gains, norm_biases)
        )

    saved = forward(span, slopes, raw, gains, biases, tokens, cotangent, segment_ids)
    layer_out, grad_tokens, grads, small = backward(span, slopes, saved)

    if span == 1:
        block = lax.axis_index("fsdp").astype(jnp.int32).reshape(1)
        outs = finish(block, grads, small, layer_out, grad_tokens)
    else:
        grads = lax.psum_scatter(
            grads, "fsdp", scatter_dimension=1, tiled=True, axis_index_groups=groups
        )
        small = lax.psum(small, "fsdp", axis_index_groups=groups)
        grads = grads.reshape(4, 2, shard_rows, 384).transpose(0, 2, 1, 3)
        grads_a = grads[0].reshape(shard_rows, 3, 4, HEAD_DIM)
        grads_f = grads[1:].reshape(3, shard_rows, 3, 256)
        shard_start = lax.axis_index("fsdp") * shard_rows
        mine = lax.dynamic_slice_in_dim(small[:4], shard_start, shard_rows, 1)
        outs = (
            layer_out,
            grad_tokens,
            grads_a[:, :, :3].transpose(1, 0, 2, 3).reshape(3, shard_rows, 192),
            grads_a[:, :, 3].reshape(shard_rows, 192).T,
            grads_f[:, :, :2].transpose(1, 2, 0, 3).reshape(shard_rows, 2, 768),
            grads_f[:, :, 2].transpose(0, 2, 1).reshape(768, shard_rows),
            mine[:2],
            mine[2:],
        )
    return outs + (jnp.sqrt(jnp.sum(small[4:], axis=1) / cells),)


def solution(mesh):
    placed = (
        P("fsdp", "tp", None),
        P("fsdp", None),
        P(None, "fsdp", "tp"),
        P("tp", "fsdp"),
        P("fsdp", None, "tp"),
        P("tp", "fsdp"),
        P(None, "fsdp"),
        P(None, "fsdp"),
        P("fsdp", "tp", None),
    )
    return jax.shard_map(
        local,
        mesh=mesh,
        in_specs=placed,
        out_specs=(
            P("fsdp", "tp", None),
            P("fsdp", "tp", None),
            P(None, "fsdp", "tp"),
            P("tp", "fsdp"),
            P("fsdp", None, "tp"),
            P("tp", "fsdp"),
            P(None, "fsdp"),
            P(None, "fsdp"),
            P(),
        ),
        check_vma=False,
    )
```

```python
from functools import partial

import jax
import jax.numpy as jnp
from jax import lax
from jax.experimental import pallas as pl
from jax.experimental.pallas import tpu as pltpu
from jax.sharding import PartitionSpec as P

HEADS = 12
HEAD_DIM = 64
MESH = pl.DeviceIdType.MESH
VMEM_LIMIT = 63 << 20
norm_eps = 1e-05
ROUNDS = 4
NT = (((1,), (1,)), ((), ()))
NN = (((1,), (0,)), ((), ()))
CHUNK = 256


class Place:
    def __init__(self, span):
        index = lax.axis_index("fsdp")
        shard = lax.axis_index("tp")
        self.span = span
        self.j = index % span
        block = index // span
        self.z = block // 2
        self.y = block % 2
        self.x = shard // 2
        self.k = shard % 2

    def shifted(self, dx=0, dy=0, dz=0, dk=0):
        x = 1 - self.x if dx else self.x
        y = 1 - self.y if dy else self.y
        z = (self.z + dz) % 4 if dz else self.z
        k = 1 - self.k if dk else self.k
        return x, y, z, k

    def device(self, dx=0, dy=0, dz=0, dk=0):
        x, y, z, k = self.shifted(dx, dy, dz, dk)
        return ((z * 2 + y) * self.span + self.j, x * 2 + k)

    def greet(self, offsets):
        barrier = pltpu.get_barrier_semaphore()
        for offset in offsets:
            pl.semaphore_signal(
                barrier, inc=1, device_id=self.device(**offset), device_id_type=MESH
            )
        pl.semaphore_wait(barrier, len(offsets))


ALL_PEERS = ({"dx": 1}, {"dy": 1}, {"dz": 1}, {"dz": 2}, {"dz": 3}, {"dk": 1})


def remote(src, dst, send, recv, device):
    return pltpu.make_async_remote_copy(
        src_ref=src, dst_ref=dst, send_sem=send, recv_sem=recv, device_id=device, device_id_type=MESH
    )


PARTS = {
    "a": pl.ds(0, 32),
    "c": pl.ds(32, 16),
    "ac": pl.ds(0, 48),
    "b": pl.ds(48, 32),
    "d": pl.ds(80, 16),
    "bd": pl.ds(48, 48),
    "": pl.ds(0, 96),
}


def dot(a, b, dims=NN):
    return lax.dot_general(a, b, dims, preferred_element_type=jnp.float32)


class Copies:
    names = ()

    def start(self, *names):
        for name in names:
            self.copy(name).start()

    def wait(self, *names):
        for name in names:
            self.copy(name).wait_recv()

    def finish(self):
        for name in self.names:
            self.copy(name).wait_send()


class GatherRound(Copies):
    names = ("z1", "z2", "z3", "ax", "by", "ay0", "bx0", "ay1", "bx1") + tuple(
        "d%d" % i for i in range(7)
    )
    names += ("cx", "cz1", "cz2", "cz3", "dy", "dz1", "dz2", "dz3")
    lines = {
        "ax": ((0, 0, "a"), {"dx": 1}),
        "by": ((0, 0, "b"), {"dy": 1}),
        "ay0": ((0, 0, "ac"), {"dy": 1}),
        "bx0": ((0, 0, "bd"), {"dx": 1}),
        "ay1": ((1, 0, "ac"), {"dy": 1}),
        "bx1": ((0, 1, "bd"), {"dx": 1}),
        "d0": ((0, 0, ""), {"dk": 1}),
        "d1": ((1, 0, "ac"), {"dk": 1}),
        "d2": ((0, 1, "bd"), {"dk": 1}),
        "d3": ((0, 1, "ac"), {"dk": 1}),
        "d4": ((1, 0, "bd"), {"dk": 1}),
        "d5": ((1, 1, "ac"), {"dk": 1}),
        "d6": ((1, 1, "bd"), {"dk": 1}),
    }
    steps = {
        3: (("ax", "cz1", "cz2", "cz3"), ("ay1", "d1")),
        4: (("by", "dz1", "dz2", "dz3"), ("bx1", "d2")),
        5: (("ay0",), ("d3",)),
        6: (("bx0",), ("d4",)),
        7: (("ay1",), ("d5",)),
        8: (("bx1",), ("d6",)),
    }
    last = 10

    def __init__(self, place, own, out, send, recv, keep):
        self.place, self.own, self.out = place, own, out
        self.send, self.recv, self.keep = send, recv, keep

    def line(self, dx, dy, part):
        x, y, z, k = self.place.shifted(dx, dy)
        return self.out.at[x, k, :, y, PARTS[part], :]

    def copy(self, name):
        place = self.place
        at = self.names.index(name)
        send, recv = self.send.at[at], self.recv.at[at]
        x, y, z, k = place.shifted()
        if name[0] == "z":
            return remote(
                self.own, self.out.at[x, k, z, y], send, recv, place.device(dz=int(name[1]))
            )
        if name in ("cx", "dy"):
            rows = PARTS[name[0]]
            return remote(
                self.own.at[rows, :],
                self.out.at[x, k, z, y, rows, :],
                send,
                recv,
                place.device(**{"d" + name[1]: 1}),
            )
        if name[:2] in ("cz", "dz"):
            x, y, z, k = place.shifted(dx=1) if name[0] == "c" else place.shifted(dy=1)
            ref = self.out.at[x, k, z, y, PARTS[name[0]], :]
            return remote(ref, ref, send, recv, place.device(dz=int(name[2])))
        where, to = self.lines[name]
        ref = self.line(*where)
        return remote(ref, ref, send, recv, place.device(**to))

    def kept(self):
        x, y, z, k = self.place.shifted()
        return pltpu.make_async_copy(self.own, self.out.at[x, k, z, y], self.keep)

    def event(self, n):
        if n == 0:
            self.kept().start()
            self.start("cx", "dy", "z1", "z2", "z3")
        elif n == 1:
            self.wait("cx", "dy")
            self.start("cz1", "cz2", "cz3", "dz1", "dz2", "dz3")
        elif n == 2:
            self.kept().wait()
            self.wait("z1", "z2", "z3")
            self.start("ax", "by", "ay0", "bx0", "d0")
        elif n == 9:
            self.wait("d0", "d2", "d3")
        elif n == 10:
            self.wait("d1", "d4", "d5", "d6")
        else:
            self.wait(*self.steps[n][0])
            self.start(*self.steps[n][1])


class NormGather(Copies):
    names = ("z1", "z2", "z3", "y")

    def __init__(self, place, own, out, send, recv, keep):
        self.place, self.own, self.out = place, own, out
        self.send, self.recv, self.keep = send, recv, keep

    def copy(self, name):
        place = self.place
        at = self.names.index(name)
        send, recv = self.send.at[at], self.recv.at[at]
        if name == "y":
            ref = self.out.at[:, place.y]
            return remote(ref, ref, send, recv, place.device(dy=1))
        return remote(
            self.own, self.out.at[place.z, place.y], send, recv, place.device(dz=int(name[1]))
        )

    def kept(self):
        return pltpu.make_async_copy(self.own, self.out.at[self.place.z, self.place.y], self.keep)


class Events:
    def __init__(self, steps):
        self.steps = list(steps)

    def run(self, count):
        for step in self.steps[:count]:
            step()
        del self.steps[:count]

    def spread(self, trips, points, count):
        total = trips * points
        return self.place(trips, points, {n * total // max(count, 1): 1 for n in range(count)})

    def place(self, trips, points, counts):
        total = trips * points
        slots = [[] for _ in range(total)]
        for number in sorted(counts):
            slots[number] += self.steps[: counts[number]]
            del self.steps[: counts[number]]

        def stop(i, point):
            for trip in range(trips):
                todo = slots[trip * points + point]
                if todo:

                    @pl.when(i == trip)
                    def _():
                        for step in todo:
                            step()

        return stop


def lane_half(tile, half):
    lane = lax.broadcasted_iota(jnp.int32, tile.shape, 1)
    keep = (lane < HEAD_DIM) if half == 0 else (lane >= HEAD_DIM)
    return jnp.where(keep, tile, jnp.zeros_like(tile))


def swap_halves(tile):
    return pltpu.roll(tile.astype(jnp.float32), HEAD_DIM, 1)


def fill_distance(dist, segments, place):
    row = segments[pl.ds(place.x, 1), :].astype(jnp.float32)
    column = jnp.broadcast_to(row, (8, 1024)).T[:, 0:1]
    for s in range(2):
        first = (2 * s + place.k) * 256
        mine = segments[pl.ds(place.x, 1), pl.ds(pl.multiple_of(first, 256), 256)].astype(jnp.float32)
        gap = lax.broadcasted_iota(jnp.int32, (1024, 256), 0) - (
            lax.broadcasted_iota(jnp.int32, (1024, 256), 1) + first
        )
        dist[:, s * 256 : (s + 1) * 256] = jnp.where(
            column == mine, jnp.abs(gap).astype(jnp.float32), 1e30
        )


def pack_attention(raw, shard):
    qkv, w_out = raw[0], raw[1]
    turned = w_out[...].astype(jnp.float32).T
    for c in range(3):
        tiles = (
            qkv[c, :, 0:128],
            jnp.concatenate(
                [
                    qkv[c, :, 128:192].astype(jnp.float32),
                    turned[:, c * HEAD_DIM : (c + 1) * HEAD_DIM],
                ],
                axis=1,
            ).astype(jnp.bfloat16),
        )
        for i in range(2):
            half, at = divmod(2 * c + i, 3)
            shard[half, :, at * 128 : at * 128 + 128] = tiles[i]


def pack_feed(raw, shard):
    w_in, w_down_t = raw[2:]
    for r in range(3):
        units = slice(r * 256, (r + 1) * 256)
        first = slice(r * 256, r * 256 + 128)
        second = slice(r * 256 + 128, r * 256 + 256)
        shard[2 + 2 * r, :, 0:256] = w_in[:, 0, units]
        shard[2 + 2 * r, :, 256:384] = w_in[:, 1, first]
        shard[3 + 2 * r, :, 0:128] = w_in[:, 1, second]
        shard[3 + 2 * r, :, 128:384] = w_down_t[:, units]


def out_weights(w):
    first = lax.broadcasted_iota(jnp.int32, (768, 128), 1) < HEAD_DIM
    left = jnp.where(first, swap_halves(w[:, 128:256]), w[:, 384:512].astype(jnp.float32))
    right = jnp.where(first, swap_halves(w[:, 640:768]), 0.0)
    return left.astype(jnp.bfloat16), right.astype(jnp.bfloat16)


def whole(ref):
    return jnp.concatenate([ref[i].reshape(768, 384) for i in range(2)], axis=1)


HEAD_SPOTS = ((0, 0), (0, 1), (1, 0))


def norm_stats(value):
    average = jnp.mean(value, axis=-1, keepdims=True)
    centered = value - average
    inv_std = lax.rsqrt(jnp.mean(centered * centered, axis=-1, keepdims=True) + norm_eps)
    return centered * inv_std, inv_std


def norm_backward(grad_val, normed, inv_std, gain_row):
    grad_norm = grad_val * gain_row
    return inv_std * (
        grad_norm
        - jnp.mean(grad_norm, axis=-1, keepdims=True)
        - normed * jnp.mean(grad_norm * normed, axis=-1, keepdims=True)
    )


ROWS = 128


def row_blocks(body):
    def step(i, carry):
        body(pl.ds(pl.multiple_of(i * ROWS, ROWS), ROWS), i)
        return carry

    lax.fori_loop(0, 512 // ROWS, step, 0)


def columns(value):
    return jnp.sum(value.reshape(value.shape[0] // 8, 8, value.shape[1]), axis=0)


def forward_kernel(
    span,
    slopes,
    raw,
    gains,
    biases,
    tok,
    cot,
    segments,
    o_weights,
    o_norms,
    o_x,
    o_cot,
    o_q,
    o_k,
    o_v,
    o_ctx,
    o_lse,
    o_kept,
    o_n1,
    o_i1,
    o_n2,
    o_i2,
    o_out,
    o_squares,
    o_h1_t,
    o_x_t,
    o_dist,
    o_wo,
    shard,
    norm_rows,
    weights,
    norms,
    xs,
    q,
    keys,
    values,
    ctx,
    h1b,
    n1,
    h1_t,
    x_t,
    wo,
    dist,
    out_t,
    acc,
    h1,
    kept,
    g_send,
    g_recv,
    g_keep,
    n_send,
    n_recv,
    n_keep,
    t_sems,
    kv_send,
    kv_recv,
    store_sems,
    kept_sems,
):
    f32, bf16 = jnp.float32, jnp.bfloat16
    place = Place(span)
    x, y, z, k = place.shifted()
    rounds = [
        GatherRound(place, shard.at[r], weights.at[r], g_send.at[r], g_recv.at[r], g_keep.at[r])
        for r in range(2 * ROUNDS)
    ]
    norm_gather = NormGather(place, norm_rows, norms, n_send, n_recv, n_keep)

    def swap(n):
        src, dst = ((tok, xs), (cot, o_cot))[n]
        return remote(
            src.at[1 - place.x],
            dst.at[place.x],
            t_sems.at[3 * n],
            t_sems.at[3 * n + 1],
            place.device(dx=1),
        )

    def stay(n):
        src, dst = ((tok, xs), (cot, o_cot))[n]
        return pltpu.make_async_copy(src.at[place.x], dst.at[place.x], t_sems.at[3 * n + 2])

    def store(n):
        src, dst = (
            (weights.at[0:2], o_weights.at[0:2]),
            (weights.at[2:4], o_weights.at[2:4]),
            (weights.at[4:6], o_weights.at[4:6]),
            (weights.at[6:8], o_weights.at[6:8]),
            (xs, o_x),
            (keys, o_k),
            (values, o_v),
            (q, o_q),
            (ctx, o_ctx),
            (n1, o_n1),
            (h1_t, o_h1_t),
            (x_t, o_x_t),
            (dist, o_dist),
            (wo, o_wo),
        )[n]
        return pltpu.make_async_copy(src, dst, store_sems.at[n])

    if len(raw) > 1:
        pack_attention(raw, shard)
    else:
        shard[...] = raw[0][...]
    place.greet(ALL_PEERS)
    rounds[0].event(0)
    swap(0).start()
    for n in range(2):
        stay(n).start()
    norm_rows[...] = jnp.zeros_like(norm_rows)
    norm_rows[0:2, 0:96] = gains[...].astype(f32)
    norm_rows[2:4, 0:96] = biases[...].astype(f32)
    block = place.z * 2 + place.y
    norm_rows[...] = pltpu.roll(norm_rows[...], block * 96, 1)
    norm_gather.kept().start()
    norm_gather.start("z1", "z2", "z3")
    if len(raw) > 1:
        pack_feed(raw, shard)

    def step(r, n):
        def go():
            rounds[r].event(n)
            if n == GatherRound.last and r % 2:
                store(r // 2).start()

        return go

    stages = {0: 0, 1: 1, 2: 1, 3: 2, 4: 2, 5: 3, 6: 3, 7: 3, 8: 3, 9: 4, 10: 4}
    order = sorted((r + stages[n], r, n) for r in range(2 * ROUNDS) for n in range(11))
    order = [(r, n) for _, r, n in order][1:]
    order = order[: order.index((7, 4)) + 1]
    order += [(7, 5), (6, 9), (7, 9), (7, 6), (7, 7), (7, 8), (6, 10), (7, 10)]
    head_part = order[: order.index((1, 10)) + 1]
    later = [at for at in head_part if at[0] >= 2 and at not in ((2, 0), (2, 1), (2, 2), (3, 0))]
    order = [at for at in head_part if at not in later] + later + order[len(head_part) :]
    begun = order.index((1, 10)) + 1
    beside_heads = order.index((3, 10)) + 1 - begun
    events = Events(step(*at) for at in order)
    events.steps.insert(order.index((7, 4)) + 1, lambda: swap(1).start())

    events.run(1)
    fill_distance(dist, segments, place)
    norm_gather.kept().wait()
    norm_gather.wait("z1", "z2", "z3")
    norm_gather.start("y")
    events.run(begun - 1)
    swap(0).wait_recv()
    stay(0).wait()
    store(4).start()
    for i in range(512 // ROWS):
        rows = pl.ds((i % 2) * ROWS, ROWS)
        x_t[:, i * ROWS : (i + 1) * ROWS] = xs[i // 2, rows, :].astype(f32).T.astype(bf16)
    store(11).start()
    store(12).start()

    def share(t, n):
        ref = (keys, values)[n].at[pl.ds(2 * t, 2), :, place.k]
        return remote(ref, ref, kv_send.at[t, n], kv_recv.at[t, n], place.device(dk=1))

    def project(t, carry):
        w = whole(weights.at[0:2, t // 2, t % 2])
        for s in range(2):
            out = dot(xs[s], w).astype(bf16)
            for i in range(2):
                cols = slice(i * 128, i * 128 + 128)
                q[2 * t + i, pl.ds(s * 256, 256), :] = out[:, cols] * bf16(HEAD_DIM**-0.5)
                keys[2 * t + i, s, k] = out[:, 256 + i * 128 : 384 + i * 128]
                values[2 * t + i, s, k] = out[:, 512 + i * 128 : 640 + i * 128]
        share(t, 0).start()
        share(t, 1).start()
        return carry

    lax.fori_loop(0, 4, project, 0)
    out_t[1, pl.ds(HEAD_DIM, HEAD_DIM), :] = jnp.zeros((HEAD_DIM, 512), f32)
    stop = events.spread(4, 7, beside_heads)

    def attend(t, carry):
        share(t, 0).wait_recv()
        share(t, 1).wait_recv()
        point = 0
        for spot, (tile, half) in enumerate(HEAD_SPOTS):
            slope = slopes[3 * t + spot]
            key = keys[2 * t + tile].reshape(1024, 128)
            rows = slice(half * HEAD_DIM, (half + 1) * HEAD_DIM)
            value_t = values[2 * t + tile].reshape(1024, 128).astype(f32).T.astype(bf16)[rows]
            for start in range(0, 512, CHUNK):
                cols = pl.ds(start, CHUNK)
                part = lane_half(q[2 * t + tile, cols, :], half)
                scores = dot(key, part, NT) - slope * dist[:, cols]
                peak = jnp.max(scores, axis=0, keepdims=True)
                expo = jnp.exp(scores - peak)
                total = jnp.sum(expo, axis=0, keepdims=True)
                out_t[tile, rows, cols] = dot(value_t, expo.astype(bf16)) / total
                o_lse[t, pl.ds(spot, 1), cols] = peak + jnp.log(total)
                stop(t, point)
                point += 1
        for tile in range(2):
            ctx[2 * t + tile] = out_t[tile].T.astype(bf16)
        left, right = out_weights(whole(weights.at[0:2, t // 2, t % 2]))
        wo[t, 0] = left
        wo[t, 1] = right
        mixed = dot(ctx[2 * t], left, NT) + dot(ctx[2 * t + 1], right, NT)

        @pl.when(t == 0)
        def _():
            acc[...] = mixed

        @pl.when(t > 0)
        def _():
            acc[...] += mixed

        stop(t, point)
        return carry

    lax.fori_loop(0, 4, attend, 0)
    for n in (5, 6, 7, 8, 13):
        store(n).start()
    norm_gather.wait("y")
    norm_sum = jnp.sum(norms[...].reshape(8, 8, 768), axis=0)
    o_norms[...] = norm_sum

    def first_norm(rows, i):
        attn = acc[rows, :]
        half = i // 2
        resid = xs[half, pl.ds(pl.multiple_of((i % 2) * ROWS, ROWS), ROWS), :].astype(f32) + attn
        normed, inv = norm_stats(resid)
        value = normed * norm_sum[0:1] + norm_sum[2:3]
        h1[rows, :] = value
        h1b[rows, :] = value.astype(bf16)
        h1_t[:, rows] = value.T.astype(bf16)
        n1[rows, :] = normed
        o_i1[rows, :] = inv
        acc[rows, :] = jnp.zeros_like(attn)
        if_first = jnp.where(i == 0, 0.0, 1.0)
        o_squares[0] = o_squares[0] * if_first + columns(attn * attn)
        o_squares[1] = o_squares[1] * if_first + columns(resid * resid)

    o_squares[...] = jnp.zeros_like(o_squares)
    row_blocks(first_norm)
    store(9).start()
    store(10).start()

    first_part = order.index((5, 10)) - begun - beside_heads
    middle = len(order) - 7 - order.index((5, 10)) - 1
    counts = {}
    for n in range(first_part):
        at = n * 8 // first_part
        counts[at] = counts.get(at, 0) + 1
    counts[8] = 1
    for n in range(middle):
        at = 9 + n * 6 // middle
        counts[at] = counts.get(at, 0) + 1
    counts[16] = 1
    counts[18] = counts[22] = 2
    counts[20] = 3
    stop_f = events.place(12, 2, counts)
    assert not events.steps

    def keep_copy(n):
        at = n // 4 * 4 + (x ^ (n % 4 // 2)) * 2 + (k ^ (n % 2))
        return pltpu.make_async_copy(kept.at[n % 2], o_kept.at[at], kept_sems.at[n % 2])

    def feed(n, carry):
        r = 1 + n // 4
        wx, wk = x ^ (n % 4 // 2), k ^ (n % 2)
        stop_f(n, 0)

        @pl.when(n >= 2)
        def _():
            keep_copy(n - 2).wait()

        ref = weights.at[pl.ds(2 * r, 2), wx, wk]
        for start in range(0, 512, CHUNK):
            rows = pl.ds(start, CHUNK)
            w = whole(ref)
            projected = dot(h1b[rows, :], w[:, :512])
            gate, up = projected[:, :256], projected[:, 256:]
            cdf = 0.5 + 0.5 * lax.erf(gate * (0.5**0.5))
            pdf = jnp.exp(-0.5 * gate * gate) * 0.3989422804014327
            act = gate * cdf
            hidden = (act * up).astype(bf16)
            kept[n % 2, 0, rows, :] = hidden
            kept[n % 2, 1, rows, :] = act.astype(bf16)
            kept[n % 2, 2, rows, :] = ((cdf + gate * pdf) * up).astype(bf16)
            acc[rows, :] += dot(hidden, w[:, 512:], NT)
        keep_copy(n).start()
        stop_f(n, 1)
        return carry

    lax.fori_loop(0, 12, feed, 0)

    def second_norm(rows, i):
        ffn = acc[rows, :]
        resid = h1[rows, :] + ffn
        normed, inv = norm_stats(resid)
        o_out[rows, :] = (normed * norm_sum[1:2] + norm_sum[3:4]).astype(bf16)
        o_n2[rows, :] = normed
        o_i2[rows, :] = inv
        o_squares[2] += columns(ffn * ffn)
        o_squares[3] += columns(resid * resid)

    row_blocks(second_norm)
    for n in (10, 11):
        keep_copy(n).wait()
    for r in rounds:
        r.finish()
    norm_gather.finish()
    for n in range(2):
        swap(n).wait_send()
    swap(1).wait_recv()
    stay(1).wait()
    for t in range(4):
        for n in range(2):
            share(t, n).wait_send()
    for n in range(14):
        store(n).wait()


def forward_refs(span, count, *refs):
    forward_kernel(span, refs[0], refs[1 : 1 + count], *refs[1 + count :])


def forward(span, slopes, raw, gains, biases, tok, cot, segments):
    f32, bf16 = jnp.float32, jnp.bfloat16
    any_space = pl.BlockSpec(memory_space=pl.ANY)
    vmem = pl.BlockSpec(memory_space=pltpu.VMEM)
    outs = (
        ((2 * ROUNDS, 2, 2, 4, 2, 96, 384), bf16, any_space),
        ((8, 768), f32, vmem),
        ((2, 256, 768), bf16, any_space),
        ((2, 256, 768), bf16, any_space),
        ((8, 512, 128), bf16, any_space),
        ((8, 2, 2, 256, 128), bf16, any_space),
        ((8, 2, 2, 256, 128), bf16, any_space),
        ((8, 512, 128), bf16, any_space),
        ((4, 8, 512), f32, vmem),
        ((12, 3, 512, 256), bf16, any_space),
        ((512, 768), f32, any_space),
        ((512, 1), f32, vmem),
        ((512, 768), f32, vmem),
        ((512, 1), f32, vmem),
        ((512, 768), bf16, vmem),
        ((4, 8, 768), f32, vmem),
        ((768, 512), bf16, any_space),
        ((768, 512), bf16, any_space),
        ((1024, 512), f32, any_space),
        ((4, 2, 768, 128), bf16, any_space),
    )
    dma = pltpu.SemaphoreType.DMA
    copies = len(GatherRound.names)
    return pl.pallas_call(
        partial(forward_refs, span, len(raw)),
        out_shape=tuple(jax.ShapeDtypeStruct(s, d) for s, d, _ in outs),
        in_specs=[pl.BlockSpec(memory_space=pltpu.SMEM)]
        + [vmem] * (len(raw) + 2)
        + [any_space, any_space, vmem],
        out_specs=tuple(spec for _, _, spec in outs),
        scratch_shapes=[
            pltpu.VMEM((2 * ROUNDS, 96, 384), bf16),
            pltpu.VMEM((8, 768), f32),
            pltpu.VMEM((2 * ROUNDS, 2, 2, 4, 2, 96, 384), bf16),
            pltpu.VMEM((4, 2, 8, 768), f32),
            pltpu.VMEM((2, 256, 768), bf16),
            pltpu.VMEM((8, 512, 128), bf16),
            pltpu.VMEM((8, 2, 2, 256, 128), bf16),
            pltpu.VMEM((8, 2, 2, 256, 128), bf16),
            pltpu.VMEM((8, 512, 128), bf16),
            pltpu.VMEM((512, 768), bf16),
            pltpu.VMEM((512, 768), f32),
            pltpu.VMEM((768, 512), bf16),
            pltpu.VMEM((768, 512), bf16),
            pltpu.VMEM((4, 2, 768, 128), bf16),
            pltpu.VMEM((1024, 512), f32),
            pltpu.VMEM((2, 128, 512), f32),
            pltpu.VMEM((512, 768), f32),
            pltpu.VMEM((512, 768), f32),
            pltpu.VMEM((2, 3, 512, 256), bf16),
            dma((2 * ROUNDS, copies)),
            dma((2 * ROUNDS, copies)),
            dma((2 * ROUNDS,)),
            dma((4,)),
            dma((4,)),
            dma,
            dma((6,)),
            dma((4, 2)),
            dma((4, 2)),
            dma((14,)),
            dma((2,)),
        ],
        compiler_params=pltpu.CompilerParams(
            collective_id=0, has_side_effects=True, vmem_limit_bytes=VMEM_LIMIT
        ),
        name="forward",
    )(slopes, *raw, gains, biases, tok, cot, segments)


class ScatterRound(Copies):
    names = ("ay1", "bx", "ay0", "ax", "by", "cx", "dy") + tuple(
        part + "z%d" % step for part in "abcd" for step in (1, 2, 3)
    )

    def __init__(self, place, held, twin, stage, landing, send, recv, pair):
        self.place, self.held, self.twin, self.stage = place, held, twin, stage
        self.ay, self.bx, self.ax, self.by, self.z, self.cz, self.dz, self.last = landing
        self.send, self.recv, self.pair = send, recv, pair

    def copy(self, name):
        p, held = self.place, self.held
        at = self.names.index(name)
        a, b, c, d = (PARTS[part] for part in "abcd")
        step = int(name[2]) if name[1] == "z" else 0
        far = (p.z + step) % 4
        ac, bd = PARTS["ac"], PARTS["bd"]
        if name in ("ay1", "ay0"):
            dx = int(name[2])
            src, dst, to = held.at[dx, :, 1 - p.y, ac, :], self.ay.at[dx], {"dy": 1}
        elif name == "bx":
            src, dst, to = held.at[1, :, :, bd, :], self.bx, {"dx": 1}
        elif name == "ax":
            src, dst, to = held.at[1, :, p.y, a, :], self.ax, {"dx": 1}
        elif name == "by":
            src, dst, to = held.at[0, :, 1 - p.y, b, :], self.by, {"dy": 1}
        elif name == "cx":
            src, dst, to = held.at[1, p.z, p.y, c, :], self.last.at[0], {"dx": 1}
        elif name == "dy":
            src, dst, to = held.at[0, p.z, 1 - p.y, d, :], self.last.at[1], {"dy": 1}
        elif name[0] == "c":
            src, dst, to = held.at[:, far, p.y, c, :], self.cz.at[step - 1], {"dz": step}
        elif name[0] == "d":
            src, dst, to = held.at[0, far, :, d, :], self.dz.at[step - 1], {"dz": step}
        else:
            rows = PARTS[name[0]]
            into = pl.ds(0, 32) if name[0] == "a" else pl.ds(32, 32)
            src, dst, to = held.at[0, far, p.y, rows, :], self.z.at[step - 1, into, :], {"dz": step}
        return remote(src, dst, self.send.at[at], self.recv.at[at], p.device(**to))

    def push(self, dx):
        return remote(
            self.stage.at[dx], self.twin.at[dx], self.pair.at[0, dx], self.pair.at[1, dx], self.place.device(dk=1)
        )

    def add(self, ref, *others):
        total = ref[...].astype(jnp.float32)
        for other in others:
            total = total + other[...].astype(jnp.float32)
        ref[...] = total.astype(jnp.bfloat16)

    def pair_sum(self, dx):
        self.push(dx).wait_recv()

        def body(i, carry):
            self.add(self.held.at[dx, i], self.twin.at[dx, i])
            return carry

        lax.fori_loop(0, 4, body, 0)
        if dx:
            self.start("bx", "ay1")
        else:
            self.start("ay0")

    def event(self, n, out=None):
        p, held = self.place, self.held
        a, b, c, d = (PARTS[part] for part in "abcd")
        ac, bd = PARTS["ac"], PARTS["bd"]
        if n == 0:
            self.wait("ay1")
            self.add(held.at[1, :, p.y, ac, :], self.ay.at[1])
            self.start("ax")
        elif n == 1:
            self.wait("bx")
            self.add(held.at[0, :, 1 - p.y, bd, :], self.bx.at[:, 1 - p.y])
            self.start("by")
            self.add(held.at[0, :, p.y, bd, :], self.bx.at[:, p.y])
            self.start("dz1", "dz2", "dz3")
        elif n == 2:
            self.wait("ay0")
            self.add(held.at[0, :, p.y, ac, :], self.ay.at[0])
            self.start("cz1", "cz2", "cz3")
        elif n == 3:
            self.wait("ax")
            self.add(held.at[0, :, p.y, a, :], self.ax)
            self.start("az1", "az2", "az3")
        elif n == 4:
            self.wait("by")
            self.add(held.at[0, :, p.y, b, :], self.by)
            self.start("bz1", "bz2", "bz3")
        elif n == 5:
            self.wait("cz1", "cz2", "cz3", "dz1", "dz2", "dz3")
            self.add(held.at[1, p.z, p.y, c, :], *[self.cz.at[i, 1] for i in range(3)])
            self.start("cx")
            self.add(held.at[0, p.z, 1 - p.y, d, :], *[self.dz.at[i, 1 - p.y] for i in range(3)])
            self.start("dy")
            self.add(held.at[0, p.z, p.y, c, :], *[self.cz.at[i, 0] for i in range(3)])
            self.add(held.at[0, p.z, p.y, d, :], *[self.dz.at[i, p.y] for i in range(3)])
        else:
            self.wait("az1", "az2", "az3", "bz1", "bz2", "bz3", "cx", "dy")
            for rows, others in (
                (a, [self.z.at[i, pl.ds(0, 32), :] for i in range(3)]),
                (b, [self.z.at[i, pl.ds(32, 32), :] for i in range(3)]),
                (c, [self.last.at[0]]),
                (d, [self.last.at[1]]),
            ):
                total = held[0, p.z, p.y, rows, :].astype(jnp.float32)
                for other in others:
                    total = total + other[...].astype(jnp.float32)
                out[rows, :] = total


def backward_kernel(
    span,
    slopes,
    i_weights,
    norms,
    i_cot,
    i_q,
    i_k,
    i_v,
    i_ctx,
    i_lse,
    i_kept,
    i_n1,
    i_i1,
    i_n2,
    i_i2,
    i_out,
    squares,
    i_h1_t,
    i_x_t,
    i_dist,
    i_wo,
    o_out,
    o_tokens,
    o_grads,
    o_small,
    w_buf,
    wo,
    kept,
    h1_t,
    f_t,
    d_rows,
    n_buf,
    d_h1,
    q,
    keys,
    values,
    ctx,
    lse,
    dist,
    d_ctx,
    d_kv,
    d_kv_in,
    dq_t,
    acc_k,
    acc_v,
    held,
    twin,
    land_ay,
    land_bx,
    land_ax,
    land_by,
    land_z,
    land_cz,
    land_dz,
    land_last,
    small,
    small_in,
    load_sems,
    step_sems,
    r_send,
    r_recv,
    r_pair,
    t_sems,
    kv_send,
    kv_recv,
    s_send,
    s_recv,
):
    f32, bf16 = jnp.float32, jnp.bfloat16
    place = Place(span)
    x, y, z, k = place.shifted()
    rounds = [
        ScatterRound(
            place,
            held.at[n],
            twin.at[n % 6],
            held.at[2 * ROUNDS + n % 2],
            [
                ref.at[n]
                for ref in (land_ay, land_bx, land_ax, land_by, land_z, land_cz, land_dz, land_last)
            ],
            r_send.at[n],
            r_recv.at[n],
            r_pair.at[n],
        )
        for n in range(2 * ROUNDS)
    ]

    def load(n):
        src, dst = (
            (i_cot, d_rows.at[1]),
            (i_n2, n_buf),
            (i_h1_t, h1_t),
            (i_x_t, h1_t),
            (i_q, q),
            (i_k, keys),
            (i_v, values),
            (i_ctx, ctx),
            (i_lse, lse),
            (i_n1, n_buf),
            (i_dist, dist),
        )[n]
        return pltpu.make_async_copy(src, dst, load_sems.at[n])

    def where(n):
        return x ^ (1 - n // 2), k ^ (1 - n % 2)

    def where_heads(n):
        return x ^ (1 - n // 2), n % 2

    def fetch(n, part):
        r = 3 - n // 4
        wx, wk = where(n % 4)
        if part == 0:
            return pltpu.make_async_copy(i_weights.at[pl.ds(2 * r, 2), wx, wk], w_buf.at[n % 2], step_sems.at[n % 2, 0])
        return pltpu.make_async_copy(
            i_kept.at[(r - 1) * 4 + wx * 2 + wk], kept.at[n % 2], step_sems.at[n % 2, 1]
        )

    for n in (0, 1):
        load(n).start()
    fetch(0, 0).start()
    fetch(0, 1).start()
    for n in (2, 4, 5, 6, 7, 8, 10):
        load(n).start()
    place.greet(ALL_PEERS)

    def swap(n):
        src, dst = ((i_out, o_out), (d_rows.at[0], o_tokens))[n]
        return remote(
            src.at[1 - place.x],
            dst.at[place.x],
            t_sems.at[3 * n],
            t_sems.at[3 * n + 1],
            place.device(dx=1),
        )

    def stay(n):
        src, dst = ((i_out, o_out), (d_rows.at[0], o_tokens))[n]
        return pltpu.make_async_copy(src.at[place.x], dst.at[place.x], t_sems.at[3 * n + 2])

    swap(0).start()
    stay(0).start()
    load(0).wait()
    load(1).wait()
    small[...] = jnp.zeros_like(small)

    def halves(ref, i):
        return ref.at[i // 2, pl.ds(pl.multiple_of((i % 2) * ROWS, ROWS), ROWS), :]

    sums = [jnp.zeros((8, 768), f32)] * 2
    for i in range(512 // ROWS):
        rows = pl.ds(i * ROWS, ROWS)
        grad = halves(d_rows.at[1], i)[...].astype(f32)
        normed = n_buf[rows, :]
        out = norm_backward(grad, normed, i_i2[rows, :], norms[1:2])
        d_h1[rows, :] = out
        halves(d_rows.at[0], i)[...] = out.astype(bf16)
        f_t[:, rows] = out.T.astype(bf16)
        sums[0] = sums[0] + columns(grad * normed)
        sums[1] = sums[1] + columns(grad)
    small[1] = sums[0]
    small[3] = sums[1]
    load(9).start()
    load(2).wait()

    def pair(n, dx):
        return lambda: rounds[n].pair_sum(dx)

    def step(n, at):
        chunk = 3 - n // 2
        return lambda: rounds[n].event(at, o_grads.at[2 * chunk + n % 2])

    def put(n, dx, theirs, value, start):
        block = value.astype(bf16).reshape(4, 2, 96, value.shape[-1])
        stop_at = start + value.shape[-1]
        for half in range(2):
            low, high = max(start, 384 * half), min(stop_at, 384 * half + 384)
            if low < high:
                slot = theirs * (2 * ROUNDS + half) + (1 - theirs) * (2 * n + half)
                held[slot, dx, :, :, :, low - 384 * half : high - 384 * half] = block[
                    :, :, :, low - start : high - start
                ]

    def pushes(n, dx):
        return [
            remote(
                held.at[2 * ROUNDS + half, dx],
                twin.at[(2 * n + half) % 6, dx],
                r_pair.at[2 * n + half, 0, dx],
                r_pair.at[2 * n + half, 1, dx],
                place.device(dk=1),
            )
            for half in range(2)
        ]

    def push(n, dx):
        for copy in pushes(n, dx):
            copy.start()

    def pushed(n, dx):
        for copy in pushes(n, dx):
            copy.wait_send()

    between = {
        5: [step(0, 0), step(1, 0)],
        6: [step(0, 1)],
        8: [step(0, 2), step(1, 1)],
        9: [step(1, 2)],
        10: [step(0, 3), step(1, 3)],
        11: [step(0, 5), step(2, 0), step(3, 0)],
    }
    after = {
        1: [pair(0, 1), pair(1, 1)],
        3: [pair(0, 0), pair(1, 0)],
        5: [pair(2, 1), pair(3, 1)],
        7: [pair(2, 0), pair(3, 0)],
        11: [pair(4, 1), pair(5, 1), pair(4, 0), pair(5, 0)],
    }

    def go(n, plan):
        for at, todo in plan.items():

            @pl.when(n == at)
            def _():
                for item in todo:
                    item()

    def feed(n, carry):
        dx = 1 - n % 4 // 2
        theirs = 1 - n % 2

        @pl.when(n < 11)
        def _():
            fetch(n + 1, 0).start()
            fetch(n + 1, 1).start()

        @pl.when(jnp.logical_and(theirs == 1, n >= 4))
        def _():
            pushed(n // 4 - 1, dx)

        fetch(n, 0).wait()
        fetch(n, 1).wait()
        w = whole(w_buf.at[n % 2])
        hold = kept.at[n % 2]
        d_ffn = d_rows[0].reshape(512, 768)
        d_hidden = dot(d_ffn, w[:, 512:])
        d_gate = (d_hidden * hold[2].astype(f32)).astype(bf16)
        d_up = (d_hidden * hold[1].astype(f32)).astype(bf16)
        d_projected = jnp.concatenate([d_gate, d_up], axis=1)
        put(n // 4, dx, theirs, dot(f_t[...], hold[0]), 512)
        go(n, between)
        put(n // 4, dx, theirs, dot(h1_t[...], d_projected), 0)

        @pl.when(theirs == 1)
        def _():
            push(n // 4, dx)

        go(n, after)
        d_h1[...] += dot(d_projected, w[:, :512], NT)
        return carry

    lax.fori_loop(0, 12, feed, 0)
    load(9).wait()
    load(3).start()
    sums = [jnp.zeros((8, 768), f32)] * 2
    for i in range(512 // ROWS):
        rows = pl.ds(i * ROWS, ROWS)
        grad = d_h1[rows, :]
        normed = n_buf[rows, :]
        out = norm_backward(grad, normed, i_i1[rows, :], norms[0:1])
        d_h1[rows, :] = out
        halves(d_rows.at[1], i)[...] = out.astype(bf16)
        f_t[:, rows] = out.T.astype(bf16)
        sums[0] = sums[0] + columns(grad * normed)
        sums[1] = sums[1] + columns(grad)
    small[0] = sums[0]
    small[2] = sums[1]
    for n in (3, 4, 5, 6, 7, 8, 10):
        load(n).wait()

    small[0] = jnp.concatenate(
        [jnp.sum(small[i], axis=0, keepdims=True) for i in range(4)]
        + [jnp.sum(squares[i], axis=0, keepdims=True) for i in range(4)],
        axis=0,
    )

    def spread(n):
        to = ({"dk": 1}, {"dx": 1}, {"dy": 1}, {"dz": 1}, {"dz": 2}, {"dz": 3})[n]
        return remote(
            small.at[min(n, 3)], small_in.at[n], s_send.at[n], s_recv.at[n], place.device(**to)
        )

    def small_step(n):
        def go():
            if 0 < n < 4:
                spread(n - 1).wait_recv()
                small[n] = small[n - 1] + small_in[n - 1]
            if n < 3:
                spread(n).start()
            if n == 3:
                for at in (3, 4, 5):
                    spread(at).start()
            if n == 4:
                for at in (3, 4, 5):
                    spread(at).wait_recv()
                total = small[3]
                result = jnp.zeros_like(total)
                for at in range(4):
                    back = (place.z - at) % 4
                    term = jnp.where(
                        back == 0,
                        total,
                        jnp.where(
                            back == 1, small_in[3], jnp.where(back == 2, small_in[4], small_in[5])
                        ),
                    )
                    result = result + term
                o_small[...] = result

        return go

    def fetch_heads(n):
        wx, wk = where_heads(n)
        return pltpu.make_async_copy(i_weights.at[0:2, wx, wk], w_buf.at[n % 2], step_sems.at[n % 2, 0])

    def fetch_wo(n):
        wx, wk = where_heads(n)
        return pltpu.make_async_copy(i_wo.at[wx * 2 + wk], wo.at[n % 2], step_sems.at[n % 2, 1])

    fetch_heads(0).start()
    fetch_wo(0).start()
    dq_t[1, pl.ds(HEAD_DIM, HEAD_DIM), :] = jnp.zeros((HEAD_DIM, 512), f32)

    def share(t):
        return remote(
            d_kv.at[t, :, :, :, 1 - place.k], d_kv_in.at[t], kv_send.at[t], kv_recv.at[t], place.device(dk=1)
        )

    beside = {
        (1, 6): [small_step(0), step(0, 4)],
        (2, 0): [step(2, 1)],
        (2, 1): [small_step(1), step(1, 5)],
        (2, 2): [step(2, 2)],
        (2, 3): [small_step(2)],
        (2, 4): [step(3, 2)],
        (2, 6): [
            small_step(3), step(1, 4), step(3, 1), step(0, 6), pair(6, 1),
            pair(7, 1),
        ],
        (3, 1): [step(2, 3), step(3, 3)],
        (3, 2): [small_step(4), step(2, 5)],
        (3, 4): [step(2, 4), step(1, 6)],
        (3, 6): [
            step(3, 5), step(3, 4), step(4, 0), step(5, 0), step(4, 1),
            step(4, 2), step(5, 2), step(2, 6), step(3, 6), step(5, 1),
            step(4, 3), step(5, 3), step(4, 5), step(4, 4),
        ],
        (4, 6): [step(6, 0), step(7, 0), step(5, 5), step(5, 4)],
    }
    first = lax.broadcasted_iota(jnp.int32, (768, 128), 1) < HEAD_DIM

    def stop(i, point):
        for (trip, at), todo in beside.items():
            if at == point:

                @pl.when(i == trip)
                def _():
                    for item in todo:
                        item()

    def attend(n):
        wx, wk = where_heads(n)
        t = wx * 2 + wk
        fetch_heads(n).wait()
        fetch_wo(n).wait()
        left, right = wo[n % 2, 0], wo[n % 2, 1]
        d_attn = d_rows[1].reshape(512, 768)
        d_ctx[0] = dot(d_attn, left).astype(bf16)
        d_ctx[1] = dot(d_attn, right).astype(bf16)
        point = 0
        for spot, (tile, half) in enumerate(HEAD_SPOTS):
            slope = slopes[3 * t + spot]
            key = keys[2 * t + tile].reshape(1024, 128)
            value = values[2 * t + tile].reshape(1024, 128)
            rows = slice(half * HEAD_DIM, (half + 1) * HEAD_DIM)
            key_t = key.astype(f32).T.astype(bf16)[rows]
            product = ctx[2 * t + tile].astype(f32) * d_ctx[tile].astype(f32)
            delta = jnp.sum(product.T[rows], axis=0, keepdims=True)
            for start in range(0, 512, CHUNK):
                cols = pl.ds(start, CHUNK)
                part = lane_half(q[2 * t + tile, cols, :], half)
                grad = lane_half(d_ctx[tile, cols, :], half)
                scores = dot(key, part, NT) - slope * dist[:, cols]
                probs = jnp.exp(scores - lse[t, pl.ds(spot, 1), cols])
                grad_probs = dot(value, grad, NT)
                term_v = dot(probs.astype(bf16), grad)
                grad_scores = (probs * (grad_probs - delta[:, start : start + CHUNK])).astype(bf16)
                term_k = dot(grad_scores, part)
                if half == 0 and start == 0:
                    acc_v[...] = term_v
                    acc_k[...] = term_k
                else:
                    acc_v[...] += term_v
                    acc_k[...] += term_k
                dq_t[tile, rows, cols] = dot(key_t, grad_scores)
                stop(n, point)
                point += 1
            if half == 1 or tile == 1:
                d_kv[t, 0, tile] = acc_k[...].astype(bf16).reshape(2, 2, 256, 128)
                d_kv[t, 1, tile] = acc_v[...].astype(bf16).reshape(2, 2, 256, 128)
        share(t).start()
        for tile in range(2):
            q[2 * t + tile] = (dq_t[tile].T * HEAD_DIM**-0.5).astype(bf16)

    def project(n):
        wx, wk = where_heads(n)
        t = wx * 2 + wk
        dx = 1 - n // 2
        theirs = wk ^ k

        @pl.when(theirs == 1)
        def _():
            pushed(2, dx)

        share(t).wait_recv()
        parts = [q[2 * t], q[2 * t + 1]]
        for kind in range(2):
            for tile in range(2):
                mine = d_kv[t, kind, tile, :, k].reshape(512, 128).astype(f32)
                mine = mine + d_kv_in[t, kind, tile].reshape(512, 128).astype(f32)
                parts.append(mine.astype(bf16))
        d_qkv = jnp.concatenate(parts, axis=1)
        d_wo = dot(f_t[...], jnp.concatenate([ctx[2 * t], ctx[2 * t + 1]], axis=1))
        turned = (swap_halves(d_wo[:, :128]), d_wo[:, :128], swap_halves(d_wo[:, 128:]))
        for kind in range(3):
            d_w = dot(h1_t[...], d_qkv[:, 256 * kind : 256 * kind + 256])
            put(3, dx, theirs, d_w[:, :128], 256 * kind)
            put(3, dx, theirs, jnp.where(first, d_w[:, 128:], turned[kind]), 256 * kind + 128)

        @pl.when(theirs == 1)
        def _():
            push(3, dx)

        d_h1[...] += dot(d_qkv, whole(w_buf.at[n % 2]), NT)

    def heads(n, carry):
        @pl.when(n < 4)
        def _():
            attend(n)

        @pl.when(n > 0)
        def _():
            project(n - 1)

        stop(n, 6)

        @pl.when(n < 3)
        def _():
            fetch_heads(n + 1).start()
            fetch_wo(n + 1).start()

        return carry

    lax.fori_loop(0, 5, heads, 0)
    for i in range(512 // ROWS):
        rows = pl.ds(i * ROWS, ROWS)
        halves(d_rows.at[0], i)[...] = d_h1[rows, :].astype(bf16)
    for n, at in (
        [(6, -1), (7, -1)]
        + [(6, 1), (4, 6), (7, 1), (6, 2), (7, 2), (5, 6), (6, 3), (7, 3)]
        + [(6, 5), (6, 4), (7, 5), (7, 4), (6, 6), (7, 6)]
    ):
        if at < 0:
            rounds[n].pair_sum(0)
        else:
            step(n, at)()
        if (n, at) == (7, -1):
            swap(1).start()
            stay(1).start()
    for n in range(6):
        spread(n).wait_send()
    for r in rounds:
        r.finish()
    for dx in range(2):
        pushed(3, dx)
    for t in range(4):
        share(t).wait_send()
    for n in range(2):
        swap(n).wait()
        stay(n).wait()


def backward(span, slopes, saved):
    f32, bf16 = jnp.float32, jnp.bfloat16
    any_space = pl.BlockSpec(memory_space=pl.ANY)
    vmem = pl.BlockSpec(memory_space=pltpu.VMEM)
    dma = pltpu.SemaphoreType.DMA
    (weights, norms, xs, cot, q, keys, values, ctx, lse, kept, n1, i1, n2, i2, out, squares) = saved[:16]
    h1_t, x_t, dist, wo = saved[16:]
    out = out.reshape(2, 256, 768)
    in_specs = [pl.BlockSpec(memory_space=pltpu.SMEM), any_space, vmem] + [any_space] * 8
    in_specs += [vmem, any_space, vmem, any_space, vmem] + [any_space] * 4
    copies = len(ScatterRound.names)
    return pl.pallas_call(
        partial(backward_kernel, span),
        out_shape=(
            jax.ShapeDtypeStruct((2, 256, 768), bf16),
            jax.ShapeDtypeStruct((2, 256, 768), bf16),
            jax.ShapeDtypeStruct((2 * ROUNDS, 96, 384), f32),
            jax.ShapeDtypeStruct((8, 768), f32),
        ),
        in_specs=in_specs,
        out_specs=(any_space, any_space, vmem, vmem),
        scratch_shapes=[
            pltpu.VMEM((2, 2, 4, 2, 96, 384), bf16),
            pltpu.VMEM((2, 2, 768, 128), bf16),
            pltpu.VMEM((2, 3, 512, 256), bf16),
            pltpu.VMEM((768, 512), bf16),
            pltpu.VMEM((768, 512), bf16),
            pltpu.VMEM((2, 2, 256, 768), bf16),
            pltpu.VMEM((512, 768), f32),
            pltpu.VMEM((512, 768), f32),
            pltpu.VMEM((8, 512, 128), bf16),
            pltpu.VMEM((8, 2, 2, 256, 128), bf16),
            pltpu.VMEM((8, 2, 2, 256, 128), bf16),
            pltpu.VMEM((8, 512, 128), bf16),
            pltpu.VMEM((4, 8, 512), f32),
            pltpu.VMEM((1024, 512), f32),
            pltpu.VMEM((2, 512, 128), bf16),
            pltpu.VMEM((4, 2, 2, 2, 2, 256, 128), bf16),
            pltpu.VMEM((4, 2, 2, 2, 256, 128), bf16),
            pltpu.VMEM((2, 128, 512), f32),
            pltpu.VMEM((1024, 128), f32),
            pltpu.VMEM((1024, 128), f32),
            pltpu.VMEM((2 * ROUNDS + 2, 2, 4, 2, 96, 384), bf16),
            pltpu.VMEM((6, 2, 4, 2, 96, 384), bf16),
            pltpu.VMEM((2 * ROUNDS, 2, 4, 48, 384), bf16),
            pltpu.VMEM((2 * ROUNDS, 4, 2, 48, 384), bf16),
            pltpu.VMEM((2 * ROUNDS, 4, 32, 384), bf16),
            pltpu.VMEM((2 * ROUNDS, 4, 32, 384), bf16),
            pltpu.VMEM((2 * ROUNDS, 3, 64, 384), bf16),
            pltpu.VMEM((2 * ROUNDS, 3, 2, 16, 384), bf16),
            pltpu.VMEM((2 * ROUNDS, 3, 2, 16, 384), bf16),
            pltpu.VMEM((2 * ROUNDS, 2, 16, 384), bf16),
            pltpu.VMEM((4, 8, 768), f32),
            pltpu.VMEM((6, 8, 768), f32),
            dma((11,)),
            dma((2, 2)),
            dma((2 * ROUNDS, copies)),
            dma((2 * ROUNDS, copies)),
            dma((2 * ROUNDS, 2, 2)),
            dma((6,)),
            dma((4,)),
            dma((4,)),
            dma((6,)),
            dma((6,)),
        ],
        compiler_params=pltpu.CompilerParams(
            collective_id=1, has_side_effects=True, vmem_limit_bytes=VMEM_LIMIT
        ),
        name="backward",
    )(
        slopes,
        weights,
        norms,
        cot,
        q,
        keys,
        values,
        ctx,
        lse,
        kept,
        n1,
        i1,
        n2,
        i2,
        out,
        squares,
        h1_t,
        x_t,
        dist,
        wo,
    )


def finish_kernel(
    block, grads, small, lo, gt, o_lo, o_gt, o_qkv, o_wout, o_win, o_down_t, o_gains, o_biases, rows, sems
):
    def move(n, src, dst):
        return pltpu.make_async_copy(src, dst, sems.at[n])

    move(0, lo, rows.at[0]).start()
    move(1, gt, rows.at[1]).start()
    turned = []

    def tile(i):
        return grads[i // 3, :, i % 3 * 128 : i % 3 * 128 + 128]

    for c in range(3):
        o_qkv[c, :, 0:128] = tile(2 * c)
        o_qkv[c, :, 128:192] = tile(2 * c + 1)[:, :HEAD_DIM]
        turned.append(tile(2 * c + 1).T[HEAD_DIM:])
    o_wout[...] = jnp.concatenate(turned, axis=0)
    move(0, lo, rows.at[0]).wait()
    move(2, rows.at[0], o_lo).start()
    move(1, gt, rows.at[1]).wait()
    move(3, rows.at[1], o_gt).start()
    for r in range(3):
        units = slice(r * 256, (r + 1) * 256)
        o_win[:, 0, units] = grads[2 + 2 * r, :, 0:256]
        o_win[:, 1, r * 256 : r * 256 + 128] = grads[2 + 2 * r, :, 256:384]
        o_win[:, 1, r * 256 + 128 : r * 256 + 256] = grads[3 + 2 * r, :, 0:128]
        o_down_t[:, units] = grads[3 + 2 * r, :, 128:384]
    mine = pltpu.roll(small[...], 768 - block[0] * 96, 1)
    o_gains[...] = mine[0:2, 0:96]
    o_biases[...] = mine[2:4, 0:96]
    move(2, rows.at[0], o_lo).wait()
    move(3, rows.at[1], o_gt).wait()


def finish(block, grads, small, lo, gt):
    any_space = pl.BlockSpec(memory_space=pl.ANY)
    vmem = pl.BlockSpec(memory_space=pltpu.VMEM)
    f32 = jnp.float32
    shape = jax.ShapeDtypeStruct
    return pl.pallas_call(
        finish_kernel,
        out_shape=(
            shape(lo.shape, lo.dtype),
            shape(gt.shape, gt.dtype),
            shape((3, 96, 192), f32),
            shape((192, 96), f32),
            shape((96, 2, 768), f32),
            shape((96, 768), f32),
            shape((2, 96), f32),
            shape((2, 96), f32),
        ),
        in_specs=[pl.BlockSpec(memory_space=pltpu.SMEM), vmem, vmem, any_space, any_space],
        out_specs=(any_space, any_space) + (vmem,) * 6,
        scratch_shapes=[pltpu.VMEM((2,) + lo.shape, lo.dtype), pltpu.SemaphoreType.DMA((4,))],
        compiler_params=pltpu.CompilerParams(vmem_limit_bytes=VMEM_LIMIT),
        name="finish",
    )(block, grads, small, lo, gt)


def local(
    tokens,
    segment_ids,
    query_key_value_weight,
    w_out,
    input_weight,
    w_down,
    norm_gains,
    norm_biases,
    cotangent,
):
    f32 = jnp.float32
    shard_rows = query_key_value_weight.shape[1]
    span = 96 // shard_rows
    slopes = jnp.asarray([2.0 ** (-8.0 * (h + 1) / HEADS) for h in range(HEADS)], f32)
    cells = float(lax.axis_size("fsdp") * 2 * 1024 * 768)
    if span == 1:
        raw = (query_key_value_weight, w_out, input_weight, w_down.T)
        gains, biases = norm_gains, norm_biases
    else:
        count = lax.axis_size("fsdp")
        groups = [list(range(i, i + span)) for i in range(0, count, span)]
        heads = query_key_value_weight.transpose(1, 0, 2).reshape(shard_rows, 3, 3, HEAD_DIM)
        w_out_t = w_out.T.reshape(shard_rows, 3, 1, HEAD_DIM)
        wa = jnp.concatenate([heads, w_out_t], axis=2).reshape(shard_rows, 1, 768)
        gate_up = input_weight.reshape(shard_rows, 2, 3, 256).transpose(0, 2, 1, 3)
        down = w_down.T.reshape(shard_rows, 3, 1, 256)
        wf = jnp.concatenate([gate_up, down], axis=2).reshape(shard_rows, 3, 768)
        shard = jnp.concatenate([wa, wf], axis=1).reshape(shard_rows, 8, 384).transpose(1, 0, 2)
        raw = (lax.all_gather(shard, "fsdp", axis=1, tiled=True, axis_index_groups=groups),)
        gains, biases = (
            lax.all_gather(rows, "fsdp", axis=1, tiled=True, axis_index_groups=groups)
            for rows in (norm_gains, norm_biases)
        )

    saved = forward(span, slopes, raw, gains, biases, tokens, cotangent, segment_ids)
    layer_out, grad_tokens, grads, small = backward(span, slopes, saved)

    if span == 1:
        block = lax.axis_index("fsdp").astype(jnp.int32).reshape(1)
        outs = finish(block, grads, small, layer_out, grad_tokens)
        outs = outs[:5] + (outs[5].T,) + outs[6:]
    else:
        grads = lax.psum_scatter(
            grads, "fsdp", scatter_dimension=1, tiled=True, axis_index_groups=groups
        )
        small = lax.psum(small, "fsdp", axis_index_groups=groups)
        grads = grads.reshape(4, 2, shard_rows, 384).transpose(0, 2, 1, 3)
        grads_a = grads[0].reshape(shard_rows, 3, 4, HEAD_DIM)
        grads_f = grads[1:].reshape(3, shard_rows, 3, 256)
        shard_start = lax.axis_index("fsdp") * shard_rows
        mine = lax.dynamic_slice_in_dim(small[:4], shard_start, shard_rows, 1)
        outs = (
            layer_out,
            grad_tokens,
            grads_a[:, :, :3].transpose(1, 0, 2, 3).reshape(3, shard_rows, 192),
            grads_a[:, :, 3].reshape(shard_rows, 192).T,
            grads_f[:, :, :2].transpose(1, 2, 0, 3).reshape(shard_rows, 2, 768),
            grads_f[:, :, 2].transpose(0, 2, 1).reshape(768, shard_rows),
            mine[:2],
            mine[2:],
        )
    return outs + (jnp.sqrt(jnp.sum(small[4:], axis=1) / cells),)


def solution(mesh):
    placed = (
        P("fsdp", "tp", None),
        P("fsdp", None),
        P(None, "fsdp", "tp"),
        P("tp", "fsdp"),
        P("fsdp", None, "tp"),
        P("tp", "fsdp"),
        P(None, "fsdp"),
        P(None, "fsdp"),
        P("fsdp", "tp", None),
    )
    return jax.shard_map(
        local,
        mesh=mesh,
        in_specs=placed,
        out_specs=(
            P("fsdp", "tp", None),
            P("fsdp", "tp", None),
            P(None, "fsdp", "tp"),
            P("tp", "fsdp"),
            P("fsdp", None, "tp"),
            P("tp", "fsdp"),
            P(None, "fsdp"),
            P(None, "fsdp"),
            P(),
        ),
        check_vma=False,
    )
```

```python
from functools import partial

import jax
import jax.numpy as jnp
from jax import lax
from jax.experimental import pallas as pl
from jax.experimental.pallas import tpu as pltpu
from jax.sharding import PartitionSpec as P

HEADS = 12
HEAD_DIM = 64
MESH = pl.DeviceIdType.MESH
VMEM_LIMIT = 63 << 20
norm_eps = 1e-05
ROUNDS = 4
NT = (((1,), (1,)), ((), ()))
NN = (((1,), (0,)), ((), ()))
CHUNK = 256


class Place:
    def __init__(self, span):
        index = lax.axis_index("fsdp")
        shard = lax.axis_index("tp")
        self.span = span
        self.j = index % span
        block = index // span
        self.z = block // 2
        self.y = block % 2
        self.x = shard // 2
        self.k = shard % 2

    def shifted(self, dx=0, dy=0, dz=0, dk=0):
        x = 1 - self.x if dx else self.x
        y = 1 - self.y if dy else self.y
        z = (self.z + dz) % 4 if dz else self.z
        k = 1 - self.k if dk else self.k
        return x, y, z, k

    def device(self, dx=0, dy=0, dz=0, dk=0):
        x, y, z, k = self.shifted(dx, dy, dz, dk)
        return ((z * 2 + y) * self.span + self.j, x * 2 + k)

    def greet(self, offsets):
        barrier = pltpu.get_barrier_semaphore()
        for offset in offsets:
            pl.semaphore_signal(
                barrier, inc=1, device_id=self.device(**offset), device_id_type=MESH
            )
        pl.semaphore_wait(barrier, len(offsets))


ALL_PEERS = ({"dx": 1}, {"dy": 1}, {"dz": 1}, {"dz": 2}, {"dz": 3}, {"dk": 1})


def remote(src, dst, send, recv, device):
    return pltpu.make_async_remote_copy(
        src_ref=src, dst_ref=dst, send_sem=send, recv_sem=recv, device_id=device, device_id_type=MESH
    )


PARTS = {
    "a": pl.ds(0, 32),
    "c": pl.ds(32, 16),
    "ac": pl.ds(0, 48),
    "b": pl.ds(48, 32),
    "d": pl.ds(80, 16),
    "bd": pl.ds(48, 48),
    "": pl.ds(0, 96),
}


def dot(a, b, dims=NN):
    return lax.dot_general(a, b, dims, preferred_element_type=jnp.float32)


class Copies:
    names = ()

    def start(self, *names):
        for name in names:
            self.copy(name).start()

    def wait(self, *names):
        for name in names:
            self.copy(name).wait_recv()

    def finish(self):
        for name in self.names:
            self.copy(name).wait_send()


class GatherRound(Copies):
    names = ("z1", "z2", "z3", "ax", "by", "ay0", "bx0", "ay1", "bx1") + tuple(
        "d%d" % i for i in range(7)
    )
    names += ("cx", "cz1", "cz2", "cz3", "dy", "dz1", "dz2", "dz3")
    lines = {
        "ax": ((0, 0, "a"), {"dx": 1}),
        "by": ((0, 0, "b"), {"dy": 1}),
        "ay0": ((0, 0, "ac"), {"dy": 1}),
        "bx0": ((0, 0, "bd"), {"dx": 1}),
        "ay1": ((1, 0, "ac"), {"dy": 1}),
        "bx1": ((0, 1, "bd"), {"dx": 1}),
        "d0": ((0, 0, ""), {"dk": 1}),
        "d1": ((1, 0, "ac"), {"dk": 1}),
        "d2": ((0, 1, "bd"), {"dk": 1}),
        "d3": ((0, 1, "ac"), {"dk": 1}),
        "d4": ((1, 0, "bd"), {"dk": 1}),
        "d5": ((1, 1, "ac"), {"dk": 1}),
        "d6": ((1, 1, "bd"), {"dk": 1}),
    }
    steps = {
        3: (("ax", "cz1", "cz2", "cz3"), ("ay1", "d1")),
        4: (("by", "dz1", "dz2", "dz3"), ("bx1", "d2")),
        5: (("ay0",), ("d3",)),
        6: (("bx0",), ("d4",)),
        7: (("ay1",), ("d5",)),
        8: (("bx1",), ("d6",)),
    }
    last = 10

    def __init__(self, place, own, out, send, recv, keep):
        self.place, self.own, self.out = place, own, out
        self.send, self.recv, self.keep = send, recv, keep

    def line(self, dx, dy, part):
        x, y, z, k = self.place.shifted(dx, dy)
        return self.out.at[x, k, :, y, PARTS[part], :]

    def copy(self, name):
        place = self.place
        at = self.names.index(name)
        send, recv = self.send.at[at], self.recv.at[at]
        x, y, z, k = place.shifted()
        if name[0] == "z":
            return remote(
                self.own, self.out.at[x, k, z, y], send, recv, place.device(dz=int(name[1]))
            )
        if name in ("cx", "dy"):
            rows = PARTS[name[0]]
            return remote(
                self.own.at[rows, :],
                self.out.at[x, k, z, y, rows, :],
                send,
                recv,
                place.device(**{"d" + name[1]: 1}),
            )
        if name[:2] in ("cz", "dz"):
            x, y, z, k = place.shifted(dx=1) if name[0] == "c" else place.shifted(dy=1)
            ref = self.out.at[x, k, z, y, PARTS[name[0]], :]
            return remote(ref, ref, send, recv, place.device(dz=int(name[2])))
        where, to = self.lines[name]
        ref = self.line(*where)
        return remote(ref, ref, send, recv, place.device(**to))

    def kept(self):
        x, y, z, k = self.place.shifted()
        return pltpu.make_async_copy(self.own, self.out.at[x, k, z, y], self.keep)

    def event(self, n):
        if n == 0:
            self.kept().start()
            self.start("cx", "dy", "z1", "z2", "z3")
        elif n == 1:
            self.wait("cx", "dy")
            self.start("cz1", "cz2", "cz3", "dz1", "dz2", "dz3")
        elif n == 2:
            self.kept().wait()
            self.wait("z1", "z2", "z3")
            self.start("ax", "by", "ay0", "bx0", "d0")
        elif n == 9:
            self.wait("d0", "d2", "d3")
        elif n == 10:
            self.wait("d1", "d4", "d5", "d6")
        else:
            self.wait(*self.steps[n][0])
            self.start(*self.steps[n][1])


class NormGather(Copies):
    names = ("z1", "z2", "z3", "y")

    def __init__(self, place, own, out, send, recv, keep):
        self.place, self.own, self.out = place, own, out
        self.send, self.recv, self.keep = send, recv, keep

    def copy(self, name):
        place = self.place
        at = self.names.index(name)
        send, recv = self.send.at[at], self.recv.at[at]
        if name == "y":
            ref = self.out.at[:, place.y]
            return remote(ref, ref, send, recv, place.device(dy=1))
        return remote(
            self.own, self.out.at[place.z, place.y], send, recv, place.device(dz=int(name[1]))
        )

    def kept(self):
        return pltpu.make_async_copy(self.own, self.out.at[self.place.z, self.place.y], self.keep)


class Events:
    def __init__(self, steps):
        self.steps = list(steps)

    def run(self, count):
        for step in self.steps[:count]:
            step()
        del self.steps[:count]

    def spread(self, trips, points, count):
        total = trips * points
        return self.place(trips, points, {n * total // max(count, 1): 1 for n in range(count)})

    def place(self, trips, points, counts):
        total = trips * points
        slots = [[] for _ in range(total)]
        for number in sorted(counts):
            slots[number] += self.steps[: counts[number]]
            del self.steps[: counts[number]]

        def stop(i, point):
            for trip in range(trips):
                todo = slots[trip * points + point]
                if todo:

                    @pl.when(i == trip)
                    def _():
                        for step in todo:
                            step()

        return stop


def lane_half(tile, half):
    lane = lax.broadcasted_iota(jnp.int32, tile.shape, 1)
    keep = (lane < HEAD_DIM) if half == 0 else (lane >= HEAD_DIM)
    return jnp.where(keep, tile, jnp.zeros_like(tile))


def swap_halves(tile):
    return pltpu.roll(tile.astype(jnp.float32), HEAD_DIM, 1)


def fill_distance(dist, segments, place):
    row = segments[pl.ds(place.x, 1), :].astype(jnp.float32)
    column = jnp.broadcast_to(row, (8, 1024)).T[:, 0:1]
    for s in range(2):
        first = (2 * s + place.k) * 256
        mine = segments[pl.ds(place.x, 1), pl.ds(pl.multiple_of(first, 256), 256)].astype(jnp.float32)
        gap = lax.broadcasted_iota(jnp.int32, (1024, 256), 0) - (
            lax.broadcasted_iota(jnp.int32, (1024, 256), 1) + first
        )
        dist[:, s * 256 : (s + 1) * 256] = jnp.where(
            column == mine, jnp.abs(gap).astype(jnp.float32), 1e30
        )


def pack_attention(raw, shard):
    qkv, w_out = raw[0], raw[1]
    turned = w_out[...].astype(jnp.float32).T
    for c in range(3):
        tiles = (
            qkv[c, :, 0:128],
            jnp.concatenate(
                [
                    qkv[c, :, 128:192].astype(jnp.float32),
                    turned[:, c * HEAD_DIM : (c + 1) * HEAD_DIM],
                ],
                axis=1,
            ).astype(jnp.bfloat16),
        )
        for i in range(2):
            half, at = divmod(2 * c + i, 3)
            shard[half, :, at * 128 : at * 128 + 128] = tiles[i]


def pack_feed(raw, shard):
    w_in, w_down_t = raw[2:]
    for r in range(3):
        units = slice(r * 256, (r + 1) * 256)
        first = slice(r * 256, r * 256 + 128)
        second = slice(r * 256 + 128, r * 256 + 256)
        shard[2 + 2 * r, :, 0:256] = w_in[:, 0, units]
        shard[2 + 2 * r, :, 256:384] = w_in[:, 1, first]
        shard[3 + 2 * r, :, 0:128] = w_in[:, 1, second]
        shard[3 + 2 * r, :, 128:384] = w_down_t[:, units]


def out_weights(w):
    first = lax.broadcasted_iota(jnp.int32, (768, 128), 1) < HEAD_DIM
    left = jnp.where(first, swap_halves(w[:, 128:256]), w[:, 384:512].astype(jnp.float32))
    right = jnp.where(first, swap_halves(w[:, 640:768]), 0.0)
    return left.astype(jnp.bfloat16), right.astype(jnp.bfloat16)


def whole(ref):
    return jnp.concatenate([ref[i].reshape(768, 384) for i in range(2)], axis=1)


HEAD_SPOTS = ((0, 0), (0, 1), (1, 0))


def norm_stats(value):
    average = jnp.mean(value, axis=-1, keepdims=True)
    centered = value - average
    inv_std = lax.rsqrt(jnp.mean(centered * centered, axis=-1, keepdims=True) + norm_eps)
    return centered * inv_std, inv_std


def norm_backward(grad_val, normed, inv_std, gain_row):
    grad_norm = grad_val * gain_row
    return inv_std * (
        grad_norm
        - jnp.mean(grad_norm, axis=-1, keepdims=True)
        - normed * jnp.mean(grad_norm * normed, axis=-1, keepdims=True)
    )


ROWS = 128


def row_blocks(body):
    def step(i, carry):
        body(pl.ds(pl.multiple_of(i * ROWS, ROWS), ROWS), i)
        return carry

    lax.fori_loop(0, 512 // ROWS, step, 0)


def columns(value):
    return jnp.sum(value.reshape(value.shape[0] // 8, 8, value.shape[1]), axis=0)


def forward_kernel(
    span,
    slopes,
    raw,
    gains,
    biases,
    tok,
    cot,
    segments,
    o_weights,
    o_norms,
    o_x,
    o_cot,
    o_q,
    o_k,
    o_v,
    o_ctx,
    o_lse,
    o_kept,
    o_n1,
    o_i1,
    o_n2,
    o_i2,
    o_out,
    o_squares,
    o_h1_t,
    o_x_t,
    o_dist,
    o_wo,
    shard,
    norm_rows,
    weights,
    norms,
    xs,
    q,
    keys,
    values,
    ctx,
    h1b,
    n1,
    h1_t,
    x_t,
    wo,
    dist,
    out_t,
    acc,
    h1,
    kept,
    g_send,
    g_recv,
    g_keep,
    n_send,
    n_recv,
    n_keep,
    t_sems,
    kv_send,
    kv_recv,
    store_sems,
    kept_sems,
):
    f32, bf16 = jnp.float32, jnp.bfloat16
    place = Place(span)
    x, y, z, k = place.shifted()
    rounds = [
        GatherRound(place, shard.at[r], weights.at[r], g_send.at[r], g_recv.at[r], g_keep.at[r])
        for r in range(2 * ROUNDS)
    ]
    norm_gather = NormGather(place, norm_rows, norms, n_send, n_recv, n_keep)

    def swap(n):
        src, dst = ((tok, xs), (cot, o_cot))[n]
        return remote(
            src.at[1 - place.x],
            dst.at[place.x],
            t_sems.at[3 * n],
            t_sems.at[3 * n + 1],
            place.device(dx=1),
        )

    def stay(n):
        src, dst = ((tok, xs), (cot, o_cot))[n]
        return pltpu.make_async_copy(src.at[place.x], dst.at[place.x], t_sems.at[3 * n + 2])

    def store(n):
        src, dst = (
            (weights.at[0:2], o_weights.at[0:2]),
            (weights.at[2:4], o_weights.at[2:4]),
            (weights.at[4:6], o_weights.at[4:6]),
            (weights.at[6:8], o_weights.at[6:8]),
            (xs, o_x),
            (keys, o_k),
            (values, o_v),
            (q, o_q),
            (ctx, o_ctx),
            (n1, o_n1),
            (h1_t, o_h1_t),
            (x_t, o_x_t),
            (dist, o_dist),
            (wo, o_wo),
        )[n]
        return pltpu.make_async_copy(src, dst, store_sems.at[n])

    if len(raw) > 1:
        pack_attention(raw, shard)
    else:
        shard[...] = raw[0][...]
    place.greet(ALL_PEERS)
    rounds[0].event(0)
    swap(0).start()
    for n in range(2):
        stay(n).start()
    norm_rows[...] = jnp.zeros_like(norm_rows)
    norm_rows[0:2, 0:96] = gains[...].astype(f32)
    norm_rows[2:4, 0:96] = biases[...].astype(f32)
    block = place.z * 2 + place.y
    norm_rows[...] = pltpu.roll(norm_rows[...], block * 96, 1)
    norm_gather.kept().start()
    norm_gather.start("z1", "z2", "z3")
    if len(raw) > 1:
        pack_feed(raw, shard)

    def step(r, n):
        def go():
            rounds[r].event(n)
            if n == GatherRound.last and r % 2:
                store(r // 2).start()

        return go

    stages = {0: 0, 1: 1, 2: 1, 3: 2, 4: 2, 5: 3, 6: 3, 7: 3, 8: 3, 9: 4, 10: 4}
    order = sorted((r + stages[n], r, n) for r in range(2 * ROUNDS) for n in range(11))
    order = [(r, n) for _, r, n in order][1:]
    order = order[: order.index((7, 4)) + 1]
    order += [(7, 5), (6, 9), (7, 9), (7, 6), (7, 7), (7, 8), (6, 10), (7, 10)]
    head_part = order[: order.index((1, 10)) + 1]
    later = [at for at in head_part if at[0] >= 2 and at not in ((2, 0), (2, 1), (2, 2), (3, 0))]
    order = [at for at in head_part if at not in later] + later + order[len(head_part) :]
    begun = order.index((1, 10)) + 1
    beside_heads = order.index((3, 10)) + 1 - begun
    events = Events(step(*at) for at in order)
    events.steps.insert(order.index((7, 4)) + 1, lambda: swap(1).start())

    events.run(1)
    fill_distance(dist, segments, place)
    norm_gather.kept().wait()
    norm_gather.wait("z1", "z2", "z3")
    norm_gather.start("y")
    events.run(begun - 1)
    swap(0).wait_recv()
    stay(0).wait()
    store(4).start()
    for i in range(512 // ROWS):
        rows = pl.ds((i % 2) * ROWS, ROWS)
        x_t[:, i * ROWS : (i + 1) * ROWS] = xs[i // 2, rows, :].astype(f32).T.astype(bf16)
    store(11).start()
    store(12).start()

    def share(t, n):
        ref = (keys, values)[n].at[pl.ds(2 * t, 2), :, place.k]
        return remote(ref, ref, kv_send.at[t, n], kv_recv.at[t, n], place.device(dk=1))

    def project(t, carry):
        w = whole(weights.at[0:2, t // 2, t % 2])
        for s in range(2):
            out = dot(xs[s], w).astype(bf16)
            for i in range(2):
                cols = slice(i * 128, i * 128 + 128)
                q[2 * t + i, pl.ds(s * 256, 256), :] = out[:, cols] * bf16(HEAD_DIM**-0.5)
                keys[2 * t + i, s, k] = out[:, 256 + i * 128 : 384 + i * 128]
                values[2 * t + i, s, k] = out[:, 512 + i * 128 : 640 + i * 128]
        share(t, 0).start()
        share(t, 1).start()
        return carry

    lax.fori_loop(0, 4, project, 0)
    out_t[1, pl.ds(HEAD_DIM, HEAD_DIM), :] = jnp.zeros((HEAD_DIM, 512), f32)
    stop = events.spread(4, 7, beside_heads)

    def attend(t, carry):
        share(t, 0).wait_recv()
        share(t, 1).wait_recv()
        point = 0
        for spot, (tile, half) in enumerate(HEAD_SPOTS):
            slope = slopes[3 * t + spot]
            key = keys[2 * t + tile].reshape(1024, 128)
            rows = slice(half * HEAD_DIM, (half + 1) * HEAD_DIM)
            value_t = values[2 * t + tile].reshape(1024, 128).astype(f32).T.astype(bf16)[rows]
            for start in range(0, 512, CHUNK):
                cols = pl.ds(start, CHUNK)
                part = lane_half(q[2 * t + tile, cols, :], half)
                scores = dot(key, part, NT) - slope * dist[:, cols]
                peak = jnp.max(scores, axis=0, keepdims=True)
                expo = jnp.exp(scores - peak)
                total = jnp.sum(expo, axis=0, keepdims=True)
                out_t[tile, rows, cols] = dot(value_t, expo.astype(bf16)) / total
                o_lse[t, pl.ds(spot, 1), cols] = peak + jnp.log(total)
                stop(t, point)
                point += 1
        for tile in range(2):
            ctx[2 * t + tile] = out_t[tile].T.astype(bf16)
        left, right = out_weights(whole(weights.at[0:2, t // 2, t % 2]))
        wo[t, 0] = left
        wo[t, 1] = right
        mixed = dot(ctx[2 * t], left, NT) + dot(ctx[2 * t + 1], right, NT)

        @pl.when(t == 0)
        def _():
            acc[...] = mixed

        @pl.when(t > 0)
        def _():
            acc[...] += mixed

        stop(t, point)
        return carry

    lax.fori_loop(0, 4, attend, 0)
    for n in (5, 6, 7, 8, 13):
        store(n).start()
    norm_gather.wait("y")
    norm_sum = jnp.sum(norms[...].reshape(8, 8, 768), axis=0)
    o_norms[...] = norm_sum

    def first_norm(rows, i):
        attn = acc[rows, :]
        half = i // 2
        resid = xs[half, pl.ds(pl.multiple_of((i % 2) * ROWS, ROWS), ROWS), :].astype(f32) + attn
        normed, inv = norm_stats(resid)
        value = normed * norm_sum[0:1] + norm_sum[2:3]
        h1[rows, :] = value
        h1b[rows, :] = value.astype(bf16)
        h1_t[:, rows] = value.T.astype(bf16)
        n1[rows, :] = normed
        o_i1[rows, :] = inv
        acc[rows, :] = jnp.zeros_like(attn)
        if_first = jnp.where(i == 0, 0.0, 1.0)
        o_squares[0] = o_squares[0] * if_first + columns(attn * attn)
        o_squares[1] = o_squares[1] * if_first + columns(resid * resid)

    o_squares[...] = jnp.zeros_like(o_squares)
    row_blocks(first_norm)
    store(9).start()
    store(10).start()

    first_part = order.index((5, 10)) - begun - beside_heads
    middle = len(order) - 7 - order.index((5, 10)) - 1
    counts = {}
    for n in range(first_part):
        at = n * 8 // first_part
        counts[at] = counts.get(at, 0) + 1
    counts[8] = 1
    for n in range(middle):
        at = 9 + n * 6 // middle
        counts[at] = counts.get(at, 0) + 1
    counts[16] = 1
    counts[18] = counts[22] = 2
    counts[20] = 3
    stop_f = events.place(12, 2, counts)
    assert not events.steps

    def keep_copy(n):
        at = n // 4 * 4 + (x ^ (n % 4 // 2)) * 2 + (k ^ (n % 2))
        return pltpu.make_async_copy(kept.at[n % 2], o_kept.at[at], kept_sems.at[n % 2])

    def feed(n, carry):
        r = 1 + n // 4
        wx, wk = x ^ (n % 4 // 2), k ^ (n % 2)
        stop_f(n, 0)

        @pl.when(n >= 2)
        def _():
            keep_copy(n - 2).wait()

        ref = weights.at[pl.ds(2 * r, 2), wx, wk]
        for start in range(0, 512, 512):
            rows = pl.ds(start, 512)
            w = whole(ref)
            projected = dot(h1b[rows, :], w[:, :512])
            gate, up = projected[:, :256], projected[:, 256:]
            cdf = 0.5 + 0.5 * lax.erf(gate * (0.5**0.5))
            pdf = jnp.exp(-0.5 * gate * gate) * 0.3989422804014327
            act = gate * cdf
            hidden = (act * up).astype(bf16)
            kept[n % 2, 0, rows, :] = hidden
            kept[n % 2, 1, rows, :] = act.astype(bf16)
            kept[n % 2, 2, rows, :] = ((cdf + gate * pdf) * up).astype(bf16)
            acc[rows, :] += dot(hidden, w[:, 512:], NT)
        keep_copy(n).start()
        stop_f(n, 1)
        return carry

    lax.fori_loop(0, 12, feed, 0)

    def second_norm(rows, i):
        ffn = acc[rows, :]
        resid = h1[rows, :] + ffn
        normed, inv = norm_stats(resid)
        o_out[rows, :] = (normed * norm_sum[1:2] + norm_sum[3:4]).astype(bf16)
        o_n2[rows, :] = normed
        o_i2[rows, :] = inv
        o_squares[2] += columns(ffn * ffn)
        o_squares[3] += columns(resid * resid)

    row_blocks(second_norm)
    for n in (10, 11):
        keep_copy(n).wait()
    for r in rounds:
        r.finish()
    norm_gather.finish()
    for n in range(2):
        swap(n).wait_send()
    swap(1).wait_recv()
    stay(1).wait()
    for t in range(4):
        for n in range(2):
            share(t, n).wait_send()
    for n in range(14):
        store(n).wait()


def forward_refs(span, count, *refs):
    forward_kernel(span, refs[0], refs[1 : 1 + count], *refs[1 + count :])


def forward(span, slopes, raw, gains, biases, tok, cot, segments):
    f32, bf16 = jnp.float32, jnp.bfloat16
    any_space = pl.BlockSpec(memory_space=pl.ANY)
    vmem = pl.BlockSpec(memory_space=pltpu.VMEM)
    outs = (
        ((2 * ROUNDS, 2, 2, 4, 2, 96, 384), bf16, any_space),
        ((8, 768), f32, vmem),
        ((2, 256, 768), bf16, any_space),
        ((2, 256, 768), bf16, any_space),
        ((8, 512, 128), bf16, any_space),
        ((8, 2, 2, 256, 128), bf16, any_space),
        ((8, 2, 2, 256, 128), bf16, any_space),
        ((8, 512, 128), bf16, any_space),
        ((4, 8, 512), f32, vmem),
        ((12, 3, 512, 256), bf16, any_space),
        ((512, 768), f32, any_space),
        ((512, 1), f32, vmem),
        ((512, 768), f32, vmem),
        ((512, 1), f32, vmem),
        ((512, 768), bf16, vmem),
        ((4, 8, 768), f32, vmem),
        ((768, 512), bf16, any_space),
        ((768, 512), bf16, any_space),
        ((1024, 512), f32, any_space),
        ((4, 2, 768, 128), bf16, any_space),
    )
    dma = pltpu.SemaphoreType.DMA
    copies = len(GatherRound.names)
    return pl.pallas_call(
        partial(forward_refs, span, len(raw)),
        out_shape=tuple(jax.ShapeDtypeStruct(s, d) for s, d, _ in outs),
        in_specs=[pl.BlockSpec(memory_space=pltpu.SMEM)]
        + [vmem] * (len(raw) + 2)
        + [any_space, any_space, vmem],
        out_specs=tuple(spec for _, _, spec in outs),
        scratch_shapes=[
            pltpu.VMEM((2 * ROUNDS, 96, 384), bf16),
            pltpu.VMEM((8, 768), f32),
            pltpu.VMEM((2 * ROUNDS, 2, 2, 4, 2, 96, 384), bf16),
            pltpu.VMEM((4, 2, 8, 768), f32),
            pltpu.VMEM((2, 256, 768), bf16),
            pltpu.VMEM((8, 512, 128), bf16),
            pltpu.VMEM((8, 2, 2, 256, 128), bf16),
            pltpu.VMEM((8, 2, 2, 256, 128), bf16),
            pltpu.VMEM((8, 512, 128), bf16),
            pltpu.VMEM((512, 768), bf16),
            pltpu.VMEM((512, 768), f32),
            pltpu.VMEM((768, 512), bf16),
            pltpu.VMEM((768, 512), bf16),
            pltpu.VMEM((4, 2, 768, 128), bf16),
            pltpu.VMEM((1024, 512), f32),
            pltpu.VMEM((2, 128, 512), f32),
            pltpu.VMEM((512, 768), f32),
            pltpu.VMEM((512, 768), f32),
            pltpu.VMEM((2, 3, 512, 256), bf16),
            dma((2 * ROUNDS, copies)),
            dma((2 * ROUNDS, copies)),
            dma((2 * ROUNDS,)),
            dma((4,)),
            dma((4,)),
            dma,
            dma((6,)),
            dma((4, 2)),
            dma((4, 2)),
            dma((14,)),
            dma((2,)),
        ],
        compiler_params=pltpu.CompilerParams(
            collective_id=0, has_side_effects=True, vmem_limit_bytes=VMEM_LIMIT
        ),
        name="forward",
    )(slopes, *raw, gains, biases, tok, cot, segments)


class ScatterRound(Copies):
    names = ("ay1", "bx", "ay0", "ax", "by", "cx", "dy") + tuple(
        part + "z%d" % step for part in "abcd" for step in (1, 2, 3)
    )

    def __init__(self, place, held, twin, stage, landing, send, recv, pair):
        self.place, self.held, self.twin, self.stage = place, held, twin, stage
        self.ay, self.bx, self.ax, self.by, self.z, self.cz, self.dz, self.last = landing
        self.send, self.recv, self.pair = send, recv, pair

    def copy(self, name):
        p, held = self.place, self.held
        at = self.names.index(name)
        a, b, c, d = (PARTS[part] for part in "abcd")
        step = int(name[2]) if name[1] == "z" else 0
        far = (p.z + step) % 4
        ac, bd = PARTS["ac"], PARTS["bd"]
        if name in ("ay1", "ay0"):
            dx = int(name[2])
            src, dst, to = held.at[dx, :, 1 - p.y, ac, :], self.ay.at[dx], {"dy": 1}
        elif name == "bx":
            src, dst, to = held.at[1, :, :, bd, :], self.bx, {"dx": 1}
        elif name == "ax":
            src, dst, to = held.at[1, :, p.y, a, :], self.ax, {"dx": 1}
        elif name == "by":
            src, dst, to = held.at[0, :, 1 - p.y, b, :], self.by, {"dy": 1}
        elif name == "cx":
            src, dst, to = held.at[1, p.z, p.y, c, :], self.last.at[0], {"dx": 1}
        elif name == "dy":
            src, dst, to = held.at[0, p.z, 1 - p.y, d, :], self.last.at[1], {"dy": 1}
        elif name[0] == "c":
            src, dst, to = held.at[:, far, p.y, c, :], self.cz.at[step - 1], {"dz": step}
        elif name[0] == "d":
            src, dst, to = held.at[0, far, :, d, :], self.dz.at[step - 1], {"dz": step}
        else:
            rows = PARTS[name[0]]
            into = pl.ds(0, 32) if name[0] == "a" else pl.ds(32, 32)
            src, dst, to = held.at[0, far, p.y, rows, :], self.z.at[step - 1, into, :], {"dz": step}
        return remote(src, dst, self.send.at[at], self.recv.at[at], p.device(**to))

    def push(self, dx):
        return remote(
            self.stage.at[dx], self.twin.at[dx], self.pair.at[0, dx], self.pair.at[1, dx], self.place.device(dk=1)
        )

    def add(self, ref, *others):
        total = ref[...].astype(jnp.float32)
        for other in others:
            total = total + other[...].astype(jnp.float32)
        ref[...] = total.astype(jnp.bfloat16)

    def pair_sum(self, dx):
        self.push(dx).wait_recv()

        def body(i, carry):
            self.add(self.held.at[dx, i], self.twin.at[dx, i])
            return carry

        lax.fori_loop(0, 4, body, 0)
        if dx:
            self.start("bx", "ay1")
        else:
            self.start("ay0")

    def event(self, n, out=None):
        p, held = self.place, self.held
        a, b, c, d = (PARTS[part] for part in "abcd")
        ac, bd = PARTS["ac"], PARTS["bd"]
        if n == 0:
            self.wait("ay1")
            self.add(held.at[1, :, p.y, ac, :], self.ay.at[1])
            self.start("ax")
        elif n == 1:
            self.wait("bx")
            self.add(held.at[0, :, 1 - p.y, bd, :], self.bx.at[:, 1 - p.y])
            self.start("by")
            self.add(held.at[0, :, p.y, bd, :], self.bx.at[:, p.y])
            self.start("dz1", "dz2", "dz3")
        elif n == 2:
            self.wait("ay0")
            self.add(held.at[0, :, p.y, ac, :], self.ay.at[0])
            self.start("cz1", "cz2", "cz3")
        elif n == 3:
            self.wait("ax")
            self.add(held.at[0, :, p.y, a, :], self.ax)
            self.start("az1", "az2", "az3")
        elif n == 4:
            self.wait("by")
            self.add(held.at[0, :, p.y, b, :], self.by)
            self.start("bz1", "bz2", "bz3")
        elif n == 5:
            self.wait("cz1", "cz2", "cz3", "dz1", "dz2", "dz3")
            self.add(held.at[1, p.z, p.y, c, :], *[self.cz.at[i, 1] for i in range(3)])
            self.start("cx")
            self.add(held.at[0, p.z, 1 - p.y, d, :], *[self.dz.at[i, 1 - p.y] for i in range(3)])
            self.start("dy")
            self.add(held.at[0, p.z, p.y, c, :], *[self.cz.at[i, 0] for i in range(3)])
            self.add(held.at[0, p.z, p.y, d, :], *[self.dz.at[i, p.y] for i in range(3)])
        else:
            self.wait("az1", "az2", "az3", "bz1", "bz2", "bz3", "cx", "dy")
            for rows, others in (
                (a, [self.z.at[i, pl.ds(0, 32), :] for i in range(3)]),
                (b, [self.z.at[i, pl.ds(32, 32), :] for i in range(3)]),
                (c, [self.last.at[0]]),
                (d, [self.last.at[1]]),
            ):
                total = held[0, p.z, p.y, rows, :].astype(jnp.float32)
                for other in others:
                    total = total + other[...].astype(jnp.float32)
                out[rows, :] = total


def backward_kernel(
    span,
    slopes,
    i_weights,
    norms,
    i_cot,
    i_q,
    i_k,
    i_v,
    i_ctx,
    i_lse,
    i_kept,
    i_n1,
    i_i1,
    i_n2,
    i_i2,
    i_out,
    squares,
    i_h1_t,
    i_x_t,
    i_dist,
    i_wo,
    o_out,
    o_tokens,
    o_grads,
    o_small,
    w_buf,
    wo,
    kept,
    h1_t,
    f_t,
    d_rows,
    n_buf,
    d_h1,
    q,
    keys,
    values,
    ctx,
    lse,
    dist,
    d_ctx,
    d_kv,
    d_kv_in,
    dq_t,
    acc_k,
    acc_v,
    held,
    twin,
    land_ay,
    land_bx,
    land_ax,
    land_by,
    land_z,
    land_cz,
    land_dz,
    land_last,
    small,
    small_in,
    load_sems,
    step_sems,
    r_send,
    r_recv,
    r_pair,
    t_sems,
    kv_send,
    kv_recv,
    s_send,
    s_recv,
):
    f32, bf16 = jnp.float32, jnp.bfloat16
    place = Place(span)
    x, y, z, k = place.shifted()
    rounds = [
        ScatterRound(
            place,
            held.at[n],
            twin.at[n % 6],
            held.at[2 * ROUNDS + n % 2],
            [
                ref.at[n]
                for ref in (land_ay, land_bx, land_ax, land_by, land_z, land_cz, land_dz, land_last)
            ],
            r_send.at[n],
            r_recv.at[n],
            r_pair.at[n],
        )
        for n in range(2 * ROUNDS)
    ]

    def load(n):
        src, dst = (
            (i_cot, d_rows.at[1]),
            (i_n2, n_buf),
            (i_h1_t, h1_t),
            (i_x_t, h1_t),
            (i_q, q),
            (i_k, keys),
            (i_v, values),
            (i_ctx, ctx),
            (i_lse, lse),
            (i_n1, n_buf),
            (i_dist, dist),
        )[n]
        return pltpu.make_async_copy(src, dst, load_sems.at[n])

    def where(n):
        return x ^ (1 - n // 2), k ^ (1 - n % 2)

    def where_heads(n):
        return x ^ (1 - n // 2), n % 2

    def fetch(n, part):
        r = 3 - n // 4
        wx, wk = where(n % 4)
        if part == 0:
            return pltpu.make_async_copy(i_weights.at[pl.ds(2 * r, 2), wx, wk], w_buf.at[n % 2], step_sems.at[n % 2, 0])
        return pltpu.make_async_copy(
            i_kept.at[(r - 1) * 4 + wx * 2 + wk], kept.at[n % 2], step_sems.at[n % 2, 1]
        )

    for n in (0, 1):
        load(n).start()
    fetch(0, 0).start()
    fetch(0, 1).start()
    for n in (2, 4, 5, 6, 7, 8, 10):
        load(n).start()
    place.greet(ALL_PEERS)

    def swap(n):
        src, dst = ((i_out, o_out), (d_rows.at[0], o_tokens))[n]
        return remote(
            src.at[1 - place.x],
            dst.at[place.x],
            t_sems.at[3 * n],
            t_sems.at[3 * n + 1],
            place.device(dx=1),
        )

    def stay(n):
        src, dst = ((i_out, o_out), (d_rows.at[0], o_tokens))[n]
        return pltpu.make_async_copy(src.at[place.x], dst.at[place.x], t_sems.at[3 * n + 2])

    swap(0).start()
    stay(0).start()
    load(0).wait()
    load(1).wait()
    small[...] = jnp.zeros_like(small)

    def halves(ref, i):
        return ref.at[i // 2, pl.ds(pl.multiple_of((i % 2) * ROWS, ROWS), ROWS), :]

    sums = [jnp.zeros((8, 768), f32)] * 2
    for i in range(512 // ROWS):
        rows = pl.ds(i * ROWS, ROWS)
        grad = halves(d_rows.at[1], i)[...].astype(f32)
        normed = n_buf[rows, :]
        out = norm_backward(grad, normed, i_i2[rows, :], norms[1:2])
        d_h1[rows, :] = out
        halves(d_rows.at[0], i)[...] = out.astype(bf16)
        f_t[:, rows] = out.T.astype(bf16)
        sums[0] = sums[0] + columns(grad * normed)
        sums[1] = sums[1] + columns(grad)
    small[1] = sums[0]
    small[3] = sums[1]
    load(9).start()
    load(2).wait()

    def pair(n, dx):
        return lambda: rounds[n].pair_sum(dx)

    def step(n, at):
        chunk = 3 - n // 2
        return lambda: rounds[n].event(at, o_grads.at[2 * chunk + n % 2])

    def put(n, dx, theirs, value, start):
        block = value.astype(bf16).reshape(4, 2, 96, value.shape[-1])
        stop_at = start + value.shape[-1]
        for half in range(2):
            low, high = max(start, 384 * half), min(stop_at, 384 * half + 384)
            if low < high:
                slot = theirs * (2 * ROUNDS + half) + (1 - theirs) * (2 * n + half)
                held[slot, dx, :, :, :, low - 384 * half : high - 384 * half] = block[
                    :, :, :, low - start : high - start
                ]

    def pushes(n, dx):
        return [
            remote(
                held.at[2 * ROUNDS + half, dx],
                twin.at[(2 * n + half) % 6, dx],
                r_pair.at[2 * n + half, 0, dx],
                r_pair.at[2 * n + half, 1, dx],
                place.device(dk=1),
            )
            for half in range(2)
        ]

    def push(n, dx):
        for copy in pushes(n, dx):
            copy.start()

    def pushed(n, dx):
        for copy in pushes(n, dx):
            copy.wait_send()

    between = {
        5: [step(0, 0), step(1, 0)],
        6: [step(0, 1)],
        8: [step(0, 2), step(1, 1)],
        9: [step(1, 2)],
        10: [step(0, 3), step(1, 3)],
        11: [step(0, 5), step(2, 0), step(3, 0)],
    }
    after = {
        1: [pair(0, 1), pair(1, 1)],
        3: [pair(0, 0), pair(1, 0)],
        5: [pair(2, 1), pair(3, 1)],
        7: [pair(2, 0), pair(3, 0)],
        11: [pair(4, 1), pair(5, 1), pair(4, 0), pair(5, 0)],
    }

    def go(n, plan):
        for at, todo in plan.items():

            @pl.when(n == at)
            def _():
                for item in todo:
                    item()

    def feed(n, carry):
        dx = 1 - n % 4 // 2
        theirs = 1 - n % 2

        @pl.when(n < 11)
        def _():
            fetch(n + 1, 0).start()
            fetch(n + 1, 1).start()

        @pl.when(jnp.logical_and(theirs == 1, n >= 4))
        def _():
            pushed(n // 4 - 1, dx)

        fetch(n, 0).wait()
        fetch(n, 1).wait()
        w = whole(w_buf.at[n % 2])
        hold = kept.at[n % 2]
        d_ffn = d_rows[0].reshape(512, 768)
        d_hidden = dot(d_ffn, w[:, 512:])
        d_gate = (d_hidden * hold[2].astype(f32)).astype(bf16)
        d_up = (d_hidden * hold[1].astype(f32)).astype(bf16)
        d_projected = jnp.concatenate([d_gate, d_up], axis=1)
        put(n // 4, dx, theirs, dot(f_t[...], hold[0]), 512)
        go(n, between)
        put(n // 4, dx, theirs, dot(h1_t[...], d_projected), 0)

        @pl.when(theirs == 1)
        def _():
            push(n // 4, dx)

        go(n, after)
        d_h1[...] += dot(d_projected, w[:, :512], NT)
        return carry

    lax.fori_loop(0, 12, feed, 0)
    load(9).wait()
    load(3).start()
    sums = [jnp.zeros((8, 768), f32)] * 2
    for i in range(512 // ROWS):
        rows = pl.ds(i * ROWS, ROWS)
        grad = d_h1[rows, :]
        normed = n_buf[rows, :]
        out = norm_backward(grad, normed, i_i1[rows, :], norms[0:1])
        d_h1[rows, :] = out
        halves(d_rows.at[1], i)[...] = out.astype(bf16)
        f_t[:, rows] = out.T.astype(bf16)
        sums[0] = sums[0] + columns(grad * normed)
        sums[1] = sums[1] + columns(grad)
    small[0] = sums[0]
    small[2] = sums[1]
    for n in (3, 4, 5, 6, 7, 8, 10):
        load(n).wait()

    small[0] = jnp.concatenate(
        [jnp.sum(small[i], axis=0, keepdims=True) for i in range(4)]
        + [jnp.sum(squares[i], axis=0, keepdims=True) for i in range(4)],
        axis=0,
    )

    def spread(n):
        to = ({"dk": 1}, {"dx": 1}, {"dy": 1}, {"dz": 1}, {"dz": 2}, {"dz": 3})[n]
        return remote(
            small.at[min(n, 3)], small_in.at[n], s_send.at[n], s_recv.at[n], place.device(**to)
        )

    def small_step(n):
        def go():
            if 0 < n < 4:
                spread(n - 1).wait_recv()
                small[n] = small[n - 1] + small_in[n - 1]
            if n < 3:
                spread(n).start()
            if n == 3:
                for at in (3, 4, 5):
                    spread(at).start()
            if n == 4:
                for at in (3, 4, 5):
                    spread(at).wait_recv()
                total = small[3]
                result = jnp.zeros_like(total)
                for at in range(4):
                    back = (place.z - at) % 4
                    term = jnp.where(
                        back == 0,
                        total,
                        jnp.where(
                            back == 1, small_in[3], jnp.where(back == 2, small_in[4], small_in[5])
                        ),
                    )
                    result = result + term
                o_small[...] = result

        return go

    def fetch_heads(n):
        wx, wk = where_heads(n)
        return pltpu.make_async_copy(i_weights.at[0:2, wx, wk], w_buf.at[n % 2], step_sems.at[n % 2, 0])

    def fetch_wo(n):
        wx, wk = where_heads(n)
        return pltpu.make_async_copy(i_wo.at[wx * 2 + wk], wo.at[n % 2], step_sems.at[n % 2, 1])

    fetch_heads(0).start()
    fetch_wo(0).start()
    dq_t[1, pl.ds(HEAD_DIM, HEAD_DIM), :] = jnp.zeros((HEAD_DIM, 512), f32)

    def share(t):
        return remote(
            d_kv.at[t, :, :, :, 1 - place.k], d_kv_in.at[t], kv_send.at[t], kv_recv.at[t], place.device(dk=1)
        )

    beside = {
        (1, 6): [small_step(0), step(0, 4)],
        (2, 0): [step(2, 1)],
        (2, 1): [small_step(1), step(1, 5)],
        (2, 2): [step(2, 2)],
        (2, 3): [small_step(2)],
        (2, 4): [step(3, 2)],
        (2, 6): [
            small_step(3), step(1, 4), step(3, 1), pair(6, 1),
            pair(7, 1),
        ],
        (3, 1): [step(2, 3), step(3, 3)],
        (3, 2): [small_step(4), step(2, 5)],
        (3, 4): [step(2, 4)],
        (3, 6): [
            step(3, 5), step(3, 4), step(4, 0), step(5, 0), step(4, 1),
            step(4, 2), step(5, 2), step(5, 1),
            step(4, 3), step(5, 3), step(4, 5), step(4, 4),
        ],
        (4, 6): [step(6, 0), step(7, 0), step(5, 5), step(5, 4)],
    }
    first = lax.broadcasted_iota(jnp.int32, (768, 128), 1) < HEAD_DIM

    def stop(i, point):
        for (trip, at), todo in beside.items():
            if at == point:

                @pl.when(i == trip)
                def _():
                    for item in todo:
                        item()

    def attend(n):
        wx, wk = where_heads(n)
        t = wx * 2 + wk
        fetch_heads(n).wait()
        fetch_wo(n).wait()
        left, right = wo[n % 2, 0], wo[n % 2, 1]
        d_attn = d_rows[1].reshape(512, 768)
        d_ctx[0] = dot(d_attn, left).astype(bf16)
        d_ctx[1] = dot(d_attn, right).astype(bf16)
        point = 0
        for spot, (tile, half) in enumerate(HEAD_SPOTS):
            slope = slopes[3 * t + spot]
            key = keys[2 * t + tile].reshape(1024, 128)
            value = values[2 * t + tile].reshape(1024, 128)
            rows = slice(half * HEAD_DIM, (half + 1) * HEAD_DIM)
            key_t = key.astype(f32).T.astype(bf16)[rows]
            product = ctx[2 * t + tile].astype(f32) * d_ctx[tile].astype(f32)
            delta = jnp.sum(product.T[rows], axis=0, keepdims=True)
            for start in range(0, 512, CHUNK):
                cols = pl.ds(start, CHUNK)
                part = lane_half(q[2 * t + tile, cols, :], half)
                grad = lane_half(d_ctx[tile, cols, :], half)
                scores = dot(key, part, NT) - slope * dist[:, cols]
                probs = jnp.exp(scores - lse[t, pl.ds(spot, 1), cols])
                grad_probs = dot(value, grad, NT)
                term_v = dot(probs.astype(bf16), grad)
                grad_scores = (probs * (grad_probs - delta[:, start : start + CHUNK])).astype(bf16)
                term_k = dot(grad_scores, part)
                if half == 0 and start == 0:
                    acc_v[...] = term_v
                    acc_k[...] = term_k
                else:
                    acc_v[...] += term_v
                    acc_k[...] += term_k
                dq_t[tile, rows, cols] = dot(key_t, grad_scores)
                stop(n, point)
                point += 1
            if half == 1 or tile == 1:
                d_kv[t, 0, tile] = acc_k[...].astype(bf16).reshape(2, 2, 256, 128)
                d_kv[t, 1, tile] = acc_v[...].astype(bf16).reshape(2, 2, 256, 128)
        share(t).start()
        for tile in range(2):
            q[2 * t + tile] = (dq_t[tile].T * HEAD_DIM**-0.5).astype(bf16)

    def project(n):
        wx, wk = where_heads(n)
        t = wx * 2 + wk
        dx = 1 - n // 2
        theirs = wk ^ k

        @pl.when(theirs == 1)
        def _():
            pushed(2, dx)

        share(t).wait_recv()
        parts = [q[2 * t], q[2 * t + 1]]
        for kind in range(2):
            for tile in range(2):
                mine = d_kv[t, kind, tile, :, k].reshape(512, 128).astype(f32)
                mine = mine + d_kv_in[t, kind, tile].reshape(512, 128).astype(f32)
                parts.append(mine.astype(bf16))
        d_qkv = jnp.concatenate(parts, axis=1)
        d_wo = dot(f_t[...], jnp.concatenate([ctx[2 * t], ctx[2 * t + 1]], axis=1))
        turned = (swap_halves(d_wo[:, :128]), d_wo[:, :128], swap_halves(d_wo[:, 128:]))
        for kind in range(3):
            d_w = dot(h1_t[...], d_qkv[:, 256 * kind : 256 * kind + 256])
            put(3, dx, theirs, d_w[:, :128], 256 * kind)
            put(3, dx, theirs, jnp.where(first, d_w[:, 128:], turned[kind]), 256 * kind + 128)

        @pl.when(theirs == 1)
        def _():
            push(3, dx)

        d_h1[...] += dot(d_qkv, whole(w_buf.at[n % 2]), NT)

    def heads(n, carry):
        @pl.when(n < 4)
        def _():
            attend(n)

        @pl.when(n > 0)
        def _():
            project(n - 1)

        stop(n, 6)

        @pl.when(n < 3)
        def _():
            fetch_heads(n + 1).start()
            fetch_wo(n + 1).start()

        return carry

    lax.fori_loop(0, 5, heads, 0)
    for i in range(512 // ROWS):
        rows = pl.ds(i * ROWS, ROWS)
        halves(d_rows.at[0], i)[...] = d_h1[rows, :].astype(bf16)
    for n, at in (
        (6, -1), (7, -1), (6, 1), (7, 1), (6, 2), (7, 2), (6, 3), (7, 3),
        (6, 5), (6, 4), (7, 5), (7, 4), (0, 6), (1, 6), (2, 6), (3, 6),
        (4, 6), (5, 6), (6, 6), (7, 6),
    ):
        if at < 0:
            rounds[n].pair_sum(0)
        else:
            step(n, at)()
        if (n, at) == (7, -1):
            swap(1).start()
            stay(1).start()
    for n in range(6):
        spread(n).wait_send()
    for r in rounds:
        r.finish()
    for dx in range(2):
        pushed(3, dx)
    for t in range(4):
        share(t).wait_send()
    for n in range(2):
        swap(n).wait()
        stay(n).wait()


def backward(span, slopes, saved):
    f32, bf16 = jnp.float32, jnp.bfloat16
    any_space = pl.BlockSpec(memory_space=pl.ANY)
    vmem = pl.BlockSpec(memory_space=pltpu.VMEM)
    dma = pltpu.SemaphoreType.DMA
    (weights, norms, xs, cot, q, keys, values, ctx, lse, kept, n1, i1, n2, i2, out, squares) = saved[:16]
    h1_t, x_t, dist, wo = saved[16:]
    out = out.reshape(2, 256, 768)
    in_specs = [pl.BlockSpec(memory_space=pltpu.SMEM), any_space, vmem] + [any_space] * 8
    in_specs += [vmem, any_space, vmem, any_space, vmem] + [any_space] * 4
    copies = len(ScatterRound.names)
    return pl.pallas_call(
        partial(backward_kernel, span),
        out_shape=(
            jax.ShapeDtypeStruct((2, 256, 768), bf16),
            jax.ShapeDtypeStruct((2, 256, 768), bf16),
            jax.ShapeDtypeStruct((2 * ROUNDS, 96, 384), f32),
            jax.ShapeDtypeStruct((8, 768), f32),
        ),
        in_specs=in_specs,
        out_specs=(any_space, any_space, vmem, vmem),
        scratch_shapes=[
            pltpu.VMEM((2, 2, 4, 2, 96, 384), bf16),
            pltpu.VMEM((2, 2, 768, 128), bf16),
            pltpu.VMEM((2, 3, 512, 256), bf16),
            pltpu.VMEM((768, 512), bf16),
            pltpu.VMEM((768, 512), bf16),
            pltpu.VMEM((2, 2, 256, 768), bf16),
            pltpu.VMEM((512, 768), f32),
            pltpu.VMEM((512, 768), f32),
            pltpu.VMEM((8, 512, 128), bf16),
            pltpu.VMEM((8, 2, 2, 256, 128), bf16),
            pltpu.VMEM((8, 2, 2, 256, 128), bf16),
            pltpu.VMEM((8, 512, 128), bf16),
            pltpu.VMEM((4, 8, 512), f32),
            pltpu.VMEM((1024, 512), f32),
            pltpu.VMEM((2, 512, 128), bf16),
            pltpu.VMEM((4, 2, 2, 2, 2, 256, 128), bf16),
            pltpu.VMEM((4, 2, 2, 2, 256, 128), bf16),
            pltpu.VMEM((2, 128, 512), f32),
            pltpu.VMEM((1024, 128), f32),
            pltpu.VMEM((1024, 128), f32),
            pltpu.VMEM((2 * ROUNDS + 2, 2, 4, 2, 96, 384), bf16),
            pltpu.VMEM((6, 2, 4, 2, 96, 384), bf16),
            pltpu.VMEM((2 * ROUNDS, 2, 4, 48, 384), bf16),
            pltpu.VMEM((2 * ROUNDS, 4, 2, 48, 384), bf16),
            pltpu.VMEM((2 * ROUNDS, 4, 32, 384), bf16),
            pltpu.VMEM((2 * ROUNDS, 4, 32, 384), bf16),
            pltpu.VMEM((2 * ROUNDS, 3, 64, 384), bf16),
            pltpu.VMEM((2 * ROUNDS, 3, 2, 16, 384), bf16),
            pltpu.VMEM((2 * ROUNDS, 3, 2, 16, 384), bf16),
            pltpu.VMEM((2 * ROUNDS, 2, 16, 384), bf16),
            pltpu.VMEM((4, 8, 768), f32),
            pltpu.VMEM((6, 8, 768), f32),
            dma((11,)),
            dma((2, 2)),
            dma((2 * ROUNDS, copies)),
            dma((2 * ROUNDS, copies)),
            dma((2 * ROUNDS, 2, 2)),
            dma((6,)),
            dma((4,)),
            dma((4,)),
            dma((6,)),
            dma((6,)),
        ],
        compiler_params=pltpu.CompilerParams(
            collective_id=1, has_side_effects=True, vmem_limit_bytes=VMEM_LIMIT
        ),
        name="backward",
    )(
        slopes,
        weights,
        norms,
        cot,
        q,
        keys,
        values,
        ctx,
        lse,
        kept,
        n1,
        i1,
        n2,
        i2,
        out,
        squares,
        h1_t,
        x_t,
        dist,
        wo,
    )


def finish_kernel(
    block,
    i_grads,
    small,
    lo,
    gt,
    o_lo,
    o_gt,
    o_qkv,
    o_wout,
    o_win,
    o_down_t,
    o_gains,
    o_biases,
    rows,
    grads,
    qkv,
    wout,
    win,
    down_t,
    sems,
):
    moves = (
        (i_grads.at[0:2], grads.at[0:2]),
        (lo, rows.at[0]),
        (gt, rows.at[1]),
        (i_grads.at[2:8], grads.at[2:8]),
        (rows.at[0], o_lo),
        (rows.at[1], o_gt),
        (qkv, o_qkv),
        (wout, o_wout),
        (win, o_win),
        (down_t, o_down_t),
    )

    def move(n):
        return pltpu.make_async_copy(*moves[n], sems.at[n])

    def tile(i):
        return grads[i // 3, :, i % 3 * 128 : i % 3 * 128 + 128]

    for n in range(4):
        move(n).start()
    mine = pltpu.roll(small[...], 768 - block[0] * 96, 1)
    o_gains[...] = mine[0:2, 0:96]
    o_biases[...] = mine[2:4, 0:96]
    move(0).wait()
    turned = []
    for c in range(3):
        qkv[c, :, 0:128] = tile(2 * c)
        qkv[c, :, 128:192] = tile(2 * c + 1)[:, :HEAD_DIM]
        turned.append(tile(2 * c + 1).T[HEAD_DIM:])
    wout[...] = jnp.concatenate(turned, axis=0)
    move(6).start()
    move(7).start()
    for n in (1, 2):
        move(n).wait()
        move(n + 3).start()
    move(3).wait()
    for r in range(3):
        units = slice(r * 256, (r + 1) * 256)
        win[:, 0, units] = grads[2 + 2 * r, :, 0:256]
        win[:, 1, r * 256 : r * 256 + 128] = grads[2 + 2 * r, :, 256:384]
        win[:, 1, r * 256 + 128 : r * 256 + 256] = grads[3 + 2 * r, :, 0:128]
        down_t[:, units] = grads[3 + 2 * r, :, 128:384]
    move(8).start()
    move(9).start()
    for n in range(4, 10):
        move(n).wait()


def finish(block, grads, small, lo, gt):
    any_space = pl.BlockSpec(memory_space=pl.ANY)
    vmem = pl.BlockSpec(memory_space=pltpu.VMEM)
    f32 = jnp.float32
    shape = jax.ShapeDtypeStruct
    return pl.pallas_call(
        finish_kernel,
        out_shape=(
            shape(lo.shape, lo.dtype),
            shape(gt.shape, gt.dtype),
            shape((3, 96, 192), f32),
            shape((192, 96), f32),
            shape((96, 2, 768), f32),
            shape((96, 768), f32),
            shape((2, 96), f32),
            shape((2, 96), f32),
        ),
        in_specs=[pl.BlockSpec(memory_space=pltpu.SMEM), any_space, vmem, any_space, any_space],
        out_specs=(any_space,) * 6 + (vmem,) * 2,
        scratch_shapes=[
            pltpu.VMEM((2,) + lo.shape, lo.dtype),
            pltpu.VMEM(grads.shape, f32),
            pltpu.VMEM((3, 96, 192), f32),
            pltpu.VMEM((192, 96), f32),
            pltpu.VMEM((96, 2, 768), f32),
            pltpu.VMEM((96, 768), f32),
            pltpu.SemaphoreType.DMA((10,)),
        ],
        compiler_params=pltpu.CompilerParams(vmem_limit_bytes=VMEM_LIMIT),
        name="finish",
    )(block, grads, small, lo, gt)


def local(
    tokens,
    segment_ids,
    query_key_value_weight,
    w_out,
    input_weight,
    w_down,
    norm_gains,
    norm_biases,
    cotangent,
):
    f32 = jnp.float32
    shard_rows = query_key_value_weight.shape[1]
    span = 96 // shard_rows
    slopes = jnp.asarray([2.0 ** (-8.0 * (h + 1) / HEADS) for h in range(HEADS)], f32)
    cells = float(lax.axis_size("fsdp") * 2 * 1024 * 768)
    if span == 1:
        raw = (query_key_value_weight, w_out, input_weight, w_down.T)
        gains, biases = norm_gains, norm_biases
    else:
        count = lax.axis_size("fsdp")
        groups = [list(range(i, i + span)) for i in range(0, count, span)]
        heads = query_key_value_weight.transpose(1, 0, 2).reshape(shard_rows, 3, 3, HEAD_DIM)
        w_out_t = w_out.T.reshape(shard_rows, 3, 1, HEAD_DIM)
        wa = jnp.concatenate([heads, w_out_t], axis=2).reshape(shard_rows, 1, 768)
        gate_up = input_weight.reshape(shard_rows, 2, 3, 256).transpose(0, 2, 1, 3)
        down = w_down.T.reshape(shard_rows, 3, 1, 256)
        wf = jnp.concatenate([gate_up, down], axis=2).reshape(shard_rows, 3, 768)
        shard = jnp.concatenate([wa, wf], axis=1).reshape(shard_rows, 8, 384).transpose(1, 0, 2)
        raw = (lax.all_gather(shard, "fsdp", axis=1, tiled=True, axis_index_groups=groups),)
        gains, biases = (
            lax.all_gather(rows, "fsdp", axis=1, tiled=True, axis_index_groups=groups)
            for rows in (norm_gains, norm_biases)
        )

    saved = forward(span, slopes, raw, gains, biases, tokens, cotangent, segment_ids)
    layer_out, grad_tokens, grads, small = backward(span, slopes, saved)

    if span == 1:
        block = lax.axis_index("fsdp").astype(jnp.int32).reshape(1)
        outs = finish(block, grads, small, layer_out, grad_tokens)
        outs = outs[:5] + (outs[5].T,) + outs[6:]
    else:
        grads = lax.psum_scatter(
            grads, "fsdp", scatter_dimension=1, tiled=True, axis_index_groups=groups
        )
        small = lax.psum(small, "fsdp", axis_index_groups=groups)
        grads = grads.reshape(4, 2, shard_rows, 384).transpose(0, 2, 1, 3)
        grads_a = grads[0].reshape(shard_rows, 3, 4, HEAD_DIM)
        grads_f = grads[1:].reshape(3, shard_rows, 3, 256)
        shard_start = lax.axis_index("fsdp") * shard_rows
        mine = lax.dynamic_slice_in_dim(small[:4], shard_start, shard_rows, 1)
        outs = (
            layer_out,
            grad_tokens,
            grads_a[:, :, :3].transpose(1, 0, 2, 3).reshape(3, shard_rows, 192),
            grads_a[:, :, 3].reshape(shard_rows, 192).T,
            grads_f[:, :, :2].transpose(1, 2, 0, 3).reshape(shard_rows, 2, 768),
            grads_f[:, :, 2].transpose(0, 2, 1).reshape(768, shard_rows),
            mine[:2],
            mine[2:],
        )
    return outs + (jnp.sqrt(jnp.sum(small[4:], axis=1) / cells),)


def solution(mesh):
    placed = (
        P("fsdp", "tp", None),
        P("fsdp", None),
        P(None, "fsdp", "tp"),
        P("tp", "fsdp"),
        P("fsdp", None, "tp"),
        P("tp", "fsdp"),
        P(None, "fsdp"),
        P(None, "fsdp"),
        P("fsdp", "tp", None),
    )
    return jax.shard_map(
        local,
        mesh=mesh,
        in_specs=placed,
        out_specs=(
            P("fsdp", "tp", None),
            P("fsdp", "tp", None),
            P(None, "fsdp", "tp"),
            P("tp", "fsdp"),
            P("fsdp", None, "tp"),
            P("tp", "fsdp"),
            P(None, "fsdp"),
            P(None, "fsdp"),
            P(),
        ),
        check_vma=False,
    )
```

```python
from functools import partial

import jax
import jax.numpy as jnp
from jax import lax
from jax.experimental import pallas as pl
from jax.experimental.pallas import tpu as pltpu
from jax.sharding import PartitionSpec as P

HEADS = 12
HEAD_DIM = 64
MESH = pl.DeviceIdType.MESH
VMEM_LIMIT = 63 << 20
norm_eps = 1e-05
ROUNDS = 4
NT = (((1,), (1,)), ((), ()))
NN = (((1,), (0,)), ((), ()))
CHUNK = 256


class Place:
    def __init__(self, span):
        index = lax.axis_index("fsdp")
        shard = lax.axis_index("tp")
        self.span = span
        self.j = index % span
        block = index // span
        self.z = block // 2
        self.y = block % 2
        self.x = shard // 2
        self.k = shard % 2

    def shifted(self, dx=0, dy=0, dz=0, dk=0):
        x = 1 - self.x if dx else self.x
        y = 1 - self.y if dy else self.y
        z = (self.z + dz) % 4 if dz else self.z
        k = 1 - self.k if dk else self.k
        return x, y, z, k

    def device(self, dx=0, dy=0, dz=0, dk=0):
        x, y, z, k = self.shifted(dx, dy, dz, dk)
        return ((z * 2 + y) * self.span + self.j, x * 2 + k)

    def greet(self, offsets):
        barrier = pltpu.get_barrier_semaphore()
        for offset in offsets:
            pl.semaphore_signal(
                barrier, inc=1, device_id=self.device(**offset), device_id_type=MESH
            )
        pl.semaphore_wait(barrier, len(offsets))


ALL_PEERS = ({"dx": 1}, {"dy": 1}, {"dz": 1}, {"dz": 2}, {"dz": 3}, {"dk": 1})


def remote(src, dst, send, recv, device):
    return pltpu.make_async_remote_copy(
        src_ref=src, dst_ref=dst, send_sem=send, recv_sem=recv, device_id=device, device_id_type=MESH
    )


PARTS = {
    "a": pl.ds(0, 32),
    "c": pl.ds(32, 16),
    "ac": pl.ds(0, 48),
    "b": pl.ds(48, 32),
    "d": pl.ds(80, 16),
    "bd": pl.ds(48, 48),
    "": pl.ds(0, 96),
}


def dot(a, b, dims=NN):
    return lax.dot_general(a, b, dims, preferred_element_type=jnp.float32)


class Copies:
    names = ()

    def start(self, *names):
        for name in names:
            self.copy(name).start()

    def wait(self, *names):
        for name in names:
            self.copy(name).wait_recv()

    def finish(self):
        for name in self.names:
            self.copy(name).wait_send()


class GatherRound(Copies):
    names = ("z1", "z2", "z3", "ax", "by", "ay0", "bx0", "ay1", "bx1") + tuple(
        "d%d" % i for i in range(7)
    )
    names += ("cx", "cz1", "cz2", "cz3", "dy", "dz1", "dz2", "dz3")
    lines = {
        "ax": ((0, 0, "a"), {"dx": 1}),
        "by": ((0, 0, "b"), {"dy": 1}),
        "ay0": ((0, 0, "ac"), {"dy": 1}),
        "bx0": ((0, 0, "bd"), {"dx": 1}),
        "ay1": ((1, 0, "ac"), {"dy": 1}),
        "bx1": ((0, 1, "bd"), {"dx": 1}),
        "d0": ((0, 0, ""), {"dk": 1}),
        "d1": ((1, 0, "ac"), {"dk": 1}),
        "d2": ((0, 1, "bd"), {"dk": 1}),
        "d3": ((0, 1, "ac"), {"dk": 1}),
        "d4": ((1, 0, "bd"), {"dk": 1}),
        "d5": ((1, 1, "ac"), {"dk": 1}),
        "d6": ((1, 1, "bd"), {"dk": 1}),
    }
    steps = {
        3: (("ax", "cz1", "cz2", "cz3"), ("ay1", "d1")),
        4: (("by", "dz1", "dz2", "dz3"), ("bx1", "d2")),
        5: (("ay0",), ("d3",)),
        6: (("bx0",), ("d4",)),
        7: (("ay1",), ("d5",)),
        8: (("bx1",), ("d6",)),
    }
    last = 10

    def __init__(self, place, own, out, send, recv, keep):
        self.place, self.own, self.out = place, own, out
        self.send, self.recv, self.keep = send, recv, keep

    def line(self, dx, dy, part):
        x, y, z, k = self.place.shifted(dx, dy)
        return self.out.at[x, k, :, y, PARTS[part], :]

    def copy(self, name):
        place = self.place
        at = self.names.index(name)
        send, recv = self.send.at[at], self.recv.at[at]
        x, y, z, k = place.shifted()
        if name[0] == "z":
            return remote(
                self.own, self.out.at[x, k, z, y], send, recv, place.device(dz=int(name[1]))
            )
        if name in ("cx", "dy"):
            rows = PARTS[name[0]]
            return remote(
                self.own.at[rows, :],
                self.out.at[x, k, z, y, rows, :],
                send,
                recv,
                place.device(**{"d" + name[1]: 1}),
            )
        if name[:2] in ("cz", "dz"):
            x, y, z, k = place.shifted(dx=1) if name[0] == "c" else place.shifted(dy=1)
            ref = self.out.at[x, k, z, y, PARTS[name[0]], :]
            return remote(ref, ref, send, recv, place.device(dz=int(name[2])))
        where, to = self.lines[name]
        ref = self.line(*where)
        return remote(ref, ref, send, recv, place.device(**to))

    def kept(self):
        x, y, z, k = self.place.shifted()
        return pltpu.make_async_copy(self.own, self.out.at[x, k, z, y], self.keep)

    def event(self, n):
        if n == 0:
            self.kept().start()
            self.start("cx", "dy", "z1", "z2", "z3")
        elif n == 1:
            self.wait("cx", "dy")
            self.start("cz1", "cz2", "cz3", "dz1", "dz2", "dz3")
        elif n == 2:
            self.kept().wait()
            self.wait("z1", "z2", "z3")
            self.start("ax", "by", "ay0", "bx0", "d0")
        elif n == 9:
            self.wait("d0", "d2", "d3")
        elif n == 10:
            self.wait("d1", "d4", "d5", "d6")
        else:
            self.wait(*self.steps[n][0])
            self.start(*self.steps[n][1])


class NormGather(Copies):
    names = ("z1", "z2", "z3", "y")

    def __init__(self, place, own, out, send, recv, keep):
        self.place, self.own, self.out = place, own, out
        self.send, self.recv, self.keep = send, recv, keep

    def copy(self, name):
        place = self.place
        at = self.names.index(name)
        send, recv = self.send.at[at], self.recv.at[at]
        if name == "y":
            ref = self.out.at[:, place.y]
            return remote(ref, ref, send, recv, place.device(dy=1))
        return remote(
            self.own, self.out.at[place.z, place.y], send, recv, place.device(dz=int(name[1]))
        )

    def kept(self):
        return pltpu.make_async_copy(self.own, self.out.at[self.place.z, self.place.y], self.keep)


class Events:
    def __init__(self, steps):
        self.steps = list(steps)

    def run(self, count):
        for step in self.steps[:count]:
            step()
        del self.steps[:count]

    def spread(self, trips, points, count):
        total = trips * points
        return self.place(trips, points, {n * total // max(count, 1): 1 for n in range(count)})

    def place(self, trips, points, counts):
        total = trips * points
        slots = [[] for _ in range(total)]
        for number in sorted(counts):
            slots[number] += self.steps[: counts[number]]
            del self.steps[: counts[number]]

        def stop(i, point):
            for trip in range(trips):
                todo = slots[trip * points + point]
                if todo:

                    @pl.when(i == trip)
                    def _():
                        for step in todo:
                            step()

        return stop


def lane_half(tile, half):
    lane = lax.broadcasted_iota(jnp.int32, tile.shape, 1)
    keep = (lane < HEAD_DIM) if half == 0 else (lane >= HEAD_DIM)
    return jnp.where(keep, tile, jnp.zeros_like(tile))


def swap_halves(tile):
    return pltpu.roll(tile.astype(jnp.float32), HEAD_DIM, 1)


def fill_distance(dist, segments, place):
    row = segments[pl.ds(place.x, 1), :].astype(jnp.float32)
    column = jnp.broadcast_to(row, (8, 1024)).T[:, 0:1]
    for s in range(2):
        first = (2 * s + place.k) * 256
        mine = segments[pl.ds(place.x, 1), pl.ds(pl.multiple_of(first, 256), 256)].astype(jnp.float32)
        gap = lax.broadcasted_iota(jnp.int32, (1024, 256), 0) - (
            lax.broadcasted_iota(jnp.int32, (1024, 256), 1) + first
        )
        dist[:, s * 256 : (s + 1) * 256] = jnp.where(
            column == mine, jnp.abs(gap).astype(jnp.float32), 1e30
        )


def pack_attention(raw, shard):
    qkv, w_out = raw[0], raw[1]
    turned = w_out[...].astype(jnp.float32).T
    for c in range(3):
        tiles = (
            qkv[c, :, 0:128],
            jnp.concatenate(
                [
                    qkv[c, :, 128:192].astype(jnp.float32),
                    turned[:, c * HEAD_DIM : (c + 1) * HEAD_DIM],
                ],
                axis=1,
            ).astype(jnp.bfloat16),
        )
        for i in range(2):
            half, at = divmod(2 * c + i, 3)
            shard[half, :, at * 128 : at * 128 + 128] = tiles[i]


def pack_feed(raw, shard):
    w_in, w_down_t = raw[2:]
    for r in range(3):
        units = slice(r * 256, (r + 1) * 256)
        first = slice(r * 256, r * 256 + 128)
        second = slice(r * 256 + 128, r * 256 + 256)
        shard[2 + 2 * r, :, 0:256] = w_in[:, 0, units]
        shard[2 + 2 * r, :, 256:384] = w_in[:, 1, first]
        shard[3 + 2 * r, :, 0:128] = w_in[:, 1, second]
        shard[3 + 2 * r, :, 128:384] = w_down_t[:, units]


def out_weights(w):
    first = lax.broadcasted_iota(jnp.int32, (768, 128), 1) < HEAD_DIM
    left = jnp.where(first, swap_halves(w[:, 128:256]), w[:, 384:512].astype(jnp.float32))
    right = jnp.where(first, swap_halves(w[:, 640:768]), 0.0)
    return left.astype(jnp.bfloat16), right.astype(jnp.bfloat16)


def whole(ref):
    return jnp.concatenate([ref[i].reshape(768, 384) for i in range(2)], axis=1)


HEAD_SPOTS = ((0, 0), (0, 1), (1, 0))


def norm_stats(value):
    average = jnp.mean(value, axis=-1, keepdims=True)
    centered = value - average
    inv_std = lax.rsqrt(jnp.mean(centered * centered, axis=-1, keepdims=True) + norm_eps)
    return centered * inv_std, inv_std


def norm_backward(grad_val, normed, inv_std, gain_row):
    grad_norm = grad_val * gain_row
    return inv_std * (
        grad_norm
        - jnp.mean(grad_norm, axis=-1, keepdims=True)
        - normed * jnp.mean(grad_norm * normed, axis=-1, keepdims=True)
    )


ROWS = 128


def row_blocks(body):
    def step(i, carry):
        body(pl.ds(pl.multiple_of(i * ROWS, ROWS), ROWS), i)
        return carry

    lax.fori_loop(0, 512 // ROWS, step, 0)


def columns(value):
    return jnp.sum(value.reshape(value.shape[0] // 8, 8, value.shape[1]), axis=0)


def forward_kernel(
    span,
    slopes,
    raw,
    gains,
    biases,
    tok,
    cot,
    segments,
    o_weights,
    o_norms,
    o_x,
    o_cot,
    o_q,
    o_k,
    o_v,
    o_ctx,
    o_lse,
    o_kept,
    o_n1,
    o_i1,
    o_n2,
    o_i2,
    o_out,
    o_squares,
    o_h1_t,
    o_x_t,
    o_dist,
    o_wo,
    shard,
    norm_rows,
    weights,
    norms,
    xs,
    q,
    keys,
    values,
    ctx,
    h1b,
    n1,
    h1_t,
    x_t,
    wo,
    dist,
    out_t,
    acc,
    h1,
    kept,
    g_send,
    g_recv,
    g_keep,
    n_send,
    n_recv,
    n_keep,
    t_sems,
    kv_send,
    kv_recv,
    store_sems,
    kept_sems,
):
    f32, bf16 = jnp.float32, jnp.bfloat16
    place = Place(span)
    x, y, z, k = place.shifted()
    rounds = [
        GatherRound(place, shard.at[r], weights.at[r], g_send.at[r], g_recv.at[r], g_keep.at[r])
        for r in range(2 * ROUNDS)
    ]
    norm_gather = NormGather(place, norm_rows, norms, n_send, n_recv, n_keep)

    def swap(n):
        src, dst = ((tok, xs), (cot, o_cot))[n]
        return remote(
            src.at[1 - place.x],
            dst.at[place.x],
            t_sems.at[3 * n],
            t_sems.at[3 * n + 1],
            place.device(dx=1),
        )

    def stay(n):
        src, dst = ((tok, xs), (cot, o_cot))[n]
        return pltpu.make_async_copy(src.at[place.x], dst.at[place.x], t_sems.at[3 * n + 2])

    def store(n):
        src, dst = (
            (weights.at[0:2], o_weights.at[0:2]),
            (weights.at[2:4], o_weights.at[2:4]),
            (weights.at[4:6], o_weights.at[4:6]),
            (weights.at[6:8], o_weights.at[6:8]),
            (xs, o_x),
            (keys, o_k),
            (values, o_v),
            (q, o_q),
            (ctx, o_ctx),
            (n1, o_n1),
            (h1_t, o_h1_t),
            (x_t, o_x_t),
            (dist, o_dist),
            (wo, o_wo),
        )[n]
        return pltpu.make_async_copy(src, dst, store_sems.at[n])

    if len(raw) > 1:
        pack_attention(raw, shard)
    else:
        shard[...] = raw[0][...]
    place.greet(ALL_PEERS)
    rounds[0].event(0)
    swap(0).start()
    for n in range(2):
        stay(n).start()
    norm_rows[...] = jnp.zeros_like(norm_rows)
    norm_rows[0:2, 0:96] = gains[...].astype(f32)
    norm_rows[2:4, 0:96] = biases[...].astype(f32)
    block = place.z * 2 + place.y
    norm_rows[...] = pltpu.roll(norm_rows[...], block * 96, 1)
    norm_gather.kept().start()
    norm_gather.start("z1", "z2", "z3")
    if len(raw) > 1:
        pack_feed(raw, shard)

    def step(r, n):
        def go():
            rounds[r].event(n)
            if n == GatherRound.last and r % 2:
                store(r // 2).start()

        return go

    stages = {0: 0, 1: 1, 2: 1, 3: 2, 4: 2, 5: 3, 6: 3, 7: 3, 8: 3, 9: 4, 10: 4}
    order = sorted((r + stages[n], r, n) for r in range(2 * ROUNDS) for n in range(11))
    order = [(r, n) for _, r, n in order][1:]
    order = order[: order.index((7, 4)) + 1]
    order += [(7, 5), (6, 9), (7, 9), (7, 6), (7, 7), (7, 8), (6, 10), (7, 10)]
    head_part = order[: order.index((1, 10)) + 1]
    later = [at for at in head_part if at[0] >= 2 and at not in ((2, 0), (2, 1), (2, 2), (3, 0))]
    order = [at for at in head_part if at not in later] + later + order[len(head_part) :]
    begun = order.index((1, 10)) + 1
    beside_heads = order.index((3, 10)) + 1 - begun
    events = Events(step(*at) for at in order)
    events.steps.insert(order.index((7, 4)) + 1, lambda: swap(1).start())

    events.run(1)
    fill_distance(dist, segments, place)
    norm_gather.kept().wait()
    norm_gather.wait("z1", "z2", "z3")
    norm_gather.start("y")
    events.run(begun - 1)
    swap(0).wait_recv()
    stay(0).wait()
    store(4).start()
    for i in range(512 // ROWS):
        rows = pl.ds((i % 2) * ROWS, ROWS)
        x_t[:, i * ROWS : (i + 1) * ROWS] = xs[i // 2, rows, :].astype(f32).T.astype(bf16)
    store(11).start()
    store(12).start()

    def share(t, n):
        ref = (keys, values)[n].at[pl.ds(2 * t, 2), :, place.k]
        return remote(ref, ref, kv_send.at[t, n], kv_recv.at[t, n], place.device(dk=1))

    def project(t, carry):
        w = whole(weights.at[0:2, t // 2, t % 2])
        for s in range(2):
            out = dot(xs[s], w).astype(bf16)
            for i in range(2):
                cols = slice(i * 128, i * 128 + 128)
                q[2 * t + i, pl.ds(s * 256, 256), :] = out[:, cols] * bf16(HEAD_DIM**-0.5)
                keys[2 * t + i, s, k] = out[:, 256 + i * 128 : 384 + i * 128]
                values[2 * t + i, s, k] = out[:, 512 + i * 128 : 640 + i * 128]
        share(t, 0).start()
        share(t, 1).start()
        return carry

    lax.fori_loop(0, 4, project, 0)
    out_t[1, pl.ds(HEAD_DIM, HEAD_DIM), :] = jnp.zeros((HEAD_DIM, 512), f32)
    stop = events.spread(4, 7, beside_heads)

    def attend(t, carry):
        share(t, 0).wait_recv()
        share(t, 1).wait_recv()
        point = 0
        for spot, (tile, half) in enumerate(HEAD_SPOTS):
            slope = slopes[3 * t + spot]
            key = keys[2 * t + tile].reshape(1024, 128)
            rows = slice(half * HEAD_DIM, (half + 1) * HEAD_DIM)
            value_t = values[2 * t + tile].reshape(1024, 128).astype(f32).T.astype(bf16)[rows]
            for start in range(0, 512, CHUNK):
                cols = pl.ds(start, CHUNK)
                part = lane_half(q[2 * t + tile, cols, :], half)
                scores = dot(key, part, NT) - slope * dist[:, cols]
                peak = jnp.max(scores, axis=0, keepdims=True)
                expo = jnp.exp(scores - peak)
                total = jnp.sum(expo, axis=0, keepdims=True)
                out_t[tile, rows, cols] = dot(value_t, expo.astype(bf16)) / total
                o_lse[t, pl.ds(spot, 1), cols] = peak + jnp.log(total)
                stop(t, point)
                point += 1
        for tile in range(2):
            ctx[2 * t + tile] = out_t[tile].T.astype(bf16)
        left, right = out_weights(whole(weights.at[0:2, t // 2, t % 2]))
        wo[t, 0] = left
        wo[t, 1] = right
        mixed = dot(ctx[2 * t], left, NT) + dot(ctx[2 * t + 1], right, NT)

        @pl.when(t == 0)
        def _():
            acc[...] = mixed

        @pl.when(t > 0)
        def _():
            acc[...] += mixed

        stop(t, point)
        return carry

    lax.fori_loop(0, 4, attend, 0)
    for n in (5, 6, 7, 8, 13):
        store(n).start()
    norm_gather.wait("y")
    norm_sum = jnp.sum(norms[...].reshape(8, 8, 768), axis=0)
    o_norms[...] = norm_sum

    def first_norm(rows, i):
        attn = acc[rows, :]
        half = i // 2
        resid = xs[half, pl.ds(pl.multiple_of((i % 2) * ROWS, ROWS), ROWS), :].astype(f32) + attn
        normed, inv = norm_stats(resid)
        value = normed * norm_sum[0:1] + norm_sum[2:3]
        h1[rows, :] = value
        h1b[rows, :] = value.astype(bf16)
        h1_t[:, rows] = value.T.astype(bf16)
        n1[rows, :] = normed
        o_i1[rows, :] = inv
        acc[rows, :] = jnp.zeros_like(attn)
        if_first = jnp.where(i == 0, 0.0, 1.0)
        o_squares[0] = o_squares[0] * if_first + columns(attn * attn)
        o_squares[1] = o_squares[1] * if_first + columns(resid * resid)

    o_squares[...] = jnp.zeros_like(o_squares)
    row_blocks(first_norm)
    store(9).start()
    store(10).start()

    first_part = order.index((5, 10)) - begun - beside_heads
    middle = len(order) - 7 - order.index((5, 10)) - 1
    counts = {}
    for n in range(first_part):
        at = n * 8 // first_part
        counts[at] = counts.get(at, 0) + 1
    counts[8] = 1
    for n in range(middle):
        at = 9 + n * 6 // middle
        counts[at] = counts.get(at, 0) + 1
    counts[16] = 1
    counts[18] = counts[22] = 2
    counts[20] = 3
    stop_f = events.place(12, 2, counts)
    assert not events.steps

    def keep_copy(n):
        at = n // 4 * 4 + (x ^ (n % 4 // 2)) * 2 + (k ^ (n % 2))
        return pltpu.make_async_copy(kept.at[n % 2], o_kept.at[at], kept_sems.at[n % 2])

    def feed(n, carry):
        r = 1 + n // 4
        wx, wk = x ^ (n % 4 // 2), k ^ (n % 2)
        stop_f(n, 0)

        @pl.when(n >= 2)
        def _():
            keep_copy(n - 2).wait()

        ref = weights.at[pl.ds(2 * r, 2), wx, wk]
        for start in range(0, 512, 512):
            rows = pl.ds(start, 512)
            w = whole(ref)
            projected = dot(h1b[rows, :], w[:, :512])
            gate, up = projected[:, :256], projected[:, 256:]
            cdf = 0.5 + 0.5 * lax.erf(gate * (0.5**0.5))
            pdf = jnp.exp(-0.5 * gate * gate) * 0.3989422804014327
            act = gate * cdf
            hidden = (act * up).astype(bf16)
            kept[n % 2, 0, rows, :] = hidden
            kept[n % 2, 1, rows, :] = act.astype(bf16)
            kept[n % 2, 2, rows, :] = ((cdf + gate * pdf) * up).astype(bf16)
            acc[rows, :] += dot(hidden, w[:, 512:], NT)
        keep_copy(n).start()
        stop_f(n, 1)
        return carry

    lax.fori_loop(0, 12, feed, 0)

    def second_norm(rows, i):
        ffn = acc[rows, :]
        resid = h1[rows, :] + ffn
        normed, inv = norm_stats(resid)
        o_out[rows, :] = (normed * norm_sum[1:2] + norm_sum[3:4]).astype(bf16)
        o_n2[rows, :] = normed
        o_i2[rows, :] = inv
        o_squares[2] += columns(ffn * ffn)
        o_squares[3] += columns(resid * resid)

    row_blocks(second_norm)
    for n in (10, 11):
        keep_copy(n).wait()
    for r in rounds:
        r.finish()
    norm_gather.finish()
    for n in range(2):
        swap(n).wait_send()
    swap(1).wait_recv()
    stay(1).wait()
    for t in range(4):
        for n in range(2):
            share(t, n).wait_send()
    for n in range(14):
        store(n).wait()


def forward_refs(span, count, *refs):
    forward_kernel(span, refs[0], refs[1 : 1 + count], *refs[1 + count :])


def forward(span, slopes, raw, gains, biases, tok, cot, segments):
    f32, bf16 = jnp.float32, jnp.bfloat16
    any_space = pl.BlockSpec(memory_space=pl.ANY)
    vmem = pl.BlockSpec(memory_space=pltpu.VMEM)
    outs = (
        ((2 * ROUNDS, 2, 2, 4, 2, 96, 384), bf16, any_space),
        ((8, 768), f32, vmem),
        ((2, 256, 768), bf16, any_space),
        ((2, 256, 768), bf16, any_space),
        ((8, 512, 128), bf16, any_space),
        ((8, 2, 2, 256, 128), bf16, any_space),
        ((8, 2, 2, 256, 128), bf16, any_space),
        ((8, 512, 128), bf16, any_space),
        ((4, 8, 512), f32, vmem),
        ((12, 3, 512, 256), bf16, any_space),
        ((512, 768), f32, any_space),
        ((512, 1), f32, vmem),
        ((512, 768), f32, vmem),
        ((512, 1), f32, vmem),
        ((512, 768), bf16, vmem),
        ((4, 8, 768), f32, vmem),
        ((768, 512), bf16, any_space),
        ((768, 512), bf16, any_space),
        ((1024, 512), f32, any_space),
        ((4, 2, 768, 128), bf16, any_space),
    )
    dma = pltpu.SemaphoreType.DMA
    copies = len(GatherRound.names)
    return pl.pallas_call(
        partial(forward_refs, span, len(raw)),
        out_shape=tuple(jax.ShapeDtypeStruct(s, d) for s, d, _ in outs),
        in_specs=[pl.BlockSpec(memory_space=pltpu.SMEM)]
        + [vmem] * (len(raw) + 2)
        + [any_space, any_space, vmem],
        out_specs=tuple(spec for _, _, spec in outs),
        scratch_shapes=[
            pltpu.VMEM((2 * ROUNDS, 96, 384), bf16),
            pltpu.VMEM((8, 768), f32),
            pltpu.VMEM((2 * ROUNDS, 2, 2, 4, 2, 96, 384), bf16),
            pltpu.VMEM((4, 2, 8, 768), f32),
            pltpu.VMEM((2, 256, 768), bf16),
            pltpu.VMEM((8, 512, 128), bf16),
            pltpu.VMEM((8, 2, 2, 256, 128), bf16),
            pltpu.VMEM((8, 2, 2, 256, 128), bf16),
            pltpu.VMEM((8, 512, 128), bf16),
            pltpu.VMEM((512, 768), bf16),
            pltpu.VMEM((512, 768), f32),
            pltpu.VMEM((768, 512), bf16),
            pltpu.VMEM((768, 512), bf16),
            pltpu.VMEM((4, 2, 768, 128), bf16),
            pltpu.VMEM((1024, 512), f32),
            pltpu.VMEM((2, 128, 512), f32),
            pltpu.VMEM((512, 768), f32),
            pltpu.VMEM((512, 768), f32),
            pltpu.VMEM((2, 3, 512, 256), bf16),
            dma((2 * ROUNDS, copies)),
            dma((2 * ROUNDS, copies)),
            dma((2 * ROUNDS,)),
            dma((4,)),
            dma((4,)),
            dma,
            dma((6,)),
            dma((4, 2)),
            dma((4, 2)),
            dma((14,)),
            dma((2,)),
        ],
        compiler_params=pltpu.CompilerParams(
            collective_id=0, has_side_effects=True, vmem_limit_bytes=VMEM_LIMIT
        ),
        name="forward",
    )(slopes, *raw, gains, biases, tok, cot, segments)


class ScatterRound(Copies):
    names = ("ay1", "bx", "ay0", "ax", "by", "cx", "dy") + tuple(
        part + "z%d" % step for part in "abcd" for step in (1, 2, 3)
    )

    def __init__(self, place, held, twin, stage, landing, send, recv, pair):
        self.place, self.held, self.twin, self.stage = place, held, twin, stage
        self.ay, self.bx, self.ax, self.by, self.z, self.cz, self.dz, self.last = landing
        self.send, self.recv, self.pair = send, recv, pair

    def copy(self, name):
        p, held = self.place, self.held
        at = self.names.index(name)
        a, b, c, d = (PARTS[part] for part in "abcd")
        step = int(name[2]) if name[1] == "z" else 0
        far = (p.z + step) % 4
        ac, bd = PARTS["ac"], PARTS["bd"]
        if name in ("ay1", "ay0"):
            dx = int(name[2])
            src, dst, to = held.at[dx, :, 1 - p.y, ac, :], self.ay.at[dx], {"dy": 1}
        elif name == "bx":
            src, dst, to = held.at[1, :, :, bd, :], self.bx, {"dx": 1}
        elif name == "ax":
            src, dst, to = held.at[1, :, p.y, a, :], self.ax, {"dx": 1}
        elif name == "by":
            src, dst, to = held.at[0, :, 1 - p.y, b, :], self.by, {"dy": 1}
        elif name == "cx":
            src, dst, to = held.at[1, p.z, p.y, c, :], self.last.at[0], {"dx": 1}
        elif name == "dy":
            src, dst, to = held.at[0, p.z, 1 - p.y, d, :], self.last.at[1], {"dy": 1}
        elif name[0] == "c":
            src, dst, to = held.at[:, far, p.y, c, :], self.cz.at[step - 1], {"dz": step}
        elif name[0] == "d":
            src, dst, to = held.at[0, far, :, d, :], self.dz.at[step - 1], {"dz": step}
        else:
            rows = PARTS[name[0]]
            into = pl.ds(0, 32) if name[0] == "a" else pl.ds(32, 32)
            src, dst, to = held.at[0, far, p.y, rows, :], self.z.at[step - 1, into, :], {"dz": step}
        return remote(src, dst, self.send.at[at], self.recv.at[at], p.device(**to))

    def push(self, dx):
        return remote(
            self.stage.at[dx], self.twin.at[dx], self.pair.at[0, dx], self.pair.at[1, dx], self.place.device(dk=1)
        )

    def add(self, ref, *others):
        total = ref[...].astype(jnp.float32)
        for other in others:
            total = total + other[...].astype(jnp.float32)
        ref[...] = total.astype(jnp.bfloat16)

    def pair_sum(self, dx):
        self.push(dx).wait_recv()

        def body(i, carry):
            self.add(self.held.at[dx, i], self.twin.at[dx, i])
            return carry

        lax.fori_loop(0, 4, body, 0)
        if dx:
            self.start("bx", "ay1")
        else:
            self.start("ay0")

    def event(self, n, out=None):
        p, held = self.place, self.held
        a, b, c, d = (PARTS[part] for part in "abcd")
        ac, bd = PARTS["ac"], PARTS["bd"]
        if n == 0:
            self.wait("ay1")
            self.add(held.at[1, :, p.y, ac, :], self.ay.at[1])
            self.start("ax")
        elif n == 1:
            self.wait("bx")
            self.add(held.at[0, :, 1 - p.y, bd, :], self.bx.at[:, 1 - p.y])
            self.start("by")
            self.add(held.at[0, :, p.y, bd, :], self.bx.at[:, p.y])
            self.start("dz1", "dz2", "dz3")
        elif n == 2:
            self.wait("ay0")
            self.add(held.at[0, :, p.y, ac, :], self.ay.at[0])
            self.start("cz1", "cz2", "cz3")
        elif n == 3:
            self.wait("ax")
            self.add(held.at[0, :, p.y, a, :], self.ax)
            self.start("az1", "az2", "az3")
        elif n == 4:
            self.wait("by")
            self.add(held.at[0, :, p.y, b, :], self.by)
            self.start("bz1", "bz2", "bz3")
        elif n == 5:
            self.wait("cz1", "cz2", "cz3", "dz1", "dz2", "dz3")
            self.add(held.at[1, p.z, p.y, c, :], *[self.cz.at[i, 1] for i in range(3)])
            self.start("cx")
            self.add(held.at[0, p.z, 1 - p.y, d, :], *[self.dz.at[i, 1 - p.y] for i in range(3)])
            self.start("dy")
            self.add(held.at[0, p.z, p.y, c, :], *[self.cz.at[i, 0] for i in range(3)])
            self.add(held.at[0, p.z, p.y, d, :], *[self.dz.at[i, p.y] for i in range(3)])
        else:
            self.wait("az1", "az2", "az3", "bz1", "bz2", "bz3", "cx", "dy")
            for rows, others in (
                (a, [self.z.at[i, pl.ds(0, 32), :] for i in range(3)]),
                (b, [self.z.at[i, pl.ds(32, 32), :] for i in range(3)]),
                (c, [self.last.at[0]]),
                (d, [self.last.at[1]]),
            ):
                total = held[0, p.z, p.y, rows, :].astype(jnp.float32)
                for other in others:
                    total = total + other[...].astype(jnp.float32)
                out[rows, :] = total


def backward_kernel(
    span,
    slopes,
    i_weights,
    norms,
    i_cot,
    i_q,
    i_k,
    i_v,
    i_ctx,
    i_lse,
    i_kept,
    i_n1,
    i_i1,
    i_n2,
    i_i2,
    i_out,
    squares,
    i_h1_t,
    i_x_t,
    i_dist,
    i_wo,
    o_out,
    o_tokens,
    o_grads,
    o_small,
    w_buf,
    wo,
    kept,
    h1_t,
    f_t,
    d_rows,
    n_buf,
    d_h1,
    q,
    keys,
    values,
    ctx,
    lse,
    dist,
    d_ctx,
    d_kv,
    d_kv_in,
    dq_t,
    acc_k,
    acc_v,
    held,
    twin,
    land_ay,
    land_bx,
    land_ax,
    land_by,
    land_z,
    land_cz,
    land_dz,
    land_last,
    small,
    small_in,
    load_sems,
    step_sems,
    r_send,
    r_recv,
    r_pair,
    t_sems,
    kv_send,
    kv_recv,
    s_send,
    s_recv,
):
    f32, bf16 = jnp.float32, jnp.bfloat16
    place = Place(span)
    x, y, z, k = place.shifted()
    rounds = [
        ScatterRound(
            place,
            held.at[n],
            twin.at[n % 6],
            held.at[2 * ROUNDS + n % 2],
            [
                ref.at[n]
                for ref in (land_ay, land_bx, land_ax, land_by, land_z, land_cz, land_dz, land_last)
            ],
            r_send.at[n],
            r_recv.at[n],
            r_pair.at[n],
        )
        for n in range(2 * ROUNDS)
    ]

    def load(n):
        src, dst = (
            (i_cot, d_rows.at[1]),
            (i_n2, n_buf),
            (i_h1_t, h1_t),
            (i_x_t, h1_t),
            (i_q, q),
            (i_k, keys),
            (i_v, values),
            (i_ctx, ctx),
            (i_lse, lse),
            (i_n1, n_buf),
            (i_dist, dist),
        )[n]
        return pltpu.make_async_copy(src, dst, load_sems.at[n])

    def where(n):
        return x ^ (1 - n // 2), k ^ (1 - n % 2)

    def where_heads(n):
        return x ^ (1 - n // 2), n % 2

    def fetch(n, part):
        r = 3 - n // 4
        wx, wk = where(n % 4)
        if part == 0:
            return pltpu.make_async_copy(i_weights.at[pl.ds(2 * r, 2), wx, wk], w_buf.at[n % 2], step_sems.at[n % 2, 0])
        return pltpu.make_async_copy(
            i_kept.at[(r - 1) * 4 + wx * 2 + wk], kept.at[n % 2], step_sems.at[n % 2, 1]
        )

    for n in (0, 1):
        load(n).start()
    fetch(0, 0).start()
    fetch(0, 1).start()
    for n in (2, 4, 5, 6, 7, 8, 10):
        load(n).start()
    place.greet(ALL_PEERS)

    def swap(n):
        src, dst = ((i_out, o_out), (d_rows.at[0], o_tokens))[n]
        return remote(
            src.at[1 - place.x],
            dst.at[place.x],
            t_sems.at[3 * n],
            t_sems.at[3 * n + 1],
            place.device(dx=1),
        )

    def stay(n):
        src, dst = ((i_out, o_out), (d_rows.at[0], o_tokens))[n]
        return pltpu.make_async_copy(src.at[place.x], dst.at[place.x], t_sems.at[3 * n + 2])

    swap(0).start()
    stay(0).start()
    load(0).wait()
    load(1).wait()
    small[...] = jnp.zeros_like(small)

    def halves(ref, i):
        return ref.at[i // 2, pl.ds(pl.multiple_of((i % 2) * ROWS, ROWS), ROWS), :]

    sums = [jnp.zeros((8, 768), f32)] * 2
    for i in range(512 // ROWS):
        rows = pl.ds(i * ROWS, ROWS)
        grad = halves(d_rows.at[1], i)[...].astype(f32)
        normed = n_buf[rows, :]
        out = norm_backward(grad, normed, i_i2[rows, :], norms[1:2])
        d_h1[rows, :] = out
        halves(d_rows.at[0], i)[...] = out.astype(bf16)
        f_t[:, rows] = out.T.astype(bf16)
        sums[0] = sums[0] + columns(grad * normed)
        sums[1] = sums[1] + columns(grad)
    small[1] = sums[0]
    small[3] = sums[1]
    load(9).start()
    load(2).wait()

    def pair(n, dx):
        return lambda: rounds[n].pair_sum(dx)

    def step(n, at):
        chunk = 3 - n // 2
        return lambda: rounds[n].event(at, o_grads.at[2 * chunk + n % 2])

    def put(n, dx, theirs, value, start):
        block = value.astype(bf16).reshape(4, 2, 96, value.shape[-1])
        stop_at = start + value.shape[-1]
        for half in range(2):
            low, high = max(start, 384 * half), min(stop_at, 384 * half + 384)
            if low < high:
                slot = theirs * (2 * ROUNDS + half) + (1 - theirs) * (2 * n + half)
                held[slot, dx, :, :, :, low - 384 * half : high - 384 * half] = block[
                    :, :, :, low - start : high - start
                ]

    def pushes(n, dx):
        return [
            remote(
                held.at[2 * ROUNDS + half, dx],
                twin.at[(2 * n + half) % 6, dx],
                r_pair.at[2 * n + half, 0, dx],
                r_pair.at[2 * n + half, 1, dx],
                place.device(dk=1),
            )
            for half in range(2)
        ]

    def push(n, dx):
        for copy in pushes(n, dx):
            copy.start()

    def pushed(n, dx):
        for copy in pushes(n, dx):
            copy.wait_send()

    between = {
        5: [step(0, 0), step(1, 0)],
        6: [step(0, 1)],
        8: [step(0, 2), step(1, 1)],
        9: [step(1, 2)],
        10: [step(0, 3), step(1, 3)],
        11: [step(0, 5), step(2, 0), step(3, 0)],
    }
    after = {
        1: [pair(0, 1), pair(1, 1)],
        3: [pair(0, 0), pair(1, 0)],
        5: [pair(2, 1), pair(3, 1)],
        7: [pair(2, 0), pair(3, 0)],
        11: [pair(4, 1), pair(5, 1), pair(4, 0), pair(5, 0)],
    }

    def go(n, plan):
        for at, todo in plan.items():

            @pl.when(n == at)
            def _():
                for item in todo:
                    item()

    def feed(n, carry):
        dx = 1 - n % 4 // 2
        theirs = 1 - n % 2

        @pl.when(n < 11)
        def _():
            fetch(n + 1, 0).start()
            fetch(n + 1, 1).start()

        @pl.when(jnp.logical_and(theirs == 1, n >= 4))
        def _():
            pushed(n // 4 - 1, dx)

        fetch(n, 0).wait()
        fetch(n, 1).wait()
        w = whole(w_buf.at[n % 2])
        hold = kept.at[n % 2]
        d_ffn = d_rows[0].reshape(512, 768)
        d_hidden = dot(d_ffn, w[:, 512:])
        d_gate = (d_hidden * hold[2].astype(f32)).astype(bf16)
        d_up = (d_hidden * hold[1].astype(f32)).astype(bf16)
        d_projected = jnp.concatenate([d_gate, d_up], axis=1)
        put(n // 4, dx, theirs, dot(f_t[...], hold[0]), 512)
        go(n, between)
        put(n // 4, dx, theirs, dot(h1_t[...], d_projected), 0)

        @pl.when(theirs == 1)
        def _():
            push(n // 4, dx)

        go(n, after)
        d_h1[...] += dot(d_projected, w[:, :512], NT)
        return carry

    lax.fori_loop(0, 12, feed, 0)
    load(9).wait()
    load(3).start()
    sums = [jnp.zeros((8, 768), f32)] * 2
    for i in range(512 // ROWS):
        rows = pl.ds(i * ROWS, ROWS)
        grad = d_h1[rows, :]
        normed = n_buf[rows, :]
        out = norm_backward(grad, normed, i_i1[rows, :], norms[0:1])
        d_h1[rows, :] = out
        halves(d_rows.at[1], i)[...] = out.astype(bf16)
        f_t[:, rows] = out.T.astype(bf16)
        sums[0] = sums[0] + columns(grad * normed)
        sums[1] = sums[1] + columns(grad)
    small[0] = sums[0]
    small[2] = sums[1]
    for n in (3, 4, 5, 6, 7, 8, 10):
        load(n).wait()

    small[0] = jnp.concatenate(
        [jnp.sum(small[i], axis=0, keepdims=True) for i in range(4)]
        + [jnp.sum(squares[i], axis=0, keepdims=True) for i in range(4)],
        axis=0,
    )

    def spread(n):
        to = ({"dk": 1}, {"dx": 1}, {"dy": 1}, {"dz": 1}, {"dz": 2}, {"dz": 3})[n]
        return remote(
            small.at[min(n, 3)], small_in.at[n], s_send.at[n], s_recv.at[n], place.device(**to)
        )

    def small_step(n):
        def go():
            if 0 < n < 4:
                spread(n - 1).wait_recv()
                small[n] = small[n - 1] + small_in[n - 1]
            if n < 3:
                spread(n).start()
            if n == 3:
                for at in (3, 4, 5):
                    spread(at).start()
            if n == 4:
                for at in (3, 4, 5):
                    spread(at).wait_recv()
                total = small[3]
                result = jnp.zeros_like(total)
                for at in range(4):
                    back = (place.z - at) % 4
                    term = jnp.where(
                        back == 0,
                        total,
                        jnp.where(
                            back == 1, small_in[3], jnp.where(back == 2, small_in[4], small_in[5])
                        ),
                    )
                    result = result + term
                o_small[...] = result

        return go

    def fetch_heads(n):
        wx, wk = where_heads(n)
        return pltpu.make_async_copy(i_weights.at[0:2, wx, wk], w_buf.at[n % 2], step_sems.at[n % 2, 0])

    def fetch_wo(n):
        wx, wk = where_heads(n)
        return pltpu.make_async_copy(i_wo.at[wx * 2 + wk], wo.at[n % 2], step_sems.at[n % 2, 1])

    fetch_heads(0).start()
    fetch_wo(0).start()
    dq_t[1, pl.ds(HEAD_DIM, HEAD_DIM), :] = jnp.zeros((HEAD_DIM, 512), f32)

    def share(t):
        return remote(
            d_kv.at[t, :, :, :, 1 - place.k], d_kv_in.at[t], kv_send.at[t], kv_recv.at[t], place.device(dk=1)
        )

    beside = {
        (1, 6): [small_step(0), step(0, 4)],
        (2, 0): [step(2, 1)],
        (2, 1): [small_step(1), step(1, 5)],
        (2, 2): [step(2, 2)],
        (2, 3): [small_step(2)],
        (2, 4): [step(3, 2)],
        (2, 6): [
            small_step(3), step(1, 4), step(3, 1), step(4, 0), step(5, 0),
            pair(6, 1), pair(7, 1),
        ],
        (3, 1): [step(2, 3), step(3, 3)],
        (3, 2): [small_step(4), step(2, 5)],
        (3, 4): [step(2, 4), step(4, 2)],
        (3, 5): [step(4, 1)],
        (3, 6): [
            step(3, 4), step(5, 2), step(5, 1), step(3, 5), step(4, 3),
            step(5, 3), step(4, 4), step(4, 5),
        ],
        (4, 6): [step(6, 0), step(7, 0), step(5, 4), step(5, 5)],
    }
    first = lax.broadcasted_iota(jnp.int32, (768, 128), 1) < HEAD_DIM

    def stop(i, point):
        for (trip, at), todo in beside.items():
            if at == point:

                @pl.when(i == trip)
                def _():
                    for item in todo:
                        item()

    def attend(n):
        wx, wk = where_heads(n)
        t = wx * 2 + wk
        fetch_heads(n).wait()
        fetch_wo(n).wait()
        left, right = wo[n % 2, 0], wo[n % 2, 1]
        d_attn = d_rows[1].reshape(512, 768)
        d_ctx[0] = dot(d_attn, left).astype(bf16)
        d_ctx[1] = dot(d_attn, right).astype(bf16)
        point = 0
        for spot, (tile, half) in enumerate(HEAD_SPOTS):
            slope = slopes[3 * t + spot]
            key = keys[2 * t + tile].reshape(1024, 128)
            value = values[2 * t + tile].reshape(1024, 128)
            rows = slice(half * HEAD_DIM, (half + 1) * HEAD_DIM)
            key_t = key.astype(f32).T.astype(bf16)[rows]
            product = ctx[2 * t + tile].astype(f32) * d_ctx[tile].astype(f32)
            delta = jnp.sum(product.T[rows], axis=0, keepdims=True)
            for start in range(0, 512, CHUNK):
                cols = pl.ds(start, CHUNK)
                part = lane_half(q[2 * t + tile, cols, :], half)
                grad = lane_half(d_ctx[tile, cols, :], half)
                scores = dot(key, part, NT) - slope * dist[:, cols]
                probs = jnp.exp(scores - lse[t, pl.ds(spot, 1), cols])
                grad_probs = dot(value, grad, NT)
                term_v = dot(probs.astype(bf16), grad)
                grad_scores = (probs * (grad_probs - delta[:, start : start + CHUNK])).astype(bf16)
                term_k = dot(grad_scores, part)
                if half == 0 and start == 0:
                    acc_v[...] = term_v
                    acc_k[...] = term_k
                else:
                    acc_v[...] += term_v
                    acc_k[...] += term_k
                dq_t[tile, rows, cols] = dot(key_t, grad_scores)
                stop(n, point)
                point += 1
            if half == 1 or tile == 1:
                d_kv[t, 0, tile] = acc_k[...].astype(bf16).reshape(2, 2, 256, 128)
                d_kv[t, 1, tile] = acc_v[...].astype(bf16).reshape(2, 2, 256, 128)
        share(t).start()
        for tile in range(2):
            q[2 * t + tile] = (dq_t[tile].T * HEAD_DIM**-0.5).astype(bf16)

    def project(n):
        wx, wk = where_heads(n)
        t = wx * 2 + wk
        dx = 1 - n // 2
        theirs = wk ^ k

        @pl.when(theirs == 1)
        def _():
            pushed(2, dx)

        share(t).wait_recv()
        parts = [q[2 * t], q[2 * t + 1]]
        for kind in range(2):
            for tile in range(2):
                mine = d_kv[t, kind, tile, :, k].reshape(512, 128).astype(f32)
                mine = mine + d_kv_in[t, kind, tile].reshape(512, 128).astype(f32)
                parts.append(mine.astype(bf16))
        d_qkv = jnp.concatenate(parts, axis=1)
        d_wo = dot(f_t[...], jnp.concatenate([ctx[2 * t], ctx[2 * t + 1]], axis=1))
        turned = (swap_halves(d_wo[:, :128]), d_wo[:, :128], swap_halves(d_wo[:, 128:]))
        for kind in range(3):
            d_w = dot(h1_t[...], d_qkv[:, 256 * kind : 256 * kind + 256])
            put(3, dx, theirs, d_w[:, :128], 256 * kind)
            put(3, dx, theirs, jnp.where(first, d_w[:, 128:], turned[kind]), 256 * kind + 128)

        @pl.when(theirs == 1)
        def _():
            push(3, dx)

        d_h1[...] += dot(d_qkv, whole(w_buf.at[n % 2]), NT)

    def heads(n, carry):
        @pl.when(n < 4)
        def _():
            attend(n)

        @pl.when(n > 0)
        def _():
            project(n - 1)

        stop(n, 6)

        @pl.when(n < 3)
        def _():
            fetch_heads(n + 1).start()
            fetch_wo(n + 1).start()

        return carry

    lax.fori_loop(0, 5, heads, 0)
    for i in range(512 // ROWS):
        rows = pl.ds(i * ROWS, ROWS)
        halves(d_rows.at[0], i)[...] = d_h1[rows, :].astype(bf16)
    for n, at in (
        (6, -1), (7, -1), (6, 1), (7, 1), (6, 2), (7, 2), (6, 3), (7, 3),
        (6, 5), (6, 4), (7, 5), (7, 4), (0, 6), (1, 6), (2, 6), (3, 6),
        (4, 6), (5, 6), (6, 6), (7, 6),
    ):
        if at < 0:
            rounds[n].pair_sum(0)
        else:
            step(n, at)()
        if (n, at) == (7, -1):
            swap(1).start()
            stay(1).start()
    for n in range(6):
        spread(n).wait_send()
    for r in rounds:
        r.finish()
    for dx in range(2):
        pushed(3, dx)
    for t in range(4):
        share(t).wait_send()
    for n in range(2):
        swap(n).wait()
        stay(n).wait()


def backward(span, slopes, saved):
    f32, bf16 = jnp.float32, jnp.bfloat16
    any_space = pl.BlockSpec(memory_space=pl.ANY)
    vmem = pl.BlockSpec(memory_space=pltpu.VMEM)
    dma = pltpu.SemaphoreType.DMA
    (weights, norms, xs, cot, q, keys, values, ctx, lse, kept, n1, i1, n2, i2, out, squares) = saved[:16]
    h1_t, x_t, dist, wo = saved[16:]
    out = out.reshape(2, 256, 768)
    in_specs = [pl.BlockSpec(memory_space=pltpu.SMEM), any_space, vmem] + [any_space] * 8
    in_specs += [vmem, any_space, vmem, any_space, vmem] + [any_space] * 4
    copies = len(ScatterRound.names)
    return pl.pallas_call(
        partial(backward_kernel, span),
        out_shape=(
            jax.ShapeDtypeStruct((2, 256, 768), bf16),
            jax.ShapeDtypeStruct((2, 256, 768), bf16),
            jax.ShapeDtypeStruct((2 * ROUNDS, 96, 384), f32),
            jax.ShapeDtypeStruct((8, 768), f32),
        ),
        in_specs=in_specs,
        out_specs=(any_space, any_space, vmem, vmem),
        scratch_shapes=[
            pltpu.VMEM((2, 2, 4, 2, 96, 384), bf16),
            pltpu.VMEM((2, 2, 768, 128), bf16),
            pltpu.VMEM((2, 3, 512, 256), bf16),
            pltpu.VMEM((768, 512), bf16),
            pltpu.VMEM((768, 512), bf16),
            pltpu.VMEM((2, 2, 256, 768), bf16),
            pltpu.VMEM((512, 768), f32),
            pltpu.VMEM((512, 768), f32),
            pltpu.VMEM((8, 512, 128), bf16),
            pltpu.VMEM((8, 2, 2, 256, 128), bf16),
            pltpu.VMEM((8, 2, 2, 256, 128), bf16),
            pltpu.VMEM((8, 512, 128), bf16),
            pltpu.VMEM((4, 8, 512), f32),
            pltpu.VMEM((1024, 512), f32),
            pltpu.VMEM((2, 512, 128), bf16),
            pltpu.VMEM((4, 2, 2, 2, 2, 256, 128), bf16),
            pltpu.VMEM((4, 2, 2, 2, 256, 128), bf16),
            pltpu.VMEM((2, 128, 512), f32),
            pltpu.VMEM((1024, 128), f32),
            pltpu.VMEM((1024, 128), f32),
            pltpu.VMEM((2 * ROUNDS + 2, 2, 4, 2, 96, 384), bf16),
            pltpu.VMEM((6, 2, 4, 2, 96, 384), bf16),
            pltpu.VMEM((2 * ROUNDS, 2, 4, 48, 384), bf16),
            pltpu.VMEM((2 * ROUNDS, 4, 2, 48, 384), bf16),
            pltpu.VMEM((2 * ROUNDS, 4, 32, 384), bf16),
            pltpu.VMEM((2 * ROUNDS, 4, 32, 384), bf16),
            pltpu.VMEM((2 * ROUNDS, 3, 64, 384), bf16),
            pltpu.VMEM((2 * ROUNDS, 3, 2, 16, 384), bf16),
            pltpu.VMEM((2 * ROUNDS, 3, 2, 16, 384), bf16),
            pltpu.VMEM((2 * ROUNDS, 2, 16, 384), bf16),
            pltpu.VMEM((4, 8, 768), f32),
            pltpu.VMEM((6, 8, 768), f32),
            dma((11,)),
            dma((2, 2)),
            dma((2 * ROUNDS, copies)),
            dma((2 * ROUNDS, copies)),
            dma((2 * ROUNDS, 2, 2)),
            dma((6,)),
            dma((4,)),
            dma((4,)),
            dma((6,)),
            dma((6,)),
        ],
        compiler_params=pltpu.CompilerParams(
            collective_id=1, has_side_effects=True, vmem_limit_bytes=VMEM_LIMIT
        ),
        name="backward",
    )(
        slopes,
        weights,
        norms,
        cot,
        q,
        keys,
        values,
        ctx,
        lse,
        kept,
        n1,
        i1,
        n2,
        i2,
        out,
        squares,
        h1_t,
        x_t,
        dist,
        wo,
    )


def finish_kernel(
    block,
    i_grads,
    small,
    lo,
    gt,
    o_lo,
    o_gt,
    o_qkv,
    o_wout,
    o_win,
    o_down_t,
    o_gains,
    o_biases,
    rows,
    grads,
    qkv,
    wout,
    win,
    down_t,
    sems,
):
    moves = (
        (i_grads.at[0:2], grads.at[0:2]),
        (lo, rows.at[0]),
        (gt, rows.at[1]),
        (i_grads.at[2:8], grads.at[2:8]),
        (rows.at[0], o_lo),
        (rows.at[1], o_gt),
        (qkv, o_qkv),
        (wout, o_wout),
        (win, o_win),
        (down_t, o_down_t),
    )

    def move(n):
        return pltpu.make_async_copy(*moves[n], sems.at[n])

    def tile(i):
        return grads[i // 3, :, i % 3 * 128 : i % 3 * 128 + 128]

    for n in range(4):
        move(n).start()
    mine = pltpu.roll(small[...], 768 - block[0] * 96, 1)
    o_gains[...] = mine[0:2, 0:96]
    o_biases[...] = mine[2:4, 0:96]
    move(0).wait()
    turned = []
    for c in range(3):
        qkv[c, :, 0:128] = tile(2 * c)
        qkv[c, :, 128:192] = tile(2 * c + 1)[:, :HEAD_DIM]
        turned.append(tile(2 * c + 1).T[HEAD_DIM:])
    wout[...] = jnp.concatenate(turned, axis=0)
    move(6).start()
    move(7).start()
    for n in (1, 2):
        move(n).wait()
        move(n + 3).start()
    move(3).wait()
    for r in range(3):
        units = slice(r * 256, (r + 1) * 256)
        win[:, 0, units] = grads[2 + 2 * r, :, 0:256]
        win[:, 1, r * 256 : r * 256 + 128] = grads[2 + 2 * r, :, 256:384]
        win[:, 1, r * 256 + 128 : r * 256 + 256] = grads[3 + 2 * r, :, 0:128]
        down_t[:, units] = grads[3 + 2 * r, :, 128:384]
    move(8).start()
    move(9).start()
    for n in range(4, 10):
        move(n).wait()


def finish(block, grads, small, lo, gt):
    any_space = pl.BlockSpec(memory_space=pl.ANY)
    vmem = pl.BlockSpec(memory_space=pltpu.VMEM)
    f32 = jnp.float32
    shape = jax.ShapeDtypeStruct
    return pl.pallas_call(
        finish_kernel,
        out_shape=(
            shape(lo.shape, lo.dtype),
            shape(gt.shape, gt.dtype),
            shape((3, 96, 192), f32),
            shape((192, 96), f32),
            shape((96, 2, 768), f32),
            shape((96, 768), f32),
            shape((2, 96), f32),
            shape((2, 96), f32),
        ),
        in_specs=[pl.BlockSpec(memory_space=pltpu.SMEM), any_space, vmem, any_space, any_space],
        out_specs=(any_space,) * 6 + (vmem,) * 2,
        scratch_shapes=[
            pltpu.VMEM((2,) + lo.shape, lo.dtype),
            pltpu.VMEM(grads.shape, f32),
            pltpu.VMEM((3, 96, 192), f32),
            pltpu.VMEM((192, 96), f32),
            pltpu.VMEM((96, 2, 768), f32),
            pltpu.VMEM((96, 768), f32),
            pltpu.SemaphoreType.DMA((10,)),
        ],
        compiler_params=pltpu.CompilerParams(vmem_limit_bytes=VMEM_LIMIT),
        name="finish",
    )(block, grads, small, lo, gt)


def local(
    tokens,
    segment_ids,
    query_key_value_weight,
    w_out,
    input_weight,
    w_down,
    norm_gains,
    norm_biases,
    cotangent,
):
    f32 = jnp.float32
    shard_rows = query_key_value_weight.shape[1]
    span = 96 // shard_rows
    slopes = jnp.asarray([2.0 ** (-8.0 * (h + 1) / HEADS) for h in range(HEADS)], f32)
    cells = float(lax.axis_size("fsdp") * 2 * 1024 * 768)
    if span == 1:
        raw = (query_key_value_weight, w_out, input_weight, w_down.T)
        gains, biases = norm_gains, norm_biases
    else:
        count = lax.axis_size("fsdp")
        groups = [list(range(i, i + span)) for i in range(0, count, span)]
        heads = query_key_value_weight.transpose(1, 0, 2).reshape(shard_rows, 3, 3, HEAD_DIM)
        w_out_t = w_out.T.reshape(shard_rows, 3, 1, HEAD_DIM)
        wa = jnp.concatenate([heads, w_out_t], axis=2).reshape(shard_rows, 1, 768)
        gate_up = input_weight.reshape(shard_rows, 2, 3, 256).transpose(0, 2, 1, 3)
        down = w_down.T.reshape(shard_rows, 3, 1, 256)
        wf = jnp.concatenate([gate_up, down], axis=2).reshape(shard_rows, 3, 768)
        shard = jnp.concatenate([wa, wf], axis=1).reshape(shard_rows, 8, 384).transpose(1, 0, 2)
        raw = (lax.all_gather(shard, "fsdp", axis=1, tiled=True, axis_index_groups=groups),)
        gains, biases = (
            lax.all_gather(rows, "fsdp", axis=1, tiled=True, axis_index_groups=groups)
            for rows in (norm_gains, norm_biases)
        )

    saved = forward(span, slopes, raw, gains, biases, tokens, cotangent, segment_ids)
    layer_out, grad_tokens, grads, small = backward(span, slopes, saved)

    if span == 1:
        block = lax.axis_index("fsdp").astype(jnp.int32).reshape(1)
        outs = finish(block, grads, small, layer_out, grad_tokens)
        outs = outs[:5] + (outs[5].T,) + outs[6:]
    else:
        grads = lax.psum_scatter(
            grads, "fsdp", scatter_dimension=1, tiled=True, axis_index_groups=groups
        )
        small = lax.psum(small, "fsdp", axis_index_groups=groups)
        grads = grads.reshape(4, 2, shard_rows, 384).transpose(0, 2, 1, 3)
        grads_a = grads[0].reshape(shard_rows, 3, 4, HEAD_DIM)
        grads_f = grads[1:].reshape(3, shard_rows, 3, 256)
        shard_start = lax.axis_index("fsdp") * shard_rows
        mine = lax.dynamic_slice_in_dim(small[:4], shard_start, shard_rows, 1)
        outs = (
            layer_out,
            grad_tokens,
            grads_a[:, :, :3].transpose(1, 0, 2, 3).reshape(3, shard_rows, 192),
            grads_a[:, :, 3].reshape(shard_rows, 192).T,
            grads_f[:, :, :2].transpose(1, 2, 0, 3).reshape(shard_rows, 2, 768),
            grads_f[:, :, 2].transpose(0, 2, 1).reshape(768, shard_rows),
            mine[:2],
            mine[2:],
        )
    return outs + (jnp.sqrt(jnp.sum(small[4:], axis=1) / cells),)


def solution(mesh):
    placed = (
        P("fsdp", "tp", None),
        P("fsdp", None),
        P(None, "fsdp", "tp"),
        P("tp", "fsdp"),
        P("fsdp", None, "tp"),
        P("tp", "fsdp"),
        P(None, "fsdp"),
        P(None, "fsdp"),
        P("fsdp", "tp", None),
    )
    return jax.shard_map(
        local,
        mesh=mesh,
        in_specs=placed,
        out_specs=(
            P("fsdp", "tp", None),
            P("fsdp", "tp", None),
            P(None, "fsdp", "tp"),
            P("tp", "fsdp"),
            P("fsdp", None, "tp"),
            P("tp", "fsdp"),
            P(None, "fsdp"),
            P(None, "fsdp"),
            P(),
        ),
        check_vma=False,
    )
```
